32 devices in a mesh: section: 2 (over core), dp: 4 (over z), tensor: 4 (over y, x).
Axes of the slice: x: 2, y: 2, z: 4, core: 2. Of those that a mesh axis runs over, the one named last changes fastest.
Arguments:
- tokens: bfloat16 [2, 3072, 1152], P(None, ('dp', 'tensor')), may hold values from -6 to 6
- cotangent: bfloat16 [2, 3072, 1152], P(None, ('dp', 'tensor')), may hold values from -6 to 6
- cond: bfloat16 [24, 1152], P('dp'), may hold values from -6 to 6
- patch_item: int32 [2, 3072], P(None, 'dp'), may hold values from -1 to 23, as said below
- patch_pos: int32 [2, 2, 3072], P(None, None, 'dp'), may hold values from 0 to 19, as said below
- w_qkv: bfloat16 [2, 3, 1152, 1152], P('section', None, None, 'tensor'), may hold values from -0.1875 to 0.1875
- w_out: bfloat16 [2, 1152, 1152], P('section', 'tensor'), may hold values from -0.75 to 0.75
- w_gate_up: bfloat16 [2, 2, 1152, 3072], P('section', None, None, 'tensor'), may hold values from -0.1875 to 0.1875
- w_down: bfloat16 [2, 3072, 1152], P('section', 'tensor'), may hold values from -0.109375 to 0.109375
- qk_gain: bfloat16 [2, 2, 72], P('section'), may hold values from 0.5 to 1.5
- ada_weight: bfloat16 [2, 1152, 6912], P('section', None, 'tensor'), may hold values from -0.1875 to 0.1875
- ada_bias: bfloat16 [2, 6912], P('section', 'tensor'), may hold values from -3 to 3
Outputs:
- layer_out: bfloat16 [2, 2, 3072, 1152], P('section', None, ('dp', 'tensor'))
- input_grads: float32 [2, 2, 3072, 1152], P('section', None, ('dp', 'tensor'))
- cond_grad: float32 [24, 1152], P('dp')
- g_qkv: float32 [2, 3, 1152, 1152], P('section', None, 'dp', 'tensor')
- g_out: float32 [2, 1152, 1152], P('section', 'tensor', 'dp')
- g_gate_up: float32 [2, 2, 1152, 3072], P('section', None, 'dp', 'tensor')
- g_down: float32 [2, 3072, 1152], P('section', 'tensor', 'dp')
- g_qk_gain: float32 [2, 2, 72], P('section')
- g_ada_weight: float32 [2, 1152, 6912], P('section', 'dp', 'tensor')
- g_ada_bias: float32 [2, 6912], P('section', ('tensor', 'dp'))
The draws below stay inside these ranges and needn't reach their ends.
Inputs may be any that keep to these rules, and one draw needn't show every extreme that they name: `patch_item`: each micro-batch sequence of 768 slots holds 3 whole items one after another, each of 240 or 256 slots, then padding slots marked -1. The items of data shard d and micro-batch m are numbered (d * 2 + m) * 3 + j in order. patch_pos[0] and patch_pos[1] are a patch's row and column in its item's grid, in row-major order within the item; padding slots have 0 and 0.
All inputs are finite; a program needn't handle non-finite values.
Results may differ from the reference program's by a relative error of at most 0.015.
Values may be sent and summed in bfloat16 or wider, within the bound.
A program may use at most 256 MiB of HBM per device.

```python
import jax
import jax.numpy as jnp
from jax import lax

D = 1152
HEADS = 16
HEAD = 72
FF = 3072
GRID_H = 12
GRID_W = 20
GRID_SIDE = 16
ITEMS_MB = 3
MICRO = 2
ROWS_MB = 768
ROWS_ALL = 3072
ITEMS = 24
N_DP = 4


def patch_layout(key):
    shape_key = jax.random.fold_in(key, 11)
    grid_kinds = jax.random.randint(shape_key, (MICRO, N_DP, ITEMS_MB), 0, 2)
    grid_kinds = grid_kinds.at[0, 0, 0].set(0).at[0, 0, 1].set(1)
    lengths = jnp.where(grid_kinds == 0, GRID_H * GRID_W, GRID_SIDE * GRID_SIDE)
    widths = jnp.where(grid_kinds == 0, GRID_W, GRID_SIDE)
    end_rows = jnp.cumsum(lengths, axis=-1)
    start_rows = end_rows - lengths
    row_places = jnp.arange(ROWS_MB, dtype=jnp.int32)
    inside = (row_places[None, None, None, :] >= start_rows[..., None]) & (row_places[None, None, None, :] < end_rows[..., None])
    inside_int = inside.astype(jnp.int32)
    slot_index = jnp.sum(inside_int * jnp.arange(ITEMS_MB, dtype=jnp.int32)[None, None, :, None], axis=2)
    is_live = jnp.sum(inside_int, axis=2) > 0
    begin_row = jnp.sum(inside_int * start_rows[..., None], axis=2)
    width_here = jnp.maximum(jnp.sum(inside_int * widths[..., None], axis=2), 1)
    offsets = row_places[None, None, :] - begin_row
    micro_ids = jnp.arange(MICRO, dtype=jnp.int32)[:, None, None]
    shard_ids = jnp.arange(N_DP, dtype=jnp.int32)[None, :, None]
    item_ids = jnp.where(is_live, (shard_ids * MICRO + micro_ids) * ITEMS_MB + slot_index, -1)
    row_pos = jnp.where(is_live, offsets // width_here, 0)
    col_pos = jnp.where(is_live, offsets % width_here, 0)
    return (item_ids.reshape(MICRO, N_DP * ROWS_MB), jnp.stack([row_pos, col_pos]).reshape(2, MICRO, N_DP * ROWS_MB))


def draw_patch_item(key, part):
    return patch_layout(key)[0]


def draw_patch_pos(key, part):
    return patch_layout(key)[1]


def block_levels(rng, shape, shards, least, top_value):
    factor_of = 1.0
    for axis_at, parts in shards:
        draws = jax.random.uniform(jax.random.fold_in(jax.random.fold_in(rng, 6), axis_at), (parts,), jnp.float32, least / len(shards), top_value / len(shards))
        factor_of = factor_of * jnp.repeat(jnp.exp(draws), shape[axis_at] // parts).reshape((-1,) + (1,) * (len(shape) - 1 - axis_at))
    return factor_of


def gaussian(key, dims, width, most, cuts=(), kind=jnp.bfloat16):
    values = width * jax.random.normal(key, dims, jnp.float32)
    if cuts:
        values = values * block_levels(key, dims, cuts, -0.22, 0.18)
    return jnp.clip(values, -most, most).astype(kind)


def setup_inputs(seed: int = 0) -> dict:
    streams_of = jax.random.split(jax.random.key(seed), 13)
    tokens = gaussian(streams_of[0], (MICRO, ROWS_ALL, D), 1.0, 6.0, ((1, 16),))
    cotangent = gaussian(streams_of[1], (MICRO, ROWS_ALL, D), 1.0, 6.0, ((1, 16),))
    cond = gaussian(streams_of[2], (ITEMS, D), 1.0, 6.0, ((0, 4),))
    patch_item = draw_patch_item(jax.random.fold_in(streams_of[12], 71), 0)
    patch_pos = draw_patch_pos(jax.random.fold_in(streams_of[12], 71), 0)
    w_qkv = gaussian(streams_of[5], (2, 3, D, D), D ** -0.5, 0.1875, ((0, 2), (3, 4)))
    w_out = gaussian(streams_of[6], (2, D, D), (D // 16) ** -0.5, 0.75, ((0, 2), (1, 4)))
    w_gate_up = gaussian(streams_of[7], (2, 2, D, FF), D ** -0.5, 0.1875, ((0, 2), (3, 4)))
    w_down = gaussian(streams_of[8], (2, FF, D), FF ** -0.5, 0.109375, ((0, 2), (1, 4)))
    qk_gain = jnp.clip(1.0 + 0.1 * jax.random.normal(streams_of[9], (2, 2, HEAD), jnp.float32), 0.5, 1.5).astype(jnp.bfloat16)
    ada_weight = gaussian(streams_of[10], (2, D, 6 * D), D ** -0.5, 0.1875, ((0, 2), (2, 4)))
    ada_bias = gaussian(streams_of[11], (2, 6 * D), 0.5, 3.0, ((0, 2), (1, 4)))
    return {"tokens": tokens, "cotangent": cotangent, "cond": cond, "patch_item": patch_item, "patch_pos": patch_pos, "w_qkv": w_qkv, "w_out": w_out, "w_gate_up": w_gate_up, "w_down": w_down, "qk_gain": qk_gain, "ada_weight": ada_weight, "ada_bias": ada_bias}


@jax.custom_vjp
def low(v):
    return lax.optimization_barrier(v.astype(jnp.bfloat16)).astype(jnp.float32)

@jax.custom_vjp
def low_back(v):
    return v

def low_keep(v):
    return (low(v), None)

def low_pass(kept, grad):
    return (grad,)

def back_keep(v):
    return (v, None)

def back_low(kept, grad):
    return (low(grad),)
low.defvjp(low_keep, low_pass)
low_back.defvjp(back_keep, back_low)
EPS = 1e-06
PRECISE = lax.Precision.HIGHEST

def normed(values_in):
    return values_in * lax.rsqrt(lax.optimization_barrier(jnp.mean(values_in * values_in, axis=-1, keepdims=True)) + EPS)

def swish(values_in):
    return values_in * jax.nn.sigmoid(values_in)

def angle_tables(row_pos, col_pos, head_size):
    quarter = head_size // 4
    frequency = 10000.0 ** (-jnp.arange(quarter, dtype=jnp.float32) / quarter)
    row_angle = row_pos.astype(jnp.float32)[:, None] * frequency[None, :]
    col_angle = col_pos.astype(jnp.float32)[:, None] * frequency[None, :]
    return (jnp.cos(row_angle), jnp.sin(row_angle), jnp.cos(col_angle), jnp.sin(col_angle))

def turn_half(half_part, cos_table, sine_table, direction):
    quarter = half_part.shape[-1] // 2
    leading = half_part[..., :quarter]
    trailing = half_part[..., quarter:]
    cosine = cos_table[:, None, :]
    sine_part = direction * sine_table[:, None, :]
    return jnp.concatenate([leading * cosine - trailing * sine_part, trailing * cosine + leading * sine_part], axis=-1)

def rotate(values_in, tables, direction):
    half_size = values_in.shape[-1] // 2
    return jnp.concatenate([turn_half(values_in[..., :half_size], tables[0], tables[1], direction), turn_half(values_in[..., half_size:], tables[2], tables[3], direction)], axis=-1)

def seq_layer(weights, inputs, mod_rows, item_ids, row_pos, col_pos):
    w_qkv, w_out, w_gate_up, w_down, qk_gain = weights
    seq_rows = inputs.shape[0]
    h_one = low(normed(inputs) * (1.0 + mod_rows[:, 1]) + mod_rows[:, 0])
    projected = low_back(jnp.einsum('sd,kde->kse', h_one, w_qkv, precision=PRECISE))
    shape_heads = (seq_rows, HEADS, HEAD)
    tables = angle_tables(row_pos, col_pos, HEAD)
    queries = low(rotate(normed(projected[0].reshape(shape_heads)) * qk_gain[0], tables, 1.0))
    keys_att = low(rotate(normed(projected[1].reshape(shape_heads)) * qk_gain[1], tables, 1.0))
    values_att = low(projected[2].reshape(shape_heads))
    scores = low_back(jnp.einsum('qhe,khe->hqk', queries, keys_att, precision=PRECISE) * HEAD ** (-0.5))
    same_item = item_ids[:, None] == item_ids[None, :]
    scores = jnp.where(same_item[None], scores, -1e+30)
    row_max = lax.optimization_barrier(jnp.max(scores, axis=-1, keepdims=True))
    shifted_exp = jnp.exp(scores - row_max)
    attn_probs = low(shifted_exp / lax.optimization_barrier(jnp.sum(shifted_exp, axis=-1, keepdims=True)))
    attended = low(low_back(jnp.einsum('hqk,khe->qhe', attn_probs, values_att, precision=PRECISE).reshape(seq_rows, D)))
    mixed = inputs + mod_rows[:, 2] * low_back(jnp.dot(attended, w_out, precision=PRECISE, preferred_element_type=jnp.float32))
    h_two = low(normed(mixed) * (1.0 + mod_rows[:, 4]) + mod_rows[:, 3])
    gate_proj = low_back(jnp.dot(h_two, w_gate_up[0], precision=PRECISE, preferred_element_type=jnp.float32))
    up_proj = low_back(jnp.dot(h_two, w_gate_up[1], precision=PRECISE, preferred_element_type=jnp.float32))
    hidden = low(swish(gate_proj) * up_proj)
    return mixed + mod_rows[:, 5] * low_back(jnp.dot(hidden, w_down, precision=PRECISE, preferred_element_type=jnp.float32))

def layer_apply(weights, ada_w, ada_b, cond_in, inputs, patch_item, row_all, col_all):
    modulation = jnp.dot(low(swish(cond_in)), ada_w, precision=PRECISE, preferred_element_type=jnp.float32) + ada_b[None, :]
    seq_count = MICRO * N_DP

    def one_sequence(packed):
        seq_in, seq_items, seq_row_pos, seq_col_pos = packed
        picked = modulation[jnp.maximum(seq_items, 0)]
        mod_rows = jnp.where((seq_items >= 0)[:, None], picked, 0.0).reshape(ROWS_MB, 6, D)
        return seq_layer(weights, seq_in, mod_rows, seq_items, seq_row_pos, seq_col_pos)
    results = lax.map(jax.checkpoint(one_sequence), (inputs.reshape(seq_count, ROWS_MB, D), patch_item.reshape(seq_count, ROWS_MB), row_all.reshape(seq_count, ROWS_MB), col_all.reshape(seq_count, ROWS_MB)))
    return results.reshape(MICRO, N_DP * ROWS_MB, D)

def reference(tokens, cotangent, cond, patch_item, patch_pos, w_qkv, w_out, w_gate_up, w_down, qk_gain, ada_weight, ada_bias):

    def widen(array_in):
        return array_in.astype(jnp.float32)

    def section_params(level):
        return (widen(w_qkv[level]), widen(w_out[level]), widen(w_gate_up[level]), widen(w_down[level]), widen(qk_gain[level]))
    row_all = patch_pos[0]
    col_all = patch_pos[1]
    cond_wide = widen(cond)

    def first_layer(inputs, weights, ada_w, ada_b, cond_in):
        return layer_apply(weights, ada_w, ada_b, cond_in, inputs, patch_item, row_all, col_all)

    def second_layer(inputs, weights, ada_w, ada_b, cond_in):
        return layer_apply(weights, ada_w, ada_b, cond_in, low(low_back(inputs)), patch_item, row_all, col_all)
    out_zero, back_zero = jax.vjp(first_layer, widen(tokens), section_params(0), widen(ada_weight[0]), widen(ada_bias[0]), cond_wide)
    out_one, back_one = jax.vjp(second_layer, out_zero, section_params(1), widen(ada_weight[1]), widen(ada_bias[1]), cond_wide)
    grad_mid, grads_one, ada_w_one, ada_b_one, cond_one = back_one(widen(cotangent))
    grad_in, grads_zero, ada_w_zero, ada_b_zero, cond_zero = back_zero(grad_mid)
    layer_out = jnp.stack([out_zero, out_one]).astype(jnp.bfloat16)
    input_grads = jnp.stack([grad_in, grad_mid])

    def paired(position):
        return jnp.stack([grads_zero[position], grads_one[position]])
    return (layer_out, input_grads, cond_zero + cond_one, paired(0), paired(1), paired(2), paired(3), paired(4), jnp.stack([ada_w_zero, ada_w_one]), jnp.stack([ada_b_zero, ada_b_one]))
```

```python
import functools

import jax
import jax.numpy as jnp
from jax import lax
from jax.experimental import pallas as pl
from jax.experimental.pallas import tpu as pltpu
from jax.sharding import PartitionSpec as P

EPS = 1e-06
PRECISE = lax.Precision.HIGHEST
F32 = jnp.float32
BF = jnp.bfloat16
S, DP, T = "section", "dp", "tensor"
PAD = 128
TILE = 256


def nn(a, b):
    return jnp.dot(a, b, preferred_element_type=F32)


def nt(a, b):
    return lax.dot_general(a, b, (((1,), (1,)), ((), ())), preferred_element_type=F32)


def tn(a, b):
    return lax.dot_general(a, b, (((0,), (0,)), ((), ())), preferred_element_type=F32)


def two(dot, a, b):
    high = a.astype(BF)
    low = (a - high.astype(F32)).astype(BF)
    return dot(high, b) + dot(low, b)


def sds(shape, dtype):
    return jax.ShapeDtypeStruct(shape, dtype)


def vmem():
    return pl.BlockSpec(memory_space=pltpu.VMEM)


def anywhere():
    return pl.BlockSpec(memory_space=pl.ANY)


def ring(square):
    me = lax.axis_index(T)
    near = me + 1 - 2 * (me % 2)
    if square:
        return me, near, me + 2 - 4 * (me // 2), 3 - me
    return me, near, 3 - me, (me + 2) % 4


def greet(place):
    sem = pltpu.get_barrier_semaphore()
    for peer in (place[1], place[2]):
        pl.semaphore_signal(
            sem, inc=1, device_id={T: peer}, device_id_type=pl.DeviceIdType.MESH
        )
    pl.semaphore_wait(sem, 2)


def remote(src, dst, sems, index, peer):
    return pltpu.make_async_remote_copy(
        src_ref=src,
        dst_ref=dst,
        send_sem=sems[0].at[index],
        recv_sem=sems[1].at[index],
        device_id={T: peer},
        device_id_type=pl.DeviceIdType.MESH,
    )


def chunk_rows(chunk, rows):
    return pl.ds(pl.multiple_of(chunk * rows, rows), rows)


def gather(place, mine, whole, sems, base, use):
    me, a, b, d = place
    rows = mine.shape[0]
    half = rows // 2
    lo, hi = pl.ds(0, half), pl.ds(half, half)

    def part(chunk, upper):
        return pl.ds(pl.multiple_of(chunk * rows + upper * half, half), half)

    a0 = remote(mine.at[lo], whole.at[part(me, 0)], sems, base, a)
    b0 = remote(mine.at[hi], whole.at[part(me, 1)], sems, base + 1, b)
    a1 = remote(mine.at[hi], whole.at[part(me, 1)], sems, base + 2, a)
    b1 = remote(mine.at[lo], whole.at[part(me, 0)], sems, base + 3, b)
    for copy in (a0, b0, a1, b1):
        copy.start()
    whole[chunk_rows(me, rows), :] = mine[...]
    use(me)
    a0.wait_recv()
    b2 = remote(whole.at[part(a, 0)], whole.at[part(a, 0)], sems, base + 4, b)
    b2.start()
    b0.wait_recv()
    a2 = remote(whole.at[part(b, 1)], whole.at[part(b, 1)], sems, base + 5, a)
    a2.start()
    a1.wait_recv()
    use(a)
    b1.wait_recv()
    use(b)
    b2.wait_recv()
    a2.wait_recv()
    use(d)
    for copy in (a0, b0, a1, b1, a2, b2):
        copy.wait_send()


def scatter(place, term, bufs, sems, base):
    me, a, b, d = place
    out, into, keep, own = bufs
    half = keep.shape[1]
    lo, hi = pl.ds(0, half), pl.ds(half, half)
    out[0] = term(d).astype(BF)
    d0 = remote(out.at[0, lo], into.at[0, lo], sems, base, a)
    d1 = remote(out.at[0, hi], into.at[0, hi], sems, base + 1, b)
    d0.start()
    d1.start()
    total = term(a)
    out[1, lo] = total[:half].astype(BF)
    a0 = remote(out.at[1, lo], into.at[1, lo], sems, base + 2, a)
    a0.start()
    keep[0] = total[half:]
    total = term(b)
    out[2, hi] = total[half:].astype(BF)
    b0 = remote(out.at[2, hi], into.at[2, hi], sems, base + 3, b)
    b0.start()
    keep[1] = total[:half]
    own[...] = term(me)
    d1.wait_recv()
    out[1, hi] = (keep[0] + into[0, hi].astype(F32)).astype(BF)
    a1 = remote(out.at[1, hi], into.at[1, hi], sems, base + 4, a)
    a1.start()
    d0.wait_recv()
    out[2, lo] = (keep[1] + into[0, lo].astype(F32)).astype(BF)
    b1 = remote(out.at[2, lo], into.at[2, lo], sems, base + 5, b)
    b1.start()
    for copy in (a0, b0, a1, b1):
        copy.wait_recv()
    for copy in (d0, d1, a0, b0, a1, b1):
        copy.wait_send()


def scattered(bufs, rows):
    return bufs[3][rows] + bufs[1][1, rows].astype(F32) + bufs[1][2, rows].astype(F32)


def scatter_scratch(rows, width):
    return [
        pltpu.VMEM((3, rows, width), BF),
        pltpu.VMEM((3, rows, width), BF),
        pltpu.VMEM((2, rows // 2, width), F32),
        pltpu.VMEM((rows, width), F32),
    ]


def dma_sems(count):
    return [pltpu.SemaphoreType.DMA((count,)), pltpu.SemaphoreType.DMA((count,))]


def layer_weights(own, other, layer, dst, sem):
    mine = lax.axis_index(S) == layer

    @pl.when(mine)
    def _():
        pltpu.make_async_copy(own, dst, sem).start()

    @pl.when(jnp.logical_not(mine))
    def _():
        pltpu.make_async_copy(other, dst, sem).start()

    return pltpu.make_async_copy(own, dst, sem)


def over_blocks(rows, fn):
    step = rows // 4

    def body(i, carry):
        fn(pl.ds(pl.multiple_of(i * step, step), step))
        return carry

    lax.fori_loop(0, 4, body, 0)


def mod_rows(sel, mod, which, width):
    cols = pl.ds(which * width, width)
    total = sel[:, 0:1] * mod[0:1, cols]
    for item in (1, 2):
        total = total + sel[:, item : item + 1] * mod[item : item + 1, cols]
    return total


def item_sums(sel, values):
    high = values.astype(BF)
    low = (values - high.astype(F32)).astype(BF)
    sel_b = sel.astype(BF)
    return tn(sel_b, high) + tn(sel_b, low)


def normed(values):
    inverse = lax.rsqrt(jnp.mean(values * values, axis=-1, keepdims=True) + EPS)
    return values * inverse, inverse


def norm_back(incoming, normal, inverse):
    return inverse * (incoming - normal * jnp.mean(incoming * normal, axis=-1, keepdims=True))


def qkv_kernel(layer, square, x, sel, mod, w_own, w_other, whole, proj, h, w, ssem, rsem, wsem):
    place = ring(square)
    width = x.shape[1]
    load = layer_weights(w_own, w_other, layer, w, wsem)
    greet(place)

    def prepare(rows):
        normal, _ = normed(x[rows].astype(F32))
        shift = mod_rows(sel[rows], mod, 0, width)
        scale = mod_rows(sel[rows], mod, 1, width)
        h[rows] = (normal * (1.0 + scale) + shift).astype(BF)

    over_blocks(x.shape[0], prepare)
    waited = []

    def use(chunk):
        if not waited:
            load.wait()
            waited.append(1)
        rows = chunk_rows(chunk, x.shape[0])
        for k in range(3):
            proj[k, rows] = nn(whole[rows], w[k])

    gather(place, h, whole, (ssem, rsem), 0, use)


def mlp_kernel(layer, square, att, x, sel, mod, wo0, wo1, wg0, wg1, wd0, wd1, br1, x1, whole,
               gate, up, hidden, br2, y, h, wo, wg, wd, o1, i1, k1, s1, o2, i2, k2, s2,
               ssem, rsem, wsem):
    place = ring(square)
    rows_here, width = x.shape
    load_o = layer_weights(wo0, wo1, layer, wo, wsem.at[0])
    load_g = layer_weights(wg0, wg1, layer, wg, wsem.at[1])
    load_d = layer_weights(wd0, wd1, layer, wd, wsem.at[2])
    greet(place)
    sems = (ssem, rsem)
    load_o.wait()
    first = (o1, i1, k1, s1)
    scatter(place, lambda c: nn(att[chunk_rows(c, rows_here)], wo[...]), first, sems, 0)

    def between(rows):
        branch = scattered(first, rows)
        br1[rows] = branch
        mixed = x[rows].astype(F32) + mod_rows(sel[rows], mod, 2, width) * branch
        x1[rows] = mixed
        normal, _ = normed(mixed)
        shift = mod_rows(sel[rows], mod, 3, width)
        scale = mod_rows(sel[rows], mod, 4, width)
        h[rows] = (normal * (1.0 + scale) + shift).astype(BF)

    over_blocks(rows_here, between)
    load_g.wait()

    def use(chunk):
        rows = chunk_rows(chunk, rows_here)
        gate[rows] = nn(whole[rows], wg[0])
        up[rows] = nn(whole[rows], wg[1])
        g = gate[rows]
        hidden[rows] = (g * jax.nn.sigmoid(g) * up[rows]).astype(BF)

    gather(place, h, whole, sems, 6, use)
    load_d.wait()
    second = (o2, i2, k2, s2)
    scatter(place, lambda c: nn(hidden[chunk_rows(c, rows_here)], wd[...]), second, sems, 12)

    def finish(rows):
        branch = scattered(second, rows)
        br2[rows] = branch
        y[rows] = (x1[rows] + mod_rows(sel[rows], mod, 5, width) * branch).astype(BF)

    over_blocks(rows_here, finish)


def mlp_back_kernel(layer, square, dy, br2, br1, x1, sel, mod, gate_h, up_h, wo0, wo1, wg0, wg1,
                    wd0, wd1, whole2, dgate, dup, whole1, datt, dx1, dmod, h, h1, gate, up, wo,
                    wg, wd, o1, i1, k1, s1, ssem, rsem, wsem):
    place = ring(square)
    rows_here, width = dy.shape
    load_d = layer_weights(wd0, wd1, layer, wd, wsem.at[0])
    load_gate = pltpu.make_async_copy(gate_h, gate, wsem.at[1])
    load_gate.start()
    load_up = pltpu.make_async_copy(up_h, up, wsem.at[2])
    load_up.start()
    load_g = layer_weights(wg0, wg1, layer, wg, wsem.at[3])
    load_o = layer_weights(wo0, wo1, layer, wo, wsem.at[4])
    greet(place)
    sems = (ssem, rsem)
    dmod[...] = jnp.zeros_like(dmod)

    def prepare(rows):
        incoming = dy[rows].astype(F32)
        h[rows] = (incoming * mod_rows(sel[rows], mod, 5, width)).astype(BF)
        dmod[3] += item_sums(sel[rows], incoming * br2[rows])

    over_blocks(rows_here, prepare)
    waited = []

    def use(chunk):
        if not waited:
            load_d.wait()
            load_gate.wait()
            load_up.wait()
            waited.append(1)
        rows = chunk_rows(chunk, rows_here)
        d_hidden = nt(whole2[rows], wd[...])
        g = gate[rows]
        s = jax.nn.sigmoid(g)
        dgate[rows] = (d_hidden * up[rows] * s * (1.0 + g * (1.0 - s))).astype(BF)
        dup[rows] = (d_hidden * g * s).astype(BF)

    gather(place, h, whole2, sems, 0, use)
    load_g.wait()
    bufs = (o1, i1, k1, s1)

    def term(chunk):
        rows = chunk_rows(chunk, rows_here)
        return nt(dgate[rows], wg[0]) + nt(dup[rows], wg[1])

    scatter(place, term, bufs, sems, 6)

    def between(rows):
        d_h = scattered(bufs, rows)
        normal, inverse = normed(x1[rows])
        scale = mod_rows(sel[rows], mod, 4, width)
        d_mixed = dy[rows].astype(F32) + norm_back(d_h * (1.0 + scale), normal, inverse)
        dx1[rows] = d_mixed
        h1[rows] = (d_mixed * mod_rows(sel[rows], mod, 2, width)).astype(BF)
        dmod[1] += item_sums(sel[rows], d_h)
        dmod[2] += item_sums(sel[rows], d_h * normal)
        dmod[0] += item_sums(sel[rows], d_mixed * br1[rows])

    over_blocks(rows_here, between)
    load_o.wait()

    def use_out(chunk):
        rows = chunk_rows(chunk, rows_here)
        datt[rows] = nt(whole1[rows], wo[...]).astype(BF)

    gather(place, h1, whole1, sems, 12, use_out)


def qkv_back_kernel(layer, square, dproj, x, dx1, sel, mod, w_own, w_other, du, du_b, dmod, w,
                    o1, i1, k1, s1, ssem, rsem, wsem):
    place = ring(square)
    rows_here, width = x.shape
    load = layer_weights(w_own, w_other, layer, w, wsem)
    greet(place)
    dmod[...] = jnp.zeros_like(dmod)
    load.wait()
    bufs = (o1, i1, k1, s1)

    def term(chunk):
        rows = chunk_rows(chunk, rows_here)
        return nt(dproj[0, rows], w[0]) + nt(dproj[1, rows], w[1]) + nt(dproj[2, rows], w[2])

    scatter(place, term, bufs, (ssem, rsem), 0)

    def finish(rows):
        d_h = scattered(bufs, rows)
        normal, inverse = normed(x[rows].astype(F32))
        scale = mod_rows(sel[rows], mod, 1, width)
        total = dx1[rows] + norm_back(d_h * (1.0 + scale), normal, inverse)
        du[rows] = total
        du_b[rows] = total.astype(BF)
        dmod[0] += item_sums(sel[rows], d_h)
        dmod[1] += item_sums(sel[rows], d_h * normal)

    over_blocks(rows_here, finish)


def ring_call(kernel, ident, outs, scratch, args, spaces):
    return pl.pallas_call(
        kernel,
        out_shape=outs,
        in_specs=[vmem() if s else anywhere() for s in spaces],
        out_specs=[vmem()] * len(outs),
        scratch_shapes=scratch,
        compiler_params=pltpu.CompilerParams(
            collective_id=ident, has_side_effects=True, vmem_limit_bytes=60 * 2**20
        ),
    )(*args)


def attention_kernel(spans, proj, gain, cosine, sine, turn, spread, ones, q, k, v, att, padded):
    heads = spread.shape[1] // PAD
    head = proj.shape[2] // heads
    scale = head ** (-0.5)
    rows = proj.shape[1]

    def units(at):
        for which, dst in ((0, q), (1, k)):
            normal, _ = unit(proj[which, at], ones[...], head)
            gained = normal * gain[which]
            turned = gained * cosine[at] + two(nn, gained, turn[...]) * sine[at]
            dst[at] = nn(turned.astype(BF), spread[...]).astype(BF)
        v[at] = nn(proj[2, at].astype(BF), spread[...]).astype(BF)

    over_blocks(rows, units)
    for item in range(3):
        start = pl.multiple_of(spans[item], 16)
        length = spans[4 + item]
        at = pl.ds(start, TILE)
        valid = lax.broadcasted_iota(jnp.int32, (TILE, TILE), 1) < length
        for n in range(heads):
            lanes = slice(n * PAD, (n + 1) * PAD)
            padded[at, lanes] = softmax_rows(q[at, lanes], k[at, lanes], v[at, lanes], valid, scale)
    first = rows - 48
    start = spans[3]
    at = pl.ds(first, 48)
    valid = first + lax.broadcasted_iota(jnp.int32, (48, 48), 1) >= start
    live = first + lax.broadcasted_iota(jnp.int32, (48, PAD), 0) >= start
    for n in range(heads):
        lanes = slice(n * PAD, (n + 1) * PAD)
        new = softmax_rows(q[at, lanes], k[at, lanes], v[at, lanes], valid, scale)
        padded[at, lanes] = jnp.where(live, new, padded[at, lanes])
    att[...] = nt(padded[...], spread[...]).astype(BF)


def unit(proj, ones, head):
    inverse = lax.rsqrt(two(nn, proj * proj, ones) * (1.0 / head) + EPS)
    return proj * inverse, inverse


def softmax_rows(query, key, value, valid, scale):
    scores = jnp.where(valid, nt(query, key) * scale, -1e30)
    raised = jnp.exp(scores - jnp.max(scores, axis=1, keepdims=True))
    probs = raised / jnp.sum(raised, axis=1, keepdims=True)
    return nn(probs.astype(BF), value).astype(BF)


def back_tile(query, key, value, grad, keys, queries, scale):
    scores = jnp.where(keys, nt(key, query) * scale, -1e30)
    raised = jnp.exp(scores - jnp.max(scores, axis=0, keepdims=True))
    probs = jnp.where(queries, raised / jnp.sum(raised, axis=0, keepdims=True), 0.0)
    d_value = nn(probs.astype(BF), grad)
    d_probs = nt(value, grad)
    inner = jnp.sum(probs * d_probs, axis=0, keepdims=True)
    d_scores = (probs * (d_probs - inner)).astype(BF)
    return tn(d_scores, key) * scale, nn(d_scores, query) * scale, d_value


def attention_back_kernel(spans, q, k, v, datt, proj, gain, cosine, sine, turn, spread, ones,
                          dproj, dgain, grad, dq, dk, dv):
    heads = spread.shape[1] // PAD
    rows, packed = datt.shape
    head = packed // heads
    scale = head ** (-0.5)
    grad[...] = nn(datt[...], spread[...]).astype(BF)
    for item in range(3):
        start = pl.multiple_of(spans[item], 16)
        length = spans[4 + item]
        at = pl.ds(start, TILE)
        keys = lax.broadcasted_iota(jnp.int32, (TILE, TILE), 0) < length
        queries = lax.broadcasted_iota(jnp.int32, (TILE, TILE), 1) < length
        for n in range(heads):
            lanes = slice(n * PAD, (n + 1) * PAD)
            parts = back_tile(
                q[at, lanes], k[at, lanes], v[at, lanes], grad[at, lanes], keys, queries, scale
            )
            dq[at, lanes], dk[at, lanes], dv[at, lanes] = parts
    first = rows - 48
    start = spans[3]
    at = pl.ds(first, 48)
    keys = first + lax.broadcasted_iota(jnp.int32, (48, 48), 0) >= start
    queries = first + lax.broadcasted_iota(jnp.int32, (48, 48), 1) >= start
    live = first + lax.broadcasted_iota(jnp.int32, (48, PAD), 0) >= start
    for n in range(heads):
        lanes = slice(n * PAD, (n + 1) * PAD)
        parts = back_tile(
            q[at, lanes], k[at, lanes], v[at, lanes], grad[at, lanes], keys, queries, scale
        )
        for new, dst in zip(parts, (dq, dk, dv)):
            dst[at, lanes] = jnp.where(live, new, dst[at, lanes])
    dgain[...] = jnp.zeros_like(dgain)

    def finish(at):
        for which, src in ((0, dq), (1, dk)):
            flat = two(nt, src[at], spread[...])
            back = flat * cosine[at] - two(nn, flat, turn[...]) * sine[at]
            normal, inverse = unit(proj[which, at], ones[...], head)
            dgain[which] += jnp.sum(back * normal, axis=0, keepdims=True)
            gained = back * gain[which]
            mean = two(nn, gained * normal, ones[...]) * (1.0 / head)
            dproj[which, at] = (inverse * (gained - normal * mean)).astype(BF)
        dproj[2, at] = nt(dv[at].astype(BF), spread[...]).astype(BF)

    over_blocks(rows, finish)


def local_call(kernel, outs, scratch, spans, args):
    return pl.pallas_call(
        kernel,
        out_shape=outs,
        in_specs=[pl.BlockSpec(memory_space=pltpu.SMEM)] + [vmem()] * len(args),
        out_specs=[vmem()] * len(outs),
        scratch_shapes=scratch,
        compiler_params=pltpu.CompilerParams(vmem_limit_bytes=60 * 2**20),
    )(spans, *args)


def swap(array):
    return lax.ppermute(array, S, [(0, 1), (1, 0)])


def head_tables(positions, packed, head):
    quarter = head // 4
    frequency = 10000.0 ** (-jnp.arange(quarter, dtype=F32) / quarter)
    lane = jnp.arange(packed) % head
    per_lane = frequency[lane % quarter][None, :]
    place = jnp.where((lane // (2 * quarter) == 0)[None, :], positions[0][:, None], positions[1][:, None])
    angle = place.astype(F32) * per_lane
    rows = jnp.arange(packed)[:, None]
    cols = jnp.arange(packed)[None, :]
    early = (cols % (2 * quarter)) < quarter
    turn = jnp.where(early & (rows == cols + quarter), -1.0, 0.0)
    turn = turn + jnp.where(~early & (rows == cols - quarter), 1.0, 0.0)
    heads = packed // head
    wide = jnp.arange(heads * PAD)[None, :]
    spread = (rows // head == wide // PAD) & (rows % head == wide % PAD)
    ones = rows // head == cols // head
    return jnp.cos(angle), jnp.sin(angle), turn.astype(BF), spread.astype(BF), ones.astype(BF)


def halves(pack, section, dp):
    wide = pack.reshape(dp, 2, -1, pack.shape[1])
    mine = lax.dynamic_index_in_dim(wide, section, 1, keepdims=False)
    theirs = lax.dynamic_index_in_dim(wide, 1 - section, 1, keepdims=False)
    return mine, theirs


def reduced(pack, section, dp):
    mine, theirs = halves(pack.astype(BF), section, dp)
    total = (mine.astype(F32) + swap(theirs).astype(F32)).astype(BF)
    return lax.psum_scatter(total, DP, scatter_dimension=0, tiled=True)[0]


def own_layer(section, pair):
    first = section == 0
    keep = jnp.where(first, pair[0], pair[1])
    got = swap(jnp.where(first, pair[1], pair[0]))
    return jnp.where(first, jnp.concatenate([keep, got]), jnp.concatenate([got, keep])).astype(F32)


def per_device(square, dp, tokens, cotangent, cond, patch_item, patch_pos, w_qkv, w_out, w_gate_up,
               w_down, qk_gain, ada_weight, ada_bias):
    section = lax.axis_index(S)
    first = section == 0
    rows, width = tokens.shape[1:]
    seq = patch_item.shape[1]
    items = cond.shape[0]
    per_micro = items // 2
    head = qk_gain.shape[-1]
    packed = w_qkv.shape[-1]
    heads = packed // head
    hidden_here = w_down.shape[1]
    own = (w_qkv[0], w_out[0], w_gate_up[0], w_down[0])
    other = tuple(swap(w) for w in own)

    cond_wide = cond.astype(F32)
    cond_sigmoid = jax.nn.sigmoid(cond_wide)
    lifted = (cond_wide * cond_sigmoid).astype(BF)
    mod_part = nn(lifted, ada_weight[0]) + ada_bias[0].astype(F32)[None, :]
    mod_all = lax.all_gather(mod_part, (S, T)).reshape(2, 4, 2, per_micro, -1)
    mod_mine = lax.dynamic_index_in_dim(mod_all, section, 2, keepdims=False)
    mod_mine = jnp.swapaxes(mod_mine, 1, 2).reshape(2, per_micro, -1)
    mod_mine = jnp.pad(mod_mine, ((0, 0), (0, 8 - per_micro), (0, 0)))
    gains = lax.all_gather(qk_gain[0], S).astype(F32)
    gains = jnp.tile(gains, (1, 1, heads)).reshape(2, 2, 1, packed)
    lifted_all = lax.all_gather(lifted, DP, tiled=True)

    ids = lax.dynamic_index_in_dim(patch_item, section, 0, keepdims=False)
    ids = jnp.where(ids >= 0, ids - lax.axis_index(DP) * items - section * per_micro, -1)
    counts = jnp.sum((ids[None, :] == jnp.arange(3)[:, None]).astype(jnp.int32), axis=1)
    starts = jnp.concatenate([jnp.zeros((1,), jnp.int32), jnp.cumsum(counts)]).astype(jnp.int32)
    spans = jnp.concatenate([starts, counts, jnp.zeros((1,), jnp.int32)])
    local_ids = lax.dynamic_slice_in_dim(ids, lax.axis_index(T) * rows, rows)
    sel = (local_ids[:, None] == jnp.arange(8)[None, :]).astype(F32)
    positions = lax.dynamic_index_in_dim(patch_pos, section, 1, keepdims=False)
    tables = head_tables(positions, packed, head)

    x = lax.dynamic_index_in_dim(tokens, section, 0, keepdims=False)
    kept = []
    for layer in range(2):
        mod = mod_mine[layer]
        whole1, proj = ring_call(
            functools.partial(qkv_kernel, layer, square),
            layer,
            [sds((seq, width), BF), sds((3, seq, packed), F32)],
            [pltpu.VMEM((rows, width), BF), pltpu.VMEM((3, width, packed), BF)]
            + dma_sems(6)
            + [pltpu.SemaphoreType.DMA],
            (x, sel, mod, own[0], other[0]),
            (1, 1, 1, 0, 0),
        )
        q, k, v, att = local_call(
            attention_kernel,
            [sds((seq, heads * PAD), BF)] * 3 + [sds((seq, packed), BF)],
            [pltpu.VMEM((seq, heads * PAD), BF)],
            spans,
            (proj, gains[layer]) + tables,
        )
        br1, x1, whole2, gate, up, hidden, br2, y = ring_call(
            functools.partial(mlp_kernel, layer, square),
            2 + layer,
            [
                sds((rows, width), F32),
                sds((rows, width), F32),
                sds((seq, width), BF),
                sds((seq, hidden_here), F32),
                sds((seq, hidden_here), F32),
                sds((seq, hidden_here), BF),
                sds((rows, width), F32),
                sds((rows, width), BF),
            ],
            [
                pltpu.VMEM((rows, width), BF),
                pltpu.VMEM((packed, width), BF),
                pltpu.VMEM((2, width, hidden_here), BF),
                pltpu.VMEM((hidden_here, width), BF),
            ]
            + scatter_scratch(rows, width)
            + scatter_scratch(rows, width)
            + dma_sems(18)
            + [pltpu.SemaphoreType.DMA((3,))],
            (att, x, sel, mod, own[1], other[1], own[2], other[2], own[3], other[3]),
            (1, 1, 1, 1) + (0,) * 6,
        )
        kept.append((x, whole1, proj, q, k, v, att, br1, x1, whole2, gate, up, hidden, br2, y))
        x = y

    dy = lax.dynamic_index_in_dim(cotangent, section, 0, keepdims=False)
    packs = [None, None]
    d_mods = [None, None]
    d_gains = [None, None]
    d_inputs = [None, None]
    for layer in (1, 0):
        x, whole1, proj, q, k, v, att, br1, x1, whole2, gate, up, hidden, br2, y = kept[layer]
        mod = mod_mine[layer]
        rows2, dgate, dup, rows1, datt, dx1, dmod_a = ring_call(
            functools.partial(mlp_back_kernel, layer, square),
            4 + layer,
            [
                sds((seq, width), BF),
                sds((seq, hidden_here), BF),
                sds((seq, hidden_here), BF),
                sds((seq, width), BF),
                sds((seq, packed), BF),
                sds((rows, width), F32),
                sds((4, 8, width), F32),
            ],
            [
                pltpu.VMEM((rows, width), BF),
                pltpu.VMEM((rows, width), BF),
                pltpu.VMEM((seq, hidden_here), F32),
                pltpu.VMEM((seq, hidden_here), F32),
                pltpu.VMEM((packed, width), BF),
                pltpu.VMEM((2, width, hidden_here), BF),
                pltpu.VMEM((hidden_here, width), BF),
            ]
            + scatter_scratch(rows, width)
            + dma_sems(18)
            + [pltpu.SemaphoreType.DMA((5,))],
            (dy, br2, br1, x1, sel, mod, gate, up, own[1], other[1], own[2], other[2], own[3],
             other[3]),
            (1,) * 6 + (0,) * 8,
        )
        grads_mlp = jnp.concatenate(
            [tn(whole2, dgate).astype(BF), tn(whole2, dup).astype(BF), tn(rows2, hidden).astype(BF)],
            axis=1,
        )
        pack_mlp = reduced(grads_mlp, section, dp)
        dproj, dgain = local_call(
            attention_back_kernel,
            [sds((3, seq, packed), BF), sds((2, 1, packed), F32)],
            [pltpu.VMEM((seq, heads * PAD), BF)] + [pltpu.VMEM((seq, heads * PAD), F32)] * 3,
            spans,
            (q, k, v, datt, proj, gains[layer]) + tables,
        )
        du, du_b, dmod_b = ring_call(
            functools.partial(qkv_back_kernel, layer, square),
            6 + layer,
            [sds((rows, width), F32), sds((rows, width), BF), sds((2, 8, width), F32)],
            [pltpu.VMEM((3, width, packed), BF)]
            + scatter_scratch(rows, width)
            + dma_sems(6)
            + [pltpu.SemaphoreType.DMA],
            (dproj, x, dx1, sel, mod, own[0], other[0]),
            (1,) * 5 + (0,) * 2,
        )
        grads_att = jnp.concatenate(
            [tn(whole1, dproj[0]).astype(BF), tn(whole1, dproj[1]).astype(BF),
             tn(whole1, dproj[2]).astype(BF), tn(rows1, att).astype(BF)],
            axis=1,
        )
        pack_att = reduced(grads_att, section, dp)
        packs[layer] = (pack_mlp, pack_att)
        d_mods[layer] = jnp.concatenate([dmod_b, dmod_a])[:, :per_micro]
        d_gains[layer] = dgain
        d_inputs[layer] = du_b if layer else du
        dy = du_b

    d_mod = jnp.stack(d_mods).swapaxes(1, 2).reshape(2 * per_micro, -1)
    d_mod = lax.psum_scatter(d_mod, T, scatter_dimension=1, tiled=True).reshape(2, per_micro, -1)
    keep = jnp.where(first, d_mod[0], d_mod[1])
    got = swap(jnp.where(first, d_mod[1], d_mod[0]))
    mod_grads = jnp.where(first, jnp.concatenate([keep, got]), jnp.concatenate([got, keep]))
    mod_grads_all = lax.all_gather(mod_grads, DP, tiled=True)
    dp_index = lax.axis_index(DP)
    part = width // dp
    lifted_part = lax.dynamic_slice_in_dim(lifted_all, dp_index * part, part, 1).astype(F32)
    g_ada_w = lax.dot_general(lifted_part, mod_grads_all, (((0,), (0,)), ((), ())), precision=PRECISE)
    bias_part = ada_bias.shape[1] // dp
    g_ada_b = lax.dynamic_slice_in_dim(jnp.sum(mod_grads_all, axis=0), dp_index * bias_part, bias_part)
    d_lifted = lax.dot_general(
        mod_grads, ada_weight[0].astype(F32), (((1,), (1,)), ((), ())), precision=PRECISE
    )
    cond_grad = (
        lax.psum(d_lifted, (S, T)) * cond_sigmoid * (1.0 + cond_wide * (1.0 - cond_sigmoid))
    )
    gain_sums = jnp.stack(d_gains).reshape(2, 2, heads, head).sum(axis=2)
    gain_sums = lax.psum(gain_sums, (S, DP, T))
    gain_total = lax.dynamic_index_in_dim(gain_sums, section, 0)

    mlp = own_layer(section, (packs[0][0], packs[1][0]))
    attn = own_layer(section, (packs[0][1], packs[1][1]))
    f = hidden_here
    g_gate_up = jnp.stack([mlp[:, :f], mlp[:, f : 2 * f]])[None]
    g_down = mlp[:, 2 * f :].T[None]
    g_qkv = jnp.stack([attn[:, k * packed : (k + 1) * packed] for k in range(3)])[None]
    g_out = attn[:, 3 * packed :].T[None]

    outs = jnp.where(first, kept[0][-1], kept[1][-1])
    outs_got = swap(jnp.where(first, kept[1][-1], kept[0][-1]))
    layer_out = jnp.where(first, jnp.stack([outs, outs_got]), jnp.stack([outs_got, outs]))
    wide_mid = d_inputs[1].astype(F32)
    back_keep = jnp.where(first, d_inputs[0], wide_mid)
    back_got = swap(jnp.where(first, wide_mid, d_inputs[0]))
    in_grads = jnp.where(first, jnp.stack([back_keep, back_got]), jnp.stack([back_got, back_keep]))
    return (
        layer_out[None],
        in_grads[None],
        cond_grad,
        g_qkv,
        g_out,
        g_gate_up,
        g_down,
        gain_total,
        g_ada_w[None],
        g_ada_b[None],
    )


def solution(mesh):
    both = (DP, T)
    in_specs = (
        P(None, both, None),
        P(None, both, None),
        P(DP, None),
        P(None, DP),
        P(None, None, DP),
        P(S, None, None, T),
        P(S, T, None),
        P(S, None, None, T),
        P(S, T, None),
        P(S, None, None),
        P(S, None, T),
        P(S, T),
    )
    out_specs = (
        P(S, None, both, None),
        P(S, None, both, None),
        P(DP, None),
        P(S, None, DP, T),
        P(S, T, DP),
        P(S, None, DP, T),
        P(S, T, DP),
        P(S, None, None),
        P(S, DP, T),
        P(S, (T, DP)),
    )
    dp = mesh.shape[DP]
    return jax.shard_map(
        functools.partial(per_device, dp <= 4, dp),
        mesh=mesh,
        in_specs=in_specs,
        out_specs=out_specs,
        check_vma=False,
    )
```

```python
import functools

import jax
import jax.numpy as jnp
import numpy as np
from jax import lax
from jax.experimental import pallas as pl
from jax.experimental.pallas import tpu as pltpu
from jax.sharding import PartitionSpec as P

EPS = 1e-06
PRECISE = lax.Precision.HIGHEST
F32 = jnp.float32
BF = jnp.bfloat16
S, DP, T = "section", "dp", "tensor"
PAD = 128
TILE = 256


def nn(a, b):
    return jnp.dot(a, b, preferred_element_type=F32)


def nt(a, b):
    return lax.dot_general(a, b, (((1,), (1,)), ((), ())), preferred_element_type=F32)


def tn(a, b):
    return lax.dot_general(a, b, (((0,), (0,)), ((), ())), preferred_element_type=F32)


def two(dot, a, b):
    high = a.astype(BF)
    low = (a - high.astype(F32)).astype(BF)
    return dot(high, b) + dot(low, b)


def sds(shape, dtype):
    return jax.ShapeDtypeStruct(shape, dtype)


def vmem():
    return pl.BlockSpec(memory_space=pltpu.VMEM)


def anywhere():
    return pl.BlockSpec(memory_space=pl.ANY)


def ring(square):
    me = lax.axis_index(T)
    near = me + 1 - 2 * (me % 2)
    if square:
        return me, near, me + 2 - 4 * (me // 2), 3 - me
    return me, near, 3 - me, (me + 2) % 4


def greet(place):
    sem = pltpu.get_barrier_semaphore()
    for peer in (place[1], place[2]):
        pl.semaphore_signal(
            sem, inc=1, device_id={T: peer}, device_id_type=pl.DeviceIdType.MESH
        )
    pl.semaphore_wait(sem, 2)


def remote(src, dst, sems, index, peer):
    return pltpu.make_async_remote_copy(
        src_ref=src,
        dst_ref=dst,
        send_sem=sems[0].at[index],
        recv_sem=sems[1].at[index],
        device_id={T: peer},
        device_id_type=pl.DeviceIdType.MESH,
    )


def chunk_rows(chunk, rows):
    return pl.ds(pl.multiple_of(chunk * rows, rows), rows)


def gather(place, mine, whole, sems, base, use, fill=()):
    me, a, b, d = place
    rows = mine.shape[0]
    half = rows // 2
    lo, hi = pl.ds(0, half), pl.ds(half, half)

    def part(chunk, upper):
        return pl.ds(pl.multiple_of(chunk * rows + upper * half, half), half)

    a0 = remote(mine.at[lo], whole.at[part(me, 0)], sems, base, a)
    b0 = remote(mine.at[hi], whole.at[part(me, 1)], sems, base + 1, b)
    a1 = remote(mine.at[hi], whole.at[part(me, 1)], sems, base + 2, a)
    b1 = remote(mine.at[lo], whole.at[part(me, 0)], sems, base + 3, b)
    for copy in (a0, b0, a1, b1):
        copy.start()
    whole[chunk_rows(me, rows), :] = mine[...]
    use(me)
    for work in fill[:1]:
        work()
    a0.wait_recv()
    b2 = remote(whole.at[part(a, 0)], whole.at[part(a, 0)], sems, base + 4, b)
    b2.start()
    b0.wait_recv()
    a2 = remote(whole.at[part(b, 1)], whole.at[part(b, 1)], sems, base + 5, a)
    a2.start()
    a1.wait_recv()
    use(a)
    b1.wait_recv()
    use(b)
    for work in fill[1:]:
        work()
    b2.wait_recv()
    a2.wait_recv()
    use(d)
    for copy in (a0, b0, a1, b1, a2, b2):
        copy.wait_send()


def scatter(place, term, bufs, sems, base, fill=()):
    me, a, b, d = place
    out, into, keep, own = bufs
    half = keep.shape[1]
    lo, hi = pl.ds(0, half), pl.ds(half, half)
    out[0] = term(d).astype(BF)
    d0 = remote(out.at[0, lo], into.at[0, lo], sems, base, a)
    d1 = remote(out.at[0, hi], into.at[0, hi], sems, base + 1, b)
    d0.start()
    d1.start()
    total = term(a)
    out[1, lo] = total[:half].astype(BF)
    a0 = remote(out.at[1, lo], into.at[1, lo], sems, base + 2, a)
    a0.start()
    keep[0] = total[half:]
    total = term(b)
    out[2, hi] = total[half:].astype(BF)
    b0 = remote(out.at[2, hi], into.at[2, hi], sems, base + 3, b)
    b0.start()
    keep[1] = total[:half]
    own[...] = term(me)
    for work in fill[:1]:
        work()
    d1.wait_recv()
    out[1, hi] = (keep[0] + into[0, hi].astype(F32)).astype(BF)
    a1 = remote(out.at[1, hi], into.at[1, hi], sems, base + 4, a)
    a1.start()
    d0.wait_recv()
    out[2, lo] = (keep[1] + into[0, lo].astype(F32)).astype(BF)
    b1 = remote(out.at[2, lo], into.at[2, lo], sems, base + 5, b)
    b1.start()
    for work in fill[1:]:
        work()
    for copy in (a0, b0, a1, b1):
        copy.wait_recv()
    for copy in (d0, d1, a0, b0, a1, b1):
        copy.wait_send()


def scattered(bufs, rows):
    return bufs[3][rows] + bufs[1][1, rows].astype(F32) + bufs[1][2, rows].astype(F32)


def scatter_scratch(rows, width):
    return [
        pltpu.VMEM((3, rows, width), BF),
        pltpu.VMEM((3, rows, width), BF),
        pltpu.VMEM((2, rows // 2, width), F32),
        pltpu.VMEM((rows, width), F32),
    ]


def dma_sems(count):
    return [pltpu.SemaphoreType.DMA((count,)), pltpu.SemaphoreType.DMA((count,))]


def layer_weights(own, other, layer, dst, sem):
    mine = lax.axis_index(S) == layer

    @pl.when(mine)
    def _():
        pltpu.make_async_copy(own, dst, sem).start()

    @pl.when(jnp.logical_not(mine))
    def _():
        pltpu.make_async_copy(other, dst, sem).start()

    return pltpu.make_async_copy(own, dst, sem)


def over_blocks(rows, fn):
    step = rows // 4

    def body(i, carry):
        fn(pl.ds(pl.multiple_of(i * step, step), step))
        return carry

    lax.fori_loop(0, 4, body, 0)


def mod_rows(sel, mod, which):
    total = sel[:, 0:1] * mod[which, 0:1]
    for item in (1, 2):
        total = total + sel[:, item : item + 1] * mod[which, item : item + 1]
    return total


def add_sums(dmod, block, sel, values):
    sums = item_sums(sel, values)
    half = dmod.shape[2]
    dmod[2 * block] += sums[:, :half]
    dmod[2 * block + 1] += sums[:, half:]


def weight_grad(x, y, flipped, col, mine, theirs):
    dp, part, _ = mine.shape
    section = lax.axis_index(S)
    width = y.shape[1]
    block = 256 if width % 256 == 0 else width
    if x is not None:
        flipped[...] = x[...].T

    def one(at, to):
        grad = nn(flipped[...], y[:, at]).astype(BF).reshape(dp, 2, part, -1)
        first = section == 0

        for target, half in ((mine, 0), (theirs, 1)):

            @pl.when(first)
            def _(target=target, half=half):
                target[:, :, to] = grad[:, half]

            @pl.when(jnp.logical_not(first))
            def _(target=target, half=half):
                target[:, :, to] = grad[:, 1 - half]

    for i in range(width // block):
        one(pl.ds(i * block, block), pl.ds(col + i * block, block))


def item_sums(sel, values):
    high = values.astype(BF)
    low = (values - high.astype(F32)).astype(BF)
    sel_b = sel.astype(BF)
    return tn(sel_b, high) + tn(sel_b, low)


def normed(values):
    inverse = lax.rsqrt(jnp.mean(values * values, axis=-1, keepdims=True) + EPS)
    return values * inverse, inverse


def norm_back(incoming, normal, inverse):
    return inverse * (incoming - normal * jnp.mean(incoming * normal, axis=-1, keepdims=True))


def qkv_kernel(layer, square, x, sel, mod, w_own, w_other, whole, proj, h, w, ssem, rsem, wsem):
    place = ring(square)
    width = x.shape[1]
    load = layer_weights(w_own, w_other, layer, w, wsem)
    greet(place)

    def prepare(rows):
        normal, _ = normed(x[rows].astype(F32))
        shift = mod_rows(sel[rows], mod, 0)
        scale = mod_rows(sel[rows], mod, 1)
        h[rows] = (normal * (1.0 + scale) + shift).astype(BF)

    over_blocks(x.shape[0], prepare)
    waited = []

    def use(chunk):
        if not waited:
            load.wait()
            waited.append(1)
        rows = chunk_rows(chunk, x.shape[0])
        for k in range(3):
            proj[k, rows] = nt(whole[rows], w[k])

    gather(place, h, whole, (ssem, rsem), 0, use)


def mlp_kernel(layer, square, att, x, sel, mod, wo0, wo1, wg0, wg1, wd0, wd1, br1, x1, whole,
               gate, up, hidden, br2, y, h, wo, wg, wd, o1, i1, k1, s1, o2, i2, k2, s2,
               ssem, rsem, wsem):
    place = ring(square)
    rows_here, width = x.shape
    load_o = layer_weights(wo0, wo1, layer, wo, wsem.at[0])
    load_g = layer_weights(wg0, wg1, layer, wg, wsem.at[1])
    load_d = layer_weights(wd0, wd1, layer, wd, wsem.at[2])
    greet(place)
    sems = (ssem, rsem)
    load_o.wait()
    first = (o1, i1, k1, s1)
    scatter(place, lambda c: nn(att[chunk_rows(c, rows_here)], wo[...]), first, sems, 0)

    def between(rows):
        branch = scattered(first, rows)
        br1[rows] = branch
        mixed = x[rows].astype(F32) + mod_rows(sel[rows], mod, 2) * branch
        x1[rows] = mixed
        normal, _ = normed(mixed)
        shift = mod_rows(sel[rows], mod, 3)
        scale = mod_rows(sel[rows], mod, 4)
        h[rows] = (normal * (1.0 + scale) + shift).astype(BF)

    over_blocks(rows_here, between)
    load_g.wait()

    def use(chunk):
        rows = chunk_rows(chunk, rows_here)
        gate[rows] = nn(whole[rows], wg[0])
        up[rows] = nn(whole[rows], wg[1])
        g = gate[rows]
        hidden[rows] = (g * jax.nn.sigmoid(g) * up[rows]).astype(BF)

    gather(place, h, whole, sems, 6, use)
    load_d.wait()
    second = (o2, i2, k2, s2)
    scatter(place, lambda c: nn(hidden[chunk_rows(c, rows_here)], wd[...]), second, sems, 12)

    def finish(rows):
        branch = scattered(second, rows)
        br2[rows] = branch
        y[rows] = (x1[rows] + mod_rows(sel[rows], mod, 5) * branch).astype(BF)

    over_blocks(rows_here, finish)


def mlp_back_kernel(layer, square, dy, br2, br1, x1, sel, mod, gate_h, up_h, hidden_h, rows_h,
                    wo0, wo1, wg0, wg1, wd0, wd1, whole1, datt, dx1, dmod, mine, theirs, h, h1,
                    whole2, dgate, dup, gate, up, hidden, saved, flipped, wo, wg, wd, o1, i1, k1,
                    s1, ssem, rsem, wsem):
    place = ring(square)
    rows_here, width = dy.shape
    load_d = layer_weights(wd0, wd1, layer, wd, wsem.at[0])
    load_gate = pltpu.make_async_copy(gate_h, gate, wsem.at[1])
    load_gate.start()
    load_up = pltpu.make_async_copy(up_h, up, wsem.at[2])
    load_up.start()
    load_g = layer_weights(wg0, wg1, layer, wg, wsem.at[3])
    load_o = layer_weights(wo0, wo1, layer, wo, wsem.at[4])
    load_hidden = pltpu.make_async_copy(hidden_h, hidden, wsem.at[5])
    load_hidden.start()
    load_rows = pltpu.make_async_copy(rows_h, saved, wsem.at[6])
    load_rows.start()
    greet(place)
    sems = (ssem, rsem)
    dmod[...] = jnp.zeros_like(dmod)

    def prepare(rows):
        incoming = dy[rows].astype(F32)
        h[rows] = (incoming * mod_rows(sel[rows], mod, 5)).astype(BF)
        add_sums(dmod, 3, sel[rows], incoming * br2[rows])

    over_blocks(rows_here, prepare)
    waited = []

    def use(chunk):
        if not waited:
            load_d.wait()
            load_gate.wait()
            load_up.wait()
            waited.append(1)
        rows = chunk_rows(chunk, rows_here)
        d_hidden = nt(whole2[rows], wd[...])
        g = gate[rows]
        s = jax.nn.sigmoid(g)
        dgate[rows] = (d_hidden * up[rows] * s * (1.0 + g * (1.0 - s))).astype(BF)
        dup[rows] = (d_hidden * g * s).astype(BF)

    gather(place, h, whole2, sems, 0, use)
    load_g.wait()
    load_hidden.wait()
    bufs = (o1, i1, k1, s1)
    f = hidden.shape[1]

    def term(chunk):
        rows = chunk_rows(chunk, rows_here)
        return nt(dgate[rows], wg[0]) + nt(dup[rows], wg[1])

    def grad_down():
        weight_grad(whole2, hidden, flipped, 2 * f, mine, theirs)

    scatter(place, term, bufs, sems, 6, (grad_down,))

    def between(rows):
        d_h = scattered(bufs, rows)
        normal, inverse = normed(x1[rows])
        scale = mod_rows(sel[rows], mod, 4)
        d_mixed = dy[rows].astype(F32) + norm_back(d_h * (1.0 + scale), normal, inverse)
        dx1[rows] = d_mixed
        h1[rows] = (d_mixed * mod_rows(sel[rows], mod, 2)).astype(BF)
        add_sums(dmod, 1, sel[rows], d_h)
        add_sums(dmod, 2, sel[rows], d_h * normal)
        add_sums(dmod, 0, sel[rows], d_mixed * br1[rows])

    over_blocks(rows_here, between)
    load_o.wait()
    load_rows.wait()

    def use_out(chunk):
        rows = chunk_rows(chunk, rows_here)
        datt[rows] = nt(whole1[rows], wo[...]).astype(BF)

    def grad_gate():
        weight_grad(saved, dgate, flipped, 0, mine, theirs)

    def grad_up():
        weight_grad(None, dup, flipped, f, mine, theirs)

    gather(place, h1, whole1, sems, 12, use_out, (grad_gate, grad_up))


def qkv_back_kernel(layer, square, dproj, x, dx1, sel, mod, part, prev, w_own, w_other, du, du_b,
                    dmod, w, o1, i1, k1, s1, ssem, rsem, wsem):
    place = ring(square)
    rows_here, width = x.shape
    load = layer_weights(w_own, w_other, layer, w, wsem)
    greet(place)
    here = dmod.at[layer]
    dmod[1 - layer] = prev[...]
    here[pl.ds(0, 4)] = jnp.zeros_like(prev[pl.ds(0, 4)])
    here[pl.ds(4, 8)] = part[...]
    load.wait()
    bufs = (o1, i1, k1, s1)

    def term(chunk):
        rows = chunk_rows(chunk, rows_here)
        return nn(dproj[0, rows], w[0]) + nn(dproj[1, rows], w[1]) + nn(dproj[2, rows], w[2])

    scatter(place, term, bufs, (ssem, rsem), 0)

    def finish(rows):
        d_h = scattered(bufs, rows)
        normal, inverse = normed(x[rows].astype(F32))
        scale = mod_rows(sel[rows], mod, 1)
        total = dx1[rows] + norm_back(d_h * (1.0 + scale), normal, inverse)
        du[rows] = total
        du_b[rows] = total.astype(BF)
        add_sums(here, 0, sel[rows], d_h)
        add_sums(here, 1, sel[rows], d_h * normal)

    over_blocks(rows_here, finish)


def cell():
    return 4 * lax.axis_index(S) + lax.axis_index(T)


def cell_id(index):
    return {S: index // 4, T: index % 4}


def greet_all(dp):
    sem = pltpu.get_barrier_semaphore()
    here, shard = cell(), lax.axis_index(DP)
    for k in range(1, 8):
        pl.semaphore_signal(
            sem, inc=1, device_id=cell_id((here + k) % 8), device_id_type=pl.DeviceIdType.MESH
        )
    for k in range(1, dp):
        pl.semaphore_signal(
            sem, inc=1, device_id={DP: (shard + k) % dp}, device_id_type=pl.DeviceIdType.MESH
        )
    pl.semaphore_wait(sem, 7 + dp - 1)


def push(src, dst, sems, index, device):
    copy = pltpu.make_async_remote_copy(
        src_ref=src,
        dst_ref=dst,
        send_sem=sems[0].at[index],
        recv_sem=sems[1].at[index],
        device_id=device,
        device_id_type=pl.DeviceIdType.MESH,
    )
    copy.start()
    return copy


def head_kernel(dp, lifted, ada_h, bias, mod, lifted_all, ada, parts, got, ssem, rsem, wsem):
    load = pltpu.make_async_copy(ada_h, ada, wsem)
    load.start()
    greet_all(dp)
    sems = (ssem, rsem)
    here, shard = cell(), lax.axis_index(DP)
    copies = []
    lifted_all[shard] = lifted[...]
    for k in range(1, dp):
        copies.append(
            push(lifted, lifted_all.at[shard], sems, 6 + k, {DP: (shard + k) % dp})
        )
    load.wait()
    half = parts.shape[3]
    for micro in range(2):
        for j in range(3):
            rows = lifted[pl.ds(micro * 8, 8)].astype(BF)
            parts[micro, j] = nt(rows, ada[pl.ds(j * half, half)]) + bias[j]
    for k in range(1, 8):
        peer = (here + k) % 8
        copies.append(push(parts.at[peer // 4], got.at[here], sems, k - 1, cell_id(peer)))
    got[here] = parts[lax.axis_index(S)]
    for copy in copies:
        copy.wait_recv()
    for layer in range(2):
        for block in range(6):
            for side in range(2):
                n = 2 * block + side
                mod[layer, block, :, pl.ds(side * half, half)] = got[4 * layer + n // 3, n % 3]
    for copy in copies:
        copy.wait_send()


def tail_kernel(dp, dmod, dgain, lifted_part, ada_h, ada_grad, bias_grad, dl_sum, gain_sum, ada,
                got, got_gain, total, total_gain, every, every_gain, lifts, ssem, rsem, wsem):
    load = pltpu.make_async_copy(ada_h, ada, wsem)
    load.start()
    greet_all(dp)
    sems = (ssem, rsem)
    here, shard = cell(), lax.axis_index(DP)
    section, place = lax.axis_index(S), lax.axis_index(T)
    sends, arrivals = [], []
    for k in range(1, 8):
        peer = (here + k) % 8
        to = cell_id(peer)
        arrivals.append(
            push(dmod.at[peer // 4, pl.ds(3 * (peer % 4), 3)], got.at[here], sems, k - 1, to)
        )
        arrivals.append(push(dgain.at[peer // 4], got_gain.at[here], sems, 6 + k, to))
    got[here] = dmod[section, pl.ds(3 * place, 3)]
    got_gain[here] = dgain[section]
    for copy in arrivals:
        copy.wait_recv()
    sends += arrivals
    for micro in range(2):
        total[micro] = (got[4 * micro] + got[4 * micro + 1]) + (got[4 * micro + 2] + got[4 * micro + 3])
    gain = got_gain[0]
    for k in range(1, 8):
        gain = gain + got_gain[k]
    total_gain[...] = gain
    arrivals = []
    for k in range(1, dp):
        to = {DP: (shard + k) % dp}
        arrivals.append(push(total, every.at[shard], sems, 13 + k, to))
        arrivals.append(push(total_gain, every_gain.at[shard], sems, 12 + dp + k, to))
    every[shard] = total[...]
    every_gain[shard] = total_gain[...]
    load.wait()
    half = total.shape[3]
    for micro in range(2):
        lift = two(nn, total[micro, 0], ada[pl.ds(0, half)])
        for j in range(1, 3):
            lift = lift + two(nn, total[micro, j], ada[pl.ds(j * half, half)])
        lifts[here, micro] = lift
    base = 13 + 2 * (dp - 1)
    lift_copies = []
    for k in range(1, 8):
        lift_copies.append(
            push(lifts.at[here], lifts.at[here], sems, base + k, cell_id((here + k) % 8))
        )
    for copy in arrivals:
        copy.wait_recv()
    sends += arrivals
    gain = every_gain[0]
    for k in range(1, dp):
        gain = gain + every_gain[k]
    gain_sum[...] = gain
    for j in range(3):
        bias = jnp.zeros((1, half), F32)
        grad = jnp.zeros((lifted_part.shape[2], half), F32)
        for k in range(dp):
            for micro in range(2):
                block = every[k, micro, j]
                bias = bias + jnp.sum(block, axis=0, keepdims=True)
                high = block.astype(BF)
                low = (block - high.astype(F32)).astype(BF)
                rows = lifted_part[2 * k + micro].astype(BF)
                grad = grad + tn(rows, high) + tn(rows, low)
        bias_grad[j] = bias
        ada_grad[:, pl.ds(j * half, half)] = grad
    for copy in lift_copies:
        copy.wait_recv()
    sends += lift_copies
    lift = lifts[0]
    for k in range(1, 8):
        lift = lift + lifts[k]
    dl_sum[...] = lift
    for copy in sends:
        copy.wait_send()


def ring_call(kernel, ident, outs, scratch, args, spaces):
    return pl.pallas_call(
        kernel,
        out_shape=outs,
        in_specs=[vmem() if s else anywhere() for s in spaces],
        out_specs=[vmem()] * len(outs),
        scratch_shapes=scratch,
        compiler_params=pltpu.CompilerParams(
            collective_id=ident, has_side_effects=True, vmem_limit_bytes=60 * 2**20
        ),
    )(*args)


def attention_kernel(spans, proj, gain, cosine, sine, turn, spread, ones, q, k, v, att, padded):
    heads = spread.shape[1] // PAD
    head = proj.shape[2] // heads
    scale = head ** (-0.5)
    rows = proj.shape[1]

    def units(at):
        for which, dst in ((0, q), (1, k)):
            normal, _ = unit(proj[which, at], ones[...], head)
            gained = normal * gain[which]
            turned = gained * cosine[at] + two(nn, gained, turn[...]) * sine[at]
            dst[at] = nn(turned.astype(BF), spread[...]).astype(BF)
        v[at] = nn(proj[2, at].astype(BF), spread[...]).astype(BF)

    over_blocks(rows, units)
    for item in range(3):
        start = pl.multiple_of(spans[item], 16)
        length = spans[4 + item]
        at = pl.ds(start, TILE)
        valid = lax.broadcasted_iota(jnp.int32, (TILE, TILE), 1) < length
        for n in range(heads):
            lanes = slice(n * PAD, (n + 1) * PAD)
            padded[at, lanes] = softmax_rows(q[at, lanes], k[at, lanes], v[at, lanes], valid, scale)
    first = rows - 48
    start = spans[3]
    at = pl.ds(first, 48)
    valid = first + lax.broadcasted_iota(jnp.int32, (48, 48), 1) >= start
    live = first + lax.broadcasted_iota(jnp.int32, (48, PAD), 0) >= start
    for n in range(heads):
        lanes = slice(n * PAD, (n + 1) * PAD)
        new = softmax_rows(q[at, lanes], k[at, lanes], v[at, lanes], valid, scale)
        padded[at, lanes] = jnp.where(live, new, padded[at, lanes])
    att[...] = nt(padded[...], spread[...]).astype(BF)


def unit(proj, ones, head):
    inverse = lax.rsqrt(two(nn, proj * proj, ones) * (1.0 / head) + EPS)
    return proj * inverse, inverse


def softmax_rows(query, key, value, valid, scale):
    scores = jnp.where(valid, nt(query, key) * scale, -1e30)
    raised = jnp.exp(scores - jnp.max(scores, axis=1, keepdims=True))
    probs = raised / jnp.sum(raised, axis=1, keepdims=True)
    return nn(probs.astype(BF), value).astype(BF)


def back_tile(query, key, value, grad, keys, queries, scale):
    scores = jnp.where(keys, nt(key, query) * scale, -1e30)
    raised = jnp.exp(scores - jnp.max(scores, axis=0, keepdims=True))
    probs = jnp.where(queries, raised / jnp.sum(raised, axis=0, keepdims=True), 0.0)
    d_value = nn(probs.astype(BF), grad)
    d_probs = nt(value, grad)
    inner = jnp.sum(probs * d_probs, axis=0, keepdims=True)
    d_scores = (probs * (d_probs - inner)).astype(BF)
    return tn(d_scores, key) * scale, nn(d_scores, query) * scale, d_value


def attention_back_kernel(spans, q, k, v, datt, proj, gain, whole, att, rows1, cosine, sine, turn,
                          spread, ones, dproj, dgain, mine, theirs, grad, dq, dk, dv, flipped):
    heads = spread.shape[1] // PAD
    rows, packed = datt.shape
    head = packed // heads
    scale = head ** (-0.5)
    grad[...] = nn(datt[...], spread[...]).astype(BF)
    for item in range(3):
        start = pl.multiple_of(spans[item], 16)
        length = spans[4 + item]
        at = pl.ds(start, TILE)
        keys = lax.broadcasted_iota(jnp.int32, (TILE, TILE), 0) < length
        queries = lax.broadcasted_iota(jnp.int32, (TILE, TILE), 1) < length
        for n in range(heads):
            lanes = slice(n * PAD, (n + 1) * PAD)
            parts = back_tile(
                q[at, lanes], k[at, lanes], v[at, lanes], grad[at, lanes], keys, queries, scale
            )
            dq[at, lanes], dk[at, lanes], dv[at, lanes] = parts
    first = rows - 48
    start = spans[3]
    at = pl.ds(first, 48)
    keys = first + lax.broadcasted_iota(jnp.int32, (48, 48), 0) >= start
    queries = first + lax.broadcasted_iota(jnp.int32, (48, 48), 1) >= start
    live = first + lax.broadcasted_iota(jnp.int32, (48, PAD), 0) >= start
    for n in range(heads):
        lanes = slice(n * PAD, (n + 1) * PAD)
        parts = back_tile(
            q[at, lanes], k[at, lanes], v[at, lanes], grad[at, lanes], keys, queries, scale
        )
        for new, dst in zip(parts, (dq, dk, dv)):
            dst[at, lanes] = jnp.where(live, new, dst[at, lanes])
    dgain[...] = jnp.zeros_like(dgain)

    def finish(at):
        for which, src in ((0, dq), (1, dk)):
            flat = two(nt, src[at], spread[...])
            back = flat * cosine[at] - two(nn, flat, turn[...]) * sine[at]
            normal, inverse = unit(proj[which, at], ones[...], head)
            dgain[which] += jnp.sum(back * normal, axis=0, keepdims=True)
            gained = back * gain[which]
            mean = two(nn, gained * normal, ones[...]) * (1.0 / head)
            dproj[which, at] = (inverse * (gained - normal * mean)).astype(BF)
        dproj[2, at] = nt(dv[at].astype(BF), spread[...]).astype(BF)

    over_blocks(rows, finish)
    for which in range(3):
        weight_grad(
            None if which else whole, dproj.at[which], flipped, which * packed, mine, theirs
        )
    weight_grad(rows1, att, flipped, 3 * packed, mine, theirs)


def local_call(kernel, outs, scratch, spans, args):
    return pl.pallas_call(
        kernel,
        out_shape=outs,
        in_specs=[pl.BlockSpec(memory_space=pltpu.SMEM)] + [vmem()] * len(args),
        out_specs=[vmem()] * len(outs),
        scratch_shapes=scratch,
        compiler_params=pltpu.CompilerParams(vmem_limit_bytes=60 * 2**20),
    )(spans, *args)


def swap(array):
    return lax.ppermute(array, S, [(0, 1), (1, 0)])


def head_tables(positions, packed, head):
    quarter = head // 4
    frequency = np.float32(10000.0) ** (-np.arange(quarter, dtype=np.float32) / quarter)
    lane = np.arange(packed) % head
    angle = np.arange(32, dtype=np.float32)[:, None] * frequency[lane % quarter][None, :]
    by_row = (lane // (2 * quarter) == 0)[None, :]
    table = np.concatenate([np.where(by_row, t, 0.0) for t in (np.cos(angle), np.sin(angle))], axis=1)
    other = np.concatenate([np.where(by_row, 0.0, t) for t in (np.cos(angle), np.sin(angle))], axis=1)
    table = jnp.asarray(np.concatenate([table, other]).astype(np.float32))
    slots = jnp.arange(32)[None, :]
    hot = jnp.concatenate(
        [positions[0][:, None] == slots, positions[1][:, None] == slots], axis=1
    ).astype(F32)
    both = jnp.dot(hot, table, precision=PRECISE)
    rows = np.arange(packed)[:, None]
    cols = np.arange(packed)[None, :]
    early = (cols % (2 * quarter)) < quarter
    turn = np.where(early & (rows == cols + quarter), -1.0, 0.0)
    turn = turn + np.where(~early & (rows == cols - quarter), 1.0, 0.0)
    heads = packed // head
    wide = np.arange(heads * PAD)[None, :]
    spread = (rows // head == wide // PAD) & (rows % head == wide % PAD)
    ones = rows // head == cols // head
    lanes = tuple(jnp.asarray(m.astype(np.float32)).astype(BF) for m in (turn, spread, ones))
    return (both[:, :packed], both[:, packed:]) + lanes


def reduced(mine, theirs):
    total = (mine.astype(F32) + swap(theirs).astype(F32)).astype(BF)
    return lax.psum_scatter(total, DP, scatter_dimension=0, tiled=True)[0]


def own_layer(section, pair):
    first = section == 0
    keep = jnp.where(first, pair[0], pair[1])
    got = swap(jnp.where(first, pair[1], pair[0]))
    return jnp.where(first, jnp.concatenate([keep, got]), jnp.concatenate([got, keep])).astype(F32)


def per_device(square, dp, tokens, cotangent, cond, patch_item, patch_pos, w_qkv, w_out, w_gate_up,
               w_down, qk_gain, ada_weight, ada_bias):
    section = lax.axis_index(S)
    first = section == 0
    rows, width = tokens.shape[1:]
    seq = patch_item.shape[1]
    items = cond.shape[0]
    per_micro = items // 2
    head = qk_gain.shape[-1]
    packed = w_qkv.shape[-1]
    heads = packed // head
    hidden_here = w_down.shape[1]
    own = (jnp.swapaxes(w_qkv[0], 1, 2), w_out[0], w_gate_up[0], w_down[0])
    other = tuple(swap(w) for w in own)

    cond_wide = cond.astype(F32)
    cond_sigmoid = jax.nn.sigmoid(cond_wide)
    lifted = (cond_wide * cond_sigmoid).astype(BF).astype(F32).reshape(2, per_micro, width)
    lifted = jnp.pad(lifted, ((0, 0), (0, 8 - per_micro), (0, 0))).reshape(16, width)
    ada = ada_weight[0].T
    half = width // 2
    bias = ada_bias.astype(F32).reshape(3, 1, half)
    mods, lifted_all = ring_call(
        functools.partial(head_kernel, dp),
        8,
        [sds((2, 6, 8, width), F32), sds((dp, 16, width), F32)],
        [
            pltpu.VMEM((3 * half, width), BF),
            pltpu.VMEM((2, 3, 8, half), F32),
            pltpu.VMEM((8, 3, 8, half), F32),
        ]
        + dma_sems(6 + dp)
        + [pltpu.SemaphoreType.DMA],
        (lifted, ada, bias),
        (1, 0, 1),
    )
    gains = lax.all_gather(qk_gain[0], S).astype(F32)
    gains = jnp.tile(gains, (1, 1, heads)).reshape(2, 2, 1, packed)
    part = width // dp
    shard = lax.axis_index(DP)
    lifted_part = lax.dynamic_slice_in_dim(lifted_all, shard * part, part, 2)
    lifted_part = lifted_part.reshape(2 * dp, 8, part)

    ids = lax.dynamic_index_in_dim(patch_item, section, 0, keepdims=False)
    ids = jnp.where(ids >= 0, ids - lax.axis_index(DP) * items - section * per_micro, -1)
    counts = jnp.sum((ids[None, :] == jnp.arange(3)[:, None]).astype(jnp.int32), axis=1)
    starts = jnp.concatenate([jnp.zeros((1,), jnp.int32), jnp.cumsum(counts)]).astype(jnp.int32)
    spans = jnp.concatenate([starts, counts, jnp.zeros((1,), jnp.int32)])
    local_ids = lax.dynamic_slice_in_dim(ids, lax.axis_index(T) * rows, rows)
    sel = (local_ids[:, None] == jnp.arange(8)[None, :]).astype(F32)
    positions = lax.dynamic_index_in_dim(patch_pos, section, 1, keepdims=False)
    tables = head_tables(positions, packed, head)

    x = lax.dynamic_index_in_dim(tokens, section, 0, keepdims=False)
    kept = []
    for layer in range(2):
        mod = mods[layer]
        whole1, proj = ring_call(
            functools.partial(qkv_kernel, layer, square),
            layer,
            [sds((seq, width), BF), sds((3, seq, packed), F32)],
            [pltpu.VMEM((rows, width), BF), pltpu.VMEM((3, packed, width), BF)]
            + dma_sems(6)
            + [pltpu.SemaphoreType.DMA],
            (x, sel, mod, own[0], other[0]),
            (1, 1, 1, 0, 0),
        )
        q, k, v, att = local_call(
            attention_kernel,
            [sds((seq, heads * PAD), BF)] * 3 + [sds((seq, packed), BF)],
            [pltpu.VMEM((seq, heads * PAD), BF)],
            spans,
            (proj, gains[layer]) + tables,
        )
        br1, x1, whole2, gate, up, hidden, br2, y = ring_call(
            functools.partial(mlp_kernel, layer, square),
            2 + layer,
            [
                sds((rows, width), F32),
                sds((rows, width), F32),
                sds((seq, width), BF),
                sds((seq, hidden_here), F32),
                sds((seq, hidden_here), F32),
                sds((seq, hidden_here), BF),
                sds((rows, width), F32),
                sds((rows, width), BF),
            ],
            [
                pltpu.VMEM((rows, width), BF),
                pltpu.VMEM((packed, width), BF),
                pltpu.VMEM((2, width, hidden_here), BF),
                pltpu.VMEM((hidden_here, width), BF),
            ]
            + scatter_scratch(rows, width)
            + scatter_scratch(rows, width)
            + dma_sems(18)
            + [pltpu.SemaphoreType.DMA((3,))],
            (att, x, sel, mod, own[1], other[1], own[2], other[2], own[3], other[3]),
            (1, 1, 1, 1) + (0,) * 6,
        )
        kept.append((x, whole1, proj, q, k, v, att, br1, x1, whole2, gate, up, hidden, br2, y))
        x = y

    dy = lax.dynamic_index_in_dim(cotangent, section, 0, keepdims=False)
    packs = [None, None]
    prev = jnp.zeros((12, 8, half), F32)
    d_gains = [None, None]
    d_inputs = [None, None]
    for layer in (1, 0):
        x, whole1, proj, q, k, v, att, br1, x1, whole2, gate, up, hidden, br2, y = kept[layer]
        mod = mods[layer]
        rows1, datt, dx1, dmod_a, mine, theirs = ring_call(
            functools.partial(mlp_back_kernel, layer, square),
            4 + layer,
            [
                sds((seq, width), BF),
                sds((seq, packed), BF),
                sds((rows, width), F32),
                sds((8, 8, half), F32),
                sds((dp, part // 2, 3 * hidden_here), BF),
                sds((dp, part // 2, 3 * hidden_here), BF),
            ],
            [
                pltpu.VMEM((rows, width), BF),
                pltpu.VMEM((rows, width), BF),
                pltpu.VMEM((seq, width), BF),
                pltpu.VMEM((seq, hidden_here), BF),
                pltpu.VMEM((seq, hidden_here), BF),
                pltpu.VMEM((seq, hidden_here), F32),
                pltpu.VMEM((seq, hidden_here), F32),
                pltpu.VMEM((seq, hidden_here), BF),
                pltpu.VMEM((seq, width), BF),
                pltpu.VMEM((width, seq), BF),
                pltpu.VMEM((packed, width), BF),
                pltpu.VMEM((2, width, hidden_here), BF),
                pltpu.VMEM((hidden_here, width), BF),
            ]
            + scatter_scratch(rows, width)
            + dma_sems(18)
            + [pltpu.SemaphoreType.DMA((7,))],
            (dy, br2, br1, x1, sel, mod, gate, up, hidden, whole2, own[1], other[1], own[2],
             other[2], own[3], other[3]),
            (1,) * 6 + (0,) * 10,
        )
        pack_mlp = reduced(mine, theirs)
        dproj, dgain, mine, theirs = local_call(
            attention_back_kernel,
            [
                sds((3, seq, packed), BF),
                sds((2, 1, packed), F32),
                sds((dp, part // 2, 4 * packed), BF),
                sds((dp, part // 2, 4 * packed), BF),
            ],
            [pltpu.VMEM((seq, heads * PAD), BF)]
            + [pltpu.VMEM((seq, heads * PAD), F32)] * 3
            + [pltpu.VMEM((width, seq), BF)],
            spans,
            (q, k, v, datt, proj, gains[layer], whole1, att, rows1) + tables,
        )
        pack_att = reduced(mine, theirs)
        du, du_b, d_mod = ring_call(
            functools.partial(qkv_back_kernel, layer, square),
            6 + layer,
            [sds((rows, width), F32), sds((rows, width), BF), sds((2, 12, 8, half), F32)],
            [pltpu.VMEM((3, packed, width), BF)]
            + scatter_scratch(rows, width)
            + dma_sems(6)
            + [pltpu.SemaphoreType.DMA],
            (dproj, x, dx1, sel, mod, dmod_a, prev, own[0], other[0]),
            (1,) * 7 + (0,) * 2,
        )
        prev = d_mod[1]
        packs[layer] = (pack_mlp, pack_att)
        d_gains[layer] = dgain
        d_inputs[layer] = du_b if layer else du
        dy = du_b

    gain_parts = jnp.pad(jnp.stack(d_gains).reshape(2, 2, packed), ((0, 0), (0, 6), (0, 0)))
    g_ada_w, bias_grad, dl_sum, gain_sum = ring_call(
        functools.partial(tail_kernel, dp),
        9,
        [
            sds((part, 3 * half), F32),
            sds((3, 1, half), F32),
            sds((2, 8, width), F32),
            sds((8, packed), F32),
        ],
        [
            pltpu.VMEM((3 * half, width), BF),
            pltpu.VMEM((8, 3, 8, half), F32),
            pltpu.VMEM((8, 8, packed), F32),
            pltpu.VMEM((2, 3, 8, half), F32),
            pltpu.VMEM((8, packed), F32),
            pltpu.VMEM((dp, 2, 3, 8, half), F32),
            pltpu.VMEM((dp, 8, packed), F32),
            pltpu.VMEM((8, 2, 8, width), F32),
        ]
        + dma_sems(13 + 2 * (dp - 1) + 8)
        + [pltpu.SemaphoreType.DMA],
        (d_mod, gain_parts, lifted_part, ada),
        (1, 1, 1, 0),
    )
    bias_part = ada_bias.shape[1] // dp
    g_ada_b = lax.dynamic_slice_in_dim(bias_grad.reshape(-1), shard * bias_part, bias_part)
    cond_grad = dl_sum[:, :per_micro].reshape(items, width) * cond_sigmoid
    cond_grad = cond_grad * (1.0 + cond_wide * (1.0 - cond_sigmoid))
    gain_total = gain_sum[:2].reshape(1, 2, heads, head).sum(axis=2)

    mlp = own_layer(section, (packs[0][0], packs[1][0]))
    attn = own_layer(section, (packs[0][1], packs[1][1]))
    f = hidden_here
    g_gate_up = jnp.stack([mlp[:, :f], mlp[:, f : 2 * f]])[None]
    g_down = mlp[:, 2 * f :].T[None]
    g_qkv = jnp.stack([attn[:, k * packed : (k + 1) * packed] for k in range(3)])[None]
    g_out = attn[:, 3 * packed :].T[None]

    outs = jnp.where(first, kept[0][-1], kept[1][-1])
    outs_got = swap(jnp.where(first, kept[1][-1], kept[0][-1]))
    layer_out = jnp.where(first, jnp.stack([outs, outs_got]), jnp.stack([outs_got, outs]))
    wide_mid = d_inputs[1].astype(F32)
    back_keep = jnp.where(first, d_inputs[0], wide_mid)
    back_got = swap(jnp.where(first, wide_mid, d_inputs[0]))
    in_grads = jnp.where(first, jnp.stack([back_keep, back_got]), jnp.stack([back_got, back_keep]))
    return (
        layer_out[None],
        in_grads[None],
        cond_grad,
        g_qkv,
        g_out,
        g_gate_up,
        g_down,
        gain_total,
        g_ada_w[None],
        g_ada_b[None],
    )


def solution(mesh):
    both = (DP, T)
    in_specs = (
        P(None, both, None),
        P(None, both, None),
        P(DP, None),
        P(None, DP),
        P(None, None, DP),
        P(S, None, None, T),
        P(S, T, None),
        P(S, None, None, T),
        P(S, T, None),
        P(S, None, None),
        P(S, None, T),
        P(S, T),
    )
    out_specs = (
        P(S, None, both, None),
        P(S, None, both, None),
        P(DP, None),
        P(S, None, DP, T),
        P(S, T, DP),
        P(S, None, DP, T),
        P(S, T, DP),
        P(S, None, None),
        P(S, DP, T),
        P(S, (T, DP)),
    )
    dp = mesh.shape[DP]
    return jax.shard_map(
        functools.partial(per_device, dp <= 4, dp),
        mesh=mesh,
        in_specs=in_specs,
        out_specs=out_specs,
        check_vma=False,
    )
```

```python
import functools

import jax
import jax.numpy as jnp
import numpy as np
from jax import lax
from jax.experimental import pallas as pl
from jax.experimental.pallas import tpu as pltpu
from jax.sharding import PartitionSpec as P


EPS = 1e-06
F32 = jnp.float32
BF = jnp.bfloat16
S, DP, T = "section", "dp", "tensor"
PAD = 128
LANES = 384
TILE = 256


def nn(a, b):
    return jnp.dot(a, b, preferred_element_type=F32)


def nt(a, b):
    return lax.dot_general(a, b, (((1,), (1,)), ((), ())), preferred_element_type=F32)


def tn(a, b):
    return lax.dot_general(a, b, (((0,), (0,)), ((), ())), preferred_element_type=F32)


def two(dot, a, b):
    high = a.astype(BF)
    low = (a - high.astype(F32)).astype(BF)
    return dot(high, b) + dot(low, b)


def sds(shape, dtype):
    return jax.ShapeDtypeStruct(shape, dtype)


def vmem():
    return pl.BlockSpec(memory_space=pltpu.VMEM)


def anywhere():
    return pl.BlockSpec(memory_space=pl.ANY)


def ring(square):
    me = lax.axis_index(T)
    near = me + 1 - 2 * (me % 2)
    if square:
        return me, near, me + 2 - 4 * (me // 2), 3 - me
    return me, near, 3 - me, (me + 2) % 4


def greet(place, partner=False):
    sem = pltpu.get_barrier_semaphore()
    for peer in (place[1], place[2]):
        pl.semaphore_signal(
            sem, inc=1, device_id={T: peer}, device_id_type=pl.DeviceIdType.MESH
        )
    if partner:
        pl.semaphore_signal(
            sem, inc=1, device_id={S: 1 - lax.axis_index(S)}, device_id_type=pl.DeviceIdType.MESH
        )
    pl.semaphore_wait(sem, 3 if partner else 2)


def remote(src, dst, sems, index, peer):
    return pltpu.make_async_remote_copy(
        src_ref=src,
        dst_ref=dst,
        send_sem=sems[0].at[index],
        recv_sem=sems[1].at[index],
        device_id={T: peer},
        device_id_type=pl.DeviceIdType.MESH,
    )


def chunk_rows(chunk, rows):
    return pl.ds(pl.multiple_of(chunk * rows, rows), rows)


def gather(place, mine, whole, sems, base, use, fill=()):
    me, a, b, d = place
    rows = mine.shape[0]
    half = rows // 2
    lo, hi = pl.ds(0, half), pl.ds(half, half)

    def part(chunk, upper):
        return pl.ds(pl.multiple_of(chunk * rows + upper * half, half), half)

    a0 = remote(mine.at[lo], whole.at[part(me, 0)], sems, base, a)
    b0 = remote(mine.at[hi], whole.at[part(me, 1)], sems, base + 1, b)
    a1 = remote(mine.at[hi], whole.at[part(me, 1)], sems, base + 2, a)
    b1 = remote(mine.at[lo], whole.at[part(me, 0)], sems, base + 3, b)
    for copy in (a0, b0, a1, b1):
        copy.start()
    whole[chunk_rows(me, rows), :] = mine[...]
    use(me)
    for work in fill[:1]:
        work()
    a0.wait_recv()
    b2 = remote(whole.at[part(a, 0)], whole.at[part(a, 0)], sems, base + 4, b)
    b2.start()
    b0.wait_recv()
    a2 = remote(whole.at[part(b, 1)], whole.at[part(b, 1)], sems, base + 5, a)
    a2.start()
    a1.wait_recv()
    use(a)
    b1.wait_recv()
    use(b)
    for work in fill[1:]:
        work()
    b2.wait_recv()
    a2.wait_recv()
    use(d)
    for copy in (a0, b0, a1, b1, a2, b2):
        copy.wait_send()


def scatter(place, term, bufs, sems, base, fill=()):
    me, a, b, d = place
    out, into, keep, own = bufs
    half = keep.shape[1]
    lo, hi = pl.ds(0, half), pl.ds(half, half)
    out[0] = term(d).astype(BF)
    d0 = remote(out.at[0, lo], into.at[0, lo], sems, base, a)
    d1 = remote(out.at[0, hi], into.at[0, hi], sems, base + 1, b)
    d0.start()
    d1.start()
    total = term(a)
    out[1, lo] = total[:half].astype(BF)
    a0 = remote(out.at[1, lo], into.at[1, lo], sems, base + 2, a)
    a0.start()
    keep[0] = total[half:]
    total = term(b)
    out[2, hi] = total[half:].astype(BF)
    b0 = remote(out.at[2, hi], into.at[2, hi], sems, base + 3, b)
    b0.start()
    keep[1] = total[:half]
    own[...] = term(me)
    for work in fill[:1]:
        work()
    d1.wait_recv()
    out[1, hi] = (keep[0] + into[0, hi].astype(F32)).astype(BF)
    a1 = remote(out.at[1, hi], into.at[1, hi], sems, base + 4, a)
    a1.start()
    d0.wait_recv()
    out[2, lo] = (keep[1] + into[0, lo].astype(F32)).astype(BF)
    b1 = remote(out.at[2, lo], into.at[2, lo], sems, base + 5, b)
    b1.start()
    for work in fill[1:]:
        work()
    for copy in (a0, b0, a1, b1):
        copy.wait_recv()
    for copy in (d0, d1, a0, b0, a1, b1):
        copy.wait_send()


def scattered(bufs, rows):
    return bufs[3][rows] + bufs[1][1, rows].astype(F32) + bufs[1][2, rows].astype(F32)


def scatter_scratch(rows, width):
    return [
        pltpu.VMEM((3, rows, width), BF),
        pltpu.VMEM((3, rows, width), BF),
        pltpu.VMEM((2, rows // 2, width), F32),
        pltpu.VMEM((rows, width), F32),
    ]


def dma_sems(count):
    return [pltpu.SemaphoreType.DMA((count,)), pltpu.SemaphoreType.DMA((count,))]


def layer_weights(own, other, layer, dst, sem):
    mine = lax.axis_index(S) == layer

    @pl.when(mine)
    def _():
        pltpu.make_async_copy(own, dst, sem).start()

    @pl.when(jnp.logical_not(mine))
    def _():
        pltpu.make_async_copy(other, dst, sem).start()

    return pltpu.make_async_copy(own, dst, sem)


def over_blocks(rows, fn):
    step = rows // 4

    def body(i, carry):
        fn(pl.ds(pl.multiple_of(i * step, step), step))
        return carry

    lax.fori_loop(0, 4, body, 0)


def mod_rows(sel, mod, which):
    total = sel[:, 0:1] * mod[which, 0:1]
    for item in (1, 2):
        total = total + sel[:, item : item + 1] * mod[which, item : item + 1]
    return total


def add_sums(dmod, block, sel, values):
    sums = item_sums(sel, values)
    half = dmod.shape[2]
    dmod[2 * block] += sums[:, :half]
    dmod[2 * block + 1] += sums[:, half:]


def weight_grad(x, y, flipped, col, packs, index):
    mine, theirs, _ = packs
    dp, part, _ = mine.shape
    first = lax.axis_index(S) == 0
    width = y.shape[1]
    block = 256 if width % 256 == 0 else width
    if x is not None:
        flipped[...] = x[...].T
    for i in range(width // block):
        to = pl.ds(col + i * block, block)
        grad = nn(flipped[...], y[:, pl.ds(i * block, block)]).astype(BF)
        grad = grad.reshape(dp, 2, part, block)

        @pl.when(first)
        def _():
            mine[:, :, to] = grad[:, 0]
            theirs[:, :, to] = grad[:, 1]

        @pl.when(jnp.logical_not(first))
        def _():
            mine[:, :, to] = grad[:, 1]
            theirs[:, :, to] = grad[:, 0]

    return index, col, width


def send_half(packs, sems, job):
    index, col, width = job
    at = pl.ds(col, width)
    return push(
        packs[1].at[:, :, at], packs[2].at[:, :, at], sems, index, {S: 1 - lax.axis_index(S)}
    )


def add_halves(packs, copies, total):
    for copy in copies:
        copy.wait_recv()
    for k in range(total.shape[0]):
        total[k] = (packs[0][k].astype(F32) + packs[2][k].astype(F32)).astype(BF)
    for copy in copies:
        copy.wait_send()


def item_sums(sel, values):
    high = values.astype(BF)
    low = (values - high.astype(F32)).astype(BF)
    sel_b = sel.astype(BF)
    return tn(sel_b, high) + tn(sel_b, low)


def normed(values):
    inverse = lax.rsqrt(jnp.mean(values * values, axis=-1, keepdims=True) + EPS)
    return values * inverse, inverse


def norm_back(incoming, normal, inverse):
    return inverse * (incoming - normal * jnp.mean(incoming * normal, axis=-1, keepdims=True))


def qkv_kernel(layer, square, x, sel, mod, w_own, w_other, whole, proj, h, w, ssem, rsem, wsem):
    place = ring(square)
    load = layer_weights(w_own, w_other, layer, w, wsem)
    greet(place)

    def prepare(rows):
        normal, _ = normed(x[rows].astype(F32))
        shift = mod_rows(sel[rows], mod, 0)
        scale = mod_rows(sel[rows], mod, 1)
        h[rows] = (normal * (1.0 + scale) + shift).astype(BF)

    over_blocks(x.shape[0], prepare)
    waited = []

    def use(chunk):
        if not waited:
            load.wait()
            waited.append(1)
        rows = chunk_rows(chunk, x.shape[0])
        for k in range(3):
            proj[k, rows] = nt(whole[rows], w[k])

    gather(place, h, whole, (ssem, rsem), 0, use)


def mlp_kernel(layer, square, att, x, sel, mod, wo0, wo1, wg0, wg1, wd0, wd1, br1, x1, whole,
               gate, up, hidden, br2, y, h, wo, wg, wd, o1, i1, k1, s1, o2, i2, k2, s2,
               ssem, rsem, wsem):
    place = ring(square)
    rows_here, _ = x.shape
    load_o = layer_weights(wo0, wo1, layer, wo, wsem.at[0])
    load_g = layer_weights(wg0, wg1, layer, wg, wsem.at[1])
    load_d = layer_weights(wd0, wd1, layer, wd, wsem.at[2])
    greet(place)
    sems = (ssem, rsem)
    load_o.wait()
    first = (o1, i1, k1, s1)
    scatter(place, lambda c: nn(att[chunk_rows(c, rows_here)], wo[...]), first, sems, 0)

    def between(rows):
        branch = scattered(first, rows)
        br1[rows] = branch
        mixed = x[rows].astype(F32) + mod_rows(sel[rows], mod, 2) * branch
        x1[rows] = mixed
        normal, _ = normed(mixed)
        shift = mod_rows(sel[rows], mod, 3)
        scale = mod_rows(sel[rows], mod, 4)
        h[rows] = (normal * (1.0 + scale) + shift).astype(BF)

    over_blocks(rows_here, between)
    load_g.wait()

    def use(chunk):
        rows = chunk_rows(chunk, rows_here)
        gate[rows] = nn(whole[rows], wg[0])
        up[rows] = nn(whole[rows], wg[1])
        g = gate[rows]
        hidden[rows] = (g * jax.nn.sigmoid(g) * up[rows]).astype(BF)

    gather(place, h, whole, sems, 6, use)
    load_d.wait()
    second = (o2, i2, k2, s2)
    scatter(place, lambda c: nn(hidden[chunk_rows(c, rows_here)], wd[...]), second, sems, 12)

    def finish(rows):
        branch = scattered(second, rows)
        br2[rows] = branch
        y[rows] = (x1[rows] + mod_rows(sel[rows], mod, 5) * branch).astype(BF)

    over_blocks(rows_here, finish)


def mlp_back_kernel(layer, square, dy, br2, br1, x1, sel, mod, gate_h, up_h, hidden_h, rows_h,
                    wo0, wo1, wg0, wg1, wd0, wd1, whole1, datt, dx1, dmod, total, mine, theirs,
                    got, h, h1, whole2, dgate, dup, gate, up, hidden, saved, flipped, wo, wg, wd, o1, i1, k1,
                    s1, ssem, rsem, wsem):
    place = ring(square)
    rows_here, _ = dy.shape
    load_d = layer_weights(wd0, wd1, layer, wd, wsem.at[0])
    load_gate = pltpu.make_async_copy(gate_h, gate, wsem.at[1])
    load_gate.start()
    load_up = pltpu.make_async_copy(up_h, up, wsem.at[2])
    load_up.start()
    load_g = layer_weights(wg0, wg1, layer, wg, wsem.at[3])
    load_o = layer_weights(wo0, wo1, layer, wo, wsem.at[4])
    load_hidden = pltpu.make_async_copy(hidden_h, hidden, wsem.at[5])
    load_hidden.start()
    load_rows = pltpu.make_async_copy(rows_h, saved, wsem.at[6])
    load_rows.start()
    greet(place, True)
    sems = (ssem, rsem)
    dmod[...] = jnp.zeros_like(dmod)

    def prepare(rows):
        incoming = dy[rows].astype(F32)
        h[rows] = (incoming * mod_rows(sel[rows], mod, 5)).astype(BF)
        add_sums(dmod, 3, sel[rows], incoming * br2[rows])

    over_blocks(rows_here, prepare)
    waited = []

    def use(chunk):
        if not waited:
            load_d.wait()
            load_gate.wait()
            load_up.wait()
            waited.append(1)
        rows = chunk_rows(chunk, rows_here)
        d_hidden = nt(whole2[rows], wd[...])
        g = gate[rows]
        s = jax.nn.sigmoid(g)
        dgate[rows] = (d_hidden * up[rows] * s * (1.0 + g * (1.0 - s))).astype(BF)
        dup[rows] = (d_hidden * g * s).astype(BF)

    gather(place, h, whole2, sems, 0, use)
    load_g.wait()
    load_hidden.wait()
    bufs = (o1, i1, k1, s1)
    f = hidden.shape[1]

    def term(chunk):
        rows = chunk_rows(chunk, rows_here)
        return nt(dgate[rows], wg[0]) + nt(dup[rows], wg[1])

    packs = (mine, theirs, got)
    copies = []

    def grad(index, x, y, col):
        job = weight_grad(x, y, flipped, col, packs, index)
        copies.append(send_half(packs, sems, job))

    def grad_down():
        grad(18, whole2, hidden, 2 * f)

    scatter(place, term, bufs, sems, 6, (grad_down,))

    def between(rows):
        d_h = scattered(bufs, rows)
        normal, inverse = normed(x1[rows])
        scale = mod_rows(sel[rows], mod, 4)
        d_mixed = dy[rows].astype(F32) + norm_back(d_h * (1.0 + scale), normal, inverse)
        dx1[rows] = d_mixed
        h1[rows] = (d_mixed * mod_rows(sel[rows], mod, 2)).astype(BF)
        add_sums(dmod, 1, sel[rows], d_h)
        add_sums(dmod, 2, sel[rows], d_h * normal)
        add_sums(dmod, 0, sel[rows], d_mixed * br1[rows])

    over_blocks(rows_here, between)
    load_o.wait()
    load_rows.wait()

    def use_out(chunk):
        rows = chunk_rows(chunk, rows_here)
        datt[rows] = nt(whole1[rows], wo[...]).astype(BF)

    def grad_gate():
        grad(19, saved, dgate, 0)

    def grad_up():
        grad(20, None, dup, f)

    gather(place, h1, whole1, sems, 12, use_out, (grad_gate, grad_up))
    add_halves(packs, copies, total)


def qkv_back_kernel(layer, square, dproj, x, dx1, sel, mod, part, prev, w_own, w_other, whole_h,
                    att_h, rows1_h, du, du_b, dmod, total, w, whole, att, rows1, flipped, mine,
                    theirs, got, o1, i1, k1, s1, ssem, rsem, wsem):
    place = ring(square)
    rows_here, _ = x.shape
    load = layer_weights(w_own, w_other, layer, w, wsem.at[0])
    loads = []
    for n, (src, dst) in enumerate(((whole_h, whole), (att_h, att), (rows1_h, rows1))):
        loads.append(pltpu.make_async_copy(src, dst, wsem.at[1 + n]))
        loads[n].start()
    greet(place, True)
    here = dmod.at[layer]
    dmod[1 - layer] = prev[...]
    here[pl.ds(0, 4)] = jnp.zeros_like(prev[pl.ds(0, 4)])
    here[pl.ds(4, 8)] = part[...]
    load.wait()
    bufs = (o1, i1, k1, s1)
    sems = (ssem, rsem)
    packs = (mine, theirs, got)
    packed = att.shape[1]
    copies = []

    def term(chunk):
        rows = chunk_rows(chunk, rows_here)
        return nn(dproj[0, rows], w[0]) + nn(dproj[1, rows], w[1]) + nn(dproj[2, rows], w[2])

    def grad_in():
        loads[0].wait()
        for k in range(3):
            weight_grad(None if k else whole, dproj.at[k], flipped, k * packed, packs, 6)

    def grad_out():
        loads[1].wait()
        loads[2].wait()
        weight_grad(rows1, att, flipped, 3 * packed, packs, 6)
        copies.append(send_half(packs, sems, (6, 0, 4 * packed)))

    scatter(place, term, bufs, sems, 0, (grad_in, grad_out))

    def finish(rows):
        d_h = scattered(bufs, rows)
        normal, inverse = normed(x[rows].astype(F32))
        scale = mod_rows(sel[rows], mod, 1)
        total_rows = dx1[rows] + norm_back(d_h * (1.0 + scale), normal, inverse)
        du[rows] = total_rows
        du_b[rows] = total_rows.astype(BF)
        add_sums(here, 0, sel[rows], d_h)
        add_sums(here, 1, sel[rows], d_h * normal)

    over_blocks(rows_here, finish)
    add_halves(packs, copies, total)


def cell():
    return 4 * lax.axis_index(S) + lax.axis_index(T)


def cell_id(index):
    return {S: index // 4, T: index % 4}


def greet_all(dp):
    sem = pltpu.get_barrier_semaphore()
    here, shard = cell(), lax.axis_index(DP)
    for k in range(1, 8):
        pl.semaphore_signal(
            sem, inc=1, device_id=cell_id((here + k) % 8), device_id_type=pl.DeviceIdType.MESH
        )
    for k in range(1, dp):
        pl.semaphore_signal(
            sem, inc=1, device_id={DP: (shard + k) % dp}, device_id_type=pl.DeviceIdType.MESH
        )
    pl.semaphore_wait(sem, 7 + dp - 1)


def push(src, dst, sems, index, device):
    copy = pltpu.make_async_remote_copy(
        src_ref=src,
        dst_ref=dst,
        send_sem=sems[0].at[index],
        recv_sem=sems[1].at[index],
        device_id=device,
        device_id_type=pl.DeviceIdType.MESH,
    )
    copy.start()
    return copy


def head_kernel(dp, lifted, ada_h, bias, gain, items, pos, tables, mod, lifted_all, gains, sel,
                both, spans, ada, parts, got, wide, tall, ssem, rsem, wsem):
    load = pltpu.make_async_copy(ada_h, ada, wsem)
    load.start()
    greet_all(dp)
    sems = (ssem, rsem)
    here, shard, section = cell(), lax.axis_index(DP), lax.axis_index(S)
    copies = [push(gain, gains.at[section], sems, 6 + dp, {S: 1 - section})]
    gains[section] = gain[...]
    lifted_all[shard] = lifted[...]
    for k in range(1, dp):
        copies.append(
            push(lifted, lifted_all.at[shard], sems, 6 + k, {DP: (shard + k) % dp})
        )
    load.wait()
    half = parts.shape[3]
    for micro in range(2):
        for j in range(3):
            rows = lifted[pl.ds(micro * 8, 8)].astype(BF)
            parts[micro, j] = nt(rows, ada[pl.ds(j * half, half)]) + bias[j]
    for k in range(1, 8):
        peer = (here + k) % 8
        copies.append(push(parts.at[peer // 4], got.at[here], sems, k - 1, cell_id(peer)))
    got[here] = parts[section]
    rows_here = sel.shape[0]
    base = shard * 6 + section * 3
    seq = items.shape[1]
    line = items[pl.ds(section, 1), :]
    wide[...] = jnp.zeros_like(wide)
    wide[0:1] = (line - base).astype(F32)
    wide[1:2] = pos[0, pl.ds(section, 1), :].astype(F32)
    wide[2:3] = pos[1, pl.ds(section, 1), :].astype(F32)
    start = 0
    spans[0] = 0
    for j in range(3):
        count = jnp.sum((wide[0:1] == j).astype(F32)).astype(jnp.int32)
        spans[4 + j] = count
        start = start + count
        spans[1 + j] = start
    spans[7] = 0
    tall[...] = wide[...].T
    own = tall[pl.ds(pl.multiple_of(lax.axis_index(T) * rows_here, rows_here), rows_here), :]
    lane = lax.broadcasted_iota(jnp.int32, (rows_here, 8), 1).astype(F32)
    sel[...] = ((own[:, 0:1] == lane) & (lane < 3.0)).astype(F32)
    lane = lax.broadcasted_iota(jnp.int32, (seq, 64), 1).astype(F32)
    hot = jnp.where(lane < 32.0, tall[:, 1:2], tall[:, 2:3] + 32.0) == lane
    hot = hot.astype(F32).astype(BF)
    both[...] = (nn(hot, tables[0]) + nn(hot, tables[1])) + nn(hot, tables[2])
    for copy in copies:
        copy.wait_recv()
    for layer in range(2):
        for block in range(6):
            for side in range(2):
                n = 2 * block + side
                mod[layer, block, :, pl.ds(side * half, half)] = got[4 * layer + n // 3, n % 3]
    for copy in copies:
        copy.wait_send()


def tail_kernel(dp, dmod, dgain, lifted_part, ada_h, ada_grad, bias_grad, dl_sum, gain_sum, ada,
                got, got_gain, total, total_gain, every, every_gain, lifts, ssem, rsem, wsem):
    load = pltpu.make_async_copy(ada_h, ada, wsem)
    load.start()
    greet_all(dp)
    sems = (ssem, rsem)
    here, shard = cell(), lax.axis_index(DP)
    section, place = lax.axis_index(S), lax.axis_index(T)
    sends, arrivals = [], []
    for k in range(1, 8):
        peer = (here + k) % 8
        to = cell_id(peer)
        arrivals.append(
            push(dmod.at[peer // 4, pl.ds(3 * (peer % 4), 3)], got.at[here], sems, k - 1, to)
        )
        arrivals.append(push(dgain.at[peer // 4], got_gain.at[here], sems, 6 + k, to))
    got[here] = dmod[section, pl.ds(3 * place, 3)]
    got_gain[here] = dgain[section]
    for copy in arrivals:
        copy.wait_recv()
    sends += arrivals
    for micro in range(2):
        total[micro] = (got[4 * micro] + got[4 * micro + 1]) + (got[4 * micro + 2] + got[4 * micro + 3])
    gain = got_gain[0]
    for k in range(1, 8):
        gain = gain + got_gain[k]
    total_gain[...] = gain
    arrivals = []
    for k in range(1, dp):
        to = {DP: (shard + k) % dp}
        arrivals.append(push(total, every.at[shard], sems, 13 + k, to))
        arrivals.append(push(total_gain, every_gain.at[shard], sems, 12 + dp + k, to))
    every[shard] = total[...]
    every_gain[shard] = total_gain[...]
    load.wait()
    half = total.shape[3]
    for micro in range(2):
        lift = two(nn, total[micro, 0], ada[pl.ds(0, half)])
        for j in range(1, 3):
            lift = lift + two(nn, total[micro, j], ada[pl.ds(j * half, half)])
        lifts[here, micro] = lift
    base = 13 + 2 * (dp - 1)
    lift_copies = []
    for k in range(1, 8):
        lift_copies.append(
            push(lifts.at[here], lifts.at[here], sems, base + k, cell_id((here + k) % 8))
        )
    for copy in arrivals:
        copy.wait_recv()
    sends += arrivals
    gain = every_gain[0]
    for k in range(1, dp):
        gain = gain + every_gain[k]
    gain_sum[...] = gain
    for j in range(3):
        bias = jnp.zeros((1, half), F32)
        grad = jnp.zeros((lifted_part.shape[2], half), F32)
        for k in range(dp):
            for micro in range(2):
                block = every[k, micro, j]
                bias = bias + jnp.sum(block, axis=0, keepdims=True)
                high = block.astype(BF)
                low = (block - high.astype(F32)).astype(BF)
                rows = lifted_part[2 * k + micro].astype(BF)
                grad = grad + tn(rows, high) + tn(rows, low)
        bias_grad[j] = bias
        ada_grad[:, pl.ds(j * half, half)] = grad
    for copy in lift_copies:
        copy.wait_recv()
    sends += lift_copies
    lift = lifts[0]
    for k in range(1, 8):
        lift = lift + lifts[k]
    dl_sum[...] = lift
    for copy in sends:
        copy.wait_send()


def price(micros):
    return pl.CostEstimate(flops=0, bytes_accessed=int(micros * 3.5e6), transcendentals=0)


def ring_call(kernel, ident, micros, outs, scratch, args, spaces, scalar=-1):
    return pl.pallas_call(
        kernel,
        out_shape=outs,
        in_specs=[vmem() if s else anywhere() for s in spaces],
        out_specs=[
            pl.BlockSpec(memory_space=pltpu.SMEM) if n == scalar else vmem()
            for n in range(len(outs))
        ],
        scratch_shapes=scratch,
        compiler_params=pltpu.CompilerParams(
            collective_id=ident, has_side_effects=True, vmem_limit_bytes=60 * 2**20
        ),
        cost_estimate=price(micros),
    )(*args)


def attention_kernel(spans, proj, gain, both, turn, spread, ones, q, k, v, att, padded):
    heads = spread.shape[1] // PAD
    packed = proj.shape[2]
    head = packed // heads
    scale = head ** (-0.5)
    rows = proj.shape[1]

    def units(at):
        for which, dst in ((0, q), (1, k)):
            normal, _ = unit(proj[which, at], ones[...], head)
            gained = normal * gain[which : which + 1]
            turned = gained * both[at, 0:packed]
            turned = turned + two(nn, gained, turn[...]) * both[at, LANES : LANES + packed]
            dst[at] = nn(turned.astype(BF), spread[...]).astype(BF)
        v[at] = nn(proj[2, at].astype(BF), spread[...]).astype(BF)

    over_blocks(rows, units)
    for item in range(3):
        start = pl.multiple_of(spans[item], 16)
        length = spans[4 + item]
        at = pl.ds(start, TILE)
        valid = lax.broadcasted_iota(jnp.int32, (TILE, TILE), 1) < length
        for n in range(heads):
            lanes = slice(n * PAD, (n + 1) * PAD)
            padded[at, lanes] = softmax_rows(q[at, lanes], k[at, lanes], v[at, lanes], valid, scale)
    first = rows - 48
    start = spans[3]
    at = pl.ds(first, 48)
    valid = first + lax.broadcasted_iota(jnp.int32, (48, 48), 1) >= start
    live = first + lax.broadcasted_iota(jnp.int32, (48, PAD), 0) >= start
    for n in range(heads):
        lanes = slice(n * PAD, (n + 1) * PAD)
        new = softmax_rows(q[at, lanes], k[at, lanes], v[at, lanes], valid, scale)
        padded[at, lanes] = jnp.where(live, new, padded[at, lanes])
    att[...] = nt(padded[...], spread[...]).astype(BF)


def unit(proj, ones, head):
    inverse = lax.rsqrt(two(nn, proj * proj, ones) * (1.0 / head) + EPS)
    return proj * inverse, inverse


def softmax_rows(query, key, value, valid, scale):
    scores = jnp.where(valid, nt(query, key) * scale, -1e30)
    raised = jnp.exp(scores - jnp.max(scores, axis=1, keepdims=True))
    probs = raised / jnp.sum(raised, axis=1, keepdims=True)
    return nn(probs.astype(BF), value).astype(BF)


def back_tile(query, key, value, grad, keys, queries, scale):
    scores = jnp.where(keys, nt(key, query) * scale, -1e30)
    raised = jnp.exp(scores - jnp.max(scores, axis=0, keepdims=True))
    probs = jnp.where(queries, raised / jnp.sum(raised, axis=0, keepdims=True), 0.0)
    d_value = nn(probs.astype(BF), grad)
    d_probs = nt(value, grad)
    inner = jnp.sum(probs * d_probs, axis=0, keepdims=True)
    d_scores = (probs * (d_probs - inner)).astype(BF)
    return tn(d_scores, key) * scale, nn(d_scores, query) * scale, d_value


def attention_back_kernel(spans, q, k, v, datt, proj, gain, both, turn, spread, ones, dproj,
                          dgain, grad, dq, dk, dv):
    heads = spread.shape[1] // PAD
    rows, packed = datt.shape
    head = packed // heads
    scale = head ** (-0.5)
    grad[...] = nn(datt[...], spread[...]).astype(BF)
    for item in range(3):
        start = pl.multiple_of(spans[item], 16)
        length = spans[4 + item]
        at = pl.ds(start, TILE)
        keys = lax.broadcasted_iota(jnp.int32, (TILE, TILE), 0) < length
        queries = lax.broadcasted_iota(jnp.int32, (TILE, TILE), 1) < length
        for n in range(heads):
            lanes = slice(n * PAD, (n + 1) * PAD)
            parts = back_tile(
                q[at, lanes], k[at, lanes], v[at, lanes], grad[at, lanes], keys, queries, scale
            )
            dq[at, lanes], dk[at, lanes], dv[at, lanes] = parts
    first = rows - 48
    start = spans[3]
    at = pl.ds(first, 48)
    keys = first + lax.broadcasted_iota(jnp.int32, (48, 48), 0) >= start
    queries = first + lax.broadcasted_iota(jnp.int32, (48, 48), 1) >= start
    live = first + lax.broadcasted_iota(jnp.int32, (48, PAD), 0) >= start
    for n in range(heads):
        lanes = slice(n * PAD, (n + 1) * PAD)
        parts = back_tile(
            q[at, lanes], k[at, lanes], v[at, lanes], grad[at, lanes], keys, queries, scale
        )
        for new, dst in zip(parts, (dq, dk, dv)):
            dst[at, lanes] = jnp.where(live, new, dst[at, lanes])
    dgain[...] = jnp.zeros_like(dgain)

    def finish(at):
        for which, src in ((0, dq), (1, dk)):
            flat = two(nt, src[at], spread[...])
            back = flat * both[at, 0:packed]
            back = back - two(nn, flat, turn[...]) * both[at, LANES : LANES + packed]
            normal, inverse = unit(proj[which, at], ones[...], head)
            dgain[which] += jnp.sum(back * normal, axis=0, keepdims=True)
            gained = back * gain[which : which + 1]
            mean = two(nn, gained * normal, ones[...]) * (1.0 / head)
            dproj[which, at] = (inverse * (gained - normal * mean)).astype(BF)
        dproj[2, at] = nt(dv[at].astype(BF), spread[...]).astype(BF)

    over_blocks(rows, finish)


def local_call(kernel, micros, outs, scratch, spans, args):
    return pl.pallas_call(
        kernel,
        out_shape=outs,
        in_specs=[pl.BlockSpec(memory_space=pltpu.SMEM)] + [vmem()] * len(args),
        out_specs=[vmem()] * len(outs),
        scratch_shapes=scratch,
        compiler_params=pltpu.CompilerParams(vmem_limit_bytes=60 * 2**20),
        cost_estimate=price(micros),
    )(spans, *args)


def swap(array):
    return lax.ppermute(array, S, [(0, 1), (1, 0)])


def head_tables(packed, head):
    quarter = head // 4
    frequency = np.float32(10000.0) ** (-np.arange(quarter, dtype=np.float32) / quarter)
    lane = np.arange(packed) % head
    angle = np.arange(32, dtype=np.float32)[:, None] * frequency[lane % quarter][None, :]
    by_row = (lane // (2 * quarter) == 0)[None, :]
    table = np.zeros((64, 2 * LANES), np.float32)
    for n, values in enumerate((np.cos(angle), np.sin(angle))):
        at = slice(n * LANES, n * LANES + packed)
        table[:32, at] = np.where(by_row, values, 0.0)
        table[32:, at] = np.where(by_row, 0.0, values)
    table = jnp.asarray(table)
    parts = []
    for _ in range(3):
        parts.append(lax.reduce_precision(table, 8, 7).astype(BF))
        table = table - parts[-1].astype(F32)
    rows = np.arange(packed)[:, None]
    cols = np.arange(packed)[None, :]
    early = (cols % (2 * quarter)) < quarter
    turn = np.where(early & (rows == cols + quarter), -1.0, 0.0)
    turn = turn + np.where(~early & (rows == cols - quarter), 1.0, 0.0)
    heads = packed // head
    wide = np.arange(heads * PAD)[None, :]
    spread = (rows // head == wide // PAD) & (rows % head == wide % PAD)
    ones = rows // head == cols // head
    lanes = tuple(jnp.asarray(m.astype(np.float32)).astype(BF) for m in (turn, spread, ones))
    return jnp.stack(parts), lanes


def reduced(total):
    return lax.psum_scatter(total, DP, scatter_dimension=0, tiled=True)[0]


def own_layer(section, pair):
    first = section == 0
    keep = jnp.where(first, pair[0], pair[1])
    got = swap(jnp.where(first, pair[1], pair[0]))
    return jnp.where(first, jnp.concatenate([keep, got]), jnp.concatenate([got, keep])).astype(F32)


def per_device(square, dp, tokens, cotangent, cond, patch_item, patch_pos, w_qkv, w_out, w_gate_up,
               w_down, qk_gain, ada_weight, ada_bias):
    section = lax.axis_index(S)
    first = section == 0
    rows, width = tokens.shape[1:]
    seq = patch_item.shape[1]
    items = cond.shape[0]
    per_micro = items // 2
    head = qk_gain.shape[-1]
    packed = w_qkv.shape[-1]
    heads = packed // head
    hidden_here = w_down.shape[1]
    own = (jnp.swapaxes(w_qkv[0], 1, 2), w_out[0], w_gate_up[0], w_down[0])
    other = tuple(swap(w) for w in own)

    cond_wide = cond.astype(F32)
    cond_sigmoid = jax.nn.sigmoid(cond_wide)
    lifted = (cond_wide * cond_sigmoid).astype(BF).astype(F32).reshape(2, per_micro, width)
    lifted = jnp.pad(lifted, ((0, 0), (0, 8 - per_micro), (0, 0))).reshape(16, width)
    ada = ada_weight[0].T
    half = width // 2
    bias = ada_bias.astype(F32).reshape(3, 1, half)
    gain = jnp.tile(qk_gain[0].astype(F32), (1, heads))
    gain = jnp.pad(gain, ((0, 6), (0, 0)))
    trig, lanes = head_tables(packed, head)
    mods, lifted_all, gains, sel, both, spans = ring_call(
        functools.partial(head_kernel, dp),
        8,
        12,
        [
            sds((2, 6, 8, width), F32),
            sds((dp, 16, width), F32),
            sds((2, 8, packed), F32),
            sds((rows, 8), F32),
            sds((seq, 2 * LANES), F32),
            sds((8,), jnp.int32),
        ],
        [
            pltpu.VMEM((3 * half, width), BF),
            pltpu.VMEM((2, 3, 8, half), F32),
            pltpu.VMEM((8, 3, 8, half), F32),
            pltpu.VMEM((8, seq), F32),
            pltpu.VMEM((seq, 8), F32),
        ]
        + dma_sems(7 + dp)
        + [pltpu.SemaphoreType.DMA],
        (lifted, ada, bias, gain, patch_item, patch_pos, trig),
        (1, 0, 1, 1, 1, 1, 1),
        scalar=5,
    )
    tables = (both,) + lanes
    part = width // dp
    shard = lax.axis_index(DP)
    lifted_part = lax.dynamic_slice_in_dim(lifted_all, shard * part, part, 2)
    lifted_part = lifted_part.reshape(2 * dp, 8, part)

    x = lax.dynamic_index_in_dim(tokens, section, 0, keepdims=False)
    kept = []
    for layer in range(2):
        mod = mods[layer]
        whole1, proj = ring_call(
            functools.partial(qkv_kernel, layer, square),
            layer,
            20,
            [sds((seq, width), BF), sds((3, seq, packed), F32)],
            [pltpu.VMEM((rows, width), BF), pltpu.VMEM((3, packed, width), BF)]
            + dma_sems(6)
            + [pltpu.SemaphoreType.DMA],
            (x, sel, mod, own[0], other[0]),
            (1, 1, 1, 0, 0),
        )
        q, k, v, att = local_call(
            attention_kernel,
            12,
            [sds((seq, heads * PAD), BF)] * 3 + [sds((seq, packed), BF)],
            [pltpu.VMEM((seq, heads * PAD), BF)],
            spans,
            (proj, gains[layer]) + tables,
        )
        br1, x1, whole2, gate, up, hidden, br2, y = ring_call(
            functools.partial(mlp_kernel, layer, square),
            2 + layer,
            48,
            [
                sds((rows, width), F32),
                sds((rows, width), F32),
                sds((seq, width), BF),
                sds((seq, hidden_here), F32),
                sds((seq, hidden_here), F32),
                sds((seq, hidden_here), BF),
                sds((rows, width), F32),
                sds((rows, width), BF),
            ],
            [
                pltpu.VMEM((rows, width), BF),
                pltpu.VMEM((packed, width), BF),
                pltpu.VMEM((2, width, hidden_here), BF),
                pltpu.VMEM((hidden_here, width), BF),
            ]
            + scatter_scratch(rows, width)
            + scatter_scratch(rows, width)
            + dma_sems(18)
            + [pltpu.SemaphoreType.DMA((3,))],
            (att, x, sel, mod, own[1], other[1], own[2], other[2], own[3], other[3]),
            (1, 1, 1, 1) + (0,) * 6,
        )
        kept.append((x, whole1, proj, q, k, v, att, br1, x1, whole2, gate, up, hidden, br2, y))
        x = y

    dy = lax.dynamic_index_in_dim(cotangent, section, 0, keepdims=False)
    packs = [None, None]
    prev = jnp.zeros((12, 8, half), F32)
    d_gains = [None, None]
    d_inputs = [None, None]
    for layer in (1, 0):
        x, whole1, proj, q, k, v, att, br1, x1, whole2, gate, up, hidden, br2, y = kept[layer]
        mod = mods[layer]
        rows1, datt, dx1, dmod_a, total_mlp = ring_call(
            functools.partial(mlp_back_kernel, layer, square),
            4 + layer,
            52,
            [
                sds((seq, width), BF),
                sds((seq, packed), BF),
                sds((rows, width), F32),
                sds((8, 8, half), F32),
                sds((dp, part // 2, 3 * hidden_here), BF),
            ],
            [pltpu.VMEM((dp, part // 2, 3 * hidden_here), BF)] * 3
            + [
                pltpu.VMEM((rows, width), BF),
                pltpu.VMEM((rows, width), BF),
                pltpu.VMEM((seq, width), BF),
                pltpu.VMEM((seq, hidden_here), BF),
                pltpu.VMEM((seq, hidden_here), BF),
                pltpu.VMEM((seq, hidden_here), F32),
                pltpu.VMEM((seq, hidden_here), F32),
                pltpu.VMEM((seq, hidden_here), BF),
                pltpu.VMEM((seq, width), BF),
                pltpu.VMEM((width, seq), BF),
                pltpu.VMEM((packed, width), BF),
                pltpu.VMEM((2, width, hidden_here), BF),
                pltpu.VMEM((hidden_here, width), BF),
            ]
            + scatter_scratch(rows, width)
            + dma_sems(21)
            + [pltpu.SemaphoreType.DMA((7,))],
            (dy, br2, br1, x1, sel, mod, gate, up, hidden, whole2, own[1], other[1], own[2],
             other[2], own[3], other[3]),
            (1,) * 6 + (0,) * 10,
        )
        pack_mlp = reduced(total_mlp)
        dproj, dgain = local_call(
            attention_back_kernel,
            28,
            [
                sds((3, seq, packed), BF),
                sds((2, 1, packed), F32),
            ],
            [pltpu.VMEM((seq, heads * PAD), BF)] + [pltpu.VMEM((seq, heads * PAD), F32)] * 3,
            spans,
            (q, k, v, datt, proj, gains[layer]) + tables,
        )
        du, du_b, d_mod, total_att = ring_call(
            functools.partial(qkv_back_kernel, layer, square),
            6 + layer,
            22,
            [
                sds((rows, width), F32),
                sds((rows, width), BF),
                sds((2, 12, 8, half), F32),
                sds((dp, part // 2, 4 * packed), BF),
            ],
            [
                pltpu.VMEM((3, packed, width), BF),
                pltpu.VMEM((seq, width), BF),
                pltpu.VMEM((seq, packed), BF),
                pltpu.VMEM((seq, width), BF),
                pltpu.VMEM((width, seq), BF),
            ]
            + [pltpu.VMEM((dp, part // 2, 4 * packed), BF)] * 3
            + scatter_scratch(rows, width)
            + dma_sems(7)
            + [pltpu.SemaphoreType.DMA((4,))],
            (dproj, x, dx1, sel, mod, dmod_a, prev, own[0], other[0], whole1, att, rows1),
            (1,) * 7 + (0,) * 5,
        )
        prev = d_mod[1]
        pack_att = reduced(total_att)
        packs[layer] = (pack_mlp, pack_att)
        d_gains[layer] = dgain
        d_inputs[layer] = du_b if layer else du
        dy = du_b

    gain_parts = jnp.pad(jnp.stack(d_gains).reshape(2, 2, packed), ((0, 0), (0, 6), (0, 0)))
    g_ada_w, bias_grad, dl_sum, gain_sum = ring_call(
        functools.partial(tail_kernel, dp),
        9,
        15,
        [
            sds((part, 3 * half), F32),
            sds((3, 1, half), F32),
            sds((2, 8, width), F32),
            sds((8, packed), F32),
        ],
        [
            pltpu.VMEM((3 * half, width), BF),
            pltpu.VMEM((8, 3, 8, half), F32),
            pltpu.VMEM((8, 8, packed), F32),
            pltpu.VMEM((2, 3, 8, half), F32),
            pltpu.VMEM((8, packed), F32),
            pltpu.VMEM((dp, 2, 3, 8, half), F32),
            pltpu.VMEM((dp, 8, packed), F32),
            pltpu.VMEM((8, 2, 8, width), F32),
        ]
        + dma_sems(13 + 2 * (dp - 1) + 8)
        + [pltpu.SemaphoreType.DMA],
        (d_mod, gain_parts, lifted_part, ada),
        (1, 1, 1, 0),
    )
    bias_part = ada_bias.shape[1] // dp
    g_ada_b = lax.dynamic_slice_in_dim(bias_grad.reshape(-1), shard * bias_part, bias_part)
    cond_grad = dl_sum[:, :per_micro].reshape(items, width) * cond_sigmoid
    cond_grad = cond_grad * (1.0 + cond_wide * (1.0 - cond_sigmoid))
    gain_total = gain_sum[:2].reshape(1, 2, heads, head).sum(axis=2)

    mlp = own_layer(section, (packs[0][0], packs[1][0]))
    attn = own_layer(section, (packs[0][1], packs[1][1]))
    f = hidden_here
    g_gate_up = jnp.stack([mlp[:, :f], mlp[:, f : 2 * f]])[None]
    g_down = mlp[:, 2 * f :].T[None]
    g_qkv = jnp.stack([attn[:, k * packed : (k + 1) * packed] for k in range(3)])[None]
    g_out = attn[:, 3 * packed :].T[None]

    outs = jnp.where(first, kept[0][-1], kept[1][-1])
    outs_got = swap(jnp.where(first, kept[1][-1], kept[0][-1]))
    layer_out = jnp.where(first, jnp.stack([outs, outs_got]), jnp.stack([outs_got, outs]))
    wide_mid = d_inputs[1].astype(F32)
    back_keep = jnp.where(first, d_inputs[0], wide_mid)
    back_got = swap(jnp.where(first, wide_mid, d_inputs[0]))
    in_grads = jnp.where(first, jnp.stack([back_keep, back_got]), jnp.stack([back_got, back_keep]))
    return (
        layer_out[None],
        in_grads[None],
        cond_grad,
        g_qkv,
        g_out,
        g_gate_up,
        g_down,
        gain_total,
        g_ada_w[None],
        g_ada_b[None],
    )


def solution(mesh):
    both = (DP, T)
    in_specs = (
        P(None, both, None),
        P(None, both, None),
        P(DP, None),
        P(None, DP),
        P(None, None, DP),
        P(S, None, None, T),
        P(S, T, None),
        P(S, None, None, T),
        P(S, T, None),
        P(S, None, None),
        P(S, None, T),
        P(S, T),
    )
    out_specs = (
        P(S, None, both, None),
        P(S, None, both, None),
        P(DP, None),
        P(S, None, DP, T),
        P(S, T, DP),
        P(S, None, DP, T),
        P(S, T, DP),
        P(S, None, None),
        P(S, DP, T),
        P(S, (T, DP)),
    )
    dp = mesh.shape[DP]

    def program(*args):
        return per_device(dp <= 4, dp, *args)

    return jax.shard_map(
        program, mesh=mesh, in_specs=in_specs, out_specs=out_specs, check_vma=False
    )
```

```python
import functools

import jax
import jax.numpy as jnp
import numpy as np
from jax import lax
from jax.experimental import pallas as pl
from jax.experimental.pallas import tpu as pltpu
from jax.sharding import PartitionSpec as P


EPS = 1e-06
F32 = jnp.float32
BF = jnp.bfloat16
S, DP, T = "section", "dp", "tensor"
PAD = 128
TILE = 256


def nn(a, b):
    return jnp.dot(a, b, preferred_element_type=F32)


def nt(a, b):
    return lax.dot_general(a, b, (((1,), (1,)), ((), ())), preferred_element_type=F32)


def tn(a, b):
    return lax.dot_general(a, b, (((0,), (0,)), ((), ())), preferred_element_type=F32)


def two(dot, a, b):
    high = a.astype(BF)
    low = (a - high.astype(F32)).astype(BF)
    return dot(high, b) + dot(low, b)


def sds(shape, dtype):
    return jax.ShapeDtypeStruct(shape, dtype)


def vmem():
    return pl.BlockSpec(memory_space=pltpu.VMEM)


def anywhere():
    return pl.BlockSpec(memory_space=pl.ANY)


def ring(square):
    me = lax.axis_index(T)
    near = me + 1 - 2 * (me % 2)
    if square:
        return me, near, me + 2 - 4 * (me // 2), 3 - me
    return me, near, 3 - me, (me + 2) % 4


def greet(place, partner=False):
    sem = pltpu.get_barrier_semaphore()
    for peer in (place[1], place[2]):
        pl.semaphore_signal(
            sem, inc=1, device_id={T: peer}, device_id_type=pl.DeviceIdType.MESH
        )
    if partner:
        pl.semaphore_signal(
            sem, inc=1, device_id={S: 1 - lax.axis_index(S)}, device_id_type=pl.DeviceIdType.MESH
        )
    pl.semaphore_wait(sem, 3 if partner else 2)


def remote(src, dst, sems, index, peer):
    return pltpu.make_async_remote_copy(
        src_ref=src,
        dst_ref=dst,
        send_sem=sems[0].at[index],
        recv_sem=sems[1].at[index],
        device_id={T: peer},
        device_id_type=pl.DeviceIdType.MESH,
    )


def chunk_rows(chunk, rows):
    return pl.ds(pl.multiple_of(chunk * rows, rows), rows)


def gather(place, mine, whole, sems, base, use, fill=()):
    me, a, b, d = place
    rows = mine.shape[0]
    half = rows // 2
    lo, hi = pl.ds(0, half), pl.ds(half, half)

    def part(chunk, upper):
        return pl.ds(pl.multiple_of(chunk * rows + upper * half, half), half)

    a0 = remote(mine.at[lo], whole.at[part(me, 0)], sems, base, a)
    b0 = remote(mine.at[hi], whole.at[part(me, 1)], sems, base + 1, b)
    a1 = remote(mine.at[hi], whole.at[part(me, 1)], sems, base + 2, a)
    b1 = remote(mine.at[lo], whole.at[part(me, 0)], sems, base + 3, b)
    for copy in (a0, b0, a1, b1):
        copy.start()
    whole[chunk_rows(me, rows), :] = mine[...]
    use(me)
    for work in fill[:1]:
        work()
    a0.wait_recv()
    b2 = remote(whole.at[part(a, 0)], whole.at[part(a, 0)], sems, base + 4, b)
    b2.start()
    b0.wait_recv()
    a2 = remote(whole.at[part(b, 1)], whole.at[part(b, 1)], sems, base + 5, a)
    a2.start()
    a1.wait_recv()
    use(a)
    b1.wait_recv()
    use(b)
    for work in fill[1:]:
        work()
    b2.wait_recv()
    a2.wait_recv()
    use(d)
    for copy in (a0, b0, a1, b1, a2, b2):
        copy.wait_send()


def scatter(place, term, bufs, sems, base, fill=()):
    me, a, b, d = place
    out, into, keep, own = bufs
    half = keep.shape[1]
    lo, hi = pl.ds(0, half), pl.ds(half, half)
    out[0] = term(d).astype(BF)
    d0 = remote(out.at[0, lo], into.at[0, lo], sems, base, a)
    d1 = remote(out.at[0, hi], into.at[0, hi], sems, base + 1, b)
    d0.start()
    d1.start()
    total = term(a)
    out[1, lo] = total[:half].astype(BF)
    a0 = remote(out.at[1, lo], into.at[1, lo], sems, base + 2, a)
    a0.start()
    keep[0] = total[half:]
    total = term(b)
    out[2, hi] = total[half:].astype(BF)
    b0 = remote(out.at[2, hi], into.at[2, hi], sems, base + 3, b)
    b0.start()
    keep[1] = total[:half]
    own[...] = term(me)
    for work in fill[:1]:
        work()
    d1.wait_recv()
    out[1, hi] = (keep[0] + into[0, hi].astype(F32)).astype(BF)
    a1 = remote(out.at[1, hi], into.at[1, hi], sems, base + 4, a)
    a1.start()
    d0.wait_recv()
    out[2, lo] = (keep[1] + into[0, lo].astype(F32)).astype(BF)
    b1 = remote(out.at[2, lo], into.at[2, lo], sems, base + 5, b)
    b1.start()
    for work in fill[1:]:
        work()
    for copy in (a0, b0, a1, b1):
        copy.wait_recv()
    for copy in (d0, d1, a0, b0, a1, b1):
        copy.wait_send()


def scattered(bufs, rows):
    return bufs[3][rows] + bufs[1][1, rows].astype(F32) + bufs[1][2, rows].astype(F32)


def scatter_scratch(rows, width):
    return [
        pltpu.VMEM((3, rows, width), BF),
        pltpu.VMEM((3, rows, width), BF),
        pltpu.VMEM((2, rows // 2, width), F32),
        pltpu.VMEM((rows, width), F32),
    ]


def dma_sems(count):
    return [pltpu.SemaphoreType.DMA((count,)), pltpu.SemaphoreType.DMA((count,))]


def layer_weights(own, other, layer, dst, sem):
    mine = lax.axis_index(S) == layer

    @pl.when(mine)
    def _():
        pltpu.make_async_copy(own, dst, sem).start()

    @pl.when(jnp.logical_not(mine))
    def _():
        pltpu.make_async_copy(other, dst, sem).start()

    return pltpu.make_async_copy(own, dst, sem)


def head_weights(own, other, layer, dst, sems, parts):
    mine = lax.axis_index(S) == layer
    spread = len(parts) > 1
    heads = dst.shape[-2] // PAD
    head = own.shape[-2] // heads
    clean = head // 16 * 16
    copies = ([], [])
    for n, part in enumerate(parts):
        for h in range(heads):
            to = dst.at[part] if spread else dst
            to[pl.ds(h * PAD + clean, PAD - clean)] = jnp.zeros((PAD - clean, dst.shape[-1]), BF)
            to = to.at[pl.ds(h * PAD, head)]
            for which, src in enumerate((own, other)):
                src = src.at[part] if spread else src
                copies[which].append(
                    pltpu.make_async_copy(
                        src.at[pl.ds(h * head, head)], to, sems.at[n * heads + h]
                    )
                )

    @pl.when(mine)
    def _():
        for copy in copies[0]:
            copy.start()

    @pl.when(jnp.logical_not(mine))
    def _():
        for copy in copies[1]:
            copy.start()

    return copies[0]


def arrive(copies):
    for copy in copies:
        copy.wait()


def twice(row):
    return jnp.concatenate([row, row], axis=-1)


def over_blocks(rows, fn):
    step = rows // 4

    def body(i, carry):
        fn(pl.ds(pl.multiple_of(i * step, step), step))
        return carry

    lax.fori_loop(0, 4, body, 0)


def mod_rows(sel, mod, which):
    total = sel[:, 0:1] * mod[which, 0:1]
    for item in (1, 2):
        total = total + sel[:, item : item + 1] * mod[which, item : item + 1]
    return total


def add_sums(dmod, block, sel, values):
    sums = item_sums(sel, values)
    half = dmod.shape[2]
    dmod[2 * block] += sums[:, :half]
    dmod[2 * block + 1] += sums[:, half:]


def weight_grad(x, y, flipped, col, packs, index):
    mine, theirs, _ = packs
    dp, part, _ = mine.shape
    first = lax.axis_index(S) == 0
    width = y.shape[1]
    block = 256 if width % 256 == 0 else width
    if x is not None:
        flipped[...] = x[...].T
    for i in range(width // block):
        to = pl.ds(col + i * block, block)
        grad = nn(flipped[...], y[:, pl.ds(i * block, block)]).astype(BF)
        grad = grad.reshape(dp, 2, part, block)

        @pl.when(first)
        def _():
            mine[:, :, to] = grad[:, 0]
            theirs[:, :, to] = grad[:, 1]

        @pl.when(jnp.logical_not(first))
        def _():
            mine[:, :, to] = grad[:, 1]
            theirs[:, :, to] = grad[:, 0]

    return index, col, width


def send_half(packs, sems, job):
    index, col, width = job
    at = pl.ds(col, width)
    return push(
        packs[1].at[:, :, at], packs[2].at[:, :, at], sems, index, {S: 1 - lax.axis_index(S)}
    )


def add_halves(packs, copies, total):
    for copy in copies:
        copy.wait_recv()
    for k in range(total.shape[0]):
        total[k] = (packs[0][k].astype(F32) + packs[2][k].astype(F32)).astype(BF)
    for copy in copies:
        copy.wait_send()


def item_sums(sel, values):
    high = values.astype(BF)
    low = (values - high.astype(F32)).astype(BF)
    sel_b = sel.astype(BF)
    return tn(sel_b, high) + tn(sel_b, low)


def normed(values):
    inverse = lax.rsqrt(jnp.mean(values * values, axis=-1, keepdims=True) + EPS)
    return values * inverse, inverse


def norm_back(incoming, normal, inverse):
    return inverse * (incoming - normal * jnp.mean(incoming * normal, axis=-1, keepdims=True))


def qkv_kernel(layer, square, x, sel, mod, gain, both, turn, ones, w_own, w_other, whole, proj, q,
               k, v, h, w, ssem, rsem, wsem):
    place = ring(square)
    head = w_own.shape[1] * PAD // w.shape[1]
    load = head_weights(w_own, w_other, layer, w, wsem, range(3))
    greet(place)

    def prepare(rows):
        normal, _ = normed(x[rows].astype(F32))
        shift = mod_rows(sel[rows], mod, 0)
        scale = mod_rows(sel[rows], mod, 1)
        h[rows] = (normal * (1.0 + scale) + shift).astype(BF)

    over_blocks(x.shape[0], prepare)
    waited = []

    def use(chunk):
        if not waited:
            arrive(load)
            waited.append(1)
        rows = chunk_rows(chunk, x.shape[0])
        cosine = twice(both[rows, 0:PAD])
        sine = twice(both[rows, PAD : 2 * PAD])
        for which, dst in ((0, q), (1, k)):
            full = nt(whole[rows], w[which])
            proj[which, rows] = full.astype(BF)
            for pair in range(full.shape[1] // (2 * PAD)):
                lanes = slice(pair * 2 * PAD, (pair + 1) * 2 * PAD)
                normal, _ = unit(full[:, lanes], ones[...], head)
                gained = normal * twice(gain[which : which + 1])
                dst[rows, lanes] = (gained * cosine + two(nn, gained, turn[...]) * sine).astype(BF)
        v[rows] = nt(whole[rows], w[2]).astype(BF)

    gather(place, h, whole, (ssem, rsem), 0, use)


def mlp_kernel(layer, square, att, x, sel, mod, wo0, wo1, wg0, wg1, wd0, wd1, br1, x1, whole,
               gate, up, hidden, br2, y, h, wo, wg, wd, o1, i1, k1, s1, o2, i2, k2, s2,
               ssem, rsem, wsem, osem):
    place = ring(square)
    rows_here, _ = x.shape
    load_o = head_weights(wo0, wo1, layer, wo, osem, range(1))
    load_g = layer_weights(wg0, wg1, layer, wg, wsem.at[1])
    load_d = layer_weights(wd0, wd1, layer, wd, wsem.at[2])
    greet(place)
    sems = (ssem, rsem)
    arrive(load_o)
    first = (o1, i1, k1, s1)
    scatter(place, lambda c: nn(att[chunk_rows(c, rows_here)], wo[...]), first, sems, 0)

    def between(rows):
        branch = scattered(first, rows)
        br1[rows] = branch
        mixed = x[rows].astype(F32) + mod_rows(sel[rows], mod, 2) * branch
        x1[rows] = mixed
        normal, _ = normed(mixed)
        shift = mod_rows(sel[rows], mod, 3)
        scale = mod_rows(sel[rows], mod, 4)
        h[rows] = (normal * (1.0 + scale) + shift).astype(BF)

    over_blocks(rows_here, between)
    load_g.wait()

    def use(chunk):
        rows = chunk_rows(chunk, rows_here)
        gate[rows] = nn(whole[rows], wg[0])
        up[rows] = nn(whole[rows], wg[1])
        g = gate[rows]
        hidden[rows] = (g * jax.nn.sigmoid(g) * up[rows]).astype(BF)

    gather(place, h, whole, sems, 6, use)
    load_d.wait()
    second = (o2, i2, k2, s2)
    scatter(place, lambda c: nn(hidden[chunk_rows(c, rows_here)], wd[...]), second, sems, 12)

    def finish(rows):
        branch = scattered(second, rows)
        br2[rows] = branch
        y[rows] = (x1[rows] + mod_rows(sel[rows], mod, 5) * branch).astype(BF)

    over_blocks(rows_here, finish)


def mlp_back_kernel(layer, square, dy, br2, br1, x1, sel, mod, gate_h, up_h, hidden_h, rows_h,
                    wo0, wo1, wg0, wg1, wd0, wd1, whole1, datt, dx1, dmod, total, mine, theirs,
                    got, h, h1, whole2, dgate, dup, gate, up, hidden, saved, flipped, wo, wg, wd, o1, i1, k1,
                    s1, ssem, rsem, wsem, osem):
    place = ring(square)
    rows_here, _ = dy.shape
    load_d = layer_weights(wd0, wd1, layer, wd, wsem.at[0])
    load_gate = pltpu.make_async_copy(gate_h, gate, wsem.at[1])
    load_gate.start()
    load_up = pltpu.make_async_copy(up_h, up, wsem.at[2])
    load_up.start()
    load_g = layer_weights(wg0, wg1, layer, wg, wsem.at[3])
    load_o = head_weights(wo0, wo1, layer, wo, osem, range(1))
    load_hidden = pltpu.make_async_copy(hidden_h, hidden, wsem.at[5])
    load_hidden.start()
    load_rows = pltpu.make_async_copy(rows_h, saved, wsem.at[6])
    load_rows.start()
    greet(place, True)
    sems = (ssem, rsem)
    dmod[...] = jnp.zeros_like(dmod)

    def prepare(rows):
        incoming = dy[rows].astype(F32)
        h[rows] = (incoming * mod_rows(sel[rows], mod, 5)).astype(BF)
        add_sums(dmod, 3, sel[rows], incoming * br2[rows])

    over_blocks(rows_here, prepare)
    waited = []

    def use(chunk):
        if not waited:
            load_d.wait()
            load_gate.wait()
            load_up.wait()
            waited.append(1)
        rows = chunk_rows(chunk, rows_here)
        d_hidden = nt(whole2[rows], wd[...])
        g = gate[rows]
        s = jax.nn.sigmoid(g)
        dgate[rows] = (d_hidden * up[rows] * s * (1.0 + g * (1.0 - s))).astype(BF)
        dup[rows] = (d_hidden * g * s).astype(BF)

    gather(place, h, whole2, sems, 0, use)
    load_g.wait()
    load_hidden.wait()
    bufs = (o1, i1, k1, s1)
    f = hidden.shape[1]

    def term(chunk):
        rows = chunk_rows(chunk, rows_here)
        return nt(dgate[rows], wg[0]) + nt(dup[rows], wg[1])

    packs = (mine, theirs, got)
    copies = []

    def grad(index, x, y, col):
        job = weight_grad(x, y, flipped, col, packs, index)
        copies.append(send_half(packs, sems, job))

    def grad_down():
        grad(18, whole2, hidden, 2 * f)

    scatter(place, term, bufs, sems, 6, (grad_down,))

    def between(rows):
        d_h = scattered(bufs, rows)
        normal, inverse = normed(x1[rows])
        scale = mod_rows(sel[rows], mod, 4)
        d_mixed = dy[rows].astype(F32) + norm_back(d_h * (1.0 + scale), normal, inverse)
        dx1[rows] = d_mixed
        h1[rows] = (d_mixed * mod_rows(sel[rows], mod, 2)).astype(BF)
        add_sums(dmod, 1, sel[rows], d_h)
        add_sums(dmod, 2, sel[rows], d_h * normal)
        add_sums(dmod, 0, sel[rows], d_mixed * br1[rows])

    over_blocks(rows_here, between)
    arrive(load_o)
    load_rows.wait()

    def use_out(chunk):
        rows = chunk_rows(chunk, rows_here)
        datt[rows] = nt(whole1[rows], wo[...]).astype(BF)

    def grad_gate():
        grad(19, saved, dgate, 0)

    def grad_up():
        grad(20, None, dup, f)

    gather(place, h1, whole1, sems, 12, use_out, (grad_gate, grad_up))
    add_halves(packs, copies, total)


def qkv_back_kernel(layer, square, dq, dk, dv, proj, gain, both, turn, ones, spread, x, dx1, sel,
                    mod, part, prev, w_own, w_other, whole_h, att_h, rows1_h, du, du_b, dmod, total,
                    dgain, w, whole, att, rows1, flipped, dproj, flat, mine, theirs, got, o1, i1,
                    k1, s1, ssem, rsem, wsem, hsem):
    place = ring(square)
    rows_here, _ = x.shape
    packed = spread.shape[0]
    head = packed * PAD // spread.shape[1]
    load = head_weights(w_own, w_other, layer, w, hsem, range(3))
    loads = []
    for n, (src, dst) in enumerate(((whole_h, whole), (att_h, att), (rows1_h, rows1))):
        loads.append(pltpu.make_async_copy(src, dst, wsem.at[n]))
        loads[n].start()
    greet(place, True)
    here = dmod.at[layer]
    dmod[1 - layer] = prev[...]
    here[pl.ds(0, 4)] = jnp.zeros_like(prev[pl.ds(0, 4)])
    here[pl.ds(4, 8)] = part[...]
    dgain[...] = jnp.zeros_like(dgain)
    arrive(load)
    bufs = (o1, i1, k1, s1)
    sems = (ssem, rsem)
    packs = (mine, theirs, got)
    copies = []

    def term(chunk):
        rows = chunk_rows(chunk, rows_here)
        cosine = twice(both[rows, 0:PAD])
        sine = twice(both[rows, PAD : 2 * PAD])
        for which, src in ((0, dq), (1, dk)):
            for pair in range(src.shape[1] // (2 * PAD)):
                lanes = slice(pair * 2 * PAD, (pair + 1) * 2 * PAD)
                turned = src[rows, lanes]
                back = turned.astype(F32) * cosine - nn(turned, turn[...]) * sine
                normal, inverse = unit(proj[which, rows, lanes].astype(F32), ones[...], head)
                dgain[which, :, lanes] += jnp.sum(back * normal, axis=0, keepdims=True)
                gained = back * twice(gain[which : which + 1])
                mean = two(nn, gained * normal, ones[...]) * (1.0 / head)
                dproj[which, rows, lanes] = (inverse * (gained - normal * mean)).astype(BF)
        return nn(dproj[0, rows], w[0]) + nn(dproj[1, rows], w[1]) + nn(dv[rows], w[2])

    def grad_in():
        loads[0].wait()
        for k in range(3):
            flat[...] = nt(dproj[k] if k < 2 else dv[...], spread[...]).astype(BF)
            weight_grad(None if k else whole, flat, flipped, k * packed, packs, 6)

    def grad_out():
        loads[1].wait()
        loads[2].wait()
        flat[...] = nt(att[...], spread[...]).astype(BF)
        weight_grad(rows1, flat, flipped, 3 * packed, packs, 6)
        copies.append(send_half(packs, sems, (6, 0, 4 * packed)))

    scatter(place, term, bufs, sems, 0, (grad_in, grad_out))

    def finish(rows):
        d_h = scattered(bufs, rows)
        normal, inverse = normed(x[rows].astype(F32))
        scale = mod_rows(sel[rows], mod, 1)
        total_rows = dx1[rows] + norm_back(d_h * (1.0 + scale), normal, inverse)
        du[rows] = total_rows
        du_b[rows] = total_rows.astype(BF)
        add_sums(here, 0, sel[rows], d_h)
        add_sums(here, 1, sel[rows], d_h * normal)

    over_blocks(rows_here, finish)
    add_halves(packs, copies, total)


def cell():
    return 4 * lax.axis_index(S) + lax.axis_index(T)


def cell_id(index):
    return {S: index // 4, T: index % 4}


def greet_all(dp):
    sem = pltpu.get_barrier_semaphore()
    here, shard = cell(), lax.axis_index(DP)
    for k in range(1, 8):
        pl.semaphore_signal(
            sem, inc=1, device_id=cell_id((here + k) % 8), device_id_type=pl.DeviceIdType.MESH
        )
    for k in range(1, dp):
        pl.semaphore_signal(
            sem, inc=1, device_id={DP: (shard + k) % dp}, device_id_type=pl.DeviceIdType.MESH
        )
    pl.semaphore_wait(sem, 7 + dp - 1)


def push(src, dst, sems, index, device):
    copy = pltpu.make_async_remote_copy(
        src_ref=src,
        dst_ref=dst,
        send_sem=sems[0].at[index],
        recv_sem=sems[1].at[index],
        device_id=device,
        device_id_type=pl.DeviceIdType.MESH,
    )
    copy.start()
    return copy


def head_kernel(dp, lifted, ada_h, bias, gain, items, pos, tables, mod, lifted_all, gains, sel,
                both, spans, ada, parts, got, wide, tall, ssem, rsem, wsem):
    load = pltpu.make_async_copy(ada_h, ada, wsem)
    load.start()
    greet_all(dp)
    sems = (ssem, rsem)
    here, shard, section = cell(), lax.axis_index(DP), lax.axis_index(S)
    copies = [push(gain, gains.at[section], sems, 6 + dp, {S: 1 - section})]
    gains[section] = gain[...]
    lifted_all[shard] = lifted[...]
    for k in range(1, dp):
        copies.append(
            push(lifted, lifted_all.at[shard], sems, 6 + k, {DP: (shard + k) % dp})
        )
    load.wait()
    half = parts.shape[3]
    for micro in range(2):
        for j in range(3):
            rows = lifted[pl.ds(micro * 8, 8)].astype(BF)
            parts[micro, j] = nt(rows, ada[pl.ds(j * half, half)]) + bias[j]
    for k in range(1, 8):
        peer = (here + k) % 8
        copies.append(push(parts.at[peer // 4], got.at[here], sems, k - 1, cell_id(peer)))
    got[here] = parts[section]
    rows_here = sel.shape[0]
    base = shard * 6 + section * 3
    seq = items.shape[1]
    line = items[pl.ds(section, 1), :]
    wide[...] = jnp.zeros_like(wide)
    wide[0:1] = (line - base).astype(F32)
    wide[1:2] = pos[0, pl.ds(section, 1), :].astype(F32)
    wide[2:3] = pos[1, pl.ds(section, 1), :].astype(F32)
    start = 0
    spans[0] = 0
    for j in range(3):
        count = jnp.sum((wide[0:1] == j).astype(F32)).astype(jnp.int32)
        spans[4 + j] = count
        start = start + count
        spans[1 + j] = start
    spans[7] = 0
    tall[...] = wide[...].T
    own = tall[pl.ds(pl.multiple_of(lax.axis_index(T) * rows_here, rows_here), rows_here), :]
    lane = lax.broadcasted_iota(jnp.int32, (rows_here, 8), 1).astype(F32)
    sel[...] = ((own[:, 0:1] == lane) & (lane < 3.0)).astype(F32)
    lane = lax.broadcasted_iota(jnp.int32, (seq, 64), 1).astype(F32)
    hot = jnp.where(lane < 32.0, tall[:, 1:2], tall[:, 2:3] + 32.0) == lane
    hot = hot.astype(F32).astype(BF)
    both[...] = (nn(hot, tables[0]) + nn(hot, tables[1])) + nn(hot, tables[2])
    for copy in copies:
        copy.wait_recv()
    for layer in range(2):
        for block in range(6):
            for side in range(2):
                n = 2 * block + side
                mod[layer, block, :, pl.ds(side * half, half)] = got[4 * layer + n // 3, n % 3]
    for copy in copies:
        copy.wait_send()


def tail_kernel(dp, dmod, dgain, lifted_part, ada_h, ada_grad, bias_grad, dl_sum, gain_sum, ada,
                got, got_gain, total, total_gain, every, every_gain, lifts, ssem, rsem, wsem):
    load = pltpu.make_async_copy(ada_h, ada, wsem)
    load.start()
    greet_all(dp)
    sems = (ssem, rsem)
    here, shard = cell(), lax.axis_index(DP)
    section, place = lax.axis_index(S), lax.axis_index(T)
    sends, arrivals = [], []
    for k in range(1, 8):
        peer = (here + k) % 8
        to = cell_id(peer)
        arrivals.append(
            push(dmod.at[peer // 4, pl.ds(3 * (peer % 4), 3)], got.at[here], sems, k - 1, to)
        )
        arrivals.append(push(dgain.at[peer // 4], got_gain.at[here], sems, 6 + k, to))
    got[here] = dmod[section, pl.ds(3 * place, 3)]
    got_gain[here] = dgain[section]
    for copy in arrivals:
        copy.wait_recv()
    sends += arrivals
    for micro in range(2):
        total[micro] = (got[4 * micro] + got[4 * micro + 1]) + (got[4 * micro + 2] + got[4 * micro + 3])
    gain = got_gain[0]
    for k in range(1, 8):
        gain = gain + got_gain[k]
    total_gain[...] = gain
    arrivals = []
    for k in range(1, dp):
        to = {DP: (shard + k) % dp}
        arrivals.append(push(total, every.at[shard], sems, 13 + k, to))
        arrivals.append(push(total_gain, every_gain.at[shard], sems, 12 + dp + k, to))
    every[shard] = total[...]
    every_gain[shard] = total_gain[...]
    load.wait()
    half = total.shape[3]
    for micro in range(2):
        lift = two(nn, total[micro, 0], ada[pl.ds(0, half)])
        for j in range(1, 3):
            lift = lift + two(nn, total[micro, j], ada[pl.ds(j * half, half)])
        lifts[here, micro] = lift
    base = 13 + 2 * (dp - 1)
    lift_copies = []
    for k in range(1, 8):
        lift_copies.append(
            push(lifts.at[here], lifts.at[here], sems, base + k, cell_id((here + k) % 8))
        )
    for copy in arrivals:
        copy.wait_recv()
    sends += arrivals
    gain = every_gain[0]
    for k in range(1, dp):
        gain = gain + every_gain[k]
    gain_sum[...] = gain
    for j in range(3):
        bias = jnp.zeros((1, half), F32)
        grad = jnp.zeros((lifted_part.shape[2], half), F32)
        for k in range(dp):
            for micro in range(2):
                block = every[k, micro, j]
                bias = bias + jnp.sum(block, axis=0, keepdims=True)
                high = block.astype(BF)
                low = (block - high.astype(F32)).astype(BF)
                rows = lifted_part[2 * k + micro].astype(BF)
                grad = grad + tn(rows, high) + tn(rows, low)
        bias_grad[j] = bias
        ada_grad[:, pl.ds(j * half, half)] = grad
    for copy in lift_copies:
        copy.wait_recv()
    sends += lift_copies
    lift = lifts[0]
    for k in range(1, 8):
        lift = lift + lifts[k]
    dl_sum[...] = lift
    for copy in sends:
        copy.wait_send()


def price(micros):
    return pl.CostEstimate(flops=0, bytes_accessed=int(micros * 3.5e6), transcendentals=0)


def ring_call(kernel, ident, micros, outs, scratch, args, spaces, scalar=-1):
    return pl.pallas_call(
        kernel,
        out_shape=outs,
        in_specs=[vmem() if s else anywhere() for s in spaces],
        out_specs=[
            pl.BlockSpec(memory_space=pltpu.SMEM) if n == scalar else vmem()
            for n in range(len(outs))
        ],
        scratch_shapes=scratch,
        compiler_params=pltpu.CompilerParams(
            collective_id=ident, has_side_effects=True, vmem_limit_bytes=60 * 2**20
        ),
        cost_estimate=price(micros),
    )(*args)


def attention_kernel(head, spans, q, k, v, att):
    rows, wide = q.shape
    scale = head ** (-0.5)

    def each_head(fn):
        for n in range(wide // PAD):
            fn(slice(n * PAD, (n + 1) * PAD))

    for item in range(3):
        at = pl.ds(pl.multiple_of(spans[item], 16), TILE)
        valid = lax.broadcasted_iota(jnp.int32, (TILE, TILE), 1) < spans[4 + item]

        def tile(lanes, at=at, valid=valid):
            att[at, lanes] = softmax_rows(q[at, lanes], k[at, lanes], v[at, lanes], valid, scale)

        each_head(tile)
    first = rows - 48
    start = spans[3]
    at = pl.ds(first, 48)
    valid = first + lax.broadcasted_iota(jnp.int32, (48, 48), 1) >= start
    live = first + lax.broadcasted_iota(jnp.int32, (48, PAD), 0) >= start

    def rest(lanes):
        new = softmax_rows(q[at, lanes], k[at, lanes], v[at, lanes], valid, scale)
        att[at, lanes] = jnp.where(live, new, att[at, lanes])

    each_head(rest)


def unit(proj, ones, head):
    inverse = lax.rsqrt(two(nn, proj * proj, ones) * (1.0 / head) + EPS)
    return proj * inverse, inverse


def softmax_rows(query, key, value, valid, scale):
    scores = jnp.where(valid, nt(query, key) * scale, -1e30)
    raised = jnp.exp(scores - jnp.max(scores, axis=1, keepdims=True))
    probs = raised / jnp.sum(raised, axis=1, keepdims=True)
    return nn(probs.astype(BF), value).astype(BF)


def back_tile(query, key, value, grad, keys, queries, scale):
    scores = jnp.where(keys, nt(key, query) * scale, -1e30)
    raised = jnp.exp(scores - jnp.max(scores, axis=0, keepdims=True))
    probs = jnp.where(queries, raised / jnp.sum(raised, axis=0, keepdims=True), 0.0)
    d_value = nn(probs.astype(BF), grad)
    d_probs = nt(value, grad)
    inner = jnp.sum(probs * d_probs, axis=0, keepdims=True)
    d_scores = (probs * (d_probs - inner)).astype(BF)
    return tn(d_scores, key) * scale, nn(d_scores, query) * scale, d_value


def attention_back_kernel(head, spans, q, k, v, grad, dq, dk, dv):
    rows, wide = q.shape
    scale = head ** (-0.5)

    def each_head(fn):
        for n in range(wide // PAD):
            fn(slice(n * PAD, (n + 1) * PAD))

    for item in range(3):
        at = pl.ds(pl.multiple_of(spans[item], 16), TILE)
        keys = lax.broadcasted_iota(jnp.int32, (TILE, TILE), 0) < spans[4 + item]
        queries = lax.broadcasted_iota(jnp.int32, (TILE, TILE), 1) < spans[4 + item]

        def tile(lanes, at=at, keys=keys, queries=queries):
            parts = back_tile(
                q[at, lanes], k[at, lanes], v[at, lanes], grad[at, lanes], keys, queries, scale
            )
            for new, dst in zip(parts, (dq, dk, dv)):
                dst[at, lanes] = new.astype(BF)

        each_head(tile)
    first = rows - 48
    start = spans[3]
    at = pl.ds(first, 48)
    keys = first + lax.broadcasted_iota(jnp.int32, (48, 48), 0) >= start
    queries = first + lax.broadcasted_iota(jnp.int32, (48, 48), 1) >= start
    live = first + lax.broadcasted_iota(jnp.int32, (48, PAD), 0) >= start

    def rest(lanes):
        parts = back_tile(
            q[at, lanes], k[at, lanes], v[at, lanes], grad[at, lanes], keys, queries, scale
        )
        for new, dst in zip(parts, (dq, dk, dv)):
            dst[at, lanes] = jnp.where(live, new.astype(BF), dst[at, lanes])

    each_head(rest)


def local_call(kernel, micros, outs, scratch, spans, args):
    return pl.pallas_call(
        kernel,
        out_shape=outs,
        in_specs=[pl.BlockSpec(memory_space=pltpu.SMEM)] + [vmem()] * len(args),
        out_specs=[vmem()] * len(outs),
        scratch_shapes=scratch,
        compiler_params=pltpu.CompilerParams(vmem_limit_bytes=60 * 2**20),
        cost_estimate=price(micros),
    )(spans, *args)


def swap(array):
    return lax.ppermute(array, S, [(0, 1), (1, 0)])


def head_tables(packed, head):
    quarter = head // 4
    frequency = np.float32(10000.0) ** (-np.arange(quarter, dtype=np.float32) / quarter)
    lane = np.arange(head)
    angle = np.arange(32, dtype=np.float32)[:, None] * frequency[lane % quarter][None, :]
    by_row = (lane // (2 * quarter) == 0)[None, :]
    table = np.zeros((64, 2 * PAD), np.float32)
    for n, values in enumerate((np.cos(angle), np.sin(angle))):
        at = slice(n * PAD, n * PAD + head)
        table[:32, at] = np.where(by_row, values, 0.0)
        table[32:, at] = np.where(by_row, 0.0, values)
    table = jnp.asarray(table)
    parts = []
    for _ in range(3):
        parts.append(lax.reduce_precision(table, 8, 7).astype(BF))
        table = table - parts[-1].astype(F32)
    rows = np.arange(2 * PAD)[:, None]
    cols = np.arange(2 * PAD)[None, :]
    inside = (rows // PAD == cols // PAD) & (rows % PAD < head) & (cols % PAD < head)
    row, col = rows % PAD, cols % PAD
    early = (col % (2 * quarter)) < quarter
    turn = np.where(inside & early & (row == col + quarter), -1.0, 0.0)
    turn = turn + np.where(inside & ~early & (row == col - quarter), 1.0, 0.0)
    heads = packed // head
    rows = np.arange(packed)[:, None]
    wide = np.arange(heads * PAD)[None, :]
    spread = (rows // head == wide // PAD) & (rows % head == wide % PAD)
    lanes = tuple(jnp.asarray(m.astype(np.float32)).astype(BF) for m in (turn, inside, spread))
    return jnp.stack(parts), lanes


def reduced(total):
    return lax.psum_scatter(total, DP, scatter_dimension=0, tiled=True)[0]


def own_layer(section, pair):
    first = section == 0
    keep = jnp.where(first, pair[0], pair[1])
    got = swap(jnp.where(first, pair[1], pair[0]))
    return jnp.where(first, jnp.concatenate([keep, got]), jnp.concatenate([got, keep])).astype(F32)


def per_device(square, dp, tokens, cotangent, cond, patch_item, patch_pos, w_qkv, w_out, w_gate_up,
               w_down, qk_gain, ada_weight, ada_bias):
    section = lax.axis_index(S)
    first = section == 0
    rows, width = tokens.shape[1:]
    seq = patch_item.shape[1]
    items = cond.shape[0]
    per_micro = items // 2
    head = qk_gain.shape[-1]
    packed = w_qkv.shape[-1]
    heads = packed // head
    hidden_here = w_down.shape[1]
    own = (jnp.swapaxes(w_qkv[0], 1, 2), w_out[0], w_gate_up[0], w_down[0])
    other = tuple(swap(w) for w in own)

    cond_wide = cond.astype(F32)
    cond_sigmoid = jax.nn.sigmoid(cond_wide)
    lifted = (cond_wide * cond_sigmoid).astype(BF).astype(F32).reshape(2, per_micro, width)
    lifted = jnp.pad(lifted, ((0, 0), (0, 8 - per_micro), (0, 0))).reshape(16, width)
    ada = ada_weight[0].T
    half = width // 2
    bias = ada_bias.astype(F32).reshape(3, 1, half)
    gain = jnp.pad(qk_gain[0].astype(F32), ((0, 6), (0, PAD - head)))
    trig, (turn, ones, spread) = head_tables(packed, head)
    wide = heads * PAD
    mods, lifted_all, gains, sel, both, spans = ring_call(
        functools.partial(head_kernel, dp),
        8,
        12,
        [
            sds((2, 6, 8, width), F32),
            sds((dp, 16, width), F32),
            sds((2, 8, PAD), F32),
            sds((rows, 8), F32),
            sds((seq, 2 * PAD), F32),
            sds((8,), jnp.int32),
        ],
        [
            pltpu.VMEM((3 * half, width), BF),
            pltpu.VMEM((2, 3, 8, half), F32),
            pltpu.VMEM((8, 3, 8, half), F32),
            pltpu.VMEM((8, seq), F32),
            pltpu.VMEM((seq, 8), F32),
        ]
        + dma_sems(7 + dp)
        + [pltpu.SemaphoreType.DMA],
        (lifted, ada, bias, gain, patch_item, patch_pos, trig),
        (1, 0, 1, 1, 1, 1, 1),
        scalar=5,
    )
    part = width // dp
    shard = lax.axis_index(DP)
    lifted_part = lax.dynamic_slice_in_dim(lifted_all, shard * part, part, 2)
    lifted_part = lifted_part.reshape(2 * dp, 8, part)

    x = lax.dynamic_index_in_dim(tokens, section, 0, keepdims=False)
    kept = []
    for layer in range(2):
        mod = mods[layer]
        whole1, proj, q, k, v = ring_call(
            functools.partial(qkv_kernel, layer, square),
            layer,
            20,
            [sds((seq, width), BF), sds((2, seq, wide), BF)] + [sds((seq, wide), BF)] * 3,
            [pltpu.VMEM((rows, width), BF), pltpu.VMEM((3, wide, width), BF)]
            + dma_sems(6)
            + [pltpu.SemaphoreType.DMA((3 * heads,))],
            (x, sel, mod, gains[layer], both, turn, ones, own[0], other[0]),
            (1,) * 7 + (0, 0),
        )
        (att,) = local_call(
            functools.partial(attention_kernel, head),
            6,
            [sds((seq, wide), BF)],
            [],
            spans,
            (q, k, v),
        )
        br1, x1, whole2, gate, up, hidden, br2, y = ring_call(
            functools.partial(mlp_kernel, layer, square),
            2 + layer,
            48,
            [
                sds((rows, width), F32),
                sds((rows, width), F32),
                sds((seq, width), BF),
                sds((seq, hidden_here), F32),
                sds((seq, hidden_here), F32),
                sds((seq, hidden_here), BF),
                sds((rows, width), F32),
                sds((rows, width), BF),
            ],
            [
                pltpu.VMEM((rows, width), BF),
                pltpu.VMEM((wide, width), BF),
                pltpu.VMEM((2, width, hidden_here), BF),
                pltpu.VMEM((hidden_here, width), BF),
            ]
            + scatter_scratch(rows, width)
            + scatter_scratch(rows, width)
            + dma_sems(18)
            + [pltpu.SemaphoreType.DMA((3,)), pltpu.SemaphoreType.DMA((heads,))],
            (att, x, sel, mod, own[1], other[1], own[2], other[2], own[3], other[3]),
            (1, 1, 1, 1) + (0,) * 6,
        )
        kept.append((x, whole1, proj, q, k, v, att, br1, x1, whole2, gate, up, hidden, br2, y))
        x = y

    dy = lax.dynamic_index_in_dim(cotangent, section, 0, keepdims=False)
    packs = [None, None]
    prev = jnp.zeros((12, 8, half), F32)
    d_gains = [None, None]
    d_inputs = [None, None]
    for layer in (1, 0):
        x, whole1, proj, q, k, v, att, br1, x1, whole2, gate, up, hidden, br2, y = kept[layer]
        mod = mods[layer]
        rows1, datt, dx1, dmod_a, total_mlp = ring_call(
            functools.partial(mlp_back_kernel, layer, square),
            4 + layer,
            52,
            [
                sds((seq, width), BF),
                sds((seq, wide), BF),
                sds((rows, width), F32),
                sds((8, 8, half), F32),
                sds((dp, part // 2, 3 * hidden_here), BF),
            ],
            [pltpu.VMEM((dp, part // 2, 3 * hidden_here), BF)] * 3
            + [
                pltpu.VMEM((rows, width), BF),
                pltpu.VMEM((rows, width), BF),
                pltpu.VMEM((seq, width), BF),
                pltpu.VMEM((seq, hidden_here), BF),
                pltpu.VMEM((seq, hidden_here), BF),
                pltpu.VMEM((seq, hidden_here), F32),
                pltpu.VMEM((seq, hidden_here), F32),
                pltpu.VMEM((seq, hidden_here), BF),
                pltpu.VMEM((seq, width), BF),
                pltpu.VMEM((width, seq), BF),
                pltpu.VMEM((wide, width), BF),
                pltpu.VMEM((2, width, hidden_here), BF),
                pltpu.VMEM((hidden_here, width), BF),
            ]
            + scatter_scratch(rows, width)
            + dma_sems(21)
            + [pltpu.SemaphoreType.DMA((7,)), pltpu.SemaphoreType.DMA((heads,))],
            (dy, br2, br1, x1, sel, mod, gate, up, hidden, whole2, own[1], other[1], own[2],
             other[2], own[3], other[3]),
            (1,) * 6 + (0,) * 10,
        )
        pack_mlp = reduced(total_mlp)
        dq, dk, dv = local_call(
            functools.partial(attention_back_kernel, head),
            10,
            [sds((seq, wide), BF)] * 3,
            [],
            spans,
            (q, k, v, datt),
        )
        du, du_b, d_mod, total_att, dgain = ring_call(
            functools.partial(qkv_back_kernel, layer, square),
            6 + layer,
            22,
            [
                sds((rows, width), F32),
                sds((rows, width), BF),
                sds((2, 12, 8, half), F32),
                sds((dp, part // 2, 4 * packed), BF),
                sds((2, 1, wide), F32),
            ],
            [
                pltpu.VMEM((3, wide, width), BF),
                pltpu.VMEM((seq, width), BF),
                pltpu.VMEM((seq, wide), BF),
                pltpu.VMEM((seq, width), BF),
                pltpu.VMEM((width, seq), BF),
                pltpu.VMEM((2, seq, wide), BF),
                pltpu.VMEM((seq, packed), BF),
            ]
            + [pltpu.VMEM((dp, part // 2, 4 * packed), BF)] * 3
            + scatter_scratch(rows, width)
            + dma_sems(7)
            + [pltpu.SemaphoreType.DMA((3,)), pltpu.SemaphoreType.DMA((3 * heads,))],
            (dq, dk, dv, proj, gains[layer], both, turn, ones, spread, x, dx1, sel, mod, dmod_a,
             prev, own[0], other[0], whole1, att, rows1),
            (1,) * 15 + (0,) * 5,
        )
        prev = d_mod[1]
        pack_att = reduced(total_att)
        packs[layer] = (pack_mlp, pack_att)
        d_gains[layer] = dgain
        d_inputs[layer] = du_b if layer else du
        dy = du_b

    gain_parts = jnp.pad(jnp.stack(d_gains).reshape(2, 2, wide), ((0, 0), (0, 6), (0, 0)))
    g_ada_w, bias_grad, dl_sum, gain_sum = ring_call(
        functools.partial(tail_kernel, dp),
        9,
        15,
        [
            sds((part, 3 * half), F32),
            sds((3, 1, half), F32),
            sds((2, 8, width), F32),
            sds((8, wide), F32),
        ],
        [
            pltpu.VMEM((3 * half, width), BF),
            pltpu.VMEM((8, 3, 8, half), F32),
            pltpu.VMEM((8, 8, wide), F32),
            pltpu.VMEM((2, 3, 8, half), F32),
            pltpu.VMEM((8, wide), F32),
            pltpu.VMEM((dp, 2, 3, 8, half), F32),
            pltpu.VMEM((dp, 8, wide), F32),
            pltpu.VMEM((8, 2, 8, width), F32),
        ]
        + dma_sems(13 + 2 * (dp - 1) + 8)
        + [pltpu.SemaphoreType.DMA],
        (d_mod, gain_parts, lifted_part, ada),
        (1, 1, 1, 0),
    )
    bias_part = ada_bias.shape[1] // dp
    g_ada_b = lax.dynamic_slice_in_dim(bias_grad.reshape(-1), shard * bias_part, bias_part)
    cond_grad = dl_sum[:, :per_micro].reshape(items, width) * cond_sigmoid
    cond_grad = cond_grad * (1.0 + cond_wide * (1.0 - cond_sigmoid))
    gain_total = gain_sum[:2].reshape(1, 2, heads, PAD)[..., :head].sum(axis=2)

    mlp = own_layer(section, (packs[0][0], packs[1][0]))
    attn = own_layer(section, (packs[0][1], packs[1][1]))
    f = hidden_here
    g_gate_up = jnp.stack([mlp[:, :f], mlp[:, f : 2 * f]])[None]
    g_down = mlp[:, 2 * f :].T[None]
    g_qkv = jnp.stack([attn[:, k * packed : (k + 1) * packed] for k in range(3)])[None]
    g_out = attn[:, 3 * packed :].T[None]

    outs = jnp.where(first, kept[0][-1], kept[1][-1])
    outs_got = swap(jnp.where(first, kept[1][-1], kept[0][-1]))
    layer_out = jnp.where(first, jnp.stack([outs, outs_got]), jnp.stack([outs_got, outs]))
    wide_mid = d_inputs[1].astype(F32)
    back_keep = jnp.where(first, d_inputs[0], wide_mid)
    back_got = swap(jnp.where(first, wide_mid, d_inputs[0]))
    in_grads = jnp.where(first, jnp.stack([back_keep, back_got]), jnp.stack([back_got, back_keep]))
    return (
        layer_out[None],
        in_grads[None],
        cond_grad,
        g_qkv,
        g_out,
        g_gate_up,
        g_down,
        gain_total,
        g_ada_w[None],
        g_ada_b[None],
    )


def solution(mesh):
    both = (DP, T)
    in_specs = (
        P(None, both, None),
        P(None, both, None),
        P(DP, None),
        P(None, DP),
        P(None, None, DP),
        P(S, None, None, T),
        P(S, T, None),
        P(S, None, None, T),
        P(S, T, None),
        P(S, None, None),
        P(S, None, T),
        P(S, T),
    )
    out_specs = (
        P(S, None, both, None),
        P(S, None, both, None),
        P(DP, None),
        P(S, None, DP, T),
        P(S, T, DP),
        P(S, None, DP, T),
        P(S, T, DP),
        P(S, None, None),
        P(S, DP, T),
        P(S, (T, DP)),
    )
    dp = mesh.shape[DP]

    def program(*args):
        return per_device(dp <= 4, dp, *args)

    return jax.shard_map(
        program, mesh=mesh, in_specs=in_specs, out_specs=out_specs, check_vma=False
    )
```

```python
import functools

import jax
import jax.numpy as jnp
import numpy as np
from jax import lax
from jax.experimental import pallas as pl
from jax.experimental.pallas import tpu as pltpu
from jax.sharding import PartitionSpec as P


EPS = 1e-06
F32 = jnp.float32
BF = jnp.bfloat16
S, DP, T = "section", "dp", "tensor"
PAD = 128
TILE = 256


def nn(a, b):
    return jnp.dot(a, b, preferred_element_type=F32)


def nt(a, b):
    return lax.dot_general(a, b, (((1,), (1,)), ((), ())), preferred_element_type=F32)


def tn(a, b):
    return lax.dot_general(a, b, (((0,), (0,)), ((), ())), preferred_element_type=F32)


def two(dot, a, b):
    high = a.astype(BF)
    low = (a - high.astype(F32)).astype(BF)
    return dot(high, b) + dot(low, b)


def sds(shape, dtype):
    return jax.ShapeDtypeStruct(shape, dtype)


def vmem():
    return pl.BlockSpec(memory_space=pltpu.VMEM)


def anywhere():
    return pl.BlockSpec(memory_space=pl.ANY)


def ring(square):
    me = lax.axis_index(T)
    near = me + 1 - 2 * (me % 2)
    if square:
        return me, near, me + 2 - 4 * (me // 2), 3 - me, True
    return me, near, 3 - me, (me + 2) % 4, False


def nearest_first(place, step):
    me, low = place[0], ((step + 1) // 2) % 2
    if place[4]:
        low = step % 2
    return (me % 2 + low) % 2 + 2 * ((me // 2 + step // 2) % 2)


def farthest_first(place, step):
    me, low = place[0], ((step + 1) // 2) % 2
    if place[4]:
        low = (3 - step) // 2
    return (me % 2 + low) % 2 + 2 * ((me // 2 + (step + 1) % 2) % 2)


def near_first(place, step):
    me, low = place[0], (3 - step) // 2
    if place[4]:
        low = (step + 1) % 2
    return (me % 2 + low) % 2 + 2 * ((me // 2 + ((step + 1) // 2) % 2) % 2)


def greet(place, partner=False):
    sem = pltpu.get_barrier_semaphore()
    peers = (place[1], place[2]) if place else ()
    for peer in peers:
        pl.semaphore_signal(
            sem, inc=1, device_id={T: peer}, device_id_type=pl.DeviceIdType.MESH
        )
    if partner:
        pl.semaphore_signal(
            sem, inc=1, device_id={S: 1 - lax.axis_index(S)}, device_id_type=pl.DeviceIdType.MESH
        )
    pl.semaphore_wait(sem, len(peers) + partner)


def remote(src, dst, sems, index, peer):
    return pltpu.make_async_remote_copy(
        src_ref=src,
        dst_ref=dst,
        send_sem=sems[0].at[index],
        recv_sem=sems[1].at[index],
        device_id={T: peer},
        device_id_type=pl.DeviceIdType.MESH,
    )


def chunk_rows(chunk, rows):
    return pl.ds(pl.multiple_of(chunk * rows, rows), rows)


def repeat(body, times):
    def one(step, carry):
        body(step)
        return carry

    lax.fori_loop(0, times, one, 0)


def gather(place, mine, whole, sems, base, use, ready=lambda: None, late=lambda: None, last=None):
    me, a, b, _, _ = place
    rows = mine.shape[0]
    half = rows // 2
    lo, hi = pl.ds(0, half), pl.ds(half, half)

    def part(chunk, upper):
        return whole.at[pl.ds(pl.multiple_of(chunk * rows + upper * half, half), half)]

    a0 = remote(mine.at[lo], part(me, 0), sems, base, a)
    b0 = remote(mine.at[hi], part(me, 1), sems, base + 1, b)
    a1 = remote(mine.at[hi], part(me, 1), sems, base + 2, a)
    b1 = remote(mine.at[lo], part(me, 0), sems, base + 3, b)
    b2 = remote(part(a, 0), part(a, 0), sems, base + 4, b)
    a2 = remote(part(b, 1), part(b, 1), sems, base + 5, a)
    for copy in (a0, b0, a1, b1):
        copy.start()
    whole[chunk_rows(me, rows), :] = mine[...]
    ready()

    def final():
        b2.wait_recv()
        a2.wait_recv()

    def body(step):
        @pl.when(step == 1)
        def _():
            a0.wait_recv()
            b2.start()
            b0.wait_recv()
            a2.start()
            a1.wait_recv()

        @pl.when(step == 2)
        def _():
            b1.wait_recv()

        if last is None:

            @pl.when(step == 3)
            def _():
                late()
                final()

        use(nearest_first(place, step))

    repeat(body, 4 if last is None else 3)
    if last is not None:
        last(final)
    for copy in (a0, b0, a1, b1, a2, b2):
        copy.wait_send()


def scatter(place, term, bufs, sems, base, fill=lambda: None, before=None):
    _, a, b, _, _ = place
    out, into, keep, own = bufs
    half = keep.shape[1]
    lo, hi = pl.ds(0, half), pl.ds(half, half)
    d0 = remote(out.at[0, lo], into.at[0, lo], sems, base, a)
    d1 = remote(out.at[0, hi], into.at[0, hi], sems, base + 1, b)
    a0 = remote(out.at[1, lo], into.at[1, lo], sems, base + 2, a)
    b0 = remote(out.at[2, hi], into.at[2, hi], sems, base + 3, b)
    a1 = remote(out.at[1, hi], into.at[1, hi], sems, base + 4, a)
    b1 = remote(out.at[2, lo], into.at[2, lo], sems, base + 5, b)
    at = (0, 1, 2) if before is None else (2, 0, 1)

    def body(step):
        if before is None:
            chunk = farthest_first(place, step)
        else:
            chunk = near_first(place, step)
            pl.when(step == 2)(before)
        own[...] = term(chunk)

        @pl.when(step == at[0])
        def _():
            out[0] = own[...].astype(BF)
            d0.start()
            d1.start()

        @pl.when(step == at[1])
        def _():
            out[1, lo] = own[lo].astype(BF)
            a0.start()
            keep[0] = own[hi]

        @pl.when(step == at[2])
        def _():
            out[2, hi] = own[hi].astype(BF)
            b0.start()
            keep[1] = own[lo]

    repeat(body, 4)
    d1.wait_recv()
    out[1, hi] = (keep[0] + into[0, hi].astype(F32)).astype(BF)
    a1.start()
    d0.wait_recv()
    out[2, lo] = (keep[1] + into[0, lo].astype(F32)).astype(BF)
    b1.start()
    fill()
    for copy in (a0, b0, a1, b1):
        copy.wait_recv()
    for copy in (d0, d1, a0, b0, a1, b1):
        copy.wait_send()


def gather_scatter(place, mine, whole, sems, base, use, term, bufs, ready, fill=lambda: None):
    def last(final):
        def before():
            final()
            use(place[3])

        scatter(place, term, bufs, sems, base + 6, fill, before)

    gather(place, mine, whole, sems, base, use, ready, last=last)


def scattered(bufs, rows):
    return bufs[3][rows] + bufs[1][1, rows].astype(F32) + bufs[1][2, rows].astype(F32)


def scatter_scratch(rows, width):
    return [
        pltpu.VMEM((3, rows, width), BF),
        pltpu.VMEM((3, rows, width), BF),
        pltpu.VMEM((2, rows // 2, width), F32),
        pltpu.VMEM((rows, width), F32),
    ]


def dma_sems(count):
    return [pltpu.SemaphoreType.DMA((count,)), pltpu.SemaphoreType.DMA((count,))]


def layer_weights(own, other, layer, dst, sem):
    mine = lax.axis_index(S) == layer

    @pl.when(mine)
    def _():
        pltpu.make_async_copy(own, dst, sem).start()

    @pl.when(jnp.logical_not(mine))
    def _():
        pltpu.make_async_copy(other, dst, sem).start()

    return pltpu.make_async_copy(own, dst, sem)


def head_weights(own, other, layer, dst, sems, parts):
    mine = lax.axis_index(S) == layer
    spread = len(parts) > 1
    heads = dst.shape[-2] // PAD
    head = own.shape[-2] // heads
    clean = head // 16 * 16
    copies = ([], [])
    for n, part in enumerate(parts):
        for h in range(heads):
            to = dst.at[part] if spread else dst
            to[pl.ds(h * PAD + clean, PAD - clean)] = jnp.zeros((PAD - clean, dst.shape[-1]), BF)
            to = to.at[pl.ds(h * PAD, head)]
            for which, src in enumerate((own, other)):
                src = src.at[part] if spread else src
                copies[which].append(
                    pltpu.make_async_copy(
                        src.at[pl.ds(h * head, head)], to, sems.at[n * heads + h]
                    )
                )

    @pl.when(mine)
    def _():
        for copy in copies[0]:
            copy.start()

    @pl.when(jnp.logical_not(mine))
    def _():
        for copy in copies[1]:
            copy.start()

    return copies[0]


def arrive(copies):
    for copy in copies:
        copy.wait()


def twice(row):
    return jnp.concatenate([row, row], axis=-1)


def over_blocks(rows, fn):
    step = rows // 4

    def body(i, carry):
        fn(pl.ds(pl.multiple_of(i * step, step), step))
        return carry

    lax.fori_loop(0, 4, body, 0)


def mod_rows(sel, mod, which):
    total = sel[:, 0:1] * mod[which, 0:1]
    for item in (1, 2):
        total = total + sel[:, item : item + 1] * mod[which, item : item + 1]
    return total


def add_sums(dmod, block, sel, values):
    sums = item_sums(sel, values)
    half = dmod.shape[2]
    dmod[2 * block] += sums[:, :half]
    dmod[2 * block + 1] += sums[:, half:]


def weight_grad(x, y, flipped, col, packs):
    mine, theirs, _ = packs
    dp, part, _ = mine.shape
    first = lax.axis_index(S) == 0
    width = y.shape[1]
    if x is not None:
        flipped[...] = x[...].T

    def one(to, columns):
        grad = nn(flipped[...], columns).astype(BF)
        grad = grad.reshape(dp, 2, part, columns.shape[1])

        @pl.when(first)
        def _():
            mine[:, :, to] = grad[:, 0]
            theirs[:, :, to] = grad[:, 1]

        @pl.when(jnp.logical_not(first))
        def _():
            mine[:, :, to] = grad[:, 1]
            theirs[:, :, to] = grad[:, 0]

    if width % 256:
        one(pl.ds(col, width), y[...])
        return

    def body(i, carry):
        at = pl.multiple_of(i * 256, 256)
        one(pl.ds(pl.multiple_of(col + at, 256), 256), y[:, pl.ds(at, 256)])
        return carry

    lax.fori_loop(0, width // 256, body, 0)


def send_half(packs, sems, index, col, width):
    at = pl.ds(col, width)
    return push(
        packs[1].at[:, :, at], packs[2].at[:, :, at], sems, index, {S: 1 - lax.axis_index(S)}
    )


def add_halves(packs, copies, total, col, width):
    at = pl.ds(col, width)
    for copy in copies:
        copy.wait_recv()

    def body(k):
        total[k, :, at] = (packs[0][k, :, at].astype(F32) + packs[2][k, :, at].astype(F32)).astype(BF)

    repeat(body, total.shape[0])
    for copy in copies:
        copy.wait_send()


def item_sums(sel, values):
    high = values.astype(BF)
    low = (values - high.astype(F32)).astype(BF)
    sel_b = sel.astype(BF)
    return tn(sel_b, high) + tn(sel_b, low)


def normed(values):
    inverse = lax.rsqrt(jnp.mean(values * values, axis=-1, keepdims=True) + EPS)
    return values * inverse, inverse


def norm_back(incoming, normal, inverse):
    return inverse * (incoming - normal * jnp.mean(incoming * normal, axis=-1, keepdims=True))


def qkv_kernel(layer, square, x, sel, mod, gain, both, turn, ones, w_own, w_other, whole, proj, q,
               k, v, h, w, ssem, rsem, wsem):
    place = ring(square)
    head = w_own.shape[1] * PAD // w.shape[1]
    load = head_weights(w_own, w_other, layer, w, wsem, range(3))
    greet(place)

    def prepare(rows):
        normal, _ = normed(x[rows].astype(F32))
        shift = mod_rows(sel[rows], mod, 0)
        scale = mod_rows(sel[rows], mod, 1)
        h[rows] = (normal * (1.0 + scale) + shift).astype(BF)

    over_blocks(x.shape[0], prepare)

    def use(chunk):
        rows = chunk_rows(chunk, x.shape[0])
        cosine = twice(both[rows, 0:PAD])
        sine = twice(both[rows, PAD : 2 * PAD])
        for which, dst in ((0, q), (1, k)):
            full = nt(whole[rows], w[which])
            proj[which, rows] = full.astype(BF)
            for pair in range(full.shape[1] // (2 * PAD)):
                lanes = slice(pair * 2 * PAD, (pair + 1) * 2 * PAD)
                normal, _ = unit(full[:, lanes], ones[...], head)
                gained = normal * twice(gain[which : which + 1])
                dst[rows, lanes] = (gained * cosine + two(nn, gained, turn[...]) * sine).astype(BF)
        v[rows] = nt(whole[rows], w[2]).astype(BF)

    gather(place, h, whole, (ssem, rsem), 0, use, lambda: arrive(load))


def mlp_kernel(layer, square, att, x, sel, mod, wo0, wo1, wg0, wg1, wd0, wd1, br1, x1, br2, y,
               whole_h, gate_h, up_h, hidden_h, whole, gate, up, hidden, h, wo, wg, wd, o1, i1, k1, s1, o2, i2, k2, s2,
               ssem, rsem, wsem, osem):
    place = ring(square)
    rows_here, _ = x.shape
    load_o = head_weights(wo0, wo1, layer, wo, osem, range(1))
    load_g = layer_weights(wg0, wg1, layer, wg, wsem.at[1])
    load_d = layer_weights(wd0, wd1, layer, wd, wsem.at[2])
    greet(place)
    sems = (ssem, rsem)
    arrive(load_o)
    first = (o1, i1, k1, s1)
    scatter(place, lambda c: nn(att[chunk_rows(c, rows_here)], wo[...]), first, sems, 0)

    def between(rows):
        branch = scattered(first, rows)
        br1[rows] = branch
        mixed = x[rows].astype(F32) + mod_rows(sel[rows], mod, 2) * branch
        x1[rows] = mixed
        normal, _ = normed(mixed)
        shift = mod_rows(sel[rows], mod, 3)
        scale = mod_rows(sel[rows], mod, 4)
        h[rows] = (normal * (1.0 + scale) + shift).astype(BF)

    over_blocks(rows_here, between)

    def use(chunk):
        rows = chunk_rows(chunk, rows_here)
        gate[rows] = nn(whole[rows], wg[0])
        up[rows] = nn(whole[rows], wg[1])
        g = gate[rows]
        hidden[rows] = (g * jax.nn.sigmoid(g) * up[rows]).astype(BF)

    second = (o2, i2, k2, s2)
    stores = []
    for n, (src, dst) in enumerate(
        ((whole, whole_h), (gate, gate_h), (up, up_h), (hidden, hidden_h))
    ):
        stores.append(pltpu.make_async_copy(src, dst, wsem.at[3 + n]))

    def ready():
        load_g.wait()
        load_d.wait()

    def fill():
        for copy in stores:
            copy.start()

    def term(chunk):
        return nn(hidden[chunk_rows(chunk, rows_here)], wd[...])

    gather_scatter(place, h, whole, sems, 6, use, term, second, ready, fill)

    def finish(rows):
        branch = scattered(second, rows)
        br2[rows] = branch
        y[rows] = (x1[rows] + mod_rows(sel[rows], mod, 5) * branch).astype(BF)

    over_blocks(rows_here, finish)
    arrive(stores)


def mlp_back_kernel(layer, square, dy, br2, br1, x1, sel, mod, gate_h, up_h, hidden_h, rows_h,
                    wo0, wo1, wg0, wg1, wd0, wd1, whole1, datt, dx1, dmod, total, mine, theirs,
                    got, h, h1, whole2, dgate, dup, gate, up, hidden, saved, flipped, wo, wg, wd, o1, i1, k1,
                    s1, ssem, rsem, wsem, osem):
    place = ring(square)
    rows_here, _ = dy.shape
    load_d = layer_weights(wd0, wd1, layer, wd, wsem.at[0])
    load_gate = pltpu.make_async_copy(gate_h, gate, wsem.at[1])
    load_gate.start()
    load_up = pltpu.make_async_copy(up_h, up, wsem.at[2])
    load_up.start()
    load_g = layer_weights(wg0, wg1, layer, wg, wsem.at[3])
    load_o = head_weights(wo0, wo1, layer, wo, osem, range(1))
    load_hidden = pltpu.make_async_copy(hidden_h, hidden, wsem.at[5])
    load_hidden.start()
    load_rows = pltpu.make_async_copy(rows_h, saved, wsem.at[6])
    load_rows.start()
    greet(place, True)
    sems = (ssem, rsem)
    dmod[...] = jnp.zeros_like(dmod)

    def prepare(rows):
        incoming = dy[rows].astype(F32)
        h[rows] = (incoming * mod_rows(sel[rows], mod, 5)).astype(BF)
        add_sums(dmod, 3, sel[rows], incoming * br2[rows])

    over_blocks(rows_here, prepare)

    def ready():
        arrive((load_d, load_gate, load_up, load_g, load_hidden))

    def use(chunk):
        rows = chunk_rows(chunk, rows_here)
        d_hidden = nt(whole2[rows], wd[...])
        g = gate[rows]
        s = jax.nn.sigmoid(g)
        dgate[rows] = (d_hidden * up[rows] * s * (1.0 + g * (1.0 - s))).astype(BF)
        dup[rows] = (d_hidden * g * s).astype(BF)

    bufs = (o1, i1, k1, s1)
    f = hidden.shape[1]

    def term(chunk):
        rows = chunk_rows(chunk, rows_here)
        return nt(dgate[rows], wg[0]) + nt(dup[rows], wg[1])

    packs = (mine, theirs, got)
    copies = []

    def grad(index, x, y, col):
        weight_grad(x, y, flipped, col, packs)
        copies.append(send_half(packs, sems, index, col, f))

    def grad_down():
        grad(18, whole2, hidden, 2 * f)

    gather_scatter(place, h, whole2, sems, 0, use, term, bufs, ready, grad_down)

    def between(rows):
        d_h = scattered(bufs, rows)
        normal, inverse = normed(x1[rows])
        scale = mod_rows(sel[rows], mod, 4)
        d_mixed = dy[rows].astype(F32) + norm_back(d_h * (1.0 + scale), normal, inverse)
        dx1[rows] = d_mixed
        h1[rows] = (d_mixed * mod_rows(sel[rows], mod, 2)).astype(BF)

    over_blocks(rows_here, between)

    def use_out(chunk):
        rows = chunk_rows(chunk, rows_here)
        datt[rows] = nt(whole1[rows], wo[...]).astype(BF)

    def sums():
        def one(rows):
            d_h = scattered(bufs, rows)
            normal, _ = normed(x1[rows])
            add_sums(dmod, 1, sel[rows], d_h)
            add_sums(dmod, 2, sel[rows], d_h * normal)
            add_sums(dmod, 0, sel[rows], dx1[rows] * br1[rows])

        over_blocks(rows_here, one)
        arrive(load_o)
        load_rows.wait()
        grad(19, saved, dgate, 0)

    def late():
        weight_grad(None, dup, flipped, f, packs)

    gather(place, h1, whole1, sems, 12, use_out, sums, late)
    copies.append(send_half(packs, sems, 20, f, f))
    add_halves(packs, copies[:1], total, 2 * f, f)
    add_halves(packs, copies[1:2], total, 0, f)
    add_halves(packs, copies[2:], total, f, f)


def qkv_back_kernel(layer, square, dq, dk, dv, proj, gain, both, turn, ones, spread, x, dx1, sel,
                    mod, part, prev, w_own, w_other, whole_h, att_h, rows1_h, du, du_b, dmod, total,
                    dgain, w, whole, att, rows1, flipped, dproj, flat, mine, theirs, got, o1, i1,
                    k1, s1, ssem, rsem, wsem, hsem):
    place = ring(square)
    rows_here, _ = x.shape
    packed = spread.shape[0]
    head = packed * PAD // spread.shape[1]
    load = head_weights(w_own, w_other, layer, w, hsem, range(3))
    loads = []
    for n, (src, dst) in enumerate(((whole_h, whole), (att_h, att), (rows1_h, rows1))):
        loads.append(pltpu.make_async_copy(src, dst, wsem.at[n]))
        loads[n].start()
    greet(place, True)
    here = dmod.at[layer]
    dmod[1 - layer] = prev[...]
    here[pl.ds(0, 4)] = jnp.zeros_like(prev[pl.ds(0, 4)])
    here[pl.ds(4, 8)] = part[...]
    dgain[...] = jnp.zeros_like(dgain)
    arrive(load)
    bufs = (o1, i1, k1, s1)
    sems = (ssem, rsem)
    packs = (mine, theirs, got)
    copies = []

    def term(chunk):
        rows = chunk_rows(chunk, rows_here)
        cosine = twice(both[rows, 0:PAD])
        sine = twice(both[rows, PAD : 2 * PAD])
        for which, src in ((0, dq), (1, dk)):
            for pair in range(src.shape[1] // (2 * PAD)):
                lanes = slice(pair * 2 * PAD, (pair + 1) * 2 * PAD)
                turned = src[rows, lanes]
                back = turned.astype(F32) * cosine - nn(turned, turn[...]) * sine
                normal, inverse = unit(proj[which, rows, lanes].astype(F32), ones[...], head)
                dgain[which, :, lanes] += jnp.sum(back * normal, axis=0, keepdims=True)
                gained = back * twice(gain[which : which + 1])
                mean = two(nn, gained * normal, ones[...]) * (1.0 / head)
                dproj[which, rows, lanes] = (inverse * (gained - normal * mean)).astype(BF)
        return nn(dproj[0, rows], w[0]) + nn(dproj[1, rows], w[1]) + nn(dv[rows], w[2])

    def grad_in():
        loads[0].wait()
        for k in range(3):
            flat[...] = nt(dproj[k] if k < 2 else dv[...], spread[...]).astype(BF)
            weight_grad(None if k else whole, flat, flipped, k * packed, packs)

    def grad_out():
        loads[1].wait()
        loads[2].wait()
        flat[...] = nt(att[...], spread[...]).astype(BF)
        weight_grad(rows1, flat, flipped, 3 * packed, packs)

    def grads():
        grad_in()
        grad_out()
        copies.append(send_half(packs, sems, 6, 0, 4 * packed))

    scatter(place, term, bufs, sems, 0, grads)

    def finish(rows):
        d_h = scattered(bufs, rows)
        normal, inverse = normed(x[rows].astype(F32))
        scale = mod_rows(sel[rows], mod, 1)
        total_rows = dx1[rows] + norm_back(d_h * (1.0 + scale), normal, inverse)
        du[rows] = total_rows
        du_b[rows] = total_rows.astype(BF)
        add_sums(here, 0, sel[rows], d_h)
        add_sums(here, 1, sel[rows], d_h * normal)

    over_blocks(rows_here, finish)
    add_halves(packs, copies, total, 0, 4 * packed)


def cell():
    return 4 * lax.axis_index(S) + lax.axis_index(T)


def cell_id(index):
    return {S: index // 4, T: index % 4}


def greet_all(dp):
    sem = pltpu.get_barrier_semaphore()
    here, shard = cell(), lax.axis_index(DP)
    for k in range(1, 8):
        pl.semaphore_signal(
            sem, inc=1, device_id=cell_id((here + k) % 8), device_id_type=pl.DeviceIdType.MESH
        )
    for k in range(1, dp):
        pl.semaphore_signal(
            sem, inc=1, device_id={DP: (shard + k) % dp}, device_id_type=pl.DeviceIdType.MESH
        )
    pl.semaphore_wait(sem, 7 + dp - 1)


def push(src, dst, sems, index, device):
    copy = pltpu.make_async_remote_copy(
        src_ref=src,
        dst_ref=dst,
        send_sem=sems[0].at[index],
        recv_sem=sems[1].at[index],
        device_id=device,
        device_id_type=pl.DeviceIdType.MESH,
    )
    copy.start()
    return copy


def head_kernel(dp, lifted, ada_h, bias, gain, items, pos, tables, mod, lifted_all, gains, sel,
                both, spans, ada, parts, got, wide, tall, ssem, rsem, wsem):
    load = pltpu.make_async_copy(ada_h, ada, wsem)
    load.start()
    greet_all(dp)
    sems = (ssem, rsem)
    here, shard, section = cell(), lax.axis_index(DP), lax.axis_index(S)
    copies = [push(gain, gains.at[section], sems, 6 + dp, {S: 1 - section})]
    gains[section] = gain[...]
    lifted_all[shard] = lifted[...]
    for k in range(1, dp):
        copies.append(
            push(lifted, lifted_all.at[shard], sems, 6 + k, {DP: (shard + k) % dp})
        )
    load.wait()
    half = parts.shape[3]
    for micro in range(2):
        for j in range(3):
            rows = lifted[pl.ds(micro * 8, 8)].astype(BF)
            parts[micro, j] = nt(rows, ada[pl.ds(j * half, half)]) + bias[j]
    for k in range(1, 8):
        peer = (here + k) % 8
        copies.append(push(parts.at[peer // 4], got.at[here], sems, k - 1, cell_id(peer)))
    got[here] = parts[section]
    rows_here = sel.shape[0]
    base = shard * 6 + section * 3
    seq = items.shape[1]
    line = items[pl.ds(section, 1), :]
    wide[...] = jnp.zeros_like(wide)
    wide[0:1] = (line - base).astype(F32)
    wide[1:2] = pos[0, pl.ds(section, 1), :].astype(F32)
    wide[2:3] = pos[1, pl.ds(section, 1), :].astype(F32)
    start = 0
    spans[0] = 0
    for j in range(3):
        count = jnp.sum((wide[0:1] == j).astype(F32)).astype(jnp.int32)
        spans[4 + j] = count
        start = start + count
        spans[1 + j] = start
    spans[7] = 0
    tall[...] = wide[...].T
    own = tall[pl.ds(pl.multiple_of(lax.axis_index(T) * rows_here, rows_here), rows_here), :]
    lane = lax.broadcasted_iota(jnp.int32, (rows_here, 8), 1).astype(F32)
    sel[...] = ((own[:, 0:1] == lane) & (lane < 3.0)).astype(F32)
    lane = lax.broadcasted_iota(jnp.int32, (seq, 64), 1).astype(F32)
    hot = jnp.where(lane < 32.0, tall[:, 1:2], tall[:, 2:3] + 32.0) == lane
    hot = hot.astype(F32).astype(BF)
    both[...] = (nn(hot, tables[0]) + nn(hot, tables[1])) + nn(hot, tables[2])
    for copy in copies:
        copy.wait_recv()
    for layer in range(2):
        for block in range(6):
            for side in range(2):
                n = 2 * block + side
                mod[layer, block, :, pl.ds(side * half, half)] = got[4 * layer + n // 3, n % 3]
    for copy in copies:
        copy.wait_send()


def tail_kernel(dp, dmod, dgain, lifted_part, ada_h, ada_grad, bias_grad, dl_sum, gain_sum, ada,
                got, got_gain, total, total_gain, every, every_gain, lifts, ssem, rsem, wsem):
    load = pltpu.make_async_copy(ada_h, ada, wsem)
    load.start()
    greet_all(dp)
    sems = (ssem, rsem)
    here, shard = cell(), lax.axis_index(DP)
    section, place = lax.axis_index(S), lax.axis_index(T)
    sends, arrivals = [], []
    for k in range(1, 8):
        peer = (here + k) % 8
        to = cell_id(peer)
        arrivals.append(
            push(dmod.at[peer // 4, pl.ds(3 * (peer % 4), 3)], got.at[here], sems, k - 1, to)
        )
        arrivals.append(push(dgain.at[peer // 4], got_gain.at[here], sems, 6 + k, to))
    got[here] = dmod[section, pl.ds(3 * place, 3)]
    got_gain[here] = dgain[section]
    for copy in arrivals:
        copy.wait_recv()
    sends += arrivals
    for micro in range(2):
        total[micro] = (got[4 * micro] + got[4 * micro + 1]) + (got[4 * micro + 2] + got[4 * micro + 3])
    gain = got_gain[0]
    for k in range(1, 8):
        gain = gain + got_gain[k]
    total_gain[...] = gain
    arrivals = []
    for k in range(1, dp):
        to = {DP: (shard + k) % dp}
        arrivals.append(push(total, every.at[shard], sems, 13 + k, to))
        arrivals.append(push(total_gain, every_gain.at[shard], sems, 12 + dp + k, to))
    every[shard] = total[...]
    every_gain[shard] = total_gain[...]
    load.wait()
    half = total.shape[3]
    for micro in range(2):
        lift = two(nn, total[micro, 0], ada[pl.ds(0, half)])
        for j in range(1, 3):
            lift = lift + two(nn, total[micro, j], ada[pl.ds(j * half, half)])
        lifts[here, micro] = lift
    base = 13 + 2 * (dp - 1)
    lift_copies = []
    for k in range(1, 8):
        lift_copies.append(
            push(lifts.at[here], lifts.at[here], sems, base + k, cell_id((here + k) % 8))
        )
    for copy in arrivals:
        copy.wait_recv()
    sends += arrivals
    gain = every_gain[0]
    for k in range(1, dp):
        gain = gain + every_gain[k]
    gain_sum[...] = gain
    for j in range(3):
        bias = jnp.zeros((1, half), F32)
        grad = jnp.zeros((lifted_part.shape[2], half), F32)
        for k in range(dp):
            for micro in range(2):
                block = every[k, micro, j]
                bias = bias + jnp.sum(block, axis=0, keepdims=True)
                high = block.astype(BF)
                low = (block - high.astype(F32)).astype(BF)
                rows = lifted_part[2 * k + micro].astype(BF)
                grad = grad + tn(rows, high) + tn(rows, low)
        bias_grad[j] = bias
        ada_grad[:, pl.ds(j * half, half)] = grad
    for copy in lift_copies:
        copy.wait_recv()
    sends += lift_copies
    lift = lifts[0]
    for k in range(1, 8):
        lift = lift + lifts[k]
    dl_sum[...] = lift
    for copy in sends:
        copy.wait_send()


def price(micros):
    return pl.CostEstimate(flops=0, bytes_accessed=int(micros * 3.5e6), transcendentals=0)


def ring_call(kernel, ident, micros, outs, scratch, args, spaces, scalar=-1, loose=99):
    return pl.pallas_call(
        kernel,
        out_shape=outs,
        in_specs=[vmem() if s else anywhere() for s in spaces],
        out_specs=[
            pl.BlockSpec(memory_space=pltpu.SMEM)
            if n == scalar
            else (vmem() if n < loose else anywhere())
            for n in range(len(outs))
        ],
        scratch_shapes=scratch,
        compiler_params=pltpu.CompilerParams(
            collective_id=ident, has_side_effects=True, vmem_limit_bytes=60 * 2**20
        ),
        cost_estimate=price(micros),
    )(*args)


def attention_kernel(head, spans, q, k, v, att):
    rows, wide = q.shape
    scale = head ** (-0.5)

    def each_head(fn):
        for n in range(wide // PAD):
            fn(slice(n * PAD, (n + 1) * PAD))

    def one_item(item, carry):
        at = pl.ds(pl.multiple_of(spans[item], 16), TILE)
        valid = lax.broadcasted_iota(jnp.int32, (TILE, TILE), 1) < spans[4 + item]

        def tile(lanes):
            att[at, lanes] = softmax_rows(q[at, lanes], k[at, lanes], v[at, lanes], valid, scale)

        each_head(tile)
        return carry

    lax.fori_loop(0, 3, one_item, 0)
    first = rows - 48
    start = spans[3]
    at = pl.ds(first, 48)
    valid = first + lax.broadcasted_iota(jnp.int32, (48, 48), 1) >= start
    live = first + lax.broadcasted_iota(jnp.int32, (48, PAD), 0) >= start

    def rest(lanes):
        new = softmax_rows(q[at, lanes], k[at, lanes], v[at, lanes], valid, scale)
        att[at, lanes] = jnp.where(live, new, att[at, lanes])

    each_head(rest)


def unit(proj, ones, head):
    inverse = lax.rsqrt(two(nn, proj * proj, ones) * (1.0 / head) + EPS)
    return proj * inverse, inverse


def softmax_rows(query, key, value, valid, scale):
    scores = jnp.where(valid, nt(query, key) * scale, -1e30)
    raised = jnp.exp(scores - jnp.max(scores, axis=1, keepdims=True))
    probs = raised / jnp.sum(raised, axis=1, keepdims=True)
    return nn(probs.astype(BF), value).astype(BF)


def back_tile(query, key, value, grad, keys, queries, scale):
    scores = jnp.where(keys, nt(key, query) * scale, -1e30)
    raised = jnp.exp(scores - jnp.max(scores, axis=0, keepdims=True))
    probs = jnp.where(queries, raised / jnp.sum(raised, axis=0, keepdims=True), 0.0)
    d_value = nn(probs.astype(BF), grad)
    d_probs = nt(value, grad)
    inner = jnp.sum(probs * d_probs, axis=0, keepdims=True)
    d_scores = (probs * (d_probs - inner)).astype(BF)
    return tn(d_scores, key) * scale, nn(d_scores, query) * scale, d_value


def attention_back_kernel(head, spans, q, k, v, grad, dq, dk, dv):
    rows, wide = q.shape
    scale = head ** (-0.5)

    def each_head(fn):
        for n in range(wide // PAD):
            fn(slice(n * PAD, (n + 1) * PAD))

    def one_item(item, carry):
        at = pl.ds(pl.multiple_of(spans[item], 16), TILE)
        keys = lax.broadcasted_iota(jnp.int32, (TILE, TILE), 0) < spans[4 + item]
        queries = lax.broadcasted_iota(jnp.int32, (TILE, TILE), 1) < spans[4 + item]

        def tile(lanes):
            parts = back_tile(
                q[at, lanes], k[at, lanes], v[at, lanes], grad[at, lanes], keys, queries, scale
            )
            for new, dst in zip(parts, (dq, dk, dv)):
                dst[at, lanes] = new.astype(BF)

        each_head(tile)
        return carry

    lax.fori_loop(0, 3, one_item, 0)
    first = rows - 48
    start = spans[3]
    at = pl.ds(first, 48)
    keys = first + lax.broadcasted_iota(jnp.int32, (48, 48), 0) >= start
    queries = first + lax.broadcasted_iota(jnp.int32, (48, 48), 1) >= start
    live = first + lax.broadcasted_iota(jnp.int32, (48, PAD), 0) >= start

    def rest(lanes):
        parts = back_tile(
            q[at, lanes], k[at, lanes], v[at, lanes], grad[at, lanes], keys, queries, scale
        )
        for new, dst in zip(parts, (dq, dk, dv)):
            dst[at, lanes] = jnp.where(live, new.astype(BF), dst[at, lanes])

    each_head(rest)


def local_call(kernel, micros, outs, scratch, spans, args):
    return pl.pallas_call(
        kernel,
        out_shape=outs,
        in_specs=[pl.BlockSpec(memory_space=pltpu.SMEM)] + [vmem()] * len(args),
        out_specs=[vmem()] * len(outs),
        scratch_shapes=scratch,
        compiler_params=pltpu.CompilerParams(vmem_limit_bytes=60 * 2**20),
        cost_estimate=price(micros),
    )(spans, *args)


def swap(array):
    return lax.ppermute(array, S, [(0, 1), (1, 0)])


def head_tables(packed, head):
    quarter = head // 4
    frequency = np.float32(10000.0) ** (-np.arange(quarter, dtype=np.float32) / quarter)
    lane = np.arange(head)
    angle = np.arange(32, dtype=np.float32)[:, None] * frequency[lane % quarter][None, :]
    by_row = (lane // (2 * quarter) == 0)[None, :]
    table = np.zeros((64, 2 * PAD), np.float32)
    for n, values in enumerate((np.cos(angle), np.sin(angle))):
        at = slice(n * PAD, n * PAD + head)
        table[:32, at] = np.where(by_row, values, 0.0)
        table[32:, at] = np.where(by_row, 0.0, values)
    table = jnp.asarray(table)
    parts = []
    for _ in range(3):
        parts.append(lax.reduce_precision(table, 8, 7).astype(BF))
        table = table - parts[-1].astype(F32)
    rows = np.arange(2 * PAD)[:, None]
    cols = np.arange(2 * PAD)[None, :]
    inside = (rows // PAD == cols // PAD) & (rows % PAD < head) & (cols % PAD < head)
    row, col = rows % PAD, cols % PAD
    early = (col % (2 * quarter)) < quarter
    turn = np.where(inside & early & (row == col + quarter), -1.0, 0.0)
    turn = turn + np.where(inside & ~early & (row == col - quarter), 1.0, 0.0)
    heads = packed // head
    rows = np.arange(packed)[:, None]
    wide = np.arange(heads * PAD)[None, :]
    spread = (rows // head == wide // PAD) & (rows % head == wide % PAD)
    lanes = tuple(jnp.asarray(m.astype(np.float32)).astype(BF) for m in (turn, inside, spread))
    return jnp.stack(parts), lanes


def reduced(total):
    return lax.psum_scatter(total, DP, scatter_dimension=0, tiled=True)[0]


def own_layer(section, pair):
    first = section == 0
    keep = jnp.where(first, pair[0], pair[1])
    got = swap(jnp.where(first, pair[1], pair[0]))
    return jnp.where(first, jnp.concatenate([keep, got]), jnp.concatenate([got, keep])).astype(F32)


def per_device(square, dp, tokens, cotangent, cond, patch_item, patch_pos, w_qkv, w_out, w_gate_up,
               w_down, qk_gain, ada_weight, ada_bias):
    section = lax.axis_index(S)
    first = section == 0
    rows, width = tokens.shape[1:]
    seq = patch_item.shape[1]
    items = cond.shape[0]
    per_micro = items // 2
    head = qk_gain.shape[-1]
    packed = w_qkv.shape[-1]
    heads = packed // head
    hidden_here = w_down.shape[1]
    own = (jnp.swapaxes(w_qkv[0], 1, 2), w_out[0], w_gate_up[0], w_down[0])
    other = tuple(swap(w) for w in own)

    cond_wide = cond.astype(F32)
    cond_sigmoid = jax.nn.sigmoid(cond_wide)
    lifted = (cond_wide * cond_sigmoid).astype(BF).astype(F32).reshape(2, per_micro, width)
    lifted = jnp.pad(lifted, ((0, 0), (0, 8 - per_micro), (0, 0))).reshape(16, width)
    ada = ada_weight[0].T
    half = width // 2
    bias = ada_bias.astype(F32).reshape(3, 1, half)
    gain = jnp.pad(qk_gain[0].astype(F32), ((0, 6), (0, PAD - head)))
    trig, (turn, ones, spread) = head_tables(packed, head)
    wide = heads * PAD
    mods, lifted_all, gains, sel, both, spans = ring_call(
        functools.partial(head_kernel, dp),
        8,
        12,
        [
            sds((2, 6, 8, width), F32),
            sds((dp, 16, width), F32),
            sds((2, 8, PAD), F32),
            sds((rows, 8), F32),
            sds((seq, 2 * PAD), F32),
            sds((8,), jnp.int32),
        ],
        [
            pltpu.VMEM((3 * half, width), BF),
            pltpu.VMEM((2, 3, 8, half), F32),
            pltpu.VMEM((8, 3, 8, half), F32),
            pltpu.VMEM((8, seq), F32),
            pltpu.VMEM((seq, 8), F32),
        ]
        + dma_sems(7 + dp)
        + [pltpu.SemaphoreType.DMA],
        (lifted, ada, bias, gain, patch_item, patch_pos, trig),
        (1, 0, 1, 1, 1, 1, 1),
        scalar=5,
    )
    part = width // dp
    shard = lax.axis_index(DP)
    lifted_part = lax.dynamic_slice_in_dim(lifted_all, shard * part, part, 2)
    lifted_part = lifted_part.reshape(2 * dp, 8, part)

    x = lax.dynamic_index_in_dim(tokens, section, 0, keepdims=False)
    kept = []
    for layer in range(2):
        mod = mods[layer]
        whole1, proj, q, k, v = ring_call(
            functools.partial(qkv_kernel, layer, square),
            layer,
            20,
            [sds((seq, width), BF), sds((2, seq, wide), BF)] + [sds((seq, wide), BF)] * 3,
            [pltpu.VMEM((rows, width), BF), pltpu.VMEM((3, wide, width), BF)]
            + dma_sems(6)
            + [pltpu.SemaphoreType.DMA((3 * heads,))],
            (x, sel, mod, gains[layer], both, turn, ones, own[0], other[0]),
            (1,) * 7 + (0, 0),
        )
        (att,) = local_call(
            functools.partial(attention_kernel, head),
            6,
            [sds((seq, wide), BF)],
            [],
            spans,
            (q, k, v),
        )
        br1, x1, br2, y, whole2, gate, up, hidden = ring_call(
            functools.partial(mlp_kernel, layer, square),
            2 + layer,
            48,
            [
                sds((rows, width), F32),
                sds((rows, width), F32),
                sds((rows, width), F32),
                sds((rows, width), BF),
                sds((seq, width), BF),
                sds((seq, hidden_here), F32),
                sds((seq, hidden_here), F32),
                sds((seq, hidden_here), BF),
            ],
            [
                pltpu.VMEM((seq, width), BF),
                pltpu.VMEM((seq, hidden_here), F32),
                pltpu.VMEM((seq, hidden_here), F32),
                pltpu.VMEM((seq, hidden_here), BF),
                pltpu.VMEM((rows, width), BF),
                pltpu.VMEM((wide, width), BF),
                pltpu.VMEM((2, width, hidden_here), BF),
                pltpu.VMEM((hidden_here, width), BF),
            ]
            + scatter_scratch(rows, width)
            + scatter_scratch(rows, width)
            + dma_sems(18)
            + [pltpu.SemaphoreType.DMA((7,)), pltpu.SemaphoreType.DMA((heads,))],
            (att, x, sel, mod, own[1], other[1], own[2], other[2], own[3], other[3]),
            (1, 1, 1, 1) + (0,) * 6,
            loose=4,
        )
        kept.append((x, whole1, proj, q, k, v, att, br1, x1, whole2, gate, up, hidden, br2, y))
        x = y

    dy = lax.dynamic_index_in_dim(cotangent, section, 0, keepdims=False)
    packs = [None, None]
    prev = jnp.zeros((12, 8, half), F32)
    d_gains = [None, None]
    d_inputs = [None, None]
    for layer in (1, 0):
        x, whole1, proj, q, k, v, att, br1, x1, whole2, gate, up, hidden, br2, y = kept[layer]
        mod = mods[layer]
        rows1, datt, dx1, dmod_a, total_mlp = ring_call(
            functools.partial(mlp_back_kernel, layer, square),
            4 + layer,
            52,
            [
                sds((seq, width), BF),
                sds((seq, wide), BF),
                sds((rows, width), F32),
                sds((8, 8, half), F32),
                sds((dp, part // 2, 3 * hidden_here), BF),
            ],
            [pltpu.VMEM((dp, part // 2, 3 * hidden_here), BF)] * 3
            + [
                pltpu.VMEM((rows, width), BF),
                pltpu.VMEM((rows, width), BF),
                pltpu.VMEM((seq, width), BF),
                pltpu.VMEM((seq, hidden_here), BF),
                pltpu.VMEM((seq, hidden_here), BF),
                pltpu.VMEM((seq, hidden_here), F32),
                pltpu.VMEM((seq, hidden_here), F32),
                pltpu.VMEM((seq, hidden_here), BF),
                pltpu.VMEM((seq, width), BF),
                pltpu.VMEM((width, seq), BF),
                pltpu.VMEM((wide, width), BF),
                pltpu.VMEM((2, width, hidden_here), BF),
                pltpu.VMEM((hidden_here, width), BF),
            ]
            + scatter_scratch(rows, width)
            + dma_sems(21)
            + [pltpu.SemaphoreType.DMA((7,)), pltpu.SemaphoreType.DMA((heads,))],
            (dy, br2, br1, x1, sel, mod, gate, up, hidden, whole2, own[1], other[1], own[2],
             other[2], own[3], other[3]),
            (1,) * 6 + (0,) * 10,
        )
        pack_mlp = reduced(total_mlp)
        dq, dk, dv = local_call(
            functools.partial(attention_back_kernel, head),
            10,
            [sds((seq, wide), BF)] * 3,
            [],
            spans,
            (q, k, v, datt),
        )
        du, du_b, d_mod, total_att, dgain = ring_call(
            functools.partial(qkv_back_kernel, layer, square),
            6 + layer,
            22,
            [
                sds((rows, width), F32),
                sds((rows, width), BF),
                sds((2, 12, 8, half), F32),
                sds((dp, part // 2, 4 * packed), BF),
                sds((2, 1, wide), F32),
            ],
            [
                pltpu.VMEM((3, wide, width), BF),
                pltpu.VMEM((seq, width), BF),
                pltpu.VMEM((seq, wide), BF),
                pltpu.VMEM((seq, width), BF),
                pltpu.VMEM((width, seq), BF),
                pltpu.VMEM((2, seq, wide), BF),
                pltpu.VMEM((seq, packed), BF),
            ]
            + [pltpu.VMEM((dp, part // 2, 4 * packed), BF)] * 3
            + scatter_scratch(rows, width)
            + dma_sems(7)
            + [pltpu.SemaphoreType.DMA((3,)), pltpu.SemaphoreType.DMA((3 * heads,))],
            (dq, dk, dv, proj, gains[layer], both, turn, ones, spread, x, dx1, sel, mod, dmod_a,
             prev, own[0], other[0], whole1, att, rows1),
            (1,) * 15 + (0,) * 5,
        )
        prev = d_mod[1]
        pack_att = reduced(total_att)
        packs[layer] = (pack_mlp, pack_att)
        d_gains[layer] = dgain
        d_inputs[layer] = du_b if layer else du
        dy = du_b

    gain_parts = jnp.pad(jnp.stack(d_gains).reshape(2, 2, wide), ((0, 0), (0, 6), (0, 0)))
    g_ada_w, bias_grad, dl_sum, gain_sum = ring_call(
        functools.partial(tail_kernel, dp),
        9,
        15,
        [
            sds((part, 3 * half), F32),
            sds((3, 1, half), F32),
            sds((2, 8, width), F32),
            sds((8, wide), F32),
        ],
        [
            pltpu.VMEM((3 * half, width), BF),
            pltpu.VMEM((8, 3, 8, half), F32),
            pltpu.VMEM((8, 8, wide), F32),
            pltpu.VMEM((2, 3, 8, half), F32),
            pltpu.VMEM((8, wide), F32),
            pltpu.VMEM((dp, 2, 3, 8, half), F32),
            pltpu.VMEM((dp, 8, wide), F32),
            pltpu.VMEM((8, 2, 8, width), F32),
        ]
        + dma_sems(13 + 2 * (dp - 1) + 8)
        + [pltpu.SemaphoreType.DMA],
        (d_mod, gain_parts, lifted_part, ada),
        (1, 1, 1, 0),
    )
    bias_part = ada_bias.shape[1] // dp
    g_ada_b = lax.dynamic_slice_in_dim(bias_grad.reshape(-1), shard * bias_part, bias_part)
    cond_grad = dl_sum[:, :per_micro].reshape(items, width) * cond_sigmoid
    cond_grad = cond_grad * (1.0 + cond_wide * (1.0 - cond_sigmoid))
    gain_total = gain_sum[:2].reshape(1, 2, heads, PAD)[..., :head].sum(axis=2)

    mlp = own_layer(section, (packs[0][0], packs[1][0]))
    attn = own_layer(section, (packs[0][1], packs[1][1]))
    f = hidden_here
    g_gate_up = jnp.stack([mlp[:, :f], mlp[:, f : 2 * f]])[None]
    g_down = mlp[:, 2 * f :].T[None]
    g_qkv = jnp.stack([attn[:, k * packed : (k + 1) * packed] for k in range(3)])[None]
    g_out = attn[:, 3 * packed :].T[None]

    outs = jnp.where(first, kept[0][-1], kept[1][-1])
    outs_got = swap(jnp.where(first, kept[1][-1], kept[0][-1]))
    layer_out = jnp.where(first, jnp.stack([outs, outs_got]), jnp.stack([outs_got, outs]))
    wide_mid = d_inputs[1].astype(F32)
    back_keep = jnp.where(first, d_inputs[0], wide_mid)
    back_got = swap(jnp.where(first, wide_mid, d_inputs[0]))
    in_grads = jnp.where(first, jnp.stack([back_keep, back_got]), jnp.stack([back_got, back_keep]))
    return (
        layer_out[None],
        in_grads[None],
        cond_grad,
        g_qkv,
        g_out,
        g_gate_up,
        g_down,
        gain_total,
        g_ada_w[None],
        g_ada_b[None],
    )


def solution(mesh):
    both = (DP, T)
    in_specs = (
        P(None, both, None),
        P(None, both, None),
        P(DP, None),
        P(None, DP),
        P(None, None, DP),
        P(S, None, None, T),
        P(S, T, None),
        P(S, None, None, T),
        P(S, T, None),
        P(S, None, None),
        P(S, None, T),
        P(S, T),
    )
    out_specs = (
        P(S, None, both, None),
        P(S, None, both, None),
        P(DP, None),
        P(S, None, DP, T),
        P(S, T, DP),
        P(S, None, DP, T),
        P(S, T, DP),
        P(S, None, None),
        P(S, DP, T),
        P(S, (T, DP)),
    )
    dp = mesh.shape[DP]

    def program(*args):
        return per_device(dp <= 4, dp, *args)

    return jax.shard_map(
        program, mesh=mesh, in_specs=in_specs, out_specs=out_specs, check_vma=False
    )
```

```python
import functools

import jax
import jax.numpy as jnp
import numpy as np
from jax import lax
from jax.experimental import pallas as pl
from jax.experimental.pallas import tpu as pltpu
from jax.sharding import PartitionSpec as P


EPS = 1e-06
F32 = jnp.float32
BF = jnp.bfloat16
S, DP, T = "section", "dp", "tensor"
PAD = 128
TILE = 256


def nn(a, b):
    return jnp.dot(a, b, preferred_element_type=F32)


def nt(a, b):
    return lax.dot_general(a, b, (((1,), (1,)), ((), ())), preferred_element_type=F32)


def tn(a, b):
    return lax.dot_general(a, b, (((0,), (0,)), ((), ())), preferred_element_type=F32)


def two(dot, a, b):
    high = a.astype(BF)
    low = (a - high.astype(F32)).astype(BF)
    return dot(high, b) + dot(low, b)


def sds(shape, dtype):
    return jax.ShapeDtypeStruct(shape, dtype)


def vmem():
    return pl.BlockSpec(memory_space=pltpu.VMEM)


def anywhere():
    return pl.BlockSpec(memory_space=pl.ANY)


def ring(square):
    me = lax.axis_index(T)
    near = me + 1 - 2 * (me % 2)
    if square:
        return me, near, me + 2 - 4 * (me // 2), 3 - me, True
    return me, near, 3 - me, (me + 2) % 4, False


def pieces(place, step, half):
    me, upper, moved, far = place[0], (step % 3) // 2, (step + 2) // 3, step // 3
    near = moved - far
    low = (moved, far) if place[4] else (near, near)
    found = []
    for side, high in ((0, far), (1, moved)):
        chunk = (me % 2 + low[side]) % 2 + 2 * ((me // 2 + high) % 2)
        row = (2 * chunk + (1 - upper if side else upper)) * half
        found.append(pl.ds(pl.multiple_of(row, half), half))
    return found


def joined(ref, rows):
    return jnp.concatenate([ref[rows[0]], ref[rows[1]]], axis=0)


def put(ref, rows, values):
    half = values.shape[0] // 2
    ref[rows[0]] = values[:half].astype(ref.dtype)
    ref[rows[1]] = values[half:].astype(ref.dtype)


def farthest_first(place, step):
    me, low = place[0], ((step + 1) // 2) % 2
    if place[4]:
        low = (3 - step) // 2
    return (me % 2 + low) % 2 + 2 * ((me // 2 + (step + 1) % 2) % 2)


def near_first(place, step):
    me, low = place[0], (3 - step) // 2
    if place[4]:
        low = (step + 1) % 2
    return (me % 2 + low) % 2 + 2 * ((me // 2 + ((step + 1) // 2) % 2) % 2)


def greet(place, partner=False):
    sem = pltpu.get_barrier_semaphore()
    peers = (place[1], place[2]) if place else ()
    for peer in peers:
        pl.semaphore_signal(
            sem, inc=1, device_id={T: peer}, device_id_type=pl.DeviceIdType.MESH
        )
    if partner:
        pl.semaphore_signal(
            sem, inc=1, device_id={S: 1 - lax.axis_index(S)}, device_id_type=pl.DeviceIdType.MESH
        )
    pl.semaphore_wait(sem, len(peers) + partner)


def remote(src, dst, sems, index, peer):
    return pltpu.make_async_remote_copy(
        src_ref=src,
        dst_ref=dst,
        send_sem=sems[0].at[index],
        recv_sem=sems[1].at[index],
        device_id={T: peer},
        device_id_type=pl.DeviceIdType.MESH,
    )


def chunk_rows(chunk, rows):
    return pl.ds(pl.multiple_of(chunk * rows, rows), rows)


def repeat(body, times):
    def one(step, carry):
        body(step)
        return carry

    lax.fori_loop(0, times, one, 0)


def gather(place, mine, whole, sems, base, use, ready=lambda: None, late=lambda: None, last=None):
    me, a, b, _, _ = place
    rows = mine.shape[0]
    half = rows // 2
    lo, hi = pl.ds(0, half), pl.ds(half, half)

    def part(chunk, upper):
        return whole.at[pl.ds(pl.multiple_of(chunk * rows + upper * half, half), half)]

    a0 = remote(mine.at[lo], part(me, 0), sems, base, a)
    b0 = remote(mine.at[hi], part(me, 1), sems, base + 1, b)
    a1 = remote(mine.at[hi], part(me, 1), sems, base + 2, a)
    b1 = remote(mine.at[lo], part(me, 0), sems, base + 3, b)
    b2 = remote(part(a, 0), part(a, 0), sems, base + 4, b)
    a2 = remote(part(b, 1), part(b, 1), sems, base + 5, a)
    for copy in (a0, b0, a1, b1):
        copy.start()
    whole[chunk_rows(me, rows), :] = mine[...]
    ready()

    def final():
        b2.wait_recv()
        a2.wait_recv()

    def body(step):
        @pl.when(step == 1)
        def _():
            a0.wait_recv()
            b2.start()
            b0.wait_recv()
            a2.start()

        @pl.when(step == 2)
        def _():
            a1.wait_recv()
            b1.wait_recv()

        if last is None:

            @pl.when(step == 3)
            def _():
                late()
                final()

        use(pieces(place, step, half))

    repeat(body, 4 if last is None else 3)
    if last is not None:
        last(final)
    for copy in (a0, b0, a1, b1, a2, b2):
        copy.wait_send()


def scatter(place, term, bufs, sems, base, fill=lambda: None, before=None):
    _, a, b, _, _ = place
    out, into, keep, own = bufs
    half = keep.shape[1]
    lo, hi = pl.ds(0, half), pl.ds(half, half)
    d0 = remote(out.at[0, lo], into.at[0, lo], sems, base, a)
    d1 = remote(out.at[0, hi], into.at[0, hi], sems, base + 1, b)
    a0 = remote(out.at[1, lo], into.at[1, lo], sems, base + 2, a)
    b0 = remote(out.at[2, hi], into.at[2, hi], sems, base + 3, b)
    a1 = remote(out.at[1, hi], into.at[1, hi], sems, base + 4, a)
    b1 = remote(out.at[2, lo], into.at[2, lo], sems, base + 5, b)
    at = (0, 1, 2) if before is None else (2, 0, 1)

    def body(step):
        if before is None:
            chunk = farthest_first(place, step)
        else:
            chunk = near_first(place, step)
            pl.when(step == 2)(before)
        own[...] = term(chunk)

        @pl.when(step == at[0])
        def _():
            out[0] = own[...].astype(BF)
            d0.start()
            d1.start()

        @pl.when(step == at[1])
        def _():
            out[1, lo] = own[lo].astype(BF)
            a0.start()
            keep[0] = own[hi]

        @pl.when(step == at[2])
        def _():
            out[2, hi] = own[hi].astype(BF)
            b0.start()
            keep[1] = own[lo]

    repeat(body, 4)
    d1.wait_recv()
    out[1, hi] = (keep[0] + into[0, hi].astype(F32)).astype(BF)
    a1.start()
    d0.wait_recv()
    out[2, lo] = (keep[1] + into[0, lo].astype(F32)).astype(BF)
    b1.start()
    fill()
    for copy in (a0, b0, a1, b1):
        copy.wait_recv()
    for copy in (d0, d1, a0, b0, a1, b1):
        copy.wait_send()


def gather_scatter(place, mine, whole, sems, base, use, term, bufs, ready, fill=lambda: None):
    def last(final):
        def before():
            final()
            use(pieces(place, 3, mine.shape[0] // 2))

        scatter(place, term, bufs, sems, base + 6, fill, before)

    gather(place, mine, whole, sems, base, use, ready, last=last)


def scattered(bufs, rows):
    return bufs[3][rows] + bufs[1][1, rows].astype(F32) + bufs[1][2, rows].astype(F32)


def scatter_scratch(rows, width):
    return [
        pltpu.VMEM((3, rows, width), BF),
        pltpu.VMEM((3, rows, width), BF),
        pltpu.VMEM((2, rows // 2, width), F32),
        pltpu.VMEM((rows, width), F32),
    ]


def dma_sems(count):
    return [pltpu.SemaphoreType.DMA((count,)), pltpu.SemaphoreType.DMA((count,))]


def layer_weights(own, other, layer, dst, sem):
    mine = lax.axis_index(S) == layer

    @pl.when(mine)
    def _():
        pltpu.make_async_copy(own, dst, sem).start()

    @pl.when(jnp.logical_not(mine))
    def _():
        pltpu.make_async_copy(other, dst, sem).start()

    return pltpu.make_async_copy(own, dst, sem)


def head_weights(own, other, layer, dst, sems, parts):
    mine = lax.axis_index(S) == layer
    spread = len(parts) > 1
    heads = dst.shape[-2] // PAD
    head = own.shape[-2] // heads
    clean = head // 16 * 16
    copies = ([], [])
    for n, part in enumerate(parts):
        for h in range(heads):
            to = dst.at[part] if spread else dst
            to[pl.ds(h * PAD + clean, PAD - clean)] = jnp.zeros((PAD - clean, dst.shape[-1]), BF)
            to = to.at[pl.ds(h * PAD, head)]
            for which, src in enumerate((own, other)):
                src = src.at[part] if spread else src
                copies[which].append(
                    pltpu.make_async_copy(
                        src.at[pl.ds(h * head, head)], to, sems.at[n * heads + h]
                    )
                )

    @pl.when(mine)
    def _():
        for copy in copies[0]:
            copy.start()

    @pl.when(jnp.logical_not(mine))
    def _():
        for copy in copies[1]:
            copy.start()

    return copies[0]


def arrive(copies):
    for copy in copies:
        copy.wait()


def twice(row):
    return jnp.concatenate([row, row], axis=-1)


def over_blocks(rows, fn):
    step = rows // 4

    def body(i, carry):
        fn(pl.ds(pl.multiple_of(i * step, step), step))
        return carry

    lax.fori_loop(0, 4, body, 0)


def mod_rows(sel, mod, which):
    total = sel[:, 0:1] * mod[which, 0:1]
    for item in (1, 2):
        total = total + sel[:, item : item + 1] * mod[which, item : item + 1]
    return total


def add_sums(dmod, block, sel, values):
    sums = item_sums(sel, values)
    half = dmod.shape[2]
    dmod[2 * block] += sums[:, :half]
    dmod[2 * block + 1] += sums[:, half:]


def weight_grad(x, y, flipped, col, packs):
    mine, theirs, _ = packs
    dp, part, _ = mine.shape
    first = lax.axis_index(S) == 0
    width = y.shape[1]
    if x is not None:
        flipped[...] = x[...].T

    def one(to, columns):
        grad = nn(flipped[...], columns).astype(BF)
        grad = grad.reshape(dp, 2, part, columns.shape[1])

        @pl.when(first)
        def _():
            mine[:, :, to] = grad[:, 0]
            theirs[:, :, to] = grad[:, 1]

        @pl.when(jnp.logical_not(first))
        def _():
            mine[:, :, to] = grad[:, 1]
            theirs[:, :, to] = grad[:, 0]

    if width % 256:
        one(pl.ds(col, width), y[...])
        return

    def body(i, carry):
        at = pl.multiple_of(i * 256, 256)
        one(pl.ds(pl.multiple_of(col + at, 256), 256), y[:, pl.ds(at, 256)])
        return carry

    lax.fori_loop(0, width // 256, body, 0)


def send_half(packs, sems, index, col, width):
    at = pl.ds(col, width)
    return push(
        packs[1].at[:, :, at], packs[2].at[:, :, at], sems, index, {S: 1 - lax.axis_index(S)}
    )


def add_halves(packs, copies, total, col, width):
    at = pl.ds(col, width)
    for copy in copies:
        copy.wait_recv()

    def body(k):
        total[k, :, at] = (packs[0][k, :, at].astype(F32) + packs[2][k, :, at].astype(F32)).astype(BF)

    repeat(body, total.shape[0])
    for copy in copies:
        copy.wait_send()


def item_sums(sel, values):
    high = values.astype(BF)
    low = (values - high.astype(F32)).astype(BF)
    sel_b = sel.astype(BF)
    return tn(sel_b, high) + tn(sel_b, low)


def normed(values):
    inverse = lax.rsqrt(jnp.mean(values * values, axis=-1, keepdims=True) + EPS)
    return values * inverse, inverse


def norm_back(incoming, normal, inverse):
    return inverse * (incoming - normal * jnp.mean(incoming * normal, axis=-1, keepdims=True))


def tokens_of(ref):
    return ref.at[lax.axis_index(S)] if len(ref.shape) == 3 else ref


def qkv_kernel(layer, square, x, sel, mod, gain, both, turn, ones, w_own, w_other, whole, proj, q,
               k, v, h, w, ssem, rsem, wsem):
    x, mod, gain = tokens_of(x), mod.at[layer], gain.at[layer]
    place = ring(square)
    head = w_own.shape[1] * PAD // w.shape[1]
    load = head_weights(w_own, w_other, layer, w, wsem, range(3))
    greet(place)

    def prepare(rows):
        normal, _ = normed(x[rows].astype(F32))
        shift = mod_rows(sel[rows], mod, 0)
        scale = mod_rows(sel[rows], mod, 1)
        h[rows] = (normal * (1.0 + scale) + shift).astype(BF)

    over_blocks(x.shape[0], prepare)

    def use(rows):
        held = joined(whole, rows)
        table = joined(both, rows)
        cosine = twice(table[:, 0:PAD])
        sine = twice(table[:, PAD : 2 * PAD])
        for which, dst in ((0, q), (1, k)):
            full = nt(held, w[which])
            put(proj.at[which], rows, full)
            turned = []
            for pair in range(full.shape[1] // (2 * PAD)):
                lanes = slice(pair * 2 * PAD, (pair + 1) * 2 * PAD)
                normal, _ = unit(full[:, lanes], ones[...], head)
                gained = normal * twice(gain[which : which + 1])
                turned.append(gained * cosine + two(nn, gained, turn[...]) * sine)
            put(dst, rows, jnp.concatenate(turned, axis=1))
        put(v, rows, nt(held, w[2]))

    gather(place, h, whole, (ssem, rsem), 0, use, lambda: arrive(load))


def mlp_kernel(layer, square, att, x, sel, mod, wo0, wo1, wg0, wg1, wd0, wd1, br1, x1, br2, y,
               whole_h, gate_h, up_h, hidden_h, whole, gate, up, hidden, h, wo, wg, wd, o1, i1, k1, s1, o2, i2, k2, s2,
               ssem, rsem, wsem, osem):
    x, mod = tokens_of(x), mod.at[layer]
    place = ring(square)
    rows_here, _ = x.shape
    load_o = head_weights(wo0, wo1, layer, wo, osem, range(1))
    load_g = layer_weights(wg0, wg1, layer, wg, wsem.at[1])
    load_d = layer_weights(wd0, wd1, layer, wd, wsem.at[2])
    greet(place)
    sems = (ssem, rsem)
    arrive(load_o)
    first = (o1, i1, k1, s1)
    scatter(place, lambda c: nn(att[chunk_rows(c, rows_here)], wo[...]), first, sems, 0)

    def between(rows):
        branch = scattered(first, rows)
        br1[rows] = branch
        mixed = x[rows].astype(F32) + mod_rows(sel[rows], mod, 2) * branch
        x1[rows] = mixed
        normal, _ = normed(mixed)
        shift = mod_rows(sel[rows], mod, 3)
        scale = mod_rows(sel[rows], mod, 4)
        h[rows] = (normal * (1.0 + scale) + shift).astype(BF)

    over_blocks(rows_here, between)

    def use(rows):
        held = joined(whole, rows)
        g = nn(held, wg[0])
        put(gate, rows, g)
        u = nn(held, wg[1])
        put(up, rows, u)
        put(hidden, rows, g * jax.nn.sigmoid(g) * u)

    second = (o2, i2, k2, s2)
    stores = []
    for n, (src, dst) in enumerate(
        ((whole, whole_h), (gate, gate_h), (up, up_h), (hidden, hidden_h))
    ):
        stores.append(pltpu.make_async_copy(src, dst, wsem.at[3 + n]))

    def ready():
        load_g.wait()
        load_d.wait()

    def fill():
        for copy in stores:
            copy.start()

    def term(chunk):
        return nn(hidden[chunk_rows(chunk, rows_here)], wd[...])

    gather_scatter(place, h, whole, sems, 6, use, term, second, ready, fill)

    def finish(rows):
        branch = scattered(second, rows)
        br2[rows] = branch
        y[rows] = (x1[rows] + mod_rows(sel[rows], mod, 5) * branch).astype(BF)

    over_blocks(rows_here, finish)
    arrive(stores)


def mlp_back_kernel(layer, square, dy, br2, br1, x1, sel, mod, gate_h, up_h, hidden_h, rows_h,
                    wo0, wo1, wg0, wg1, wd0, wd1, whole1, datt, dx1, dmod, total, mine, theirs,
                    got, h, h1, whole2, dgate, dup, gate, up, hidden, saved, flipped, wo, wg, wd, o1, i1, k1,
                    s1, ssem, rsem, wsem, osem):
    dy, mod = tokens_of(dy), mod.at[layer]
    place = ring(square)
    rows_here, _ = dy.shape
    load_d = layer_weights(wd0, wd1, layer, wd, wsem.at[0])
    load_gate = pltpu.make_async_copy(gate_h, gate, wsem.at[1])
    load_gate.start()
    load_up = pltpu.make_async_copy(up_h, up, wsem.at[2])
    load_up.start()
    load_g = layer_weights(wg0, wg1, layer, wg, wsem.at[3])
    load_o = head_weights(wo0, wo1, layer, wo, osem, range(1))
    load_hidden = pltpu.make_async_copy(hidden_h, hidden, wsem.at[5])
    load_hidden.start()
    load_rows = pltpu.make_async_copy(rows_h, saved, wsem.at[6])
    load_rows.start()
    greet(place, True)
    sems = (ssem, rsem)
    dmod[...] = jnp.zeros_like(dmod)

    def prepare(rows):
        incoming = dy[rows].astype(F32)
        h[rows] = (incoming * mod_rows(sel[rows], mod, 5)).astype(BF)
        add_sums(dmod, 3, sel[rows], incoming * br2[rows])

    over_blocks(rows_here, prepare)

    def ready():
        arrive((load_d, load_gate, load_up, load_g, load_hidden))

    def use(rows):
        d_hidden = nt(joined(whole2, rows), wd[...])
        g = joined(gate, rows)
        s = jax.nn.sigmoid(g)
        put(dgate, rows, d_hidden * joined(up, rows) * s * (1.0 + g * (1.0 - s)))
        put(dup, rows, d_hidden * g * s)

    bufs = (o1, i1, k1, s1)
    f = hidden.shape[1]

    def term(chunk):
        rows = chunk_rows(chunk, rows_here)
        return nt(dgate[rows], wg[0]) + nt(dup[rows], wg[1])

    packs = (mine, theirs, got)
    copies = []

    def grad(index, x, y, col):
        weight_grad(x, y, flipped, col, packs)
        copies.append(send_half(packs, sems, index, col, f))

    def grad_down():
        grad(18, whole2, hidden, 2 * f)

    gather_scatter(place, h, whole2, sems, 0, use, term, bufs, ready, grad_down)

    def between(rows):
        d_h = scattered(bufs, rows)
        normal, inverse = normed(x1[rows])
        scale = mod_rows(sel[rows], mod, 4)
        d_mixed = dy[rows].astype(F32) + norm_back(d_h * (1.0 + scale), normal, inverse)
        dx1[rows] = d_mixed
        h1[rows] = (d_mixed * mod_rows(sel[rows], mod, 2)).astype(BF)

    over_blocks(rows_here, between)

    def use_out(rows):
        put(datt, rows, nt(joined(whole1, rows), wo[...]))

    def sums():
        def one(rows):
            d_h = scattered(bufs, rows)
            normal, _ = normed(x1[rows])
            add_sums(dmod, 1, sel[rows], d_h)
            add_sums(dmod, 2, sel[rows], d_h * normal)
            add_sums(dmod, 0, sel[rows], dx1[rows] * br1[rows])

        over_blocks(rows_here, one)
        arrive(load_o)
        load_rows.wait()
        grad(19, saved, dgate, 0)

    def late():
        weight_grad(None, dup, flipped, f, packs)

    gather(place, h1, whole1, sems, 12, use_out, sums, late)
    copies.append(send_half(packs, sems, 20, f, f))
    add_halves(packs, copies[:1], total, 2 * f, f)
    add_halves(packs, copies[1:2], total, 0, f)
    add_halves(packs, copies[2:], total, f, f)


def qkv_back_kernel(layer, square, dq, dk, dv, proj, gain, both, turn, ones, spread, x, dx1, sel,
                    mod, part, prev, w_own, w_other, whole_h, att_h, rows1_h, du, du_b, dmod, total,
                    dgain, w, whole, att, rows1, flipped, dproj, flat, mine, theirs, got, o1, i1,
                    k1, s1, ssem, rsem, wsem, hsem):
    x, mod, gain = tokens_of(x), mod.at[layer], gain.at[layer]
    place = ring(square)
    rows_here, _ = x.shape
    packed = spread.shape[0]
    head = packed * PAD // spread.shape[1]
    load = head_weights(w_own, w_other, layer, w, hsem, range(3))
    loads = []
    for n, (src, dst) in enumerate(((whole_h, whole), (att_h, att), (rows1_h, rows1))):
        loads.append(pltpu.make_async_copy(src, dst, wsem.at[n]))
        loads[n].start()
    greet(place, True)
    here = dmod.at[layer]
    dmod[1 - layer] = prev[...]
    here[pl.ds(0, 4)] = jnp.zeros_like(prev[pl.ds(0, 4)])
    here[pl.ds(4, 8)] = part[...]
    dgain[...] = jnp.zeros_like(dgain)
    arrive(load)
    bufs = (o1, i1, k1, s1)
    sems = (ssem, rsem)
    packs = (mine, theirs, got)
    copies = []

    def term(chunk):
        rows = chunk_rows(chunk, rows_here)
        cosine = twice(both[rows, 0:PAD])
        sine = twice(both[rows, PAD : 2 * PAD])
        for which, src in ((0, dq), (1, dk)):
            for pair in range(src.shape[1] // (2 * PAD)):
                lanes = slice(pair * 2 * PAD, (pair + 1) * 2 * PAD)
                turned = src[rows, lanes]
                back = turned.astype(F32) * cosine - nn(turned, turn[...]) * sine
                normal, inverse = unit(proj[which, rows, lanes].astype(F32), ones[...], head)
                dgain[which, :, lanes] += jnp.sum(back * normal, axis=0, keepdims=True)
                gained = back * twice(gain[which : which + 1])
                mean = two(nn, gained * normal, ones[...]) * (1.0 / head)
                dproj[which, rows, lanes] = (inverse * (gained - normal * mean)).astype(BF)
        return nn(dproj[0, rows], w[0]) + nn(dproj[1, rows], w[1]) + nn(dv[rows], w[2])

    def grad_in():
        loads[0].wait()
        for k in range(3):
            flat[...] = nt(dproj[k] if k < 2 else dv[...], spread[...]).astype(BF)
            weight_grad(None if k else whole, flat, flipped, k * packed, packs)

    def grad_out():
        loads[1].wait()
        loads[2].wait()
        flat[...] = nt(att[...], spread[...]).astype(BF)
        weight_grad(rows1, flat, flipped, 3 * packed, packs)

    def grads():
        grad_in()
        grad_out()
        copies.append(send_half(packs, sems, 6, 0, 4 * packed))

    scatter(place, term, bufs, sems, 0, grads)

    def finish(rows):
        d_h = scattered(bufs, rows)
        normal, inverse = normed(x[rows].astype(F32))
        scale = mod_rows(sel[rows], mod, 1)
        total_rows = dx1[rows] + norm_back(d_h * (1.0 + scale), normal, inverse)
        du[rows] = total_rows
        du_b[rows] = total_rows.astype(BF)
        add_sums(here, 0, sel[rows], d_h)
        add_sums(here, 1, sel[rows], d_h * normal)

    over_blocks(rows_here, finish)
    add_halves(packs, copies, total, 0, 4 * packed)


def cell():
    return 4 * lax.axis_index(S) + lax.axis_index(T)


def cell_id(index):
    return {S: index // 4, T: index % 4}


def greet_all(dp):
    sem = pltpu.get_barrier_semaphore()
    here, shard = cell(), lax.axis_index(DP)
    for k in range(1, 8):
        pl.semaphore_signal(
            sem, inc=1, device_id=cell_id((here + k) % 8), device_id_type=pl.DeviceIdType.MESH
        )
    for k in range(1, dp):
        pl.semaphore_signal(
            sem, inc=1, device_id={DP: (shard + k) % dp}, device_id_type=pl.DeviceIdType.MESH
        )
    pl.semaphore_wait(sem, 7 + dp - 1)


def push(src, dst, sems, index, device):
    copy = pltpu.make_async_remote_copy(
        src_ref=src,
        dst_ref=dst,
        send_sem=sems[0].at[index],
        recv_sem=sems[1].at[index],
        device_id=device,
        device_id_type=pl.DeviceIdType.MESH,
    )
    copy.start()
    return copy


def head_kernel(dp, cond, ada_h, bias, gain_own, items, pos, tables, mod, lifted_all, gains, sel,
                both, spans, ada, parts, got, wide, tall, lifted, gain, ssem, rsem, wsem):
    load = pltpu.make_async_copy(ada_h, ada, wsem)
    load.start()
    lifted[...] = jnp.zeros_like(lifted)
    raw = cond[...].astype(F32)
    raw = (raw * jax.nn.sigmoid(raw)).astype(BF).astype(F32)
    lifted[0:3] = raw[0:3]
    lifted[8:11] = raw[3:6]
    gain[...] = jnp.zeros_like(gain)
    gain[0:2, 0 : gain_own.shape[1]] = gain_own[...].astype(F32)
    biases = bias[...].astype(F32)
    greet_all(dp)
    sems = (ssem, rsem)
    here, shard, section = cell(), lax.axis_index(DP), lax.axis_index(S)
    copies = [push(gain, gains.at[section], sems, 6 + dp, {S: 1 - section})]
    gains[section] = gain[...]
    lifted_all[shard] = lifted[...]
    for k in range(1, dp):
        copies.append(
            push(lifted, lifted_all.at[shard], sems, 6 + k, {DP: (shard + k) % dp})
        )
    load.wait()
    half = parts.shape[3]
    for micro in range(2):
        for j in range(3):
            rows = lifted[pl.ds(micro * 8, 8)].astype(BF)
            here_bias = biases[:, j * half : (j + 1) * half]
            parts[micro, j] = nt(rows, ada[pl.ds(j * half, half)]) + here_bias
    for k in range(1, 8):
        peer = (here + k) % 8
        copies.append(push(parts.at[peer // 4], got.at[here], sems, k - 1, cell_id(peer)))
    got[here] = parts[section]
    rows_here = sel.shape[0]
    base = shard * 6 + section * 3
    seq = items.shape[1]
    line = items[pl.ds(section, 1), :]
    wide[...] = jnp.zeros_like(wide)
    wide[0:1] = (line - base).astype(F32)
    wide[1:2] = pos[0, pl.ds(section, 1), :].astype(F32)
    wide[2:3] = pos[1, pl.ds(section, 1), :].astype(F32)
    start = 0
    spans[0] = 0
    for j in range(3):
        count = jnp.sum((wide[0:1] == j).astype(F32)).astype(jnp.int32)
        spans[4 + j] = count
        start = start + count
        spans[1 + j] = start
    spans[7] = 0
    tall[...] = wide[...].T
    own = tall[pl.ds(pl.multiple_of(lax.axis_index(T) * rows_here, rows_here), rows_here), :]
    lane = lax.broadcasted_iota(jnp.int32, (rows_here, 8), 1).astype(F32)
    sel[...] = ((own[:, 0:1] == lane) & (lane < 3.0)).astype(F32)
    lane = lax.broadcasted_iota(jnp.int32, (seq, 64), 1).astype(F32)
    hot = jnp.where(lane < 32.0, tall[:, 1:2], tall[:, 2:3] + 32.0) == lane
    hot = hot.astype(F32).astype(BF)
    both[...] = (nn(hot, tables[0]) + nn(hot, tables[1])) + nn(hot, tables[2])
    for copy in copies:
        copy.wait_recv()
    for layer in range(2):
        for block in range(6):
            for side in range(2):
                n = 2 * block + side
                mod[layer, block, :, pl.ds(side * half, half)] = got[4 * layer + n // 3, n % 3]
    for copy in copies:
        copy.wait_send()


def tail_kernel(dp, dmod, dgain, lifted_part, cond, ada_h, ada_grad, bias_grad, cond_grad, gain_grad,
                ada, bias_row, got, got_gain, total, total_gain, every, every_gain, lifts, ssem, rsem, wsem):
    load = pltpu.make_async_copy(ada_h, ada, wsem)
    load.start()
    greet_all(dp)
    sems = (ssem, rsem)
    here, shard = cell(), lax.axis_index(DP)
    section, place = lax.axis_index(S), lax.axis_index(T)
    sends, arrivals = [], []
    for k in range(1, 8):
        peer = (here + k) % 8
        to = cell_id(peer)
        arrivals.append(
            push(dmod.at[peer // 4, pl.ds(3 * (peer % 4), 3)], got.at[here], sems, k - 1, to)
        )
        arrivals.append(push(dgain.at[peer // 4], got_gain.at[here], sems, 6 + k, to))
    got[here] = dmod[section, pl.ds(3 * place, 3)]
    got_gain[here] = dgain[section]
    for copy in arrivals:
        copy.wait_recv()
    sends += arrivals
    for micro in range(2):
        total[micro] = (got[4 * micro] + got[4 * micro + 1]) + (got[4 * micro + 2] + got[4 * micro + 3])
    gain = got_gain[0]
    for k in range(1, 8):
        gain = gain + got_gain[k]
    total_gain[...] = gain
    arrivals = []
    for k in range(1, dp):
        to = {DP: (shard + k) % dp}
        arrivals.append(push(total, every.at[shard], sems, 13 + k, to))
        arrivals.append(push(total_gain, every_gain.at[shard], sems, 12 + dp + k, to))
    every[shard] = total[...]
    every_gain[shard] = total_gain[...]
    load.wait()
    half = total.shape[3]
    for micro in range(2):
        lift = two(nn, total[micro, 0], ada[pl.ds(0, half)])
        for j in range(1, 3):
            lift = lift + two(nn, total[micro, j], ada[pl.ds(j * half, half)])
        lifts[here, micro] = lift
    base = 13 + 2 * (dp - 1)
    lift_copies = []
    for k in range(1, 8):
        lift_copies.append(
            push(lifts.at[here], lifts.at[here], sems, base + k, cell_id((here + k) % 8))
        )
    for copy in arrivals:
        copy.wait_recv()
    sends += arrivals
    gain = every_gain[0]
    for k in range(1, dp):
        gain = gain + every_gain[k]
    heads = gain.shape[1] // PAD
    summed = gain[:, 0:PAD]
    for h in range(1, heads):
        summed = summed + gain[:, h * PAD : (h + 1) * PAD]
    gain_grad[...] = summed[0:2, 0 : gain_grad.shape[1]]
    for j in range(3):
        bias = jnp.zeros((1, half), F32)
        grad = jnp.zeros((lifted_part.shape[2], half), F32)
        for k in range(dp):
            for micro in range(2):
                block = every[k, micro, j]
                bias = bias + jnp.sum(block, axis=0, keepdims=True)
                high = block.astype(BF)
                low = (block - high.astype(F32)).astype(BF)
                rows = lifted_part[2 * k + micro].astype(BF)
                grad = grad + tn(rows, high) + tn(rows, low)
        bias_row[:, pl.ds(j * half, half)] = bias
        ada_grad[:, pl.ds(j * half, half)] = grad
    for copy in lift_copies:
        copy.wait_recv()
    sends += lift_copies
    lift = lifts[0]
    for k in range(1, 8):
        lift = lift + lifts[k]
    raw = cond[...].astype(F32)
    s = jax.nn.sigmoid(raw)
    factor = s * (1.0 + raw * (1.0 - s))
    cond_grad[0:3] = lift[0, 0:3] * factor[0:3]
    cond_grad[3:6] = lift[1, 0:3] * factor[3:6]
    part = bias_grad.shape[1]
    row = bias_row[...]
    total_bias = jnp.zeros((1, part), F32)
    for k in range(dp):
        chosen = (shard == k).astype(F32)
        total_bias = total_bias + row[:, k * part : (k + 1) * part] * chosen
    bias_grad[...] = total_bias
    for copy in sends:
        copy.wait_send()


def price(micros):
    return pl.CostEstimate(flops=0, bytes_accessed=int(micros * 3.5e6), transcendentals=0)


def ring_call(kernel, ident, micros, outs, scratch, args, spaces, scalar=-1, loose=99):
    return pl.pallas_call(
        kernel,
        out_shape=outs,
        in_specs=[vmem() if s else anywhere() for s in spaces],
        out_specs=[
            pl.BlockSpec(memory_space=pltpu.SMEM)
            if n == scalar
            else (vmem() if n < loose else anywhere())
            for n in range(len(outs))
        ],
        scratch_shapes=scratch,
        compiler_params=pltpu.CompilerParams(
            collective_id=ident, has_side_effects=True, vmem_limit_bytes=60 * 2**20
        ),
        cost_estimate=price(micros),
    )(*args)


def attention_kernel(head, spans, q, k, v, att):
    rows, wide = q.shape
    scale = head ** (-0.5)

    def each_head(fn):
        for n in range(wide // PAD):
            fn(slice(n * PAD, (n + 1) * PAD))

    def one_item(item, carry):
        at = pl.ds(pl.multiple_of(spans[item], 16), TILE)
        valid = lax.broadcasted_iota(jnp.int32, (TILE, TILE), 1) < spans[4 + item]

        def tile(lanes):
            att[at, lanes] = softmax_rows(q[at, lanes], k[at, lanes], v[at, lanes], valid, scale)

        each_head(tile)
        return carry

    lax.fori_loop(0, 3, one_item, 0)
    first = rows - 48
    start = spans[3]
    at = pl.ds(first, 48)
    valid = first + lax.broadcasted_iota(jnp.int32, (48, 48), 1) >= start
    live = first + lax.broadcasted_iota(jnp.int32, (48, PAD), 0) >= start

    def rest(lanes):
        new = softmax_rows(q[at, lanes], k[at, lanes], v[at, lanes], valid, scale)
        att[at, lanes] = jnp.where(live, new, att[at, lanes])

    each_head(rest)


def unit(proj, ones, head):
    inverse = lax.rsqrt(two(nn, proj * proj, ones) * (1.0 / head) + EPS)
    return proj * inverse, inverse


def softmax_rows(query, key, value, valid, scale):
    scores = jnp.where(valid, nt(query, key) * scale, -1e30)
    raised = jnp.exp(scores - jnp.max(scores, axis=1, keepdims=True))
    probs = raised / jnp.sum(raised, axis=1, keepdims=True)
    return nn(probs.astype(BF), value).astype(BF)


def back_tile(query, key, value, grad, keys, queries, scale):
    scores = jnp.where(keys, nt(key, query) * scale, -1e30)
    raised = jnp.exp(scores - jnp.max(scores, axis=0, keepdims=True))
    probs = jnp.where(queries, raised / jnp.sum(raised, axis=0, keepdims=True), 0.0)
    d_value = nn(probs.astype(BF), grad)
    d_probs = nt(value, grad)
    inner = jnp.sum(probs * d_probs, axis=0, keepdims=True)
    d_scores = (probs * (d_probs - inner)).astype(BF)
    return tn(d_scores, key) * scale, nn(d_scores, query) * scale, d_value


def attention_back_kernel(head, spans, q, k, v, grad, dq, dk, dv):
    rows, wide = q.shape
    scale = head ** (-0.5)

    def each_head(fn):
        for n in range(wide // PAD):
            fn(slice(n * PAD, (n + 1) * PAD))

    def one_item(item, carry):
        at = pl.ds(pl.multiple_of(spans[item], 16), TILE)
        keys = lax.broadcasted_iota(jnp.int32, (TILE, TILE), 0) < spans[4 + item]
        queries = lax.broadcasted_iota(jnp.int32, (TILE, TILE), 1) < spans[4 + item]

        def tile(lanes):
            parts = back_tile(
                q[at, lanes], k[at, lanes], v[at, lanes], grad[at, lanes], keys, queries, scale
            )
            for new, dst in zip(parts, (dq, dk, dv)):
                dst[at, lanes] = new.astype(BF)

        each_head(tile)
        return carry

    lax.fori_loop(0, 3, one_item, 0)
    first = rows - 48
    start = spans[3]
    at = pl.ds(first, 48)
    keys = first + lax.broadcasted_iota(jnp.int32, (48, 48), 0) >= start
    queries = first + lax.broadcasted_iota(jnp.int32, (48, 48), 1) >= start
    live = first + lax.broadcasted_iota(jnp.int32, (48, PAD), 0) >= start

    def rest(lanes):
        parts = back_tile(
            q[at, lanes], k[at, lanes], v[at, lanes], grad[at, lanes], keys, queries, scale
        )
        for new, dst in zip(parts, (dq, dk, dv)):
            dst[at, lanes] = jnp.where(live, new.astype(BF), dst[at, lanes])

    each_head(rest)


def local_call(kernel, micros, outs, scratch, spans, args):
    return pl.pallas_call(
        kernel,
        out_shape=outs,
        in_specs=[pl.BlockSpec(memory_space=pltpu.SMEM)] + [vmem()] * len(args),
        out_specs=[vmem()] * len(outs),
        scratch_shapes=scratch,
        compiler_params=pltpu.CompilerParams(vmem_limit_bytes=60 * 2**20),
        cost_estimate=price(micros),
    )(spans, *args)


def swap(array):
    return lax.ppermute(array, S, [(0, 1), (1, 0)])


def head_tables(packed, head):
    quarter = head // 4
    frequency = np.float32(10000.0) ** (-np.arange(quarter, dtype=np.float32) / quarter)
    lane = np.arange(head)
    angle = np.arange(32, dtype=np.float32)[:, None] * frequency[lane % quarter][None, :]
    by_row = (lane // (2 * quarter) == 0)[None, :]
    table = np.zeros((64, 2 * PAD), np.float32)
    for n, values in enumerate((np.cos(angle), np.sin(angle))):
        at = slice(n * PAD, n * PAD + head)
        table[:32, at] = np.where(by_row, values, 0.0)
        table[32:, at] = np.where(by_row, 0.0, values)
    table = jnp.asarray(table)
    parts = []
    for _ in range(3):
        parts.append(lax.reduce_precision(table, 8, 7).astype(BF))
        table = table - parts[-1].astype(F32)
    rows = np.arange(2 * PAD)[:, None]
    cols = np.arange(2 * PAD)[None, :]
    inside = (rows // PAD == cols // PAD) & (rows % PAD < head) & (cols % PAD < head)
    row, col = rows % PAD, cols % PAD
    early = (col % (2 * quarter)) < quarter
    turn = np.where(inside & early & (row == col + quarter), -1.0, 0.0)
    turn = turn + np.where(inside & ~early & (row == col - quarter), 1.0, 0.0)
    heads = packed // head
    rows = np.arange(packed)[:, None]
    wide = np.arange(heads * PAD)[None, :]
    spread = (rows // head == wide // PAD) & (rows % head == wide % PAD)
    lanes = tuple(jnp.asarray(m.astype(np.float32)).astype(BF) for m in (turn, inside, spread))
    return jnp.stack(parts), lanes


def reduced(total):
    return lax.psum_scatter(total, DP, scatter_dimension=0, tiled=True)[0]


def own_layer(section, pair):
    first = section == 0
    keep = jnp.where(first, pair[0], pair[1])
    got = swap(jnp.where(first, pair[1], pair[0]))
    return jnp.where(first, jnp.concatenate([keep, got]), jnp.concatenate([got, keep])).astype(F32)


def per_device(square, dp, tokens, cotangent, cond, patch_item, patch_pos, w_qkv, w_out, w_gate_up,
               w_down, qk_gain, ada_weight, ada_bias):
    section = lax.axis_index(S)
    first = section == 0
    rows, width = tokens.shape[1:]
    seq = patch_item.shape[1]
    items = cond.shape[0]
    head = qk_gain.shape[-1]
    packed = w_qkv.shape[-1]
    heads = packed // head
    hidden_here = w_down.shape[1]
    own = (jnp.swapaxes(w_qkv[0], 1, 2), w_out[0], w_gate_up[0], w_down[0])
    other = tuple(swap(w) for w in own)

    ada = ada_weight[0].T
    half = width // 2
    trig, (turn, ones, spread) = head_tables(packed, head)
    wide = heads * PAD
    mods, lifted_all, gains, sel, both, spans = ring_call(
        functools.partial(head_kernel, dp),
        8,
        12,
        [
            sds((2, 6, 8, width), F32),
            sds((dp, 16, width), F32),
            sds((2, 8, PAD), F32),
            sds((rows, 8), F32),
            sds((seq, 2 * PAD), F32),
            sds((8,), jnp.int32),
        ],
        [
            pltpu.VMEM((3 * half, width), BF),
            pltpu.VMEM((2, 3, 8, half), F32),
            pltpu.VMEM((8, 3, 8, half), F32),
            pltpu.VMEM((8, seq), F32),
            pltpu.VMEM((seq, 8), F32),
            pltpu.VMEM((16, width), F32),
            pltpu.VMEM((8, PAD), F32),
        ]
        + dma_sems(7 + dp)
        + [pltpu.SemaphoreType.DMA],
        (cond, ada, ada_bias, qk_gain[0], patch_item, patch_pos, trig),
        (1, 0, 1, 1, 1, 1, 1),
        scalar=5,
    )
    part = width // dp
    shard = lax.axis_index(DP)
    lifted_part = lax.dynamic_slice_in_dim(lifted_all, shard * part, part, 2)
    lifted_part = lifted_part.reshape(2 * dp, 8, part)

    x = tokens
    kept = []
    for layer in range(2):
        mod = mods
        whole1, proj, q, k, v = ring_call(
            functools.partial(qkv_kernel, layer, square),
            layer,
            20,
            [sds((seq, width), BF), sds((2, seq, wide), BF)] + [sds((seq, wide), BF)] * 3,
            [pltpu.VMEM((rows, width), BF), pltpu.VMEM((3, wide, width), BF)]
            + dma_sems(6)
            + [pltpu.SemaphoreType.DMA((3 * heads,))],
            (x, sel, mod, gains, both, turn, ones, own[0], other[0]),
            (1,) * 7 + (0, 0),
        )
        (att,) = local_call(
            functools.partial(attention_kernel, head),
            6,
            [sds((seq, wide), BF)],
            [],
            spans,
            (q, k, v),
        )
        br1, x1, br2, y, whole2, gate, up, hidden = ring_call(
            functools.partial(mlp_kernel, layer, square),
            2 + layer,
            48,
            [
                sds((rows, width), F32),
                sds((rows, width), F32),
                sds((rows, width), F32),
                sds((rows, width), BF),
                sds((seq, width), BF),
                sds((seq, hidden_here), F32),
                sds((seq, hidden_here), F32),
                sds((seq, hidden_here), BF),
            ],
            [
                pltpu.VMEM((seq, width), BF),
                pltpu.VMEM((seq, hidden_here), F32),
                pltpu.VMEM((seq, hidden_here), F32),
                pltpu.VMEM((seq, hidden_here), BF),
                pltpu.VMEM((rows, width), BF),
                pltpu.VMEM((wide, width), BF),
                pltpu.VMEM((2, width, hidden_here), BF),
                pltpu.VMEM((hidden_here, width), BF),
            ]
            + scatter_scratch(rows, width)
            + scatter_scratch(rows, width)
            + dma_sems(18)
            + [pltpu.SemaphoreType.DMA((7,)), pltpu.SemaphoreType.DMA((heads,))],
            (att, x, sel, mod, own[1], other[1], own[2], other[2], own[3], other[3]),
            (1, 1, 1, 1) + (0,) * 6,
            loose=4,
        )
        kept.append((x, whole1, proj, q, k, v, att, br1, x1, whole2, gate, up, hidden, br2, y))
        x = y

    dy = cotangent
    packs = [None, None]
    prev = jnp.zeros((12, 8, half), F32)
    d_gains = [None, None]
    d_inputs = [None, None]
    for layer in (1, 0):
        x, whole1, proj, q, k, v, att, br1, x1, whole2, gate, up, hidden, br2, y = kept[layer]
        mod = mods
        rows1, datt, dx1, dmod_a, total_mlp = ring_call(
            functools.partial(mlp_back_kernel, layer, square),
            4 + layer,
            52,
            [
                sds((seq, width), BF),
                sds((seq, wide), BF),
                sds((rows, width), F32),
                sds((8, 8, half), F32),
                sds((dp, part // 2, 3 * hidden_here), BF),
            ],
            [pltpu.VMEM((dp, part // 2, 3 * hidden_here), BF)] * 3
            + [
                pltpu.VMEM((rows, width), BF),
                pltpu.VMEM((rows, width), BF),
                pltpu.VMEM((seq, width), BF),
                pltpu.VMEM((seq, hidden_here), BF),
                pltpu.VMEM((seq, hidden_here), BF),
                pltpu.VMEM((seq, hidden_here), F32),
                pltpu.VMEM((seq, hidden_here), F32),
                pltpu.VMEM((seq, hidden_here), BF),
                pltpu.VMEM((seq, width), BF),
                pltpu.VMEM((width, seq), BF),
                pltpu.VMEM((wide, width), BF),
                pltpu.VMEM((2, width, hidden_here), BF),
                pltpu.VMEM((hidden_here, width), BF),
            ]
            + scatter_scratch(rows, width)
            + dma_sems(21)
            + [pltpu.SemaphoreType.DMA((7,)), pltpu.SemaphoreType.DMA((heads,))],
            (dy, br2, br1, x1, sel, mod, gate, up, hidden, whole2, own[1], other[1], own[2],
             other[2], own[3], other[3]),
            (1,) * 6 + (0,) * 10,
        )
        pack_mlp = reduced(total_mlp)
        dq, dk, dv = local_call(
            functools.partial(attention_back_kernel, head),
            10,
            [sds((seq, wide), BF)] * 3,
            [],
            spans,
            (q, k, v, datt),
        )
        du, du_b, d_mod, total_att, dgain = ring_call(
            functools.partial(qkv_back_kernel, layer, square),
            6 + layer,
            22,
            [
                sds((rows, width), F32),
                sds((rows, width), BF),
                sds((2, 12, 8, half), F32),
                sds((dp, part // 2, 4 * packed), BF),
                sds((2, 1, wide), F32),
            ],
            [
                pltpu.VMEM((3, wide, width), BF),
                pltpu.VMEM((seq, width), BF),
                pltpu.VMEM((seq, wide), BF),
                pltpu.VMEM((seq, width), BF),
                pltpu.VMEM((width, seq), BF),
                pltpu.VMEM((2, seq, wide), BF),
                pltpu.VMEM((seq, packed), BF),
            ]
            + [pltpu.VMEM((dp, part // 2, 4 * packed), BF)] * 3
            + scatter_scratch(rows, width)
            + dma_sems(7)
            + [pltpu.SemaphoreType.DMA((3,)), pltpu.SemaphoreType.DMA((3 * heads,))],
            (dq, dk, dv, proj, gains, both, turn, ones, spread, x, dx1, sel, mod, dmod_a,
             prev, own[0], other[0], whole1, att, rows1),
            (1,) * 15 + (0,) * 5,
        )
        prev = d_mod[1]
        pack_att = reduced(total_att)
        packs[layer] = (pack_mlp, pack_att)
        d_gains[layer] = dgain
        d_inputs[layer] = du_b if layer else du
        dy = du_b

    gain_parts = jnp.pad(jnp.stack(d_gains).reshape(2, 2, wide), ((0, 0), (0, 6), (0, 0)))
    bias_part = ada_bias.shape[1] // dp
    g_ada_w, g_ada_b, cond_grad, gain_total = ring_call(
        functools.partial(tail_kernel, dp),
        9,
        15,
        [
            sds((part, 3 * half), F32),
            sds((1, bias_part), F32),
            sds((items, width), F32),
            sds((2, head), F32),
        ],
        [
            pltpu.VMEM((3 * half, width), BF),
            pltpu.VMEM((1, 3 * half), F32),
            pltpu.VMEM((8, 3, 8, half), F32),
            pltpu.VMEM((8, 8, wide), F32),
            pltpu.VMEM((2, 3, 8, half), F32),
            pltpu.VMEM((8, wide), F32),
            pltpu.VMEM((dp, 2, 3, 8, half), F32),
            pltpu.VMEM((dp, 8, wide), F32),
            pltpu.VMEM((8, 2, 8, width), F32),
        ]
        + dma_sems(13 + 2 * (dp - 1) + 8)
        + [pltpu.SemaphoreType.DMA],
        (d_mod, gain_parts, lifted_part, cond, ada),
        (1, 1, 1, 1, 0),
    )

    mlp = own_layer(section, (packs[0][0], packs[1][0]))
    attn = own_layer(section, (packs[0][1], packs[1][1]))
    f = hidden_here
    g_gate_up = jnp.stack([mlp[:, :f], mlp[:, f : 2 * f]])[None]
    g_down = mlp[:, 2 * f :].T[None]
    g_qkv = jnp.stack([attn[:, k * packed : (k + 1) * packed] for k in range(3)])[None]
    g_out = attn[:, 3 * packed :].T[None]

    outs = jnp.where(first, kept[0][-1], kept[1][-1])
    outs_got = swap(jnp.where(first, kept[1][-1], kept[0][-1]))
    layer_out = jnp.where(first, jnp.stack([outs, outs_got]), jnp.stack([outs_got, outs]))
    wide_mid = d_inputs[1].astype(F32)
    back_keep = jnp.where(first, d_inputs[0], wide_mid)
    back_got = swap(jnp.where(first, wide_mid, d_inputs[0]))
    in_grads = jnp.where(first, jnp.stack([back_keep, back_got]), jnp.stack([back_got, back_keep]))
    return (
        layer_out[None],
        in_grads[None],
        cond_grad,
        g_qkv,
        g_out,
        g_gate_up,
        g_down,
        gain_total[None],
        g_ada_w[None],
        g_ada_b,
    )


def solution(mesh):
    both = (DP, T)
    in_specs = (
        P(None, both, None),
        P(None, both, None),
        P(DP, None),
        P(None, DP),
        P(None, None, DP),
        P(S, None, None, T),
        P(S, T, None),
        P(S, None, None, T),
        P(S, T, None),
        P(S, None, None),
        P(S, None, T),
        P(S, T),
    )
    out_specs = (
        P(S, None, both, None),
        P(S, None, both, None),
        P(DP, None),
        P(S, None, DP, T),
        P(S, T, DP),
        P(S, None, DP, T),
        P(S, T, DP),
        P(S, None, None),
        P(S, DP, T),
        P(S, (T, DP)),
    )
    dp = mesh.shape[DP]

    def program(*args):
        return per_device(dp <= 4, dp, *args)

    return jax.shard_map(
        program, mesh=mesh, in_specs=in_specs, out_specs=out_specs, check_vma=False
    )
```

```python
import functools

import jax
import jax.numpy as jnp
import numpy as np
from jax import lax
from jax.experimental import pallas as pl
from jax.experimental.pallas import tpu as pltpu
from jax.sharding import PartitionSpec as P


EPS = 1e-06
F32 = jnp.float32
BF = jnp.bfloat16
S, DP, T = "section", "dp", "tensor"
PAD = 128
TILE = 256


def nn(a, b):
    return jnp.dot(a, b, preferred_element_type=F32)


def nt(a, b):
    return lax.dot_general(a, b, (((1,), (1,)), ((), ())), preferred_element_type=F32)


def tn(a, b):
    return lax.dot_general(a, b, (((0,), (0,)), ((), ())), preferred_element_type=F32)


def two(dot, a, b):
    high = a.astype(BF)
    low = (a - high.astype(F32)).astype(BF)
    return dot(high, b) + dot(low, b)


def sds(shape, dtype):
    return jax.ShapeDtypeStruct(shape, dtype)


def vmem():
    return pl.BlockSpec(memory_space=pltpu.VMEM)


def anywhere():
    return pl.BlockSpec(memory_space=pl.ANY)


def ring(square):
    me = lax.axis_index(T)
    near = me + 1 - 2 * (me % 2)
    if square:
        return me, near, me + 2 - 4 * (me // 2), 3 - me, True
    return me, near, 3 - me, (me + 2) % 4, False


def pieces(place, step, half):
    me, upper, moved, far = place[0], (step % 3) // 2, (step + 2) // 3, step // 3
    near = moved - far
    low = (moved, far) if place[4] else (near, near)
    found = []
    for side, high in ((0, far), (1, moved)):
        chunk = (me % 2 + low[side]) % 2 + 2 * ((me // 2 + high) % 2)
        row = (2 * chunk + (1 - upper if side else upper)) * half
        found.append(pl.ds(pl.multiple_of(row, half), half))
    return found


def joined(ref, rows):
    return jnp.concatenate([ref[rows[0]], ref[rows[1]]], axis=0)


def put(ref, rows, values):
    half = values.shape[0] // 2
    ref[rows[0]] = values[:half].astype(ref.dtype)
    ref[rows[1]] = values[half:].astype(ref.dtype)


def farthest_first(place, step):
    me, low = place[0], ((step + 1) // 2) % 2
    if place[4]:
        low = (3 - step) // 2
    return (me % 2 + low) % 2 + 2 * ((me // 2 + (step + 1) % 2) % 2)


def near_first(place, step):
    me, low = place[0], (3 - step) // 2
    if place[4]:
        low = (step + 1) % 2
    return (me % 2 + low) % 2 + 2 * ((me // 2 + ((step + 1) // 2) % 2) % 2)


def greet(place, partner=False):
    sem = pltpu.get_barrier_semaphore()
    peers = (place[1], place[2]) if place else ()
    for peer in peers:
        pl.semaphore_signal(
            sem, inc=1, device_id={T: peer}, device_id_type=pl.DeviceIdType.MESH
        )
    if partner:
        pl.semaphore_signal(
            sem, inc=1, device_id={S: 1 - lax.axis_index(S)}, device_id_type=pl.DeviceIdType.MESH
        )
    pl.semaphore_wait(sem, len(peers) + partner)


def remote(src, dst, sems, index, peer):
    return pltpu.make_async_remote_copy(
        src_ref=src,
        dst_ref=dst,
        send_sem=sems[0].at[index],
        recv_sem=sems[1].at[index],
        device_id={T: peer},
        device_id_type=pl.DeviceIdType.MESH,
    )


def chunk_rows(chunk, rows):
    return pl.ds(pl.multiple_of(chunk * rows, rows), rows)


def repeat(body, times):
    def one(step, carry):
        body(step)
        return carry

    lax.fori_loop(0, times, one, 0)


def gather(place, mine, whole, sems, base, use, ready=lambda: None, late=lambda: None, last=None):
    me, a, b, _, _ = place
    rows = mine.shape[0]
    half = rows // 2
    lo, hi = pl.ds(0, half), pl.ds(half, half)

    def part(chunk, upper):
        return whole.at[pl.ds(pl.multiple_of(chunk * rows + upper * half, half), half)]

    a0 = remote(mine.at[lo], part(me, 0), sems, base, a)
    b0 = remote(mine.at[hi], part(me, 1), sems, base + 1, b)
    a1 = remote(mine.at[hi], part(me, 1), sems, base + 2, a)
    b1 = remote(mine.at[lo], part(me, 0), sems, base + 3, b)
    b2 = remote(part(a, 0), part(a, 0), sems, base + 4, b)
    a2 = remote(part(b, 1), part(b, 1), sems, base + 5, a)
    for copy in (a0, b0, a1, b1):
        copy.start()
    whole[chunk_rows(me, rows), :] = mine[...]
    ready()

    def final():
        b2.wait_recv()
        a2.wait_recv()

    def body(step):
        @pl.when(step == 1)
        def _():
            a0.wait_recv()
            b2.start()
            b0.wait_recv()
            a2.start()

        @pl.when(step == 2)
        def _():
            a1.wait_recv()
            b1.wait_recv()

        if last is None:

            @pl.when(step == 3)
            def _():
                late()
                final()

        use(pieces(place, step, half))

    repeat(body, 4 if last is None else 3)
    if last is not None:
        last(final)
    for copy in (a0, b0, a1, b1, a2, b2):
        copy.wait_send()


def scatter(place, term, bufs, sems, base, fill=lambda: None, before=None):
    _, a, b, _, _ = place
    out, into, keep, own = bufs
    half = keep.shape[1]
    lo, hi = pl.ds(0, half), pl.ds(half, half)
    d0 = remote(out.at[0, lo], into.at[0, lo], sems, base, a)
    d1 = remote(out.at[0, hi], into.at[0, hi], sems, base + 1, b)
    a0 = remote(out.at[1, lo], into.at[1, lo], sems, base + 2, a)
    b0 = remote(out.at[2, hi], into.at[2, hi], sems, base + 3, b)
    a1 = remote(out.at[1, hi], into.at[1, hi], sems, base + 4, a)
    b1 = remote(out.at[2, lo], into.at[2, lo], sems, base + 5, b)
    at = (0, 1, 2) if before is None else (2, 0, 1)

    def body(step):
        if before is None:
            chunk = farthest_first(place, step)
        else:
            chunk = near_first(place, step)
            pl.when(step == 2)(before)
        own[...] = term(chunk)

        @pl.when(step == at[0])
        def _():
            out[0] = own[...].astype(BF)
            d0.start()
            d1.start()

        @pl.when(step == at[1])
        def _():
            out[1, lo] = own[lo].astype(BF)
            a0.start()
            keep[0] = own[hi]

        @pl.when(step == at[2])
        def _():
            out[2, hi] = own[hi].astype(BF)
            b0.start()
            keep[1] = own[lo]

    repeat(body, 4)
    d1.wait_recv()
    out[1, hi] = (keep[0] + into[0, hi].astype(F32)).astype(BF)
    a1.start()
    d0.wait_recv()
    out[2, lo] = (keep[1] + into[0, lo].astype(F32)).astype(BF)
    b1.start()
    fill()
    for copy in (a0, b0, a1, b1):
        copy.wait_recv()
    for copy in (d0, d1, a0, b0, a1, b1):
        copy.wait_send()


def gather_scatter(place, mine, whole, sems, base, use, term, bufs, ready, fill=lambda: None):
    def last(final):
        def before():
            final()
            use(pieces(place, 3, mine.shape[0] // 2))

        scatter(place, term, bufs, sems, base + 6, fill, before)

    gather(place, mine, whole, sems, base, use, ready, last=last)


def scattered(bufs, rows):
    return bufs[3][rows] + bufs[1][1, rows].astype(F32) + bufs[1][2, rows].astype(F32)


def scatter_scratch(rows, width):
    return [
        pltpu.VMEM((3, rows, width), BF),
        pltpu.VMEM((3, rows, width), BF),
        pltpu.VMEM((2, rows // 2, width), F32),
        pltpu.VMEM((rows, width), F32),
    ]


def dma_sems(count):
    return [pltpu.SemaphoreType.DMA((count,)), pltpu.SemaphoreType.DMA((count,))]


def layer_weights(own, other, layer, dst, sem):
    mine = lax.axis_index(S) == layer

    @pl.when(mine)
    def _():
        pltpu.make_async_copy(own, dst, sem).start()

    @pl.when(jnp.logical_not(mine))
    def _():
        pltpu.make_async_copy(other, dst, sem).start()

    return pltpu.make_async_copy(own, dst, sem)


def head_weights(own, other, layer, dst, sems, parts):
    mine = lax.axis_index(S) == layer
    spread = len(parts) > 1
    heads = dst.shape[-2] // PAD
    head = own.shape[-2] // heads
    clean = head // 16 * 16
    copies = ([], [])
    for n, part in enumerate(parts):
        for h in range(heads):
            to = dst.at[part] if spread else dst
            to[pl.ds(h * PAD + clean, PAD - clean)] = jnp.zeros((PAD - clean, dst.shape[-1]), BF)
            to = to.at[pl.ds(h * PAD, head)]
            for which, src in enumerate((own, other)):
                src = src.at[part] if spread else src
                copies[which].append(
                    pltpu.make_async_copy(
                        src.at[pl.ds(h * head, head)], to, sems.at[n * heads + h]
                    )
                )

    @pl.when(mine)
    def _():
        for copy in copies[0]:
            copy.start()

    @pl.when(jnp.logical_not(mine))
    def _():
        for copy in copies[1]:
            copy.start()

    return copies[0]


def arrive(copies):
    for copy in copies:
        copy.wait()


def twice(row):
    return jnp.concatenate([row, row], axis=-1)


def over_blocks(rows, fn):
    step = rows // 4

    def body(i, carry):
        fn(pl.ds(pl.multiple_of(i * step, step), step))
        return carry

    lax.fori_loop(0, 4, body, 0)


def mod_rows(sel, mod, which):
    total = sel[:, 0:1] * mod[which, 0:1]
    for item in (1, 2):
        total = total + sel[:, item : item + 1] * mod[which, item : item + 1]
    return total


def add_sums(dmod, block, sel, values):
    sums = item_sums(sel, values)
    half = dmod.shape[2]
    dmod[2 * block] += sums[:, :half]
    dmod[2 * block + 1] += sums[:, half:]


def weight_grad(x, y, flipped, col, packs):
    mine, theirs, _ = packs
    dp, part, _ = mine.shape
    first = lax.axis_index(S) == 0
    width = y.shape[1]
    if x is not None:
        flipped[...] = x[...].T

    def one(to, columns):
        grad = nn(flipped[...], columns).astype(BF)
        grad = grad.reshape(dp, 2, part, columns.shape[1])

        @pl.when(first)
        def _():
            mine[:, :, to] = grad[:, 0]
            theirs[:, :, to] = grad[:, 1]

        @pl.when(jnp.logical_not(first))
        def _():
            mine[:, :, to] = grad[:, 1]
            theirs[:, :, to] = grad[:, 0]

    if width % 256:
        one(pl.ds(col, width), y[...])
        return

    def body(i, carry):
        at = pl.multiple_of(i * 256, 256)
        one(pl.ds(pl.multiple_of(col + at, 256), 256), y[:, pl.ds(at, 256)])
        return carry

    lax.fori_loop(0, width // 256, body, 0)


def send_half(packs, sems, index, col, width):
    at = pl.ds(col, width)
    return push(
        packs[1].at[:, :, at], packs[2].at[:, :, at], sems, index, {S: 1 - lax.axis_index(S)}
    )


def add_halves(packs, copies, total, col, width):
    at = pl.ds(col, width)
    for copy in copies:
        copy.wait_recv()

    def body(k):
        total[k, :, at] = (packs[0][k, :, at].astype(F32) + packs[2][k, :, at].astype(F32)).astype(BF)

    repeat(body, total.shape[0])
    for copy in copies:
        copy.wait_send()


def item_sums(sel, values):
    high = values.astype(BF)
    low = (values - high.astype(F32)).astype(BF)
    sel_b = sel.astype(BF)
    return tn(sel_b, high) + tn(sel_b, low)


def normed(values):
    inverse = lax.rsqrt(jnp.mean(values * values, axis=-1, keepdims=True) + EPS)
    return values * inverse, inverse


def norm_back(incoming, normal, inverse):
    return inverse * (incoming - normal * jnp.mean(incoming * normal, axis=-1, keepdims=True))


def tokens_of(ref):
    return ref.at[lax.axis_index(S)] if len(ref.shape) == 3 else ref


def qkv_kernel(layer, square, x, sel, mod, gain, both, turn, ones, w_own, w_other, whole, proj, q,
               k, v, h, w, ssem, rsem, wsem):
    x, mod, gain = tokens_of(x), mod.at[layer], gain.at[layer]
    place = ring(square)
    head = w_own.shape[1] * PAD // w.shape[1]
    load = head_weights(w_own, w_other, layer, w, wsem, range(3))
    greet(place)

    def prepare(rows):
        normal, _ = normed(x[rows].astype(F32))
        shift = mod_rows(sel[rows], mod, 0)
        scale = mod_rows(sel[rows], mod, 1)
        h[rows] = (normal * (1.0 + scale) + shift).astype(BF)

    over_blocks(x.shape[0], prepare)

    def use(rows):
        held = joined(whole, rows)
        table = joined(both, rows)
        cosine = twice(table[:, 0:PAD])
        sine = twice(table[:, PAD : 2 * PAD])
        for which, dst in ((0, q), (1, k)):
            full = nt(held, w[which])
            put(proj.at[which], rows, full)
            turned = []
            for pair in range(full.shape[1] // (2 * PAD)):
                lanes = slice(pair * 2 * PAD, (pair + 1) * 2 * PAD)
                normal, _ = unit(full[:, lanes], ones[...], head)
                gained = normal * twice(gain[which : which + 1])
                turned.append(gained * cosine + two(nn, gained, turn[...]) * sine)
            put(dst, rows, jnp.concatenate(turned, axis=1))
        put(v, rows, nt(held, w[2]))

    gather(place, h, whole, (ssem, rsem), 0, use, lambda: arrive(load))


def mlp_kernel(layer, square, att, x, sel, mod, wo0, wo1, wg0, wg1, wd0, wd1, br1, x1, br2, y,
               whole_h, gate_h, up_h, hidden_h, whole, gate, up, hidden, h, wo, wg, wd, o1, i1, k1, s1, o2, i2, k2, s2,
               ssem, rsem, wsem, osem):
    x, mod = tokens_of(x), mod.at[layer]
    place = ring(square)
    rows_here, _ = x.shape
    load_o = head_weights(wo0, wo1, layer, wo, osem, range(1))
    load_g = layer_weights(wg0, wg1, layer, wg, wsem.at[1])
    load_d = layer_weights(wd0, wd1, layer, wd, wsem.at[2])
    greet(place)
    sems = (ssem, rsem)
    arrive(load_o)
    first = (o1, i1, k1, s1)
    scatter(place, lambda c: nn(att[chunk_rows(c, rows_here)], wo[...]), first, sems, 0)

    def between(rows):
        branch = scattered(first, rows)
        br1[rows] = branch
        mixed = x[rows].astype(F32) + mod_rows(sel[rows], mod, 2) * branch
        x1[rows] = mixed
        normal, _ = normed(mixed)
        shift = mod_rows(sel[rows], mod, 3)
        scale = mod_rows(sel[rows], mod, 4)
        h[rows] = (normal * (1.0 + scale) + shift).astype(BF)

    over_blocks(rows_here, between)

    def use(rows):
        held = joined(whole, rows)
        g = nn(held, wg[0])
        put(gate, rows, g)
        u = nn(held, wg[1])
        put(up, rows, u)
        put(hidden, rows, g * jax.nn.sigmoid(g) * u)

    second = (o2, i2, k2, s2)
    stores = []
    for n, (src, dst) in enumerate(
        ((whole, whole_h), (gate, gate_h), (up, up_h), (hidden, hidden_h))
    ):
        stores.append(pltpu.make_async_copy(src, dst, wsem.at[3 + n]))

    def ready():
        load_g.wait()
        load_d.wait()

    def fill():
        for copy in stores:
            copy.start()

    def term(chunk):
        return nn(hidden[chunk_rows(chunk, rows_here)], wd[...])

    gather_scatter(place, h, whole, sems, 6, use, term, second, ready, fill)

    def finish(rows):
        branch = scattered(second, rows)
        br2[rows] = branch
        y[rows] = (x1[rows] + mod_rows(sel[rows], mod, 5) * branch).astype(BF)

    over_blocks(rows_here, finish)
    arrive(stores)


def mlp_back_kernel(layer, square, dy, br2, br1, x1, sel, mod, gate_h, up_h, hidden_h, rows_h,
                    wo0, wo1, wg0, wg1, wd0, wd1, whole1, datt, dx1, dmod, total, mine, theirs,
                    got, h, h1, whole2, dgate, dup, gate, up, hidden, saved, flipped, wo, wg, wd, o1, i1, k1,
                    s1, ssem, rsem, wsem, osem):
    dy, mod = tokens_of(dy), mod.at[layer]
    place = ring(square)
    rows_here, _ = dy.shape
    load_d = layer_weights(wd0, wd1, layer, wd, wsem.at[0])
    load_gate = pltpu.make_async_copy(gate_h, gate, wsem.at[1])
    load_gate.start()
    load_up = pltpu.make_async_copy(up_h, up, wsem.at[2])
    load_up.start()
    load_g = layer_weights(wg0, wg1, layer, wg, wsem.at[3])
    load_o = head_weights(wo0, wo1, layer, wo, osem, range(1))
    load_hidden = pltpu.make_async_copy(hidden_h, hidden, wsem.at[5])
    load_hidden.start()
    load_rows = pltpu.make_async_copy(rows_h, saved, wsem.at[6])
    load_rows.start()
    greet(place, True)
    sems = (ssem, rsem)
    dmod[...] = jnp.zeros_like(dmod)

    def prepare(rows):
        incoming = dy[rows].astype(F32)
        h[rows] = (incoming * mod_rows(sel[rows], mod, 5)).astype(BF)
        add_sums(dmod, 3, sel[rows], incoming * br2[rows])

    over_blocks(rows_here, prepare)

    def ready():
        arrive((load_d, load_gate, load_up, load_g, load_hidden))

    def use(rows):
        d_hidden = nt(joined(whole2, rows), wd[...])
        g = joined(gate, rows)
        s = jax.nn.sigmoid(g)
        put(dgate, rows, d_hidden * joined(up, rows) * s * (1.0 + g * (1.0 - s)))
        put(dup, rows, d_hidden * g * s)

    bufs = (o1, i1, k1, s1)
    f = hidden.shape[1]

    def term(chunk):
        rows = chunk_rows(chunk, rows_here)
        return nt(dgate[rows], wg[0]) + nt(dup[rows], wg[1])

    packs = (mine, theirs, got)
    copies = []

    def grad(index, x, y, col):
        weight_grad(x, y, flipped, col, packs)
        copies.append(send_half(packs, sems, index, col, f))

    def grad_down():
        grad(18, whole2, hidden, 2 * f)

    gather_scatter(place, h, whole2, sems, 0, use, term, bufs, ready, grad_down)

    def between(rows):
        d_h = scattered(bufs, rows)
        normal, inverse = normed(x1[rows])
        scale = mod_rows(sel[rows], mod, 4)
        d_mixed = dy[rows].astype(F32) + norm_back(d_h * (1.0 + scale), normal, inverse)
        dx1[rows] = d_mixed
        h1[rows] = (d_mixed * mod_rows(sel[rows], mod, 2)).astype(BF)

    over_blocks(rows_here, between)

    def use_out(rows):
        put(datt, rows, nt(joined(whole1, rows), wo[...]))

    def sums():
        def one(rows):
            d_h = scattered(bufs, rows)
            normal, _ = normed(x1[rows])
            add_sums(dmod, 1, sel[rows], d_h)
            add_sums(dmod, 2, sel[rows], d_h * normal)
            add_sums(dmod, 0, sel[rows], dx1[rows] * br1[rows])

        over_blocks(rows_here, one)
        arrive(load_o)
        load_rows.wait()
        grad(19, saved, dgate, 0)

    def late():
        weight_grad(None, dup, flipped, f, packs)

    gather(place, h1, whole1, sems, 12, use_out, sums, late)
    copies.append(send_half(packs, sems, 20, f, f))
    add_halves(packs, copies[:1], total, 2 * f, f)
    add_halves(packs, copies[1:2], total, 0, f)
    add_halves(packs, copies[2:], total, f, f)


def qkv_back_kernel(layer, square, dq, dk, dv, proj, gain, both, turn, ones, spread, x, dx1, sel,
                    mod, part, prev, w_own, w_other, whole_h, att_h, rows1_h, du, du_b, dmod, total,
                    dgain, w, whole, att, rows1, flipped, dpack, flat, mine, theirs, got, o1, i1,
                    k1, s1, ssem, rsem, wsem):
    x, mod, gain = tokens_of(x), mod.at[layer], gain.at[layer]
    place = ring(square)
    rows_here, _ = x.shape
    packed = spread.shape[0]
    head = packed * PAD // spread.shape[1]
    load = layer_weights(w_own, w_other, layer, w, wsem.at[3])
    loads = []
    for n, (src, dst) in enumerate(((whole_h, whole), (att_h, att), (rows1_h, rows1))):
        loads.append(pltpu.make_async_copy(src, dst, wsem.at[n]))
        loads[n].start()
    greet(place, True)
    here = dmod.at[layer]
    dmod[1 - layer] = prev[...]
    here[pl.ds(0, 4)] = jnp.zeros_like(prev[pl.ds(0, 4)])
    here[pl.ds(4, 8)] = part[...]
    dgain[...] = jnp.zeros_like(dgain)
    load.wait()
    bufs = (o1, i1, k1, s1)
    sems = (ssem, rsem)
    packs = (mine, theirs, got)
    copies = []

    def term(chunk):
        rows = chunk_rows(chunk, rows_here)
        cosine = twice(both[rows, 0:PAD])
        sine = twice(both[rows, PAD : 2 * PAD])
        for which, src in ((0, dq), (1, dk)):
            parts = []
            for pair in range(src.shape[1] // (2 * PAD)):
                lanes = slice(pair * 2 * PAD, (pair + 1) * 2 * PAD)
                turned = src[rows, lanes]
                back = turned.astype(F32) * cosine - nn(turned, turn[...]) * sine
                normal, inverse = unit(proj[which, rows, lanes].astype(F32), ones[...], head)
                dgain[which, :, lanes] += jnp.sum(back * normal, axis=0, keepdims=True)
                gained = back * twice(gain[which : which + 1])
                mean = two(nn, gained * normal, ones[...]) * (1.0 / head)
                parts.append((inverse * (gained - normal * mean)).astype(BF))
            full = jnp.concatenate(parts, axis=1)
            dpack[rows, which * packed : (which + 1) * packed] = nt(full, spread[...]).astype(BF)
        dpack[rows, 2 * packed : 3 * packed] = nt(dv[rows], spread[...]).astype(BF)
        return nn(dpack[rows], w[...])

    def grads():
        loads[0].wait()
        flipped[...] = whole[...].T
        for col in range(0, 3 * packed, TILE):
            size = min(TILE, 3 * packed - col)
            weight_grad(None, dpack.at[:, col : col + size], flipped, col, packs)
        loads[1].wait()
        loads[2].wait()
        flat[...] = nt(att[...], spread[...]).astype(BF)
        weight_grad(rows1, flat, flipped, 3 * packed, packs)
        copies.append(send_half(packs, sems, 6, 0, 4 * packed))

    scatter(place, term, bufs, sems, 0, grads)

    def finish(rows):
        d_h = scattered(bufs, rows)
        normal, inverse = normed(x[rows].astype(F32))
        scale = mod_rows(sel[rows], mod, 1)
        total_rows = dx1[rows] + norm_back(d_h * (1.0 + scale), normal, inverse)
        du[rows] = total_rows
        du_b[rows] = total_rows.astype(BF)
        add_sums(here, 0, sel[rows], d_h)
        add_sums(here, 1, sel[rows], d_h * normal)

    over_blocks(rows_here, finish)
    add_halves(packs, copies, total, 0, 4 * packed)


def cell():
    return 4 * lax.axis_index(S) + lax.axis_index(T)


def cell_id(index):
    return {S: index // 4, T: index % 4}


def greet_all(dp):
    sem = pltpu.get_barrier_semaphore()
    here, shard = cell(), lax.axis_index(DP)
    for k in range(1, 8):
        pl.semaphore_signal(
            sem, inc=1, device_id=cell_id((here + k) % 8), device_id_type=pl.DeviceIdType.MESH
        )
    for k in range(1, dp):
        pl.semaphore_signal(
            sem, inc=1, device_id={DP: (shard + k) % dp}, device_id_type=pl.DeviceIdType.MESH
        )
    pl.semaphore_wait(sem, 7 + dp - 1)


def push(src, dst, sems, index, device):
    copy = pltpu.make_async_remote_copy(
        src_ref=src,
        dst_ref=dst,
        send_sem=sems[0].at[index],
        recv_sem=sems[1].at[index],
        device_id=device,
        device_id_type=pl.DeviceIdType.MESH,
    )
    copy.start()
    return copy


def head_kernel(dp, cond, ada_h, bias, gain_own, items, pos, tables, mod, lifted_all, gains, sel,
                both, spans, ada, parts, got, wide, tall, lifted, gain, ssem, rsem, wsem):
    load = pltpu.make_async_copy(ada_h, ada, wsem)
    load.start()
    lifted[...] = jnp.zeros_like(lifted)
    raw = cond[...].astype(F32)
    raw = (raw * jax.nn.sigmoid(raw)).astype(BF).astype(F32)
    lifted[0:3] = raw[0:3]
    lifted[8:11] = raw[3:6]
    gain[...] = jnp.zeros_like(gain)
    gain[0:2, 0 : gain_own.shape[1]] = gain_own[...].astype(F32)
    biases = bias[...].astype(F32)
    greet_all(dp)
    sems = (ssem, rsem)
    here, shard, section = cell(), lax.axis_index(DP), lax.axis_index(S)
    copies = [push(gain, gains.at[section], sems, 6 + dp, {S: 1 - section})]
    gains[section] = gain[...]
    lifted_all[shard] = lifted[...]
    for k in range(1, dp):
        copies.append(
            push(lifted, lifted_all.at[shard], sems, 6 + k, {DP: (shard + k) % dp})
        )
    load.wait()
    half = parts.shape[3]
    for micro in range(2):
        for j in range(3):
            rows = lifted[pl.ds(micro * 8, 8)].astype(BF)
            here_bias = biases[:, j * half : (j + 1) * half]
            parts[micro, j] = nt(rows, ada[pl.ds(j * half, half)]) + here_bias
    for k in range(1, 8):
        peer = (here + k) % 8
        copies.append(push(parts.at[peer // 4], got.at[here], sems, k - 1, cell_id(peer)))
    got[here] = parts[section]
    rows_here = sel.shape[0]
    base = shard * 6 + section * 3
    seq = items.shape[1]
    line = items[pl.ds(section, 1), :]
    wide[...] = jnp.zeros_like(wide)
    wide[0:1] = (line - base).astype(F32)
    wide[1:2] = pos[0, pl.ds(section, 1), :].astype(F32)
    wide[2:3] = pos[1, pl.ds(section, 1), :].astype(F32)
    start = 0
    spans[0] = 0
    for j in range(3):
        count = jnp.sum((wide[0:1] == j).astype(F32)).astype(jnp.int32)
        spans[4 + j] = count
        start = start + count
        spans[1 + j] = start
    spans[7] = 0
    tall[...] = wide[...].T
    own = tall[pl.ds(pl.multiple_of(lax.axis_index(T) * rows_here, rows_here), rows_here), :]
    lane = lax.broadcasted_iota(jnp.int32, (rows_here, 8), 1).astype(F32)
    sel[...] = ((own[:, 0:1] == lane) & (lane < 3.0)).astype(F32)
    lane = lax.broadcasted_iota(jnp.int32, (seq, 64), 1).astype(F32)
    hot = jnp.where(lane < 32.0, tall[:, 1:2], tall[:, 2:3] + 32.0) == lane
    hot = hot.astype(F32).astype(BF)
    both[...] = (nn(hot, tables[0]) + nn(hot, tables[1])) + nn(hot, tables[2])
    for copy in copies:
        copy.wait_recv()
    for layer in range(2):
        for block in range(6):
            for side in range(2):
                n = 2 * block + side
                mod[layer, block, :, pl.ds(side * half, half)] = got[4 * layer + n // 3, n % 3]
    for copy in copies:
        copy.wait_send()


def tail_kernel(dp, dmod, dgain, lifted_part, cond, ada_h, ada_grad, bias_grad, cond_grad, gain_grad,
                ada, bias_row, got, got_gain, total, total_gain, every, every_gain, lifts, ssem, rsem, wsem):
    load = pltpu.make_async_copy(ada_h, ada, wsem)
    load.start()
    greet_all(dp)
    sems = (ssem, rsem)
    here, shard = cell(), lax.axis_index(DP)
    section, place = lax.axis_index(S), lax.axis_index(T)
    sends, arrivals = [], []
    for k in range(1, 8):
        peer = (here + k) % 8
        to = cell_id(peer)
        arrivals.append(
            push(dmod.at[peer // 4, pl.ds(3 * (peer % 4), 3)], got.at[here], sems, k - 1, to)
        )
        arrivals.append(push(dgain.at[peer // 4], got_gain.at[here], sems, 6 + k, to))
    got[here] = dmod[section, pl.ds(3 * place, 3)]
    got_gain[here] = dgain[section]
    for copy in arrivals:
        copy.wait_recv()
    sends += arrivals
    for micro in range(2):
        total[micro] = (got[4 * micro] + got[4 * micro + 1]) + (got[4 * micro + 2] + got[4 * micro + 3])
    gain = got_gain[0]
    for k in range(1, 8):
        gain = gain + got_gain[k]
    total_gain[...] = gain
    arrivals = []
    for k in range(1, dp):
        to = {DP: (shard + k) % dp}
        arrivals.append(push(total, every.at[shard], sems, 13 + k, to))
        arrivals.append(push(total_gain, every_gain.at[shard], sems, 12 + dp + k, to))
    every[shard] = total[...]
    every_gain[shard] = total_gain[...]
    load.wait()
    half = total.shape[3]
    for micro in range(2):
        lift = two(nn, total[micro, 0], ada[pl.ds(0, half)])
        for j in range(1, 3):
            lift = lift + two(nn, total[micro, j], ada[pl.ds(j * half, half)])
        lifts[here, micro] = lift
    base = 13 + 2 * (dp - 1)
    lift_copies = []
    for k in range(1, 8):
        lift_copies.append(
            push(lifts.at[here], lifts.at[here], sems, base + k, cell_id((here + k) % 8))
        )
    for copy in arrivals:
        copy.wait_recv()
    sends += arrivals
    gain = every_gain[0]
    for k in range(1, dp):
        gain = gain + every_gain[k]
    heads = gain.shape[1] // PAD
    summed = gain[:, 0:PAD]
    for h in range(1, heads):
        summed = summed + gain[:, h * PAD : (h + 1) * PAD]
    gain_grad[...] = summed[0:2, 0 : gain_grad.shape[1]]
    for j in range(3):
        bias = jnp.zeros((1, half), F32)
        grad = jnp.zeros((lifted_part.shape[2], half), F32)
        for k in range(dp):
            for micro in range(2):
                block = every[k, micro, j]
                bias = bias + jnp.sum(block, axis=0, keepdims=True)
                high = block.astype(BF)
                low = (block - high.astype(F32)).astype(BF)
                rows = lifted_part[2 * k + micro].astype(BF)
                grad = grad + tn(rows, high) + tn(rows, low)
        bias_row[:, pl.ds(j * half, half)] = bias
        ada_grad[:, pl.ds(j * half, half)] = grad
    for copy in lift_copies:
        copy.wait_recv()
    sends += lift_copies
    lift = lifts[0]
    for k in range(1, 8):
        lift = lift + lifts[k]
    raw = cond[...].astype(F32)
    s = jax.nn.sigmoid(raw)
    factor = s * (1.0 + raw * (1.0 - s))
    cond_grad[0:3] = lift[0, 0:3] * factor[0:3]
    cond_grad[3:6] = lift[1, 0:3] * factor[3:6]
    part = bias_grad.shape[1]
    row = bias_row[...]
    total_bias = jnp.zeros((1, part), F32)
    for k in range(dp):
        chosen = (shard == k).astype(F32)
        total_bias = total_bias + row[:, k * part : (k + 1) * part] * chosen
    bias_grad[...] = total_bias
    for copy in sends:
        copy.wait_send()


def price(micros):
    return pl.CostEstimate(flops=0, bytes_accessed=int(micros * 3.5e6), transcendentals=0)


def ring_call(kernel, ident, micros, outs, scratch, args, spaces, scalar=-1, loose=99):
    return pl.pallas_call(
        kernel,
        out_shape=outs,
        in_specs=[vmem() if s else anywhere() for s in spaces],
        out_specs=[
            pl.BlockSpec(memory_space=pltpu.SMEM)
            if n == scalar
            else (vmem() if n < loose else anywhere())
            for n in range(len(outs))
        ],
        scratch_shapes=scratch,
        compiler_params=pltpu.CompilerParams(
            collective_id=ident, has_side_effects=True, vmem_limit_bytes=60 * 2**20
        ),
        cost_estimate=price(micros),
    )(*args)


def attention_kernel(head, spans, q, k, v, att):
    rows, wide = q.shape
    scale = head ** (-0.5)

    def each_head(fn):
        for n in range(wide // PAD):
            fn(slice(n * PAD, (n + 1) * PAD))

    for item in range(3):
        at = pl.ds(pl.multiple_of(spans[item], 16), TILE)
        valid = lax.broadcasted_iota(jnp.int32, (TILE, TILE), 1) < spans[4 + item]

        def tile(lanes, at=at, valid=valid):
            att[at, lanes] = softmax_rows(q[at, lanes], k[at, lanes], v[at, lanes], valid, scale)

        each_head(tile)
    first = rows - 48
    start = spans[3]
    at = pl.ds(first, 48)
    valid = first + lax.broadcasted_iota(jnp.int32, (48, 48), 1) >= start
    live = first + lax.broadcasted_iota(jnp.int32, (48, PAD), 0) >= start

    def rest(lanes):
        new = softmax_rows(q[at, lanes], k[at, lanes], v[at, lanes], valid, scale)
        att[at, lanes] = jnp.where(live, new, att[at, lanes])

    each_head(rest)


def unit(proj, ones, head):
    inverse = lax.rsqrt(two(nn, proj * proj, ones) * (1.0 / head) + EPS)
    return proj * inverse, inverse


def softmax_rows(query, key, value, valid, scale):
    scores = jnp.where(valid, nt(query, key) * scale, -1e30)
    raised = jnp.exp(scores - jnp.max(scores, axis=1, keepdims=True))
    probs = raised / jnp.sum(raised, axis=1, keepdims=True)
    return nn(probs.astype(BF), value).astype(BF)


def back_tile(query, key, value, grad, keys, queries, scale):
    scores = jnp.where(keys, nt(key, query) * scale, -1e30)
    raised = jnp.exp(scores - jnp.max(scores, axis=0, keepdims=True))
    probs = jnp.where(queries, raised / jnp.sum(raised, axis=0, keepdims=True), 0.0)
    d_value = nn(probs.astype(BF), grad)
    d_probs = nt(value, grad)
    inner = jnp.sum(probs * d_probs, axis=0, keepdims=True)
    d_scores = (probs * (d_probs - inner)).astype(BF)
    return tn(d_scores, key) * scale, nn(d_scores, query) * scale, d_value


def attention_back_kernel(head, spans, q, k, v, grad, dq, dk, dv):
    rows, wide = q.shape
    scale = head ** (-0.5)

    def each_head(fn):
        for n in range(wide // PAD):
            fn(slice(n * PAD, (n + 1) * PAD))

    for item in range(3):
        at = pl.ds(pl.multiple_of(spans[item], 16), TILE)
        keys = lax.broadcasted_iota(jnp.int32, (TILE, TILE), 0) < spans[4 + item]
        queries = lax.broadcasted_iota(jnp.int32, (TILE, TILE), 1) < spans[4 + item]

        def tile(lanes, at=at, keys=keys, queries=queries):
            parts = back_tile(
                q[at, lanes], k[at, lanes], v[at, lanes], grad[at, lanes], keys, queries, scale
            )
            for new, dst in zip(parts, (dq, dk, dv)):
                dst[at, lanes] = new.astype(BF)

        each_head(tile)
    first = rows - 48
    start = spans[3]
    at = pl.ds(first, 48)
    keys = first + lax.broadcasted_iota(jnp.int32, (48, 48), 0) >= start
    queries = first + lax.broadcasted_iota(jnp.int32, (48, 48), 1) >= start
    live = first + lax.broadcasted_iota(jnp.int32, (48, PAD), 0) >= start

    def rest(lanes):
        parts = back_tile(
            q[at, lanes], k[at, lanes], v[at, lanes], grad[at, lanes], keys, queries, scale
        )
        for new, dst in zip(parts, (dq, dk, dv)):
            dst[at, lanes] = jnp.where(live, new.astype(BF), dst[at, lanes])

    each_head(rest)


def local_call(kernel, micros, outs, scratch, spans, args):
    return pl.pallas_call(
        kernel,
        out_shape=outs,
        in_specs=[pl.BlockSpec(memory_space=pltpu.SMEM)] + [vmem()] * len(args),
        out_specs=[vmem()] * len(outs),
        scratch_shapes=scratch,
        compiler_params=pltpu.CompilerParams(vmem_limit_bytes=60 * 2**20),
        cost_estimate=price(micros),
    )(spans, *args)


def swap(array):
    return lax.ppermute(array, S, [(0, 1), (1, 0)])


def head_tables(packed, head):
    quarter = head // 4
    frequency = np.float32(10000.0) ** (-np.arange(quarter, dtype=np.float32) / quarter)
    lane = np.arange(head)
    angle = np.arange(32, dtype=np.float32)[:, None] * frequency[lane % quarter][None, :]
    by_row = (lane // (2 * quarter) == 0)[None, :]
    table = np.zeros((64, 2 * PAD), np.float32)
    for n, values in enumerate((np.cos(angle), np.sin(angle))):
        at = slice(n * PAD, n * PAD + head)
        table[:32, at] = np.where(by_row, values, 0.0)
        table[32:, at] = np.where(by_row, 0.0, values)
    table = jnp.asarray(table)
    parts = []
    for _ in range(3):
        parts.append(lax.reduce_precision(table, 8, 7).astype(BF))
        table = table - parts[-1].astype(F32)
    rows = np.arange(2 * PAD)[:, None]
    cols = np.arange(2 * PAD)[None, :]
    inside = (rows // PAD == cols // PAD) & (rows % PAD < head) & (cols % PAD < head)
    row, col = rows % PAD, cols % PAD
    early = (col % (2 * quarter)) < quarter
    turn = np.where(inside & early & (row == col + quarter), -1.0, 0.0)
    turn = turn + np.where(inside & ~early & (row == col - quarter), 1.0, 0.0)
    heads = packed // head
    rows = np.arange(packed)[:, None]
    wide = np.arange(heads * PAD)[None, :]
    spread = (rows // head == wide // PAD) & (rows % head == wide % PAD)
    lanes = tuple(jnp.asarray(m.astype(np.float32)).astype(BF) for m in (turn, inside, spread))
    return jnp.stack(parts), lanes


def reduced(total):
    return lax.psum_scatter(total, DP, scatter_dimension=0, tiled=True)[0]


def own_layer(section, pair):
    first = section == 0
    keep = jnp.where(first, pair[0], pair[1])
    got = swap(jnp.where(first, pair[1], pair[0]))
    return jnp.where(first, jnp.concatenate([keep, got]), jnp.concatenate([got, keep])).astype(F32)


def per_device(square, dp, tokens, cotangent, cond, patch_item, patch_pos, w_qkv, w_out, w_gate_up,
               w_down, qk_gain, ada_weight, ada_bias):
    section = lax.axis_index(S)
    first = section == 0
    rows, width = tokens.shape[1:]
    seq = patch_item.shape[1]
    items = cond.shape[0]
    head = qk_gain.shape[-1]
    packed = w_qkv.shape[-1]
    heads = packed // head
    hidden_here = w_down.shape[1]
    own = (jnp.swapaxes(w_qkv[0], 1, 2), w_out[0], w_gate_up[0], w_down[0])
    other = tuple(swap(w) for w in own)
    flat_qkv = (own[0].reshape(3 * packed, width), other[0].reshape(3 * packed, width))

    ada = ada_weight[0].T
    half = width // 2
    trig, (turn, ones, spread) = head_tables(packed, head)
    wide = heads * PAD
    mods, lifted_all, gains, sel, both, spans = ring_call(
        functools.partial(head_kernel, dp),
        8,
        12,
        [
            sds((2, 6, 8, width), F32),
            sds((dp, 16, width), F32),
            sds((2, 8, PAD), F32),
            sds((rows, 8), F32),
            sds((seq, 2 * PAD), F32),
            sds((8,), jnp.int32),
        ],
        [
            pltpu.VMEM((3 * half, width), BF),
            pltpu.VMEM((2, 3, 8, half), F32),
            pltpu.VMEM((8, 3, 8, half), F32),
            pltpu.VMEM((8, seq), F32),
            pltpu.VMEM((seq, 8), F32),
            pltpu.VMEM((16, width), F32),
            pltpu.VMEM((8, PAD), F32),
        ]
        + dma_sems(7 + dp)
        + [pltpu.SemaphoreType.DMA],
        (cond, ada, ada_bias, qk_gain[0], patch_item, patch_pos, trig),
        (1, 0, 1, 1, 1, 1, 1),
        scalar=5,
    )
    part = width // dp
    shard = lax.axis_index(DP)
    lifted_part = lax.dynamic_slice_in_dim(lifted_all, shard * part, part, 2)
    lifted_part = lifted_part.reshape(2 * dp, 8, part)

    x = tokens
    kept = []
    for layer in range(2):
        mod = mods
        whole1, proj, q, k, v = ring_call(
            functools.partial(qkv_kernel, layer, square),
            layer,
            20,
            [sds((seq, width), BF), sds((2, seq, wide), BF)] + [sds((seq, wide), BF)] * 3,
            [pltpu.VMEM((rows, width), BF), pltpu.VMEM((3, wide, width), BF)]
            + dma_sems(6)
            + [pltpu.SemaphoreType.DMA((3 * heads,))],
            (x, sel, mod, gains, both, turn, ones, own[0], other[0]),
            (1,) * 7 + (0, 0),
        )
        (att,) = local_call(
            functools.partial(attention_kernel, head),
            6,
            [sds((seq, wide), BF)],
            [],
            spans,
            (q, k, v),
        )
        br1, x1, br2, y, whole2, gate, up, hidden = ring_call(
            functools.partial(mlp_kernel, layer, square),
            2 + layer,
            48,
            [
                sds((rows, width), F32),
                sds((rows, width), F32),
                sds((rows, width), F32),
                sds((rows, width), BF),
                sds((seq, width), BF),
                sds((seq, hidden_here), F32),
                sds((seq, hidden_here), F32),
                sds((seq, hidden_here), BF),
            ],
            [
                pltpu.VMEM((seq, width), BF),
                pltpu.VMEM((seq, hidden_here), F32),
                pltpu.VMEM((seq, hidden_here), F32),
                pltpu.VMEM((seq, hidden_here), BF),
                pltpu.VMEM((rows, width), BF),
                pltpu.VMEM((wide, width), BF),
                pltpu.VMEM((2, width, hidden_here), BF),
                pltpu.VMEM((hidden_here, width), BF),
            ]
            + scatter_scratch(rows, width)
            + scatter_scratch(rows, width)
            + dma_sems(18)
            + [pltpu.SemaphoreType.DMA((7,)), pltpu.SemaphoreType.DMA((heads,))],
            (att, x, sel, mod, own[1], other[1], own[2], other[2], own[3], other[3]),
            (1, 1, 1, 1) + (0,) * 6,
            loose=4,
        )
        kept.append((x, whole1, proj, q, k, v, att, br1, x1, whole2, gate, up, hidden, br2, y))
        x = y

    dy = cotangent
    packs = [None, None]
    prev = jnp.zeros((12, 8, half), F32)
    d_gains = [None, None]
    d_inputs = [None, None]
    for layer in (1, 0):
        x, whole1, proj, q, k, v, att, br1, x1, whole2, gate, up, hidden, br2, y = kept[layer]
        mod = mods
        rows1, datt, dx1, dmod_a, total_mlp = ring_call(
            functools.partial(mlp_back_kernel, layer, square),
            4 + layer,
            52,
            [
                sds((seq, width), BF),
                sds((seq, wide), BF),
                sds((rows, width), F32),
                sds((8, 8, half), F32),
                sds((dp, part // 2, 3 * hidden_here), BF),
            ],
            [pltpu.VMEM((dp, part // 2, 3 * hidden_here), BF)] * 3
            + [
                pltpu.VMEM((rows, width), BF),
                pltpu.VMEM((rows, width), BF),
                pltpu.VMEM((seq, width), BF),
                pltpu.VMEM((seq, hidden_here), BF),
                pltpu.VMEM((seq, hidden_here), BF),
                pltpu.VMEM((seq, hidden_here), F32),
                pltpu.VMEM((seq, hidden_here), F32),
                pltpu.VMEM((seq, hidden_here), BF),
                pltpu.VMEM((seq, width), BF),
                pltpu.VMEM((width, seq), BF),
                pltpu.VMEM((wide, width), BF),
                pltpu.VMEM((2, width, hidden_here), BF),
                pltpu.VMEM((hidden_here, width), BF),
            ]
            + scatter_scratch(rows, width)
            + dma_sems(21)
            + [pltpu.SemaphoreType.DMA((7,)), pltpu.SemaphoreType.DMA((heads,))],
            (dy, br2, br1, x1, sel, mod, gate, up, hidden, whole2, own[1], other[1], own[2],
             other[2], own[3], other[3]),
            (1,) * 6 + (0,) * 10,
        )
        pack_mlp = reduced(total_mlp)
        dq, dk, dv = local_call(
            functools.partial(attention_back_kernel, head),
            10,
            [sds((seq, wide), BF)] * 3,
            [],
            spans,
            (q, k, v, datt),
        )
        du, du_b, d_mod, total_att, dgain = ring_call(
            functools.partial(qkv_back_kernel, layer, square),
            6 + layer,
            22,
            [
                sds((rows, width), F32),
                sds((rows, width), BF),
                sds((2, 12, 8, half), F32),
                sds((dp, part // 2, 4 * packed), BF),
                sds((2, 1, wide), F32),
            ],
            [
                pltpu.VMEM((3 * packed, width), BF),
                pltpu.VMEM((seq, width), BF),
                pltpu.VMEM((seq, wide), BF),
                pltpu.VMEM((seq, width), BF),
                pltpu.VMEM((width, seq), BF),
                pltpu.VMEM((seq, 3 * packed), BF),
                pltpu.VMEM((seq, packed), BF),
            ]
            + [pltpu.VMEM((dp, part // 2, 4 * packed), BF)] * 3
            + scatter_scratch(rows, width)
            + dma_sems(7)
            + [pltpu.SemaphoreType.DMA((4,))],
            (dq, dk, dv, proj, gains, both, turn, ones, spread, x, dx1, sel, mod, dmod_a,
             prev, *flat_qkv, whole1, att, rows1),
            (1,) * 15 + (0,) * 5,
        )
        prev = d_mod[1]
        pack_att = reduced(total_att)
        packs[layer] = (pack_mlp, pack_att)
        d_gains[layer] = dgain
        d_inputs[layer] = du_b if layer else du
        dy = du_b

    gain_parts = jnp.pad(jnp.stack(d_gains).reshape(2, 2, wide), ((0, 0), (0, 6), (0, 0)))
    bias_part = ada_bias.shape[1] // dp
    g_ada_w, g_ada_b, cond_grad, gain_total = ring_call(
        functools.partial(tail_kernel, dp),
        9,
        15,
        [
            sds((part, 3 * half), F32),
            sds((1, bias_part), F32),
            sds((items, width), F32),
            sds((2, head), F32),
        ],
        [
            pltpu.VMEM((3 * half, width), BF),
            pltpu.VMEM((1, 3 * half), F32),
            pltpu.VMEM((8, 3, 8, half), F32),
            pltpu.VMEM((8, 8, wide), F32),
            pltpu.VMEM((2, 3, 8, half), F32),
            pltpu.VMEM((8, wide), F32),
            pltpu.VMEM((dp, 2, 3, 8, half), F32),
            pltpu.VMEM((dp, 8, wide), F32),
            pltpu.VMEM((8, 2, 8, width), F32),
        ]
        + dma_sems(13 + 2 * (dp - 1) + 8)
        + [pltpu.SemaphoreType.DMA],
        (d_mod, gain_parts, lifted_part, cond, ada),
        (1, 1, 1, 1, 0),
    )

    mlp = own_layer(section, (packs[0][0], packs[1][0]))
    attn = own_layer(section, (packs[0][1], packs[1][1]))
    f = hidden_here
    g_gate_up = jnp.stack([mlp[:, :f], mlp[:, f : 2 * f]])[None]
    g_down = mlp[:, 2 * f :].T[None]
    g_qkv = jnp.stack([attn[:, k * packed : (k + 1) * packed] for k in range(3)])[None]
    g_out = attn[:, 3 * packed :].T[None]

    outs = jnp.where(first, kept[0][-1], kept[1][-1])
    outs_got = swap(jnp.where(first, kept[1][-1], kept[0][-1]))
    layer_out = jnp.where(first, jnp.stack([outs, outs_got]), jnp.stack([outs_got, outs]))
    wide_mid = d_inputs[1].astype(F32)
    back_keep = jnp.where(first, d_inputs[0], wide_mid)
    back_got = swap(jnp.where(first, wide_mid, d_inputs[0]))
    in_grads = jnp.where(first, jnp.stack([back_keep, back_got]), jnp.stack([back_got, back_keep]))
    return (
        layer_out[None],
        in_grads[None],
        cond_grad,
        g_qkv,
        g_out,
        g_gate_up,
        g_down,
        gain_total[None],
        g_ada_w[None],
        g_ada_b,
    )


def solution(mesh):
    both = (DP, T)
    in_specs = (
        P(None, both, None),
        P(None, both, None),
        P(DP, None),
        P(None, DP),
        P(None, None, DP),
        P(S, None, None, T),
        P(S, T, None),
        P(S, None, None, T),
        P(S, T, None),
        P(S, None, None),
        P(S, None, T),
        P(S, T),
    )
    out_specs = (
        P(S, None, both, None),
        P(S, None, both, None),
        P(DP, None),
        P(S, None, DP, T),
        P(S, T, DP),
        P(S, None, DP, T),
        P(S, T, DP),
        P(S, None, None),
        P(S, DP, T),
        P(S, (T, DP)),
    )
    dp = mesh.shape[DP]

    def program(*args):
        return per_device(dp <= 4, dp, *args)

    return jax.shard_map(
        program, mesh=mesh, in_specs=in_specs, out_specs=out_specs, check_vma=False
    )
```

```python
import functools

import jax
import jax.numpy as jnp
import numpy as np
from jax import lax
from jax.experimental import pallas as pl
from jax.experimental.pallas import tpu as pltpu
from jax.sharding import PartitionSpec as P


EPS = 1e-06
F32 = jnp.float32
BF = jnp.bfloat16
S, DP, T = "section", "dp", "tensor"
PAD = 128
TILE = 256


def nn(a, b):
    return jnp.dot(a, b, preferred_element_type=F32)


def nt(a, b):
    return lax.dot_general(a, b, (((1,), (1,)), ((), ())), preferred_element_type=F32)


def tn(a, b):
    return lax.dot_general(a, b, (((0,), (0,)), ((), ())), preferred_element_type=F32)


def two(dot, a, b):
    high = a.astype(BF)
    low = (a - high.astype(F32)).astype(BF)
    return dot(high, b) + dot(low, b)


def sds(shape, dtype):
    return jax.ShapeDtypeStruct(shape, dtype)


def vmem():
    return pl.BlockSpec(memory_space=pltpu.VMEM)


def anywhere():
    return pl.BlockSpec(memory_space=pl.ANY)


def ring(square):
    me = lax.axis_index(T)
    near = me + 1 - 2 * (me % 2)
    if square:
        return me, near, me + 2 - 4 * (me // 2), 3 - me, True
    return me, near, 3 - me, (me + 2) % 4, False


def pieces(place, step, half):
    me, upper, moved, far = place[0], (step % 3) // 2, (step + 2) // 3, step // 3
    near = moved - far
    low = (moved, far) if place[4] else (near, near)
    found = []
    for side, high in ((0, far), (1, moved)):
        chunk = (me % 2 + low[side]) % 2 + 2 * ((me // 2 + high) % 2)
        row = (2 * chunk + (1 - upper if side else upper)) * half
        found.append(pl.ds(pl.multiple_of(row, half), half))
    return found


def joined(ref, rows):
    return jnp.concatenate([ref[rows[0]], ref[rows[1]]], axis=0)


def put(ref, rows, values):
    half = values.shape[0] // 2
    ref[rows[0]] = values[:half].astype(ref.dtype)
    ref[rows[1]] = values[half:].astype(ref.dtype)


def farthest_first(place, step):
    me, low = place[0], ((step + 1) // 2) % 2
    if place[4]:
        low = (3 - step) // 2
    return (me % 2 + low) % 2 + 2 * ((me // 2 + (step + 1) % 2) % 2)


def near_first(place, step):
    me, low = place[0], (3 - step) // 2
    if place[4]:
        low = (step + 1) % 2
    return (me % 2 + low) % 2 + 2 * ((me // 2 + ((step + 1) // 2) % 2) % 2)


def greet(place, partner=False):
    sem = pltpu.get_barrier_semaphore()
    peers = (place[1], place[2]) if place else ()
    for peer in peers:
        pl.semaphore_signal(
            sem, inc=1, device_id={T: peer}, device_id_type=pl.DeviceIdType.MESH
        )
    if partner:
        pl.semaphore_signal(
            sem, inc=1, device_id={S: 1 - lax.axis_index(S)}, device_id_type=pl.DeviceIdType.MESH
        )
    pl.semaphore_wait(sem, len(peers) + partner)


def remote(src, dst, sems, index, peer):
    return pltpu.make_async_remote_copy(
        src_ref=src,
        dst_ref=dst,
        send_sem=sems[0].at[index],
        recv_sem=sems[1].at[index],
        device_id={T: peer},
        device_id_type=pl.DeviceIdType.MESH,
    )


def chunk_rows(chunk, rows):
    return pl.ds(pl.multiple_of(chunk * rows, rows), rows)


def repeat(body, times):
    def one(step, carry):
        body(step)
        return carry

    lax.fori_loop(0, times, one, 0)


def gather(place, mine, whole, sems, base, use, ready=lambda: None, late=lambda: None, last=None):
    me, a, b, _, _ = place
    rows = mine.shape[0]
    half = rows // 2
    lo, hi = pl.ds(0, half), pl.ds(half, half)

    def part(chunk, upper):
        return whole.at[pl.ds(pl.multiple_of(chunk * rows + upper * half, half), half)]

    a0 = remote(mine.at[lo], part(me, 0), sems, base, a)
    b0 = remote(mine.at[hi], part(me, 1), sems, base + 1, b)
    a1 = remote(mine.at[hi], part(me, 1), sems, base + 2, a)
    b1 = remote(mine.at[lo], part(me, 0), sems, base + 3, b)
    b2 = remote(part(a, 0), part(a, 0), sems, base + 4, b)
    a2 = remote(part(b, 1), part(b, 1), sems, base + 5, a)
    for copy in (a0, b0, a1, b1):
        copy.start()
    whole[chunk_rows(me, rows), :] = mine[...]
    ready()

    def final():
        b2.wait_recv()
        a2.wait_recv()

    def body(step):
        @pl.when(step == 1)
        def _():
            a0.wait_recv()
            b2.start()
            b0.wait_recv()
            a2.start()

        @pl.when(step == 2)
        def _():
            a1.wait_recv()
            b1.wait_recv()

        if last is None:

            @pl.when(step == 3)
            def _():
                late()
                final()

        use(pieces(place, step, half))

    repeat(body, 4 if last is None else 3)
    if last is not None:
        last(final)
    for copy in (a0, b0, a1, b1, a2, b2):
        copy.wait_send()


def scatter(place, term, bufs, sems, base, fill=lambda: None, before=None):
    _, a, b, _, _ = place
    out, into, keep, own = bufs
    half = keep.shape[1]
    lo, hi = pl.ds(0, half), pl.ds(half, half)
    d0 = remote(out.at[0, lo], into.at[0, lo], sems, base, a)
    d1 = remote(out.at[0, hi], into.at[0, hi], sems, base + 1, b)
    a0 = remote(out.at[1, lo], into.at[1, lo], sems, base + 2, a)
    b0 = remote(out.at[2, hi], into.at[2, hi], sems, base + 3, b)
    a1 = remote(out.at[1, hi], into.at[1, hi], sems, base + 4, a)
    b1 = remote(out.at[2, lo], into.at[2, lo], sems, base + 5, b)
    at = (0, 1, 2) if before is None else (2, 0, 1)

    def body(step):
        if before is None:
            chunk = farthest_first(place, step)
        else:
            chunk = near_first(place, step)
            pl.when(step == 2)(before)
        own[...] = term(chunk)

        @pl.when(step == at[0])
        def _():
            out[0] = own[...].astype(BF)
            d0.start()
            d1.start()

        @pl.when(step == at[1])
        def _():
            out[1, lo] = own[lo].astype(BF)
            a0.start()
            keep[0] = own[hi]

        @pl.when(step == at[2])
        def _():
            out[2, hi] = own[hi].astype(BF)
            b0.start()
            keep[1] = own[lo]

    repeat(body, 4)
    d1.wait_recv()
    out[1, hi] = (keep[0] + into[0, hi].astype(F32)).astype(BF)
    a1.start()
    d0.wait_recv()
    out[2, lo] = (keep[1] + into[0, lo].astype(F32)).astype(BF)
    b1.start()
    fill()
    for copy in (a0, b0, a1, b1):
        copy.wait_recv()
    for copy in (d0, d1, a0, b0, a1, b1):
        copy.wait_send()


def gather_scatter(place, mine, whole, sems, base, use, term, bufs, ready, fill=lambda: None):
    def last(final):
        def before():
            final()
            use(pieces(place, 3, mine.shape[0] // 2))

        scatter(place, term, bufs, sems, base + 6, fill, before)

    gather(place, mine, whole, sems, base, use, ready, last=last)


def scattered(bufs, rows):
    return bufs[3][rows] + bufs[1][1, rows].astype(F32) + bufs[1][2, rows].astype(F32)


def scatter_scratch(rows, width):
    return [
        pltpu.VMEM((3, rows, width), BF),
        pltpu.VMEM((3, rows, width), BF),
        pltpu.VMEM((2, rows // 2, width), F32),
        pltpu.VMEM((rows, width), F32),
    ]


def dma_sems(count):
    return [pltpu.SemaphoreType.DMA((count,)), pltpu.SemaphoreType.DMA((count,))]


def layer_weights(own, other, layer, dst, sem):
    mine = lax.axis_index(S) == layer

    @pl.when(mine)
    def _():
        pltpu.make_async_copy(own, dst, sem).start()

    @pl.when(jnp.logical_not(mine))
    def _():
        pltpu.make_async_copy(other, dst, sem).start()

    return pltpu.make_async_copy(own, dst, sem)


def head_weights(own, other, layer, dst, sems, parts):
    mine = lax.axis_index(S) == layer
    spread = len(parts) > 1
    heads = dst.shape[-2] // PAD
    head = own.shape[-2] // heads
    clean = head // 16 * 16
    copies = ([], [])
    for n, part in enumerate(parts):
        for h in range(heads):
            to = dst.at[part] if spread else dst
            to[pl.ds(h * PAD + clean, PAD - clean)] = jnp.zeros((PAD - clean, dst.shape[-1]), BF)
            to = to.at[pl.ds(h * PAD, head)]
            for which, src in enumerate((own, other)):
                src = src.at[part] if spread else src
                copies[which].append(
                    pltpu.make_async_copy(
                        src.at[pl.ds(h * head, head)], to, sems.at[n * heads + h]
                    )
                )

    @pl.when(mine)
    def _():
        for copy in copies[0]:
            copy.start()

    @pl.when(jnp.logical_not(mine))
    def _():
        for copy in copies[1]:
            copy.start()

    return copies[0]


def arrive(copies):
    for copy in copies:
        copy.wait()


def twice(row):
    return jnp.concatenate([row, row], axis=-1)


def over_blocks(rows, fn):
    step = rows // 4

    def body(i, carry):
        fn(pl.ds(pl.multiple_of(i * step, step), step))
        return carry

    lax.fori_loop(0, 4, body, 0)


def mod_rows(sel, mod, which):
    total = sel[:, 0:1] * mod[which, 0:1]
    for item in (1, 2):
        total = total + sel[:, item : item + 1] * mod[which, item : item + 1]
    return total


def add_sums(dmod, block, sel, values):
    sums = item_sums(sel, values)
    half = dmod.shape[2]
    dmod[2 * block] += sums[:, :half]
    dmod[2 * block + 1] += sums[:, half:]


def weight_grad(x, y, flipped, col, packs):
    mine, theirs, _ = packs
    dp, part, _ = mine.shape
    first = lax.axis_index(S) == 0
    width = y.shape[1]
    if x is not None:
        flipped[...] = x[...].T

    def one(to, columns):
        grad = nn(flipped[...], columns).astype(BF)
        grad = grad.reshape(dp, 2, part, columns.shape[1])

        @pl.when(first)
        def _():
            mine[:, :, to] = grad[:, 0]
            theirs[:, :, to] = grad[:, 1]

        @pl.when(jnp.logical_not(first))
        def _():
            mine[:, :, to] = grad[:, 1]
            theirs[:, :, to] = grad[:, 0]

    if width % 256:
        one(pl.ds(col, width), y[...])
        return

    def body(i, carry):
        at = pl.multiple_of(i * 256, 256)
        one(pl.ds(pl.multiple_of(col + at, 256), 256), y[:, pl.ds(at, 256)])
        return carry

    lax.fori_loop(0, width // 256, body, 0)


def send_half(packs, sems, index, col, width):
    at = pl.ds(col, width)
    return push(
        packs[1].at[:, :, at], packs[2].at[:, :, at], sems, index, {S: 1 - lax.axis_index(S)}
    )


def add_halves(packs, copies, total, col, width):
    at = pl.ds(col, width)
    for copy in copies:
        copy.wait_recv()

    def body(k):
        total[k, :, at] = (packs[0][k, :, at].astype(F32) + packs[2][k, :, at].astype(F32)).astype(BF)

    repeat(body, total.shape[0])
    for copy in copies:
        copy.wait_send()


def item_sums(sel, values):
    high = values.astype(BF)
    low = (values - high.astype(F32)).astype(BF)
    sel_b = sel.astype(BF)
    return tn(sel_b, high) + tn(sel_b, low)


def normed(values):
    inverse = lax.rsqrt(jnp.mean(values * values, axis=-1, keepdims=True) + EPS)
    return values * inverse, inverse


def norm_back(incoming, normal, inverse):
    return inverse * (incoming - normal * jnp.mean(incoming * normal, axis=-1, keepdims=True))


def tokens_of(ref):
    return ref.at[lax.axis_index(S)] if len(ref.shape) == 3 else ref


def qkv_kernel(layer, square, x, sel, mod, gain, both, turn, ones, w_own, w_other, whole, proj, q,
               k, v, h, w, ssem, rsem, wsem):
    place = ring(square)
    load = head_weights(w_own, w_other, layer, w, wsem, range(3))
    greet(place)
    head = w_own.shape[1] * PAD // w.shape[1]
    qkv_part(
        place, head, tokens_of(x), sel, mod.at[layer], gain.at[layer], both, turn, ones, load,
        whole, proj, q, k, v, h, w, (ssem, rsem), 0
    )


def qkv_part(place, head, x, sel, mod, gain, both, turn, ones, load, whole, proj, q, k, v, h, w,
             sems, base):
    def prepare(rows):
        normal, _ = normed(x[rows].astype(F32))
        shift = mod_rows(sel[rows], mod, 0)
        scale = mod_rows(sel[rows], mod, 1)
        h[rows] = (normal * (1.0 + scale) + shift).astype(BF)

    over_blocks(x.shape[0], prepare)

    def use(rows):
        held = joined(whole, rows)
        table = joined(both, rows)
        cosine = twice(table[:, 0:PAD])
        sine = twice(table[:, PAD : 2 * PAD])
        for which, dst in ((0, q), (1, k)):
            full = nt(held, w[which])
            put(proj.at[which], rows, full)
            turned = []
            for pair in range(full.shape[1] // (2 * PAD)):
                lanes = slice(pair * 2 * PAD, (pair + 1) * 2 * PAD)
                normal, _ = unit(full[:, lanes], ones[...], head)
                gained = normal * twice(gain[which : which + 1])
                turned.append(gained * cosine + two(nn, gained, turn[...]) * sine)
            put(dst, rows, jnp.concatenate(turned, axis=1))
        put(v, rows, nt(held, w[2]))

    gather(place, h, whole, sems, base, use, lambda: arrive(load))


def mlp_qkv_kernel(layer, square, att, x, sel, mod, wo0, wo1, wg0, wg1, wd0, wd1, gain, both, turn,
                   ones, w_own, w_other, br1, x1, br2, y, whole_q, proj, q, k, v, whole_h, gate_h,
                   up_h, hidden_h, whole, gate, up, hidden, h, wo, wg, wd, o1, i1, k1, s1, o2, i2,
                   k2, s2, ssem, rsem, wsem, osem, w, hsem):
    place = ring(square)
    load = head_weights(w_own, w_other, layer + 1, w, hsem, range(3))
    mlp_kernel(
        layer, square, att, x, sel, mod, wo0, wo1, wg0, wg1, wd0, wd1, br1, x1, br2, y, whole_h,
        gate_h, up_h, hidden_h, whole, gate, up, hidden, h, wo, wg, wd, o1, i1, k1, s1, o2, i2, k2,
        s2, ssem, rsem, wsem, osem
    )
    head = w_own.shape[1] * PAD // w.shape[1]
    qkv_part(
        place, head, y, sel, mod.at[layer + 1], gain.at[layer + 1], both, turn, ones, load, whole_q,
        proj, q, k, v, h, w, (ssem, rsem), 18
    )


def mlp_kernel(layer, square, att, x, sel, mod, wo0, wo1, wg0, wg1, wd0, wd1, br1, x1, br2, y,
               whole_h, gate_h, up_h, hidden_h, whole, gate, up, hidden, h, wo, wg, wd, o1, i1, k1, s1, o2, i2, k2, s2,
               ssem, rsem, wsem, osem):
    x, mod = tokens_of(x), mod.at[layer]
    place = ring(square)
    rows_here, _ = x.shape
    load_o = head_weights(wo0, wo1, layer, wo, osem, range(1))
    load_g = layer_weights(wg0, wg1, layer, wg, wsem.at[1])
    load_d = layer_weights(wd0, wd1, layer, wd, wsem.at[2])
    greet(place)
    sems = (ssem, rsem)
    arrive(load_o)
    first = (o1, i1, k1, s1)
    scatter(place, lambda c: nn(att[chunk_rows(c, rows_here)], wo[...]), first, sems, 0)

    def between(rows):
        branch = scattered(first, rows)
        br1[rows] = branch
        mixed = x[rows].astype(F32) + mod_rows(sel[rows], mod, 2) * branch
        x1[rows] = mixed
        normal, _ = normed(mixed)
        shift = mod_rows(sel[rows], mod, 3)
        scale = mod_rows(sel[rows], mod, 4)
        h[rows] = (normal * (1.0 + scale) + shift).astype(BF)

    over_blocks(rows_here, between)

    def use(rows):
        held = joined(whole, rows)
        g = nn(held, wg[0])
        put(gate, rows, g)
        u = nn(held, wg[1])
        put(up, rows, u)
        put(hidden, rows, g * jax.nn.sigmoid(g) * u)

    second = (o2, i2, k2, s2)
    stores = []
    for n, (src, dst) in enumerate(
        ((whole, whole_h), (gate, gate_h), (up, up_h), (hidden, hidden_h))
    ):
        stores.append(pltpu.make_async_copy(src, dst, wsem.at[3 + n]))

    def ready():
        load_g.wait()
        load_d.wait()

    def fill():
        for copy in stores:
            copy.start()

    def term(chunk):
        return nn(hidden[chunk_rows(chunk, rows_here)], wd[...])

    gather_scatter(place, h, whole, sems, 6, use, term, second, ready, fill)

    def finish(rows):
        branch = scattered(second, rows)
        br2[rows] = branch
        y[rows] = (x1[rows] + mod_rows(sel[rows], mod, 5) * branch).astype(BF)

    over_blocks(rows_here, finish)
    arrive(stores)


def mlp_back_kernel(layer, square, dy, br2, br1, x1, sel, mod, gate_h, up_h, hidden_h, rows_h,
                    wo0, wo1, wg0, wg1, wd0, wd1, whole1, datt, dx1, dmod, total, mine, theirs,
                    got, h, h1, whole2, dgate, dup, gate, up, hidden, saved, flipped, wo, wg, wd, o1, i1, k1,
                    s1, ssem, rsem, wsem, osem):
    dy, mod = tokens_of(dy), mod.at[layer]
    place = ring(square)
    rows_here, _ = dy.shape
    load_d = layer_weights(wd0, wd1, layer, wd, wsem.at[0])
    load_gate = pltpu.make_async_copy(gate_h, gate, wsem.at[1])
    load_gate.start()
    load_up = pltpu.make_async_copy(up_h, up, wsem.at[2])
    load_up.start()
    load_g = layer_weights(wg0, wg1, layer, wg, wsem.at[3])
    load_o = head_weights(wo0, wo1, layer, wo, osem, range(1))
    load_hidden = pltpu.make_async_copy(hidden_h, hidden, wsem.at[5])
    load_hidden.start()
    load_rows = pltpu.make_async_copy(rows_h, saved, wsem.at[6])
    load_rows.start()
    greet(place, True)
    sems = (ssem, rsem)
    dmod[...] = jnp.zeros_like(dmod)

    def prepare(rows):
        incoming = dy[rows].astype(F32)
        h[rows] = (incoming * mod_rows(sel[rows], mod, 5)).astype(BF)
        add_sums(dmod, 3, sel[rows], incoming * br2[rows])

    over_blocks(rows_here, prepare)

    def ready():
        arrive((load_d, load_gate, load_up, load_g, load_hidden))

    def use(rows):
        d_hidden = nt(joined(whole2, rows), wd[...])
        g = joined(gate, rows)
        s = jax.nn.sigmoid(g)
        put(dgate, rows, d_hidden * joined(up, rows) * s * (1.0 + g * (1.0 - s)))
        put(dup, rows, d_hidden * g * s)

    bufs = (o1, i1, k1, s1)
    f = hidden.shape[1]

    def term(chunk):
        rows = chunk_rows(chunk, rows_here)
        return nt(dgate[rows], wg[0]) + nt(dup[rows], wg[1])

    packs = (mine, theirs, got)
    copies = []

    def grad(index, x, y, col):
        weight_grad(x, y, flipped, col, packs)
        copies.append(send_half(packs, sems, index, col, f))

    def grad_down():
        grad(18, whole2, hidden, 2 * f)

    gather_scatter(place, h, whole2, sems, 0, use, term, bufs, ready, grad_down)

    def between(rows):
        d_h = scattered(bufs, rows)
        normal, inverse = normed(x1[rows])
        scale = mod_rows(sel[rows], mod, 4)
        d_mixed = dy[rows].astype(F32) + norm_back(d_h * (1.0 + scale), normal, inverse)
        dx1[rows] = d_mixed
        h1[rows] = (d_mixed * mod_rows(sel[rows], mod, 2)).astype(BF)

    over_blocks(rows_here, between)

    def use_out(rows):
        put(datt, rows, nt(joined(whole1, rows), wo[...]))

    def sums():
        def one(rows):
            d_h = scattered(bufs, rows)
            normal, _ = normed(x1[rows])
            add_sums(dmod, 1, sel[rows], d_h)
            add_sums(dmod, 2, sel[rows], d_h * normal)
            add_sums(dmod, 0, sel[rows], dx1[rows] * br1[rows])

        over_blocks(rows_here, one)
        arrive(load_o)
        load_rows.wait()
        grad(19, saved, dgate, 0)

    def late():
        weight_grad(None, dup, flipped, f, packs)

    gather(place, h1, whole1, sems, 12, use_out, sums, late)
    copies.append(send_half(packs, sems, 20, f, f))
    add_halves(packs, copies[:1], total, 2 * f, f)
    add_halves(packs, copies[1:2], total, 0, f)
    add_halves(packs, copies[2:], total, f, f)


def qkv_back_kernel(layer, square, dq, dk, dv, proj, gain, both, turn, ones, spread, x, dx1, sel,
                    mod, part, prev, w_own, w_other, whole_h, att_h, rows1_h, du, du_b, dmod, total,
                    dgain, w, whole, att, rows1, flipped, dpack, flat, mine, theirs, got, o1, i1,
                    k1, s1, ssem, rsem, wsem):
    x, mod, gain = tokens_of(x), mod.at[layer], gain.at[layer]
    place = ring(square)
    rows_here, _ = x.shape
    packed = spread.shape[0]
    head = packed * PAD // spread.shape[1]
    load = layer_weights(w_own, w_other, layer, w, wsem.at[3])
    loads = []
    for n, (src, dst) in enumerate(((whole_h, whole), (att_h, att), (rows1_h, rows1))):
        loads.append(pltpu.make_async_copy(src, dst, wsem.at[n]))
        loads[n].start()
    greet(place, True)
    here = dmod.at[layer]
    dmod[1 - layer] = prev[...]
    here[pl.ds(0, 4)] = jnp.zeros_like(prev[pl.ds(0, 4)])
    here[pl.ds(4, 8)] = part[...]
    dgain[...] = jnp.zeros_like(dgain)
    load.wait()
    bufs = (o1, i1, k1, s1)
    sems = (ssem, rsem)
    packs = (mine, theirs, got)
    copies = []

    def term(chunk):
        rows = chunk_rows(chunk, rows_here)
        cosine = twice(both[rows, 0:PAD])
        sine = twice(both[rows, PAD : 2 * PAD])
        for which, src in ((0, dq), (1, dk)):
            parts = []
            for pair in range(src.shape[1] // (2 * PAD)):
                lanes = slice(pair * 2 * PAD, (pair + 1) * 2 * PAD)
                turned = src[rows, lanes]
                back = turned.astype(F32) * cosine - nn(turned, turn[...]) * sine
                normal, inverse = unit(proj[which, rows, lanes].astype(F32), ones[...], head)
                dgain[which, :, lanes] += jnp.sum(back * normal, axis=0, keepdims=True)
                gained = back * twice(gain[which : which + 1])
                mean = two(nn, gained * normal, ones[...]) * (1.0 / head)
                parts.append((inverse * (gained - normal * mean)).astype(BF))
            full = jnp.concatenate(parts, axis=1)
            dpack[rows, which * packed : (which + 1) * packed] = nt(full, spread[...]).astype(BF)
        dpack[rows, 2 * packed : 3 * packed] = nt(dv[rows], spread[...]).astype(BF)
        return nn(dpack[rows], w[...])

    def grads():
        loads[0].wait()
        flipped[...] = whole[...].T
        for col in range(0, 3 * packed, TILE):
            size = min(TILE, 3 * packed - col)
            weight_grad(None, dpack.at[:, col : col + size], flipped, col, packs)
        loads[1].wait()
        loads[2].wait()
        flat[...] = nt(att[...], spread[...]).astype(BF)
        weight_grad(rows1, flat, flipped, 3 * packed, packs)
        copies.append(send_half(packs, sems, 6, 0, 4 * packed))

    scatter(place, term, bufs, sems, 0, grads)

    def finish(rows):
        d_h = scattered(bufs, rows)
        normal, inverse = normed(x[rows].astype(F32))
        scale = mod_rows(sel[rows], mod, 1)
        total_rows = dx1[rows] + norm_back(d_h * (1.0 + scale), normal, inverse)
        du[rows] = total_rows
        du_b[rows] = total_rows.astype(BF)
        add_sums(here, 0, sel[rows], d_h)
        add_sums(here, 1, sel[rows], d_h * normal)

    over_blocks(rows_here, finish)
    add_halves(packs, copies, total, 0, 4 * packed)


def cell():
    return 4 * lax.axis_index(S) + lax.axis_index(T)


def cell_id(index):
    return {S: index // 4, T: index % 4}


def greet_all(dp):
    sem = pltpu.get_barrier_semaphore()
    here, shard = cell(), lax.axis_index(DP)
    for k in range(1, 8):
        pl.semaphore_signal(
            sem, inc=1, device_id=cell_id((here + k) % 8), device_id_type=pl.DeviceIdType.MESH
        )
    for k in range(1, dp):
        pl.semaphore_signal(
            sem, inc=1, device_id={DP: (shard + k) % dp}, device_id_type=pl.DeviceIdType.MESH
        )
    pl.semaphore_wait(sem, 7 + dp - 1)


def push(src, dst, sems, index, device):
    copy = pltpu.make_async_remote_copy(
        src_ref=src,
        dst_ref=dst,
        send_sem=sems[0].at[index],
        recv_sem=sems[1].at[index],
        device_id=device,
        device_id_type=pl.DeviceIdType.MESH,
    )
    copy.start()
    return copy


def head_kernel(dp, cond, ada_h, bias, gain_own, items, pos, tables, mod, lifted_all, gains, sel,
                both, spans, ada, parts, got, wide, tall, lifted, gain, ssem, rsem, wsem):
    load = pltpu.make_async_copy(ada_h, ada, wsem)
    load.start()
    lifted[...] = jnp.zeros_like(lifted)
    raw = cond[...].astype(F32)
    raw = (raw * jax.nn.sigmoid(raw)).astype(BF).astype(F32)
    lifted[0:3] = raw[0:3]
    lifted[8:11] = raw[3:6]
    gain[...] = jnp.zeros_like(gain)
    gain[0:2, 0 : gain_own.shape[1]] = gain_own[...].astype(F32)
    biases = bias[...].astype(F32)
    greet_all(dp)
    sems = (ssem, rsem)
    here, shard, section = cell(), lax.axis_index(DP), lax.axis_index(S)
    copies = [push(gain, gains.at[section], sems, 6 + dp, {S: 1 - section})]
    gains[section] = gain[...]
    lifted_all[shard] = lifted[...]
    for k in range(1, dp):
        copies.append(
            push(lifted, lifted_all.at[shard], sems, 6 + k, {DP: (shard + k) % dp})
        )
    load.wait()
    half = parts.shape[3]
    for micro in range(2):
        for j in range(3):
            rows = lifted[pl.ds(micro * 8, 8)].astype(BF)
            here_bias = biases[:, j * half : (j + 1) * half]
            parts[micro, j] = nt(rows, ada[pl.ds(j * half, half)]) + here_bias
    for k in range(1, 8):
        peer = (here + k) % 8
        copies.append(push(parts.at[peer // 4], got.at[here], sems, k - 1, cell_id(peer)))
    got[here] = parts[section]
    rows_here = sel.shape[0]
    base = shard * 6 + section * 3
    seq = items.shape[1]
    line = items[pl.ds(section, 1), :]
    wide[...] = jnp.zeros_like(wide)
    wide[0:1] = (line - base).astype(F32)
    wide[1:2] = pos[0, pl.ds(section, 1), :].astype(F32)
    wide[2:3] = pos[1, pl.ds(section, 1), :].astype(F32)
    start = 0
    spans[0] = 0
    for j in range(3):
        count = jnp.sum((wide[0:1] == j).astype(F32)).astype(jnp.int32)
        spans[4 + j] = count
        start = start + count
        spans[1 + j] = start
    spans[7] = 0
    tall[...] = wide[...].T
    own = tall[pl.ds(pl.multiple_of(lax.axis_index(T) * rows_here, rows_here), rows_here), :]
    lane = lax.broadcasted_iota(jnp.int32, (rows_here, 8), 1).astype(F32)
    sel[...] = ((own[:, 0:1] == lane) & (lane < 3.0)).astype(F32)
    lane = lax.broadcasted_iota(jnp.int32, (seq, 64), 1).astype(F32)
    hot = jnp.where(lane < 32.0, tall[:, 1:2], tall[:, 2:3] + 32.0) == lane
    hot = hot.astype(F32).astype(BF)
    both[...] = (nn(hot, tables[0]) + nn(hot, tables[1])) + nn(hot, tables[2])
    for copy in copies:
        copy.wait_recv()
    for layer in range(2):
        for block in range(6):
            for side in range(2):
                n = 2 * block + side
                mod[layer, block, :, pl.ds(side * half, half)] = got[4 * layer + n // 3, n % 3]
    for copy in copies:
        copy.wait_send()


def tail_kernel(dp, dmod, dgain, lifted_part, cond, ada_h, ada_grad, bias_grad, cond_grad, gain_grad,
                ada, bias_row, got, got_gain, total, total_gain, every, every_gain, lifts, ssem, rsem, wsem):
    load = pltpu.make_async_copy(ada_h, ada, wsem)
    load.start()
    greet_all(dp)
    sems = (ssem, rsem)
    here, shard = cell(), lax.axis_index(DP)
    section, place = lax.axis_index(S), lax.axis_index(T)
    sends, arrivals = [], []
    for k in range(1, 8):
        peer = (here + k) % 8
        to = cell_id(peer)
        arrivals.append(
            push(dmod.at[peer // 4, pl.ds(3 * (peer % 4), 3)], got.at[here], sems, k - 1, to)
        )
        arrivals.append(push(dgain.at[peer // 4], got_gain.at[here], sems, 6 + k, to))
    got[here] = dmod[section, pl.ds(3 * place, 3)]
    got_gain[here] = dgain[section]
    for copy in arrivals:
        copy.wait_recv()
    sends += arrivals
    total[...] = jnp.zeros_like(total)
    for micro in range(2):
        summed = (got[4 * micro] + got[4 * micro + 1]) + (got[4 * micro + 2] + got[4 * micro + 3])
        total[:, 3 * micro : 3 * micro + 3] = summed[:, 0:3]
    gain = got_gain[0]
    for k in range(1, 8):
        gain = gain + got_gain[k]
    total_gain[...] = gain
    arrivals = []
    for k in range(1, dp):
        to = {DP: (shard + k) % dp}
        arrivals.append(push(total, every.at[shard], sems, 13 + k, to))
        arrivals.append(push(total_gain, every_gain.at[shard], sems, 12 + dp + k, to))
    every[shard] = total[...]
    every_gain[shard] = total_gain[...]
    load.wait()
    half = total.shape[2]
    lift = two(nn, total[0], ada[pl.ds(0, half)])
    for j in range(1, 3):
        lift = lift + two(nn, total[j], ada[pl.ds(j * half, half)])
    lifts[here] = lift
    base = 13 + 2 * (dp - 1)
    lift_copies = []
    for k in range(1, 8):
        lift_copies.append(
            push(lifts.at[here], lifts.at[here], sems, base + k, cell_id((here + k) % 8))
        )
    for copy in arrivals:
        copy.wait_recv()
    sends += arrivals
    gain = every_gain[0]
    for k in range(1, dp):
        gain = gain + every_gain[k]
    heads = gain.shape[1] // PAD
    summed = gain[:, 0:PAD]
    for h in range(1, heads):
        summed = summed + gain[:, h * PAD : (h + 1) * PAD]
    gain_grad[...] = summed[0:2, 0 : gain_grad.shape[1]]
    for j in range(3):
        bias = jnp.zeros((1, half), F32)
        grad = jnp.zeros((lifted_part.shape[2], half), F32)
        for k in range(dp):
            block = every[k, j, 0:6]
            bias = bias + jnp.sum(block, axis=0, keepdims=True)
            high = block.astype(BF)
            low = (block - high.astype(F32)).astype(BF)
            rows = jnp.concatenate([lifted_part[2 * k, 0:3], lifted_part[2 * k + 1, 0:3]], axis=0)
            rows = rows.astype(BF)
            grad = grad + tn(rows, high) + tn(rows, low)
        bias_row[:, pl.ds(j * half, half)] = bias
        ada_grad[:, pl.ds(j * half, half)] = grad
    for copy in lift_copies:
        copy.wait_recv()
    sends += lift_copies
    lift = lifts[0]
    for k in range(1, 8):
        lift = lift + lifts[k]
    raw = cond[...].astype(F32)
    s = jax.nn.sigmoid(raw)
    factor = s * (1.0 + raw * (1.0 - s))
    cond_grad[...] = lift[0:6] * factor
    part = bias_grad.shape[1]
    row = bias_row[...]
    total_bias = jnp.zeros((1, part), F32)
    for k in range(dp):
        chosen = (shard == k).astype(F32)
        total_bias = total_bias + row[:, k * part : (k + 1) * part] * chosen
    bias_grad[...] = total_bias
    for copy in sends:
        copy.wait_send()


def price(micros):
    return pl.CostEstimate(flops=0, bytes_accessed=int(micros * 3.5e6), transcendentals=0)


def ring_call(kernel, ident, micros, outs, scratch, args, spaces, scalar=-1, loose=99):
    return pl.pallas_call(
        kernel,
        out_shape=outs,
        in_specs=[vmem() if s else anywhere() for s in spaces],
        out_specs=[
            pl.BlockSpec(memory_space=pltpu.SMEM)
            if n == scalar
            else (vmem() if n < loose else anywhere())
            for n in range(len(outs))
        ],
        scratch_shapes=scratch,
        compiler_params=pltpu.CompilerParams(
            collective_id=ident, has_side_effects=True, vmem_limit_bytes=60 * 2**20
        ),
        cost_estimate=price(micros),
    )(*args)


def attention_kernel(head, spans, q, k, v, att):
    rows, wide = q.shape
    scale = head ** (-0.5)

    def each_head(fn):
        for n in range(wide // PAD):
            fn(slice(n * PAD, (n + 1) * PAD))

    for item in range(3):
        at = pl.ds(pl.multiple_of(spans[item], 16), TILE)
        valid = lax.broadcasted_iota(jnp.int32, (TILE, TILE), 1) < spans[4 + item]

        def tile(lanes, at=at, valid=valid):
            att[at, lanes] = softmax_rows(q[at, lanes], k[at, lanes], v[at, lanes], valid, scale)

        each_head(tile)
    first = rows - 48
    start = spans[3]
    at = pl.ds(first, 48)
    valid = first + lax.broadcasted_iota(jnp.int32, (48, 48), 1) >= start
    live = first + lax.broadcasted_iota(jnp.int32, (48, PAD), 0) >= start

    def rest(lanes):
        new = softmax_rows(q[at, lanes], k[at, lanes], v[at, lanes], valid, scale)
        att[at, lanes] = jnp.where(live, new, att[at, lanes])

    each_head(rest)


def unit(proj, ones, head):
    inverse = lax.rsqrt(two(nn, proj * proj, ones) * (1.0 / head) + EPS)
    return proj * inverse, inverse


def softmax_rows(query, key, value, valid, scale):
    scores = jnp.where(valid, nt(query, key) * scale, -1e30)
    raised = jnp.exp(scores - jnp.max(scores, axis=1, keepdims=True))
    probs = raised / jnp.sum(raised, axis=1, keepdims=True)
    return nn(probs.astype(BF), value).astype(BF)


def back_tile(query, key, value, grad, keys, queries, scale):
    scores = jnp.where(keys, nt(key, query) * scale, -1e30)
    raised = jnp.exp(scores - jnp.max(scores, axis=0, keepdims=True))
    probs = jnp.where(queries, raised / jnp.sum(raised, axis=0, keepdims=True), 0.0)
    d_value = nn(probs.astype(BF), grad)
    d_probs = nt(value, grad)
    inner = jnp.sum(probs * d_probs, axis=0, keepdims=True)
    d_scores = (probs * (d_probs - inner)).astype(BF)
    return tn(d_scores, key) * scale, nn(d_scores, query) * scale, d_value


def attention_back_kernel(head, spans, q, k, v, grad, dq, dk, dv):
    rows, wide = q.shape
    scale = head ** (-0.5)

    def each_head(fn):
        for n in range(wide // PAD):
            fn(slice(n * PAD, (n + 1) * PAD))

    for item in range(3):
        at = pl.ds(pl.multiple_of(spans[item], 16), TILE)
        keys = lax.broadcasted_iota(jnp.int32, (TILE, TILE), 0) < spans[4 + item]
        queries = lax.broadcasted_iota(jnp.int32, (TILE, TILE), 1) < spans[4 + item]

        def tile(lanes, at=at, keys=keys, queries=queries):
            parts = back_tile(
                q[at, lanes], k[at, lanes], v[at, lanes], grad[at, lanes], keys, queries, scale
            )
            for new, dst in zip(parts, (dq, dk, dv)):
                dst[at, lanes] = new.astype(BF)

        each_head(tile)
    first = rows - 48
    start = spans[3]
    at = pl.ds(first, 48)
    keys = first + lax.broadcasted_iota(jnp.int32, (48, 48), 0) >= start
    queries = first + lax.broadcasted_iota(jnp.int32, (48, 48), 1) >= start
    live = first + lax.broadcasted_iota(jnp.int32, (48, PAD), 0) >= start

    def rest(lanes):
        parts = back_tile(
            q[at, lanes], k[at, lanes], v[at, lanes], grad[at, lanes], keys, queries, scale
        )
        for new, dst in zip(parts, (dq, dk, dv)):
            dst[at, lanes] = jnp.where(live, new.astype(BF), dst[at, lanes])

    each_head(rest)


def local_call(kernel, micros, outs, scratch, spans, args):
    return pl.pallas_call(
        kernel,
        out_shape=outs,
        in_specs=[pl.BlockSpec(memory_space=pltpu.SMEM)] + [vmem()] * len(args),
        out_specs=[vmem()] * len(outs),
        scratch_shapes=scratch,
        compiler_params=pltpu.CompilerParams(vmem_limit_bytes=60 * 2**20),
        cost_estimate=price(micros),
    )(spans, *args)


def swap(array):
    return lax.ppermute(array, S, [(0, 1), (1, 0)])


def head_tables(packed, head):
    quarter = head // 4
    frequency = np.float32(10000.0) ** (-np.arange(quarter, dtype=np.float32) / quarter)
    lane = np.arange(head)
    angle = np.arange(32, dtype=np.float32)[:, None] * frequency[lane % quarter][None, :]
    by_row = (lane // (2 * quarter) == 0)[None, :]
    table = np.zeros((64, 2 * PAD), np.float32)
    for n, values in enumerate((np.cos(angle), np.sin(angle))):
        at = slice(n * PAD, n * PAD + head)
        table[:32, at] = np.where(by_row, values, 0.0)
        table[32:, at] = np.where(by_row, 0.0, values)
    table = jnp.asarray(table)
    parts = []
    for _ in range(3):
        parts.append(lax.reduce_precision(table, 8, 7).astype(BF))
        table = table - parts[-1].astype(F32)
    rows = np.arange(2 * PAD)[:, None]
    cols = np.arange(2 * PAD)[None, :]
    inside = (rows // PAD == cols // PAD) & (rows % PAD < head) & (cols % PAD < head)
    row, col = rows % PAD, cols % PAD
    early = (col % (2 * quarter)) < quarter
    turn = np.where(inside & early & (row == col + quarter), -1.0, 0.0)
    turn = turn + np.where(inside & ~early & (row == col - quarter), 1.0, 0.0)
    heads = packed // head
    rows = np.arange(packed)[:, None]
    wide = np.arange(heads * PAD)[None, :]
    spread = (rows // head == wide // PAD) & (rows % head == wide % PAD)
    lanes = tuple(jnp.asarray(m.astype(np.float32)).astype(BF) for m in (turn, inside, spread))
    return jnp.stack(parts), lanes


def reduced(total):
    return lax.psum_scatter(total, DP, scatter_dimension=0, tiled=True)[0]


def own_layer(section, pair):
    first = section == 0
    keep = jnp.where(first, pair[0], pair[1])
    got = swap(jnp.where(first, pair[1], pair[0]))
    return jnp.where(first, jnp.concatenate([keep, got]), jnp.concatenate([got, keep])).astype(F32)


def per_device(square, dp, tokens, cotangent, cond, patch_item, patch_pos, w_qkv, w_out, w_gate_up,
               w_down, qk_gain, ada_weight, ada_bias):
    section = lax.axis_index(S)
    first = section == 0
    rows, width = tokens.shape[1:]
    seq = patch_item.shape[1]
    items = cond.shape[0]
    head = qk_gain.shape[-1]
    packed = w_qkv.shape[-1]
    heads = packed // head
    hidden_here = w_down.shape[1]
    own = (jnp.swapaxes(w_qkv[0], 1, 2), w_out[0], w_gate_up[0], w_down[0])
    other = tuple(swap(w) for w in own)
    flat_qkv = (own[0].reshape(3 * packed, width), other[0].reshape(3 * packed, width))

    ada = ada_weight[0].T
    half = width // 2
    trig, (turn, ones, spread) = head_tables(packed, head)
    wide = heads * PAD
    mods, lifted_all, gains, sel, both, spans = ring_call(
        functools.partial(head_kernel, dp),
        8,
        12,
        [
            sds((2, 6, 8, width), F32),
            sds((dp, 16, width), F32),
            sds((2, 8, PAD), F32),
            sds((rows, 8), F32),
            sds((seq, 2 * PAD), F32),
            sds((8,), jnp.int32),
        ],
        [
            pltpu.VMEM((3 * half, width), BF),
            pltpu.VMEM((2, 3, 8, half), F32),
            pltpu.VMEM((8, 3, 8, half), F32),
            pltpu.VMEM((8, seq), F32),
            pltpu.VMEM((seq, 8), F32),
            pltpu.VMEM((16, width), F32),
            pltpu.VMEM((8, PAD), F32),
        ]
        + dma_sems(7 + dp)
        + [pltpu.SemaphoreType.DMA],
        (cond, ada, ada_bias, qk_gain[0], patch_item, patch_pos, trig),
        (1, 0, 1, 1, 1, 1, 1),
        scalar=5,
    )
    part = width // dp
    shard = lax.axis_index(DP)
    lifted_part = lax.dynamic_slice_in_dim(lifted_all, shard * part, part, 2)
    lifted_part = lifted_part.reshape(2 * dp, 8, part)

    x = tokens
    kept = []
    held = ring_call(
        functools.partial(qkv_kernel, 0, square),
        0,
        20,
        [sds((seq, width), BF), sds((2, seq, wide), BF)] + [sds((seq, wide), BF)] * 3,
        [pltpu.VMEM((rows, width), BF), pltpu.VMEM((3, wide, width), BF)]
        + dma_sems(6)
        + [pltpu.SemaphoreType.DMA((3 * heads,))],
        (x, sel, mods, gains, both, turn, ones, own[0], other[0]),
        (1,) * 7 + (0, 0),
    )
    for layer in range(2):
        whole1, proj, q, k, v = held
        (att,) = local_call(
            functools.partial(attention_kernel, head),
            6,
            [sds((seq, wide), BF)],
            [],
            spans,
            (q, k, v),
        )
        small = [sds((rows, width), F32)] * 3 + [sds((rows, width), BF)]
        large = [
            sds((seq, width), BF),
            sds((seq, hidden_here), F32),
            sds((seq, hidden_here), F32),
            sds((seq, hidden_here), BF),
        ]
        scratch = (
            [pltpu.VMEM(t.shape, t.dtype) for t in large]
            + [
                pltpu.VMEM((rows, width), BF),
                pltpu.VMEM((wide, width), BF),
                pltpu.VMEM((2, width, hidden_here), BF),
                pltpu.VMEM((hidden_here, width), BF),
            ]
            + scatter_scratch(rows, width)
            + scatter_scratch(rows, width)
            + dma_sems(18 if layer else 24)
            + [pltpu.SemaphoreType.DMA((7,)), pltpu.SemaphoreType.DMA((heads,))]
        )
        weights = (own[1], other[1], own[2], other[2], own[3], other[3])
        if layer:
            outs = ring_call(
                functools.partial(mlp_kernel, layer, square),
                3,
                48,
                small + large,
                scratch,
                (att, x, sel, mods) + weights,
                (1,) * 4 + (0,) * 6,
                loose=4,
            )
        else:
            outs = ring_call(
                functools.partial(mlp_qkv_kernel, layer, square),
                2,
                70,
                small
                + [sds((seq, width), BF), sds((2, seq, wide), BF)]
                + [sds((seq, wide), BF)] * 3
                + large,
                scratch
                + [pltpu.VMEM((3, wide, width), BF), pltpu.SemaphoreType.DMA((3 * heads,))],
                (att, x, sel, mods) + weights + (gains, both, turn, ones, own[0], other[0]),
                (1,) * 4 + (0,) * 6 + (1,) * 4 + (0, 0),
                loose=9,
            )
            held = outs[4:9]
        br1, x1, br2, y = outs[:4]
        whole2, gate, up, hidden = outs[-4:]
        kept.append((x, whole1, proj, q, k, v, att, br1, x1, whole2, gate, up, hidden, br2, y))
        x = y

    dy = cotangent
    packs = [None, None]
    prev = jnp.zeros((12, 8, half), F32)
    d_gains = [None, None]
    d_inputs = [None, None]
    for layer in (1, 0):
        x, whole1, proj, q, k, v, att, br1, x1, whole2, gate, up, hidden, br2, y = kept[layer]
        mod = mods
        rows1, datt, dx1, dmod_a, total_mlp = ring_call(
            functools.partial(mlp_back_kernel, layer, square),
            4 + layer,
            52,
            [
                sds((seq, width), BF),
                sds((seq, wide), BF),
                sds((rows, width), F32),
                sds((8, 8, half), F32),
                sds((dp, part // 2, 3 * hidden_here), BF),
            ],
            [pltpu.VMEM((dp, part // 2, 3 * hidden_here), BF)] * 3
            + [
                pltpu.VMEM((rows, width), BF),
                pltpu.VMEM((rows, width), BF),
                pltpu.VMEM((seq, width), BF),
                pltpu.VMEM((seq, hidden_here), BF),
                pltpu.VMEM((seq, hidden_here), BF),
                pltpu.VMEM((seq, hidden_here), F32),
                pltpu.VMEM((seq, hidden_here), F32),
                pltpu.VMEM((seq, hidden_here), BF),
                pltpu.VMEM((seq, width), BF),
                pltpu.VMEM((width, seq), BF),
                pltpu.VMEM((wide, width), BF),
                pltpu.VMEM((2, width, hidden_here), BF),
                pltpu.VMEM((hidden_here, width), BF),
            ]
            + scatter_scratch(rows, width)
            + dma_sems(21)
            + [pltpu.SemaphoreType.DMA((7,)), pltpu.SemaphoreType.DMA((heads,))],
            (dy, br2, br1, x1, sel, mod, gate, up, hidden, whole2, own[1], other[1], own[2],
             other[2], own[3], other[3]),
            (1,) * 6 + (0,) * 10,
        )
        pack_mlp = reduced(total_mlp)
        dq, dk, dv = local_call(
            functools.partial(attention_back_kernel, head),
            10,
            [sds((seq, wide), BF)] * 3,
            [],
            spans,
            (q, k, v, datt),
        )
        du, du_b, d_mod, total_att, dgain = ring_call(
            functools.partial(qkv_back_kernel, layer, square),
            6 + layer,
            22,
            [
                sds((rows, width), F32),
                sds((rows, width), BF),
                sds((2, 12, 8, half), F32),
                sds((dp, part // 2, 4 * packed), BF),
                sds((2, 1, wide), F32),
            ],
            [
                pltpu.VMEM((3 * packed, width), BF),
                pltpu.VMEM((seq, width), BF),
                pltpu.VMEM((seq, wide), BF),
                pltpu.VMEM((seq, width), BF),
                pltpu.VMEM((width, seq), BF),
                pltpu.VMEM((seq, 3 * packed), BF),
                pltpu.VMEM((seq, packed), BF),
            ]
            + [pltpu.VMEM((dp, part // 2, 4 * packed), BF)] * 3
            + scatter_scratch(rows, width)
            + dma_sems(7)
            + [pltpu.SemaphoreType.DMA((4,))],
            (dq, dk, dv, proj, gains, both, turn, ones, spread, x, dx1, sel, mod, dmod_a,
             prev, *flat_qkv, whole1, att, rows1),
            (1,) * 15 + (0,) * 5,
        )
        prev = d_mod[1]
        pack_att = reduced(total_att)
        packs[layer] = (pack_mlp, pack_att)
        d_gains[layer] = dgain
        d_inputs[layer] = du_b if layer else du
        dy = du_b

    gain_parts = jnp.pad(jnp.stack(d_gains).reshape(2, 2, wide), ((0, 0), (0, 6), (0, 0)))
    bias_part = ada_bias.shape[1] // dp
    g_ada_w, g_ada_b, cond_grad, gain_total = ring_call(
        functools.partial(tail_kernel, dp),
        9,
        15,
        [
            sds((part, 3 * half), F32),
            sds((1, bias_part), F32),
            sds((items, width), F32),
            sds((2, head), F32),
        ],
        [
            pltpu.VMEM((3 * half, width), BF),
            pltpu.VMEM((1, 3 * half), F32),
            pltpu.VMEM((8, 3, 8, half), F32),
            pltpu.VMEM((8, 8, wide), F32),
            pltpu.VMEM((3, 8, half), F32),
            pltpu.VMEM((8, wide), F32),
            pltpu.VMEM((dp, 3, 8, half), F32),
            pltpu.VMEM((dp, 8, wide), F32),
            pltpu.VMEM((8, 8, width), F32),
        ]
        + dma_sems(13 + 2 * (dp - 1) + 8)
        + [pltpu.SemaphoreType.DMA],
        (d_mod, gain_parts, lifted_part, cond, ada),
        (1, 1, 1, 1, 0),
    )

    f = hidden_here
    ready = lax.optimization_barrier((packs[0][0], packs[1][0], cond_grad))
    cond_grad = ready[2]
    mlp = own_layer(section, ready[:2])
    g_gate_up = jnp.stack([mlp[:, :f], mlp[:, f : 2 * f]])[None]
    g_down = mlp[:, 2 * f :].T[None]
    attn = own_layer(section, (packs[0][1], packs[1][1]))
    g_qkv = jnp.stack([attn[:, k * packed : (k + 1) * packed] for k in range(3)])[None]
    g_out = attn[:, 3 * packed :].T[None]

    outs = jnp.where(first, kept[0][-1], kept[1][-1])
    outs_got = swap(jnp.where(first, kept[1][-1], kept[0][-1]))
    layer_out = jnp.where(first, jnp.stack([outs, outs_got]), jnp.stack([outs_got, outs]))
    wide_mid = d_inputs[1].astype(F32)
    back_keep = jnp.where(first, d_inputs[0], wide_mid)
    back_got = swap(jnp.where(first, wide_mid, d_inputs[0]))
    in_grads = jnp.where(first, jnp.stack([back_keep, back_got]), jnp.stack([back_got, back_keep]))
    return (
        layer_out[None],
        in_grads[None],
        cond_grad,
        g_qkv,
        g_out,
        g_gate_up,
        g_down,
        gain_total[None],
        g_ada_w[None],
        g_ada_b,
    )


def solution(mesh):
    both = (DP, T)
    in_specs = (
        P(None, both, None),
        P(None, both, None),
        P(DP, None),
        P(None, DP),
        P(None, None, DP),
        P(S, None, None, T),
        P(S, T, None),
        P(S, None, None, T),
        P(S, T, None),
        P(S, None, None),
        P(S, None, T),
        P(S, T),
    )
    out_specs = (
        P(S, None, both, None),
        P(S, None, both, None),
        P(DP, None),
        P(S, None, DP, T),
        P(S, T, DP),
        P(S, None, DP, T),
        P(S, T, DP),
        P(S, None, None),
        P(S, DP, T),
        P(S, (T, DP)),
    )
    dp = mesh.shape[DP]

    def program(*args):
        return per_device(dp <= 4, dp, *args)

    return jax.shard_map(
        program, mesh=mesh, in_specs=in_specs, out_specs=out_specs, check_vma=False
    )
```

```python
import functools

import jax
import jax.numpy as jnp
import numpy as np
from jax import lax
from jax.experimental import pallas as pl
from jax.experimental.pallas import tpu as pltpu
from jax.sharding import PartitionSpec as P


EPS = 1e-06
F32 = jnp.float32
BF = jnp.bfloat16
S, DP, T = "section", "dp", "tensor"
PAD = 128
TILE = 256


def nn(a, b):
    return jnp.dot(a, b, preferred_element_type=F32)


def nt(a, b):
    return lax.dot_general(a, b, (((1,), (1,)), ((), ())), preferred_element_type=F32)


def tn(a, b):
    return lax.dot_general(a, b, (((0,), (0,)), ((), ())), preferred_element_type=F32)


def two(dot, a, b):
    high = a.astype(BF)
    low = (a - high.astype(F32)).astype(BF)
    return dot(high, b) + dot(low, b)


def sds(shape, dtype):
    return jax.ShapeDtypeStruct(shape, dtype)


def vmem():
    return pl.BlockSpec(memory_space=pltpu.VMEM)


def anywhere():
    return pl.BlockSpec(memory_space=pl.ANY)


def ring(square):
    me = lax.axis_index(T)
    near = me + 1 - 2 * (me % 2)
    if square:
        return me, near, me + 2 - 4 * (me // 2), 3 - me, True
    return me, near, 3 - me, (me + 2) % 4, False


def pieces(place, step, half):
    me, upper, moved, far = place[0], (step % 3) // 2, (step + 2) // 3, step // 3
    near = moved - far
    low = (moved, far) if place[4] else (near, near)
    found = []
    for side, high in ((0, far), (1, moved)):
        chunk = (me % 2 + low[side]) % 2 + 2 * ((me // 2 + high) % 2)
        row = (2 * chunk + (1 - upper if side else upper)) * half
        found.append(pl.ds(pl.multiple_of(row, half), half))
    return found


def joined(ref, rows):
    return jnp.concatenate([ref[rows[0]], ref[rows[1]]], axis=0)


def put(ref, rows, values):
    half = values.shape[0] // 2
    ref[rows[0]] = values[:half].astype(ref.dtype)
    ref[rows[1]] = values[half:].astype(ref.dtype)


def farthest_first(place, step):
    me, low = place[0], ((step + 1) // 2) % 2
    if place[4]:
        low = (3 - step) // 2
    return (me % 2 + low) % 2 + 2 * ((me // 2 + (step + 1) % 2) % 2)


def near_first(place, step):
    me, low = place[0], (3 - step) // 2
    if place[4]:
        low = (step + 1) % 2
    return (me % 2 + low) % 2 + 2 * ((me // 2 + ((step + 1) // 2) % 2) % 2)


def greet(place, partner=False):
    sem = pltpu.get_barrier_semaphore()
    peers = (place[1], place[2]) if place else ()
    for peer in peers:
        pl.semaphore_signal(
            sem, inc=1, device_id={T: peer}, device_id_type=pl.DeviceIdType.MESH
        )
    if partner:
        pl.semaphore_signal(
            sem, inc=1, device_id={S: 1 - lax.axis_index(S)}, device_id_type=pl.DeviceIdType.MESH
        )
    pl.semaphore_wait(sem, len(peers) + partner)


def remote(src, dst, sems, index, peer):
    return pltpu.make_async_remote_copy(
        src_ref=src,
        dst_ref=dst,
        send_sem=sems[0].at[index],
        recv_sem=sems[1].at[index],
        device_id={T: peer},
        device_id_type=pl.DeviceIdType.MESH,
    )


def chunk_rows(chunk, rows):
    return pl.ds(pl.multiple_of(chunk * rows, rows), rows)


def repeat(body, times):
    def one(step, carry):
        body(step)
        return carry

    lax.fori_loop(0, times, one, 0)


def gather(place, mine, whole, sems, base, use, ready=lambda: None, late=lambda: None, last=None):
    me, a, b, _, _ = place
    rows = mine.shape[0]
    half = rows // 2
    lo, hi = pl.ds(0, half), pl.ds(half, half)

    def part(chunk, upper):
        return whole.at[pl.ds(pl.multiple_of(chunk * rows + upper * half, half), half)]

    a0 = remote(mine.at[lo], part(me, 0), sems, base, a)
    b0 = remote(mine.at[hi], part(me, 1), sems, base + 1, b)
    a1 = remote(mine.at[hi], part(me, 1), sems, base + 2, a)
    b1 = remote(mine.at[lo], part(me, 0), sems, base + 3, b)
    b2 = remote(part(a, 0), part(a, 0), sems, base + 4, b)
    a2 = remote(part(b, 1), part(b, 1), sems, base + 5, a)
    for copy in (a0, b0, a1, b1):
        copy.start()
    whole[chunk_rows(me, rows), :] = mine[...]
    ready()

    def final():
        b2.wait_recv()
        a2.wait_recv()

    def body(step):
        @pl.when(step == 1)
        def _():
            a0.wait_recv()
            b2.start()
            b0.wait_recv()
            a2.start()

        @pl.when(step == 2)
        def _():
            a1.wait_recv()
            b1.wait_recv()

        if last is None:

            @pl.when(step == 3)
            def _():
                late()
                final()

        use(pieces(place, step, half))

    repeat(body, 4 if last is None else 3)
    if last is not None:
        last(final)
    for copy in (a0, b0, a1, b1, a2, b2):
        copy.wait_send()


def scatter(place, term, bufs, sems, base, fill=lambda: None, before=None):
    _, a, b, _, _ = place
    out, into, keep, own = bufs
    half = keep.shape[1]
    lo, hi = pl.ds(0, half), pl.ds(half, half)
    d0 = remote(out.at[0, lo], into.at[0, lo], sems, base, a)
    d1 = remote(out.at[0, hi], into.at[0, hi], sems, base + 1, b)
    a0 = remote(out.at[1, lo], into.at[1, lo], sems, base + 2, a)
    b0 = remote(out.at[2, hi], into.at[2, hi], sems, base + 3, b)
    a1 = remote(out.at[1, hi], into.at[1, hi], sems, base + 4, a)
    b1 = remote(out.at[2, lo], into.at[2, lo], sems, base + 5, b)
    at = (0, 1, 2) if before is None else (2, 0, 1)

    def body(step):
        if before is None:
            chunk = farthest_first(place, step)
        else:
            chunk = near_first(place, step)
            pl.when(step == 2)(before)
        own[...] = term(chunk)

        @pl.when(step == at[0])
        def _():
            out[0] = own[...].astype(BF)
            d0.start()
            d1.start()

        @pl.when(step == at[1])
        def _():
            out[1, lo] = own[lo].astype(BF)
            a0.start()
            keep[0] = own[hi]

        @pl.when(step == at[2])
        def _():
            out[2, hi] = own[hi].astype(BF)
            b0.start()
            keep[1] = own[lo]

    repeat(body, 4)
    d1.wait_recv()
    out[1, hi] = (keep[0] + into[0, hi].astype(F32)).astype(BF)
    a1.start()
    d0.wait_recv()
    out[2, lo] = (keep[1] + into[0, lo].astype(F32)).astype(BF)
    b1.start()
    fill()
    for copy in (a0, b0, a1, b1):
        copy.wait_recv()
    for copy in (d0, d1, a0, b0, a1, b1):
        copy.wait_send()


def gather_scatter(place, mine, whole, sems, base, use, term, bufs, ready, fill=lambda: None):
    def last(final):
        def before():
            final()
            use(pieces(place, 3, mine.shape[0] // 2))

        scatter(place, term, bufs, sems, base + 6, fill, before)

    gather(place, mine, whole, sems, base, use, ready, last=last)


def scattered(bufs, rows):
    return bufs[3][rows] + bufs[1][1, rows].astype(F32) + bufs[1][2, rows].astype(F32)


def scatter_scratch(rows, width):
    return [
        pltpu.VMEM((3, rows, width), BF),
        pltpu.VMEM((3, rows, width), BF),
        pltpu.VMEM((2, rows // 2, width), F32),
        pltpu.VMEM((rows, width), F32),
    ]


def dma_sems(count):
    return [pltpu.SemaphoreType.DMA((count,)), pltpu.SemaphoreType.DMA((count,))]


def layer_weights(own, other, layer, dst, sem):
    mine = lax.axis_index(S) == layer

    @pl.when(mine)
    def _():
        pltpu.make_async_copy(own, dst, sem).start()

    @pl.when(jnp.logical_not(mine))
    def _():
        pltpu.make_async_copy(other, dst, sem).start()

    return pltpu.make_async_copy(own, dst, sem)


def head_weights(own, other, layer, dst, sems, parts):
    mine = lax.axis_index(S) == layer
    spread = len(parts) > 1
    heads = dst.shape[-2] // PAD
    head = own.shape[-2] // heads
    clean = head // 16 * 16
    copies = ([], [])
    for n, part in enumerate(parts):
        for h in range(heads):
            to = dst.at[part] if spread else dst
            to[pl.ds(h * PAD + clean, PAD - clean)] = jnp.zeros((PAD - clean, dst.shape[-1]), BF)
            to = to.at[pl.ds(h * PAD, head)]
            for which, src in enumerate((own, other)):
                src = src.at[part] if spread else src
                copies[which].append(
                    pltpu.make_async_copy(
                        src.at[pl.ds(h * head, head)], to, sems.at[n * heads + h]
                    )
                )

    @pl.when(mine)
    def _():
        for copy in copies[0]:
            copy.start()

    @pl.when(jnp.logical_not(mine))
    def _():
        for copy in copies[1]:
            copy.start()

    return copies[0]


def arrive(copies):
    for copy in copies:
        copy.wait()


def twice(row):
    return jnp.concatenate([row, row], axis=-1)


def over_blocks(rows, fn):
    step = rows // 4

    def body(i, carry):
        fn(pl.ds(pl.multiple_of(i * step, step), step))
        return carry

    lax.fori_loop(0, 4, body, 0)


def mod_rows(sel, mod, which):
    total = sel[:, 0:1] * mod[which, 0:1]
    for item in (1, 2):
        total = total + sel[:, item : item + 1] * mod[which, item : item + 1]
    return total


def add_sums(dmod, block, sel, values):
    sums = item_sums(sel, values)
    half = dmod.shape[2]
    dmod[2 * block] += sums[:, :half]
    dmod[2 * block + 1] += sums[:, half:]


def weight_grad(x, y, flipped, col, packs):
    mine, theirs, _ = packs
    dp, part, _ = mine.shape
    first = lax.axis_index(S) == 0
    width = y.shape[1]
    if x is not None:
        flipped[...] = x[...].T

    def one(to, columns):
        grad = nn(flipped[...], columns).astype(BF)
        grad = grad.reshape(dp, 2, part, columns.shape[1])

        @pl.when(first)
        def _():
            mine[:, :, to] = grad[:, 0]
            theirs[:, :, to] = grad[:, 1]

        @pl.when(jnp.logical_not(first))
        def _():
            mine[:, :, to] = grad[:, 1]
            theirs[:, :, to] = grad[:, 0]

    if width % 256:
        one(pl.ds(col, width), y[...])
        return

    def body(i, carry):
        at = pl.multiple_of(i * 256, 256)
        one(pl.ds(pl.multiple_of(col + at, 256), 256), y[:, pl.ds(at, 256)])
        return carry

    lax.fori_loop(0, width // 256, body, 0)


def half_copy(packs, sems, index, col, width):
    at = pl.ds(col, width)
    return pltpu.make_async_remote_copy(
        src_ref=packs[1].at[:, :, at],
        dst_ref=packs[2].at[:, :, at],
        send_sem=sems[0].at[index],
        recv_sem=sems[1].at[index],
        device_id={S: 1 - lax.axis_index(S)},
        device_id_type=pl.DeviceIdType.MESH,
    )


def send_half(packs, sems, index, col, width):
    copy = half_copy(packs, sems, index, col, width)
    copy.start()
    return copy


def add_halves(packs, copies, total, col, width):
    at = pl.ds(col, width)
    for copy in copies:
        copy.wait_recv()

    def body(k):
        total[k, :, at] = (packs[0][k, :, at].astype(F32) + packs[2][k, :, at].astype(F32)).astype(BF)

    repeat(body, total.shape[0])
    for copy in copies:
        copy.wait_send()


def item_sums(sel, values):
    high = values.astype(BF)
    low = (values - high.astype(F32)).astype(BF)
    sel_b = sel.astype(BF)
    return tn(sel_b, high) + tn(sel_b, low)


def normed(values):
    inverse = lax.rsqrt(jnp.mean(values * values, axis=-1, keepdims=True) + EPS)
    return values * inverse, inverse


def norm_back(incoming, normal, inverse):
    return inverse * (incoming - normal * jnp.mean(incoming * normal, axis=-1, keepdims=True))


def tokens_of(ref):
    return ref.at[lax.axis_index(S)] if len(ref.shape) == 3 else ref


def qkv_kernel(layer, square, x, sel, mod, gain, both, turn, ones, w_own, w_other, whole, proj, q,
               k, v, h, w, ssem, rsem, wsem):
    place = ring(square)
    load = head_weights(w_own, w_other, layer, w, wsem, range(3))
    greet(place)
    head = w_own.shape[1] * PAD // w.shape[1]
    qkv_part(
        place, head, tokens_of(x), sel, mod.at[layer], gain.at[layer], both, turn, ones, load,
        whole, proj, q, k, v, h, w, (ssem, rsem), 0
    )


def qkv_part(place, head, x, sel, mod, gain, both, turn, ones, load, whole, proj, q, k, v, h, w,
             sems, base):
    def prepare(rows):
        normal, _ = normed(x[rows].astype(F32))
        shift = mod_rows(sel[rows], mod, 0)
        scale = mod_rows(sel[rows], mod, 1)
        h[rows] = (normal * (1.0 + scale) + shift).astype(BF)

    over_blocks(x.shape[0], prepare)

    def use(rows):
        held = joined(whole, rows)
        table = joined(both, rows)
        cosine = twice(table[:, 0:PAD])
        sine = twice(table[:, PAD : 2 * PAD])
        for which, dst in ((0, q), (1, k)):
            full = nt(held, w[which])
            put(proj.at[which], rows, full)
            turned = []
            for pair in range(full.shape[1] // (2 * PAD)):
                lanes = slice(pair * 2 * PAD, (pair + 1) * 2 * PAD)
                normal, _ = unit(full[:, lanes], ones[...], head)
                gained = normal * twice(gain[which : which + 1])
                turned.append(gained * cosine + two(nn, gained, turn[...]) * sine)
            put(dst, rows, jnp.concatenate(turned, axis=1))
        put(v, rows, nt(held, w[2]))

    gather(place, h, whole, sems, base, use, lambda: arrive(load))


def mlp_qkv_kernel(layer, square, att, x, sel, mod, wo0, wo1, wg0, wg1, wd0, wd1, gain, both, turn,
                   ones, w_own, w_other, br1, x1, br2, y, whole_q, proj, q, k, v, whole_h, gate_h,
                   up_h, hidden_h, whole, gate, up, hidden, h, wo, wg, wd, o1, i1, k1, s1, o2, i2,
                   k2, s2, ssem, rsem, wsem, osem, w, hsem):
    place = ring(square)
    load = head_weights(w_own, w_other, layer + 1, w, hsem, range(3))
    mlp_kernel(
        layer, square, att, x, sel, mod, wo0, wo1, wg0, wg1, wd0, wd1, br1, x1, br2, y, whole_h,
        gate_h, up_h, hidden_h, whole, gate, up, hidden, h, wo, wg, wd, o1, i1, k1, s1, o2, i2, k2,
        s2, ssem, rsem, wsem, osem
    )
    head = w_own.shape[1] * PAD // w.shape[1]
    qkv_part(
        place, head, y, sel, mod.at[layer + 1], gain.at[layer + 1], both, turn, ones, load, whole_q,
        proj, q, k, v, h, w, (ssem, rsem), 18
    )


def mlp_kernel(layer, square, att, x, sel, mod, wo0, wo1, wg0, wg1, wd0, wd1, br1, x1, br2, y,
               whole_h, gate_h, up_h, hidden_h, whole, gate, up, hidden, h, wo, wg, wd, o1, i1, k1, s1, o2, i2, k2, s2,
               ssem, rsem, wsem, osem):
    x, mod = tokens_of(x), mod.at[layer]
    place = ring(square)
    rows_here, _ = x.shape
    load_o = head_weights(wo0, wo1, layer, wo, osem, range(1))
    load_g = layer_weights(wg0, wg1, layer, wg, wsem.at[1])
    load_d = layer_weights(wd0, wd1, layer, wd, wsem.at[2])
    greet(place)
    sems = (ssem, rsem)
    arrive(load_o)
    first = (o1, i1, k1, s1)
    scatter(place, lambda c: nn(att[chunk_rows(c, rows_here)], wo[...]), first, sems, 0)

    def between(rows):
        branch = scattered(first, rows)
        br1[rows] = branch
        mixed = x[rows].astype(F32) + mod_rows(sel[rows], mod, 2) * branch
        x1[rows] = mixed
        normal, _ = normed(mixed)
        shift = mod_rows(sel[rows], mod, 3)
        scale = mod_rows(sel[rows], mod, 4)
        h[rows] = (normal * (1.0 + scale) + shift).astype(BF)

    over_blocks(rows_here, between)

    def use(rows):
        held = joined(whole, rows)
        g = nn(held, wg[0])
        put(gate, rows, g)
        u = nn(held, wg[1])
        put(up, rows, u)
        put(hidden, rows, g * jax.nn.sigmoid(g) * u)

    second = (o2, i2, k2, s2)
    stores = []
    for n, (src, dst) in enumerate(
        ((whole, whole_h), (gate, gate_h), (up, up_h), (hidden, hidden_h))
    ):
        stores.append(pltpu.make_async_copy(src, dst, wsem.at[3 + n]))

    def ready():
        load_g.wait()
        load_d.wait()

    def fill():
        for copy in stores:
            copy.start()

    def term(chunk):
        return nn(hidden[chunk_rows(chunk, rows_here)], wd[...])

    gather_scatter(place, h, whole, sems, 6, use, term, second, ready, fill)

    def finish(rows):
        branch = scattered(second, rows)
        br2[rows] = branch
        y[rows] = (x1[rows] + mod_rows(sel[rows], mod, 5) * branch).astype(BF)

    over_blocks(rows_here, finish)
    arrive(stores)


def mlp_back_kernel(layer, square, dy, br2, br1, x1, sel, mod, gate_h, up_h, hidden_h, rows_h,
                    wo0, wo1, wg0, wg1, wd0, wd1, whole1, datt, dx1, dmod, total, mine, theirs,
                    got, h, h1, whole2, dgate, dup, gate, up, hidden, saved, flipped, wo, wg, wd, o1, i1, k1,
                    s1, ssem, rsem, wsem, osem):
    dy, mod = tokens_of(dy), mod.at[layer]
    place = ring(square)
    rows_here, _ = dy.shape
    load_d = layer_weights(wd0, wd1, layer, wd, wsem.at[0])
    load_gate = pltpu.make_async_copy(gate_h, gate, wsem.at[1])
    load_gate.start()
    load_up = pltpu.make_async_copy(up_h, up, wsem.at[2])
    load_up.start()
    load_g = layer_weights(wg0, wg1, layer, wg, wsem.at[3])
    load_o = head_weights(wo0, wo1, layer, wo, osem, range(1))
    load_hidden = pltpu.make_async_copy(hidden_h, hidden, wsem.at[5])
    load_hidden.start()
    load_rows = pltpu.make_async_copy(rows_h, saved, wsem.at[6])
    load_rows.start()
    greet(place, True)
    sems = (ssem, rsem)
    dmod[...] = jnp.zeros_like(dmod)

    def prepare(rows):
        incoming = dy[rows].astype(F32)
        h[rows] = (incoming * mod_rows(sel[rows], mod, 5)).astype(BF)
        add_sums(dmod, 3, sel[rows], incoming * br2[rows])

    over_blocks(rows_here, prepare)

    def ready():
        arrive((load_d, load_gate, load_up, load_g, load_hidden))

    def use(rows):
        d_hidden = nt(joined(whole2, rows), wd[...])
        g = joined(gate, rows)
        s = jax.nn.sigmoid(g)
        put(dgate, rows, d_hidden * joined(up, rows) * s * (1.0 + g * (1.0 - s)))
        put(dup, rows, d_hidden * g * s)

    bufs = (o1, i1, k1, s1)
    f = hidden.shape[1]

    def term(chunk):
        rows = chunk_rows(chunk, rows_here)
        return nt(dgate[rows], wg[0]) + nt(dup[rows], wg[1])

    packs = (mine, theirs, got)
    copies = []

    def grad(index, x, y, col):
        weight_grad(x, y, flipped, col, packs)
        copies.append(send_half(packs, sems, index, col, f))

    def grad_down():
        grad(18, whole2, hidden, 2 * f)

    gather_scatter(place, h, whole2, sems, 0, use, term, bufs, ready, grad_down)

    def between(rows):
        d_h = scattered(bufs, rows)
        normal, inverse = normed(x1[rows])
        scale = mod_rows(sel[rows], mod, 4)
        d_mixed = dy[rows].astype(F32) + norm_back(d_h * (1.0 + scale), normal, inverse)
        dx1[rows] = d_mixed
        h1[rows] = (d_mixed * mod_rows(sel[rows], mod, 2)).astype(BF)

    over_blocks(rows_here, between)

    def use_out(rows):
        put(datt, rows, nt(joined(whole1, rows), wo[...]))

    def sums():
        def one(rows):
            d_h = scattered(bufs, rows)
            normal, _ = normed(x1[rows])
            add_sums(dmod, 1, sel[rows], d_h)
            add_sums(dmod, 2, sel[rows], d_h * normal)
            add_sums(dmod, 0, sel[rows], dx1[rows] * br1[rows])

        over_blocks(rows_here, one)
        arrive(load_o)
        load_rows.wait()
        grad(19, saved, dgate, 0)

    def late():
        weight_grad(None, dup, flipped, f, packs)
        last.start()
        add_halves(packs, copies[:1], total, 2 * f, f)
        add_halves(packs, copies[1:2], total, 0, f)

    last = half_copy(packs, sems, 20, f, f)
    gather(place, h1, whole1, sems, 12, use_out, sums, late)
    add_halves(packs, [last], total, f, f)


def qkv_back_kernel(layer, square, dq, dk, dv, proj, gain, both, turn, ones, spread, x, dx1, sel,
                    mod, part, prev, w_own, w_other, whole_h, att_h, rows1_h, du, du_b, dmod, total,
                    dgain, w, whole, att, rows1, flipped, dpack, flat, mine, theirs, got, o1, i1,
                    k1, s1, ssem, rsem, wsem):
    x, mod, gain = tokens_of(x), mod.at[layer], gain.at[layer]
    place = ring(square)
    rows_here, _ = x.shape
    packed = spread.shape[0]
    head = packed * PAD // spread.shape[1]
    load = layer_weights(w_own, w_other, layer, w, wsem.at[3])
    loads = []
    for n, (src, dst) in enumerate(((whole_h, whole), (att_h, att), (rows1_h, rows1))):
        loads.append(pltpu.make_async_copy(src, dst, wsem.at[n]))
        loads[n].start()
    greet(place, True)
    here = dmod.at[layer]
    dmod[1 - layer] = prev[...]
    here[pl.ds(0, 4)] = jnp.zeros_like(prev[pl.ds(0, 4)])
    here[pl.ds(4, 8)] = part[...]
    dgain[...] = jnp.zeros_like(dgain)
    load.wait()
    bufs = (o1, i1, k1, s1)
    sems = (ssem, rsem)
    packs = (mine, theirs, got)
    copies = []

    def term(chunk):
        rows = chunk_rows(chunk, rows_here)
        cosine = twice(both[rows, 0:PAD])
        sine = twice(both[rows, PAD : 2 * PAD])
        for which, src in ((0, dq), (1, dk)):
            parts = []
            for pair in range(src.shape[1] // (2 * PAD)):
                lanes = slice(pair * 2 * PAD, (pair + 1) * 2 * PAD)
                turned = src[rows, lanes]
                back = turned.astype(F32) * cosine - nn(turned, turn[...]) * sine
                normal, inverse = unit(proj[which, rows, lanes].astype(F32), ones[...], head, nn_low)
                dgain[which, :, lanes] += jnp.sum(back * normal, axis=0, keepdims=True)
                gained = back * twice(gain[which : which + 1])
                mean = nn_low(gained * normal, ones[...]) * (1.0 / head)
                parts.append((inverse * (gained - normal * mean)).astype(BF))
            full = jnp.concatenate(parts, axis=1)
            dpack[rows, which * packed : (which + 1) * packed] = nt(full, spread[...]).astype(BF)
        dpack[rows, 2 * packed : 3 * packed] = nt(dv[rows], spread[...]).astype(BF)
        return nn(dpack[rows], w[...])

    def grads():
        loads[0].wait()
        flipped[...] = whole[...].T
        for col in range(0, 3 * packed, TILE):
            size = min(TILE, 3 * packed - col)
            weight_grad(None, dpack.at[:, col : col + size], flipped, col, packs)
        loads[1].wait()
        loads[2].wait()
        flat[...] = nt(att[...], spread[...]).astype(BF)
        weight_grad(rows1, flat, flipped, 3 * packed, packs)
        copies.append(send_half(packs, sems, 6, 0, 4 * packed))

    scatter(place, term, bufs, sems, 0, grads)

    def finish(rows):
        d_h = scattered(bufs, rows)
        normal, inverse = normed(x[rows].astype(F32))
        scale = mod_rows(sel[rows], mod, 1)
        total_rows = dx1[rows] + norm_back(d_h * (1.0 + scale), normal, inverse)
        du[rows] = total_rows
        du_b[rows] = total_rows.astype(BF)
        add_sums(here, 0, sel[rows], d_h)
        add_sums(here, 1, sel[rows], d_h * normal)

    over_blocks(rows_here, finish)
    add_halves(packs, copies, total, 0, 4 * packed)


def cell():
    return 4 * lax.axis_index(S) + lax.axis_index(T)


def cell_id(index):
    return {S: index // 4, T: index % 4}


def greet_all(dp):
    sem = pltpu.get_barrier_semaphore()
    here, shard = cell(), lax.axis_index(DP)
    for k in range(1, 8):
        pl.semaphore_signal(
            sem, inc=1, device_id=cell_id((here + k) % 8), device_id_type=pl.DeviceIdType.MESH
        )
    for k in range(1, dp):
        pl.semaphore_signal(
            sem, inc=1, device_id={DP: (shard + k) % dp}, device_id_type=pl.DeviceIdType.MESH
        )
    pl.semaphore_wait(sem, 7 + dp - 1)


def push(src, dst, sems, index, device):
    copy = pltpu.make_async_remote_copy(
        src_ref=src,
        dst_ref=dst,
        send_sem=sems[0].at[index],
        recv_sem=sems[1].at[index],
        device_id=device,
        device_id_type=pl.DeviceIdType.MESH,
    )
    copy.start()
    return copy


def head_kernel(dp, cond, ada_h, bias, gain_own, items, pos, tables, mod, lifted_all, gains, sel,
                both, spans, ada, parts, got, wide, tall, lifted, gain, ssem, rsem, wsem):
    load = pltpu.make_async_copy(ada_h, ada, wsem)
    load.start()
    lifted[...] = jnp.zeros_like(lifted)
    raw = cond[...].astype(F32)
    raw = (raw * jax.nn.sigmoid(raw)).astype(BF).astype(F32)
    lifted[0:3] = raw[0:3]
    lifted[8:11] = raw[3:6]
    gain[...] = jnp.zeros_like(gain)
    gain[0:2, 0 : gain_own.shape[1]] = gain_own[...].astype(F32)
    biases = bias[...].astype(F32)
    greet_all(dp)
    sems = (ssem, rsem)
    here, shard, section = cell(), lax.axis_index(DP), lax.axis_index(S)
    copies = [push(gain, gains.at[section], sems, 6 + dp, {S: 1 - section})]
    gains[section] = gain[...]
    lifted_all[shard] = lifted[...]
    for k in range(1, dp):
        copies.append(
            push(lifted, lifted_all.at[shard], sems, 6 + k, {DP: (shard + k) % dp})
        )
    load.wait()
    half = parts.shape[3]
    for j in range(3):
        here_bias = biases[:, j * half : (j + 1) * half]
        made = nt(lifted[...].astype(BF), ada[pl.ds(j * half, half)]) + here_bias
        parts[0, j] = made[0:8]
        parts[1, j] = made[8:16]
    for k in range(1, 8):
        peer = (here + k) % 8
        copies.append(push(parts.at[peer // 4], got.at[here], sems, k - 1, cell_id(peer)))
    got[here] = parts[section]
    rows_here = sel.shape[0]
    base = shard * 6 + section * 3
    seq = items.shape[1]
    line = items[pl.ds(section, 1), :]
    wide[...] = jnp.zeros_like(wide)
    wide[0:1] = (line - base).astype(F32)
    wide[1:2] = pos[0, pl.ds(section, 1), :].astype(F32)
    wide[2:3] = pos[1, pl.ds(section, 1), :].astype(F32)
    start = 0
    spans[0] = 0
    for j in range(3):
        count = jnp.sum((wide[0:1] == j).astype(F32)).astype(jnp.int32)
        spans[4 + j] = count
        start = start + count
        spans[1 + j] = start
    spans[7] = 0
    tall[...] = wide[...].T
    own = tall[pl.ds(pl.multiple_of(lax.axis_index(T) * rows_here, rows_here), rows_here), :]
    lane = lax.broadcasted_iota(jnp.int32, (rows_here, 8), 1).astype(F32)
    sel[...] = ((own[:, 0:1] == lane) & (lane < 3.0)).astype(F32)
    lane = lax.broadcasted_iota(jnp.int32, (seq, 64), 1).astype(F32)
    hot = jnp.where(lane < 32.0, tall[:, 1:2], tall[:, 2:3] + 32.0) == lane
    hot = hot.astype(F32).astype(BF)
    both[...] = (nn(hot, tables[0]) + nn(hot, tables[1])) + nn(hot, tables[2])
    for copy in copies:
        copy.wait_recv()
    for layer in range(2):
        for block in range(6):
            for side in range(2):
                n = 2 * block + side
                mod[layer, block, :, pl.ds(side * half, half)] = got[4 * layer + n // 3, n % 3]
    for copy in copies:
        copy.wait_send()


def tail_kernel(dp, dmod, dgain, lifted_part, cond, ada_h, ada_grad, bias_grad, cond_grad, gain_grad,
                ada, bias_row, got, got_gain, total, total_gain, every, every_gain, lifts, ssem, rsem, wsem):
    load = pltpu.make_async_copy(ada_h, ada, wsem)
    load.start()
    greet_all(dp)
    sems = (ssem, rsem)
    here, shard = cell(), lax.axis_index(DP)
    section, place = lax.axis_index(S), lax.axis_index(T)
    sends, arrivals = [], []
    for k in range(1, 8):
        peer = (here + k) % 8
        to = cell_id(peer)
        arrivals.append(
            push(dmod.at[peer // 4, pl.ds(3 * (peer % 4), 3)], got.at[here], sems, k - 1, to)
        )
        arrivals.append(push(dgain.at[peer // 4], got_gain.at[here], sems, 6 + k, to))
    got[here] = dmod[section, pl.ds(3 * place, 3)]
    got_gain[here] = dgain[section]
    for copy in arrivals:
        copy.wait_recv()
    sends += arrivals
    total[...] = jnp.zeros_like(total)
    for micro in range(2):
        summed = (got[4 * micro] + got[4 * micro + 1]) + (got[4 * micro + 2] + got[4 * micro + 3])
        total[:, 3 * micro : 3 * micro + 3] = summed[:, 0:3]
    gain = got_gain[0]
    for k in range(1, 8):
        gain = gain + got_gain[k]
    total_gain[...] = gain
    arrivals = []
    for k in range(1, dp):
        to = {DP: (shard + k) % dp}
        arrivals.append(push(total, every.at[shard], sems, 13 + k, to))
        arrivals.append(push(total_gain, every_gain.at[shard], sems, 12 + dp + k, to))
    every[shard] = total[...]
    every_gain[shard] = total_gain[...]
    load.wait()
    half = total.shape[2]
    lift = two(nn, total[0], ada[pl.ds(0, half)])
    for j in range(1, 3):
        lift = lift + two(nn, total[j], ada[pl.ds(j * half, half)])
    lifts[here] = lift
    base = 13 + 2 * (dp - 1)
    lift_copies = []
    for k in range(1, 8):
        lift_copies.append(
            push(lifts.at[here], lifts.at[here], sems, base + k, cell_id((here + k) % 8))
        )
    for copy in arrivals:
        copy.wait_recv()
    sends += arrivals
    gain = every_gain[0]
    for k in range(1, dp):
        gain = gain + every_gain[k]
    heads = gain.shape[1] // PAD
    summed = gain[:, 0:PAD]
    for h in range(1, heads):
        summed = summed + gain[:, h * PAD : (h + 1) * PAD]
    gain_grad[...] = summed[0:2, 0 : gain_grad.shape[1]]
    for j in range(3):
        bias = jnp.zeros((1, half), F32)
        grad = jnp.zeros((lifted_part.shape[2], half), F32)
        for k in range(dp):
            block = every[k, j, 0:6]
            bias = bias + jnp.sum(block, axis=0, keepdims=True)
            high = block.astype(BF)
            low = (block - high.astype(F32)).astype(BF)
            rows = jnp.concatenate([lifted_part[2 * k, 0:3], lifted_part[2 * k + 1, 0:3]], axis=0)
            rows = rows.astype(BF)
            grad = grad + tn(rows, high) + tn(rows, low)
        bias_row[:, pl.ds(j * half, half)] = bias
        ada_grad[:, pl.ds(j * half, half)] = grad
    for copy in lift_copies:
        copy.wait_recv()
    sends += lift_copies
    lift = lifts[0]
    for k in range(1, 8):
        lift = lift + lifts[k]
    raw = cond[...].astype(F32)
    s = jax.nn.sigmoid(raw)
    factor = s * (1.0 + raw * (1.0 - s))
    cond_grad[...] = lift[0:6] * factor
    part = bias_grad.shape[1]
    row = bias_row[...]
    total_bias = jnp.zeros((1, part), F32)
    for k in range(dp):
        chosen = (shard == k).astype(F32)
        total_bias = total_bias + row[:, k * part : (k + 1) * part] * chosen
    bias_grad[...] = total_bias
    for copy in sends:
        copy.wait_send()


def price(micros):
    return pl.CostEstimate(flops=0, bytes_accessed=int(micros * 3.5e6), transcendentals=0)


def ring_call(kernel, ident, micros, outs, scratch, args, spaces, scalar=-1, loose=99):
    return pl.pallas_call(
        kernel,
        out_shape=outs,
        in_specs=[vmem() if s else anywhere() for s in spaces],
        out_specs=[
            pl.BlockSpec(memory_space=pltpu.SMEM)
            if n == scalar
            else (vmem() if n < loose else anywhere())
            for n in range(len(outs))
        ],
        scratch_shapes=scratch,
        compiler_params=pltpu.CompilerParams(
            collective_id=ident, has_side_effects=True, vmem_limit_bytes=60 * 2**20
        ),
        cost_estimate=price(micros),
    )(*args)


def attention_kernel(head, spans, q, k, v, att):
    rows, wide = q.shape
    scale = head ** (-0.5)

    def each_head(fn):
        for n in range(wide // PAD):
            fn(slice(n * PAD, (n + 1) * PAD))

    for item in range(3):
        at = pl.ds(pl.multiple_of(spans[item], 16), TILE)
        valid = lax.broadcasted_iota(jnp.int32, (TILE, TILE), 1) < spans[4 + item]

        def tile(lanes, at=at, valid=valid):
            att[at, lanes] = softmax_rows(q[at, lanes], k[at, lanes], v[at, lanes], valid, scale)

        each_head(tile)
    first = rows - 48
    start = spans[3]
    at = pl.ds(first, 48)
    valid = first + lax.broadcasted_iota(jnp.int32, (48, 48), 1) >= start
    live = first + lax.broadcasted_iota(jnp.int32, (48, PAD), 0) >= start

    def rest(lanes):
        new = softmax_rows(q[at, lanes], k[at, lanes], v[at, lanes], valid, scale)
        att[at, lanes] = jnp.where(live, new, att[at, lanes])

    each_head(rest)


def nn_low(a, b):
    return nn(a.astype(BF), b)


def nn_two(a, b):
    return two(nn, a, b)


def unit(proj, ones, head, sums=nn_two):
    inverse = lax.rsqrt(sums(proj * proj, ones) * (1.0 / head) + EPS)
    return proj * inverse, inverse


def softmax_rows(query, key, value, valid, scale):
    scores = jnp.where(valid, nt(query, key) * scale, -1e30)
    raised = jnp.exp(scores - jnp.max(scores, axis=1, keepdims=True))
    probs = raised / jnp.sum(raised, axis=1, keepdims=True)
    return nn(probs.astype(BF), value).astype(BF)


def back_tile(query, key, value, grad, keys, queries, scale):
    scores = jnp.where(keys, nt(key, query) * scale, -1e30)
    raised = jnp.exp(scores - jnp.max(scores, axis=0, keepdims=True))
    probs = jnp.where(queries, raised / jnp.sum(raised, axis=0, keepdims=True), 0.0)
    d_value = nn(probs.astype(BF), grad)
    d_probs = nt(value, grad)
    inner = jnp.sum(probs * d_probs, axis=0, keepdims=True)
    d_scores = (probs * (d_probs - inner)).astype(BF)
    return tn(d_scores, key) * scale, nn(d_scores, query) * scale, d_value


def attention_back_kernel(head, spans, q, k, v, grad, dq, dk, dv):
    rows, wide = q.shape
    scale = head ** (-0.5)

    def each_head(fn):
        for n in range(wide // PAD):
            fn(slice(n * PAD, (n + 1) * PAD))

    for item in range(3):
        at = pl.ds(pl.multiple_of(spans[item], 16), TILE)
        keys = lax.broadcasted_iota(jnp.int32, (TILE, TILE), 0) < spans[4 + item]
        queries = lax.broadcasted_iota(jnp.int32, (TILE, TILE), 1) < spans[4 + item]

        def tile(lanes, at=at, keys=keys, queries=queries):
            parts = back_tile(
                q[at, lanes], k[at, lanes], v[at, lanes], grad[at, lanes], keys, queries, scale
            )
            for new, dst in zip(parts, (dq, dk, dv)):
                dst[at, lanes] = new.astype(BF)

        each_head(tile)
    first = rows - 48
    start = spans[3]
    at = pl.ds(first, 48)
    keys = first + lax.broadcasted_iota(jnp.int32, (48, 48), 0) >= start
    queries = first + lax.broadcasted_iota(jnp.int32, (48, 48), 1) >= start
    live = first + lax.broadcasted_iota(jnp.int32, (48, PAD), 0) >= start

    def rest(lanes):
        parts = back_tile(
            q[at, lanes], k[at, lanes], v[at, lanes], grad[at, lanes], keys, queries, scale
        )
        for new, dst in zip(parts, (dq, dk, dv)):
            dst[at, lanes] = jnp.where(live, new.astype(BF), dst[at, lanes])

    each_head(rest)


def local_call(kernel, micros, outs, scratch, spans, args):
    return pl.pallas_call(
        kernel,
        out_shape=outs,
        in_specs=[pl.BlockSpec(memory_space=pltpu.SMEM)] + [vmem()] * len(args),
        out_specs=[vmem()] * len(outs),
        scratch_shapes=scratch,
        compiler_params=pltpu.CompilerParams(vmem_limit_bytes=60 * 2**20),
        cost_estimate=price(micros),
    )(spans, *args)


def swap(array):
    return lax.ppermute(array, S, [(0, 1), (1, 0)])


def head_tables(packed, head):
    quarter = head // 4
    frequency = np.float32(10000.0) ** (-np.arange(quarter, dtype=np.float32) / quarter)
    lane = np.arange(head)
    angle = np.arange(32, dtype=np.float32)[:, None] * frequency[lane % quarter][None, :]
    by_row = (lane // (2 * quarter) == 0)[None, :]
    table = np.zeros((64, 2 * PAD), np.float32)
    for n, values in enumerate((np.cos(angle), np.sin(angle))):
        at = slice(n * PAD, n * PAD + head)
        table[:32, at] = np.where(by_row, values, 0.0)
        table[32:, at] = np.where(by_row, 0.0, values)
    table = jnp.asarray(table)
    parts = []
    for _ in range(3):
        parts.append(lax.reduce_precision(table, 8, 7).astype(BF))
        table = table - parts[-1].astype(F32)
    rows = np.arange(2 * PAD)[:, None]
    cols = np.arange(2 * PAD)[None, :]
    inside = (rows // PAD == cols // PAD) & (rows % PAD < head) & (cols % PAD < head)
    row, col = rows % PAD, cols % PAD
    early = (col % (2 * quarter)) < quarter
    turn = np.where(inside & early & (row == col + quarter), -1.0, 0.0)
    turn = turn + np.where(inside & ~early & (row == col - quarter), 1.0, 0.0)
    heads = packed // head
    rows = np.arange(packed)[:, None]
    wide = np.arange(heads * PAD)[None, :]
    spread = (rows // head == wide // PAD) & (rows % head == wide % PAD)
    lanes = tuple(jnp.asarray(m.astype(np.float32)).astype(BF) for m in (turn, inside, spread))
    return jnp.stack(parts), lanes


def reduced(total):
    return lax.psum_scatter(total, DP, scatter_dimension=0, tiled=True)[0]


def own_layer(section, pair):
    first = section == 0
    keep = jnp.where(first, pair[0], pair[1])
    got = swap(jnp.where(first, pair[1], pair[0]))
    return jnp.where(first, jnp.concatenate([keep, got]), jnp.concatenate([got, keep])).astype(F32)


def per_device(square, dp, tokens, cotangent, cond, patch_item, patch_pos, w_qkv, w_out, w_gate_up,
               w_down, qk_gain, ada_weight, ada_bias):
    section = lax.axis_index(S)
    first = section == 0
    rows, width = tokens.shape[1:]
    seq = patch_item.shape[1]
    items = cond.shape[0]
    head = qk_gain.shape[-1]
    packed = w_qkv.shape[-1]
    heads = packed // head
    hidden_here = w_down.shape[1]
    own = (jnp.swapaxes(w_qkv[0], 1, 2), w_out[0], w_gate_up[0], w_down[0])
    other = tuple(swap(w) for w in own)
    flat_qkv = (own[0].reshape(3 * packed, width), other[0].reshape(3 * packed, width))

    ada = ada_weight[0].T
    half = width // 2
    trig, (turn, ones, spread) = head_tables(packed, head)
    wide = heads * PAD
    mods, lifted_all, gains, sel, both, spans = ring_call(
        functools.partial(head_kernel, dp),
        8,
        12,
        [
            sds((2, 6, 8, width), F32),
            sds((dp, 16, width), F32),
            sds((2, 8, PAD), F32),
            sds((rows, 8), F32),
            sds((seq, 2 * PAD), F32),
            sds((8,), jnp.int32),
        ],
        [
            pltpu.VMEM((3 * half, width), BF),
            pltpu.VMEM((2, 3, 8, half), F32),
            pltpu.VMEM((8, 3, 8, half), F32),
            pltpu.VMEM((8, seq), F32),
            pltpu.VMEM((seq, 8), F32),
            pltpu.VMEM((16, width), F32),
            pltpu.VMEM((8, PAD), F32),
        ]
        + dma_sems(7 + dp)
        + [pltpu.SemaphoreType.DMA],
        (cond, ada, ada_bias, qk_gain[0], patch_item, patch_pos, trig),
        (1, 0, 1, 1, 1, 1, 1),
        scalar=5,
    )
    part = width // dp
    shard = lax.axis_index(DP)
    lifted_part = lax.dynamic_slice_in_dim(lifted_all, shard * part, part, 2)
    lifted_part = lifted_part.reshape(2 * dp, 8, part)

    x = tokens
    kept = []
    held = ring_call(
        functools.partial(qkv_kernel, 0, square),
        0,
        20,
        [sds((seq, width), BF), sds((2, seq, wide), BF)] + [sds((seq, wide), BF)] * 3,
        [pltpu.VMEM((rows, width), BF), pltpu.VMEM((3, wide, width), BF)]
        + dma_sems(6)
        + [pltpu.SemaphoreType.DMA((3 * heads,))],
        (x, sel, mods, gains, both, turn, ones, own[0], other[0]),
        (1,) * 7 + (0, 0),
    )
    for layer in range(2):
        whole1, proj, q, k, v = held
        (att,) = local_call(
            functools.partial(attention_kernel, head),
            6,
            [sds((seq, wide), BF)],
            [],
            spans,
            (q, k, v),
        )
        small = [sds((rows, width), F32)] * 3 + [sds((rows, width), BF)]
        large = [
            sds((seq, width), BF),
            sds((seq, hidden_here), F32),
            sds((seq, hidden_here), F32),
            sds((seq, hidden_here), BF),
        ]
        scratch = (
            [pltpu.VMEM(t.shape, t.dtype) for t in large]
            + [
                pltpu.VMEM((rows, width), BF),
                pltpu.VMEM((wide, width), BF),
                pltpu.VMEM((2, width, hidden_here), BF),
                pltpu.VMEM((hidden_here, width), BF),
            ]
            + scatter_scratch(rows, width)
            + scatter_scratch(rows, width)
            + dma_sems(18 if layer else 24)
            + [pltpu.SemaphoreType.DMA((7,)), pltpu.SemaphoreType.DMA((heads,))]
        )
        weights = (own[1], other[1], own[2], other[2], own[3], other[3])
        if layer:
            outs = ring_call(
                functools.partial(mlp_kernel, layer, square),
                3,
                48,
                small + large,
                scratch,
                (att, x, sel, mods) + weights,
                (1,) * 4 + (0,) * 6,
                loose=4,
            )
        else:
            outs = ring_call(
                functools.partial(mlp_qkv_kernel, layer, square),
                2,
                70,
                small
                + [sds((seq, width), BF), sds((2, seq, wide), BF)]
                + [sds((seq, wide), BF)] * 3
                + large,
                scratch
                + [pltpu.VMEM((3, wide, width), BF), pltpu.SemaphoreType.DMA((3 * heads,))],
                (att, x, sel, mods) + weights + (gains, both, turn, ones, own[0], other[0]),
                (1,) * 4 + (0,) * 6 + (1,) * 4 + (0, 0),
                loose=9,
            )
            held = outs[4:9]
        br1, x1, br2, y = outs[:4]
        whole2, gate, up, hidden = outs[-4:]
        kept.append((x, whole1, proj, q, k, v, att, br1, x1, whole2, gate, up, hidden, br2, y))
        x = y

    dy = cotangent
    packs = [None, None]
    prev = jnp.zeros((12, 8, half), F32)
    d_gains = [None, None]
    d_inputs = [None, None]
    for layer in (1, 0):
        x, whole1, proj, q, k, v, att, br1, x1, whole2, gate, up, hidden, br2, y = kept[layer]
        mod = mods
        rows1, datt, dx1, dmod_a, total_mlp = ring_call(
            functools.partial(mlp_back_kernel, layer, square),
            4 + layer,
            52,
            [
                sds((seq, width), BF),
                sds((seq, wide), BF),
                sds((rows, width), F32),
                sds((8, 8, half), F32),
                sds((dp, part // 2, 3 * hidden_here), BF),
            ],
            [pltpu.VMEM((dp, part // 2, 3 * hidden_here), BF)] * 3
            + [
                pltpu.VMEM((rows, width), BF),
                pltpu.VMEM((rows, width), BF),
                pltpu.VMEM((seq, width), BF),
                pltpu.VMEM((seq, hidden_here), BF),
                pltpu.VMEM((seq, hidden_here), BF),
                pltpu.VMEM((seq, hidden_here), F32),
                pltpu.VMEM((seq, hidden_here), F32),
                pltpu.VMEM((seq, hidden_here), BF),
                pltpu.VMEM((seq, width), BF),
                pltpu.VMEM((width, seq), BF),
                pltpu.VMEM((wide, width), BF),
                pltpu.VMEM((2, width, hidden_here), BF),
                pltpu.VMEM((hidden_here, width), BF),
            ]
            + scatter_scratch(rows, width)
            + dma_sems(21)
            + [pltpu.SemaphoreType.DMA((7,)), pltpu.SemaphoreType.DMA((heads,))],
            (dy, br2, br1, x1, sel, mod, gate, up, hidden, whole2, own[1], other[1], own[2],
             other[2], own[3], other[3]),
            (1,) * 6 + (0,) * 10,
        )
        pack_mlp = reduced(total_mlp)
        dq, dk, dv = local_call(
            functools.partial(attention_back_kernel, head),
            10,
            [sds((seq, wide), BF)] * 3,
            [],
            spans,
            (q, k, v, datt),
        )
        du, du_b, d_mod, total_att, dgain = ring_call(
            functools.partial(qkv_back_kernel, layer, square),
            6 + layer,
            22,
            [
                sds((rows, width), F32),
                sds((rows, width), BF),
                sds((2, 12, 8, half), F32),
                sds((dp, part // 2, 4 * packed), BF),
                sds((2, 1, wide), F32),
            ],
            [
                pltpu.VMEM((3 * packed, width), BF),
                pltpu.VMEM((seq, width), BF),
                pltpu.VMEM((seq, wide), BF),
                pltpu.VMEM((seq, width), BF),
                pltpu.VMEM((width, seq), BF),
                pltpu.VMEM((seq, 3 * packed), BF),
                pltpu.VMEM((seq, packed), BF),
            ]
            + [pltpu.VMEM((dp, part // 2, 4 * packed), BF)] * 3
            + scatter_scratch(rows, width)
            + dma_sems(7)
            + [pltpu.SemaphoreType.DMA((4,))],
            (dq, dk, dv, proj, gains, both, turn, ones, spread, x, dx1, sel, mod, dmod_a,
             prev, *flat_qkv, whole1, att, rows1),
            (1,) * 15 + (0,) * 5,
        )
        prev = d_mod[1]
        pack_att = reduced(total_att)
        packs[layer] = (pack_mlp, pack_att)
        d_gains[layer] = dgain
        d_inputs[layer] = du_b if layer else du
        dy = du_b

    gain_parts = jnp.pad(jnp.stack(d_gains).reshape(2, 2, wide), ((0, 0), (0, 6), (0, 0)))
    bias_part = ada_bias.shape[1] // dp
    g_ada_w, g_ada_b, cond_grad, gain_total = ring_call(
        functools.partial(tail_kernel, dp),
        9,
        15,
        [
            sds((part, 3 * half), F32),
            sds((1, bias_part), F32),
            sds((items, width), F32),
            sds((2, head), F32),
        ],
        [
            pltpu.VMEM((3 * half, width), BF),
            pltpu.VMEM((1, 3 * half), F32),
            pltpu.VMEM((8, 3, 8, half), F32),
            pltpu.VMEM((8, 8, wide), F32),
            pltpu.VMEM((3, 8, half), F32),
            pltpu.VMEM((8, wide), F32),
            pltpu.VMEM((dp, 3, 8, half), F32),
            pltpu.VMEM((dp, 8, wide), F32),
            pltpu.VMEM((8, 8, width), F32),
        ]
        + dma_sems(13 + 2 * (dp - 1) + 8)
        + [pltpu.SemaphoreType.DMA],
        (d_mod, gain_parts, lifted_part, cond, ada),
        (1, 1, 1, 1, 0),
    )

    f = hidden_here
    ready = lax.optimization_barrier((packs[0][0], packs[1][0], cond_grad))
    cond_grad = ready[2]
    mlp = own_layer(section, ready[:2])
    g_gate_up = jnp.stack([mlp[:, :f], mlp[:, f : 2 * f]])[None]
    g_down = mlp[:, 2 * f :].T[None]
    attn = own_layer(section, (packs[0][1], packs[1][1]))
    g_qkv = jnp.stack([attn[:, k * packed : (k + 1) * packed] for k in range(3)])[None]
    g_out = attn[:, 3 * packed :].T[None]

    outs = jnp.where(first, kept[0][-1], kept[1][-1])
    outs_got = swap(jnp.where(first, kept[1][-1], kept[0][-1]))
    layer_out = jnp.where(first, jnp.stack([outs, outs_got]), jnp.stack([outs_got, outs]))
    wide_mid = d_inputs[1].astype(F32)
    back_keep = jnp.where(first, d_inputs[0], wide_mid)
    back_got = swap(jnp.where(first, wide_mid, d_inputs[0]))
    in_grads = jnp.where(first, jnp.stack([back_keep, back_got]), jnp.stack([back_got, back_keep]))
    return (
        layer_out[None],
        in_grads[None],
        cond_grad,
        g_qkv,
        g_out,
        g_gate_up,
        g_down,
        gain_total[None],
        g_ada_w[None],
        g_ada_b,
    )


def solution(mesh):
    both = (DP, T)
    in_specs = (
        P(None, both, None),
        P(None, both, None),
        P(DP, None),
        P(None, DP),
        P(None, None, DP),
        P(S, None, None, T),
        P(S, T, None),
        P(S, None, None, T),
        P(S, T, None),
        P(S, None, None),
        P(S, None, T),
        P(S, T),
    )
    out_specs = (
        P(S, None, both, None),
        P(S, None, both, None),
        P(DP, None),
        P(S, None, DP, T),
        P(S, T, DP),
        P(S, None, DP, T),
        P(S, T, DP),
        P(S, None, None),
        P(S, DP, T),
        P(S, (T, DP)),
    )
    dp = mesh.shape[DP]

    def program(*args):
        return per_device(dp <= 4, dp, *args)

    return jax.shard_map(
        program, mesh=mesh, in_specs=in_specs, out_specs=out_specs, check_vma=False
    )
```
